128 devices in a mesh: dp: 1, yax: 16 (over z, y), xax: 8 (over x, core).
Axes of the slice: x: 4, y: 4, z: 4, core: 2. Of those that a mesh axis runs over, the one named last changes fastest.
Arguments:
- hidden: bfloat16 [768, 4096], P('dp', 'xax')
- cache_len: int32 [768], P('dp')
- k_cache: bfloat16 [768, 1024, 128], P(('dp', 'yax', 'xax'))
- v_cache: bfloat16 [768, 1024, 128], P(('dp', 'yax', 'xax'))
- g_attn: float32 [4096], P('xax')
- w_query: bfloat16 [4096, 4096], P('xax', 'yax')
- w_key: bfloat16 [4096, 128], P('xax')
- w_value: bfloat16 [4096, 128], P('xax')
- w_gate: bfloat16 [4096, 16384], P('xax', 'yax')
- w_up: bfloat16 [4096, 16384], P('xax', 'yax')
- w_out: bfloat16 [4096, 4096], P('yax', 'xax')
- w_down: bfloat16 [16384, 4096], P('yax', 'xax')
- g_final: float32 [4096], P('xax')
- embedding: bfloat16 [50432, 4096], P('yax', 'xax')
Outputs:
- output 1: bfloat16 [768, 128], P(('dp', 'yax', 'xax'))
- output 2: bfloat16 [768, 128], P(('dp', 'yax', 'xax'))
- output 3: float32 [768, 50432], P('dp', ('yax', 'xax'))
- output 4: float32 [768], P('dp')
All inputs are finite; a program needn't handle non-finite values.
Results may differ from the reference program's by a relative error of at most 0.00127.
Values are sent between devices in bfloat16 or wider.
A program may use at most 1 GiB of HBM per device.

```python
import jax
import jax.numpy as jnp
from jax import lax

D = 4096
HEADS = 32
HEAD = 128
FF = 16384
VOCAB = 50432
BATCH = 768
SEQ = 1024
ROW_BLOCK = 16

EPS = 1e-6
ROPE_BASE = 10000.0


def draw_lengths(key):
    drawn = jax.random.randint(key, (BATCH,), 1, SEQ, dtype=jnp.int32)
    row_ids = jnp.arange(BATCH)
    return jnp.where(row_ids == 0, SEQ - 1, jnp.where(row_ids == 1, 1, drawn)).astype(jnp.int32)


def setup_inputs(seed: int = 0, part: int = 0) -> dict:
    base_key = jax.random.key(seed)
    shared = jax.random.split(base_key, 10)
    own = jax.random.split(jax.random.fold_in(base_key, part), 5)

    def weight(key, shape, fan_in, gain):
        return (gain * fan_in ** -0.5 * jax.random.normal(key, shape, jnp.float32)).astype(jnp.bfloat16)

    col_scale = jnp.exp(0.5 * jax.random.normal(own[0], (D,), jnp.float32))
    hidden = jax.random.normal(own[1], (BATCH, D), jnp.float32) * col_scale
    k_cache = 2.5 * jax.random.normal(own[3], (BATCH, SEQ, HEAD), jnp.float32)
    v_cache = 2.0 * jax.random.normal(own[4], (BATCH, SEQ, HEAD), jnp.float32)
    return {
        "hidden": hidden.astype(jnp.bfloat16),
        "cache_len": draw_lengths(own[2]),
        "k_cache": k_cache.astype(jnp.bfloat16),
        "v_cache": v_cache.astype(jnp.bfloat16),
        "g_attn": 1.0 + 0.3 * jax.random.normal(shared[0], (D,), jnp.float32),
        "w_query": weight(shared[1], (D, HEADS * HEAD), D, 1.0),
        "w_key": weight(shared[2], (D, HEAD), D, 1.0),
        "w_value": weight(shared[3], (D, HEAD), D, 1.0),
        "w_gate": weight(shared[4], (D, FF), D, 1.0),
        "w_up": weight(shared[5], (D, FF), D, 1.0),
        "w_out": weight(shared[6], (HEADS * HEAD, D), HEADS * HEAD, 1.0),
        "w_down": weight(shared[7], (FF, D), FF, 1.0),
        "g_final": 1.0 + 0.3 * jax.random.normal(shared[8], (D,), jnp.float32),
        "embedding": weight(shared[9], (VOCAB, D), D, 2.0),
    }


def layer_norm(values_in, gain):
    row_mean = jnp.mean(values_in, axis=-1, keepdims=True)
    row_var = jnp.mean(jnp.square(values_in - row_mean), axis=-1, keepdims=True)
    return (values_in - row_mean) * lax.rsqrt(row_var + EPS) * gain


def rope_angle(positions):
    half_dim = HEAD // 2
    inv_freq = ROPE_BASE ** (-(jnp.arange(half_dim, dtype=jnp.float32) * 2.0) / HEAD)
    return positions.astype(jnp.float32)[:, None] * inv_freq[None, :]


def rotary(values_in, angles):
    half_dim = values_in.shape[-1] // 2
    cos_a = jnp.cos(angles)
    sin_a = jnp.sin(angles)
    first = values_in[..., :half_dim]
    second = values_in[..., half_dim:]
    return jnp.concatenate([first * cos_a - second * sin_a, second * cos_a + first * sin_a], axis=-1)


def attend_block(block):
    q_blk, kc_blk, vc_blk, kn_blk, vn_blk, len_blk = block
    positions = jnp.arange(SEQ)
    at_slot = positions[None, :, None] == len_blk[:, None, None]
    keys_all = jnp.where(at_slot, kn_blk[:, None, :], kc_blk)
    values_all = jnp.where(at_slot, vn_blk[:, None, :], vc_blk)
    scores = jnp.einsum("rhe,rse->rhs", q_blk.astype(jnp.float32), keys_all.astype(jnp.float32)) * HEAD ** -0.5
    valid = positions[None, None, :] <= len_blk[:, None, None]
    scores = jnp.where(valid, scores, -jnp.inf)
    prob_all = jax.nn.softmax(scores, axis=-1).astype(jnp.bfloat16)
    mixed = jnp.einsum("rhs,rse->rhe", prob_all.astype(jnp.float32), values_all.astype(jnp.float32))
    return mixed.astype(jnp.bfloat16)


def reference(hidden, cache_len, k_cache, v_cache, g_attn, w_query, w_key, w_value,
              w_gate, w_up, w_out, w_down, g_final, embedding):
    residual = hidden.astype(jnp.float32)
    normed = layer_norm(residual, g_attn).astype(jnp.bfloat16)
    query = jnp.dot(normed, w_query, preferred_element_type=jnp.float32).astype(jnp.bfloat16)
    key_new = jnp.dot(normed, w_key, preferred_element_type=jnp.float32).astype(jnp.bfloat16)
    value_new = jnp.dot(normed, w_value, preferred_element_type=jnp.float32).astype(jnp.bfloat16)
    gate = jnp.dot(normed, w_gate, preferred_element_type=jnp.float32).astype(jnp.bfloat16)
    up_val = jnp.dot(normed, w_up, preferred_element_type=jnp.float32).astype(jnp.bfloat16)
    angles = rope_angle(cache_len)
    query = rotary(query.astype(jnp.float32).reshape(BATCH, HEADS, HEAD), angles[:, None, :]).astype(jnp.bfloat16)
    key_new = rotary(key_new.astype(jnp.float32), angles).astype(jnp.bfloat16)
    blocks = BATCH // ROW_BLOCK
    attn_out = lax.map(attend_block, (
        query.reshape(blocks, ROW_BLOCK, HEADS, HEAD),
        k_cache.reshape(blocks, ROW_BLOCK, SEQ, HEAD),
        v_cache.reshape(blocks, ROW_BLOCK, SEQ, HEAD),
        key_new.reshape(blocks, ROW_BLOCK, HEAD),
        value_new.reshape(blocks, ROW_BLOCK, HEAD),
        cache_len.reshape(blocks, ROW_BLOCK)))
    attn_out = attn_out.reshape(BATCH, HEADS * HEAD)
    mlp_act = (jax.nn.silu(gate.astype(jnp.float32)) * up_val.astype(jnp.float32)).astype(jnp.bfloat16)
    branch_sum = (jnp.dot(attn_out, w_out, preferred_element_type=jnp.float32)
                  + jnp.dot(mlp_act, w_down, preferred_element_type=jnp.float32))
    residual_out = residual + branch_sum
    final_norm = layer_norm(residual_out, g_final).astype(jnp.bfloat16)
    logits = jnp.dot(final_norm, embedding.T, preferred_element_type=jnp.float32)
    log_norm = jax.nn.logsumexp(logits, axis=-1)
    return key_new, value_new, logits - log_norm[:, None], log_norm
```

```python
import jax
import jax.numpy as jnp
from jax import lax
from jax.experimental import pallas as pl
from jax.experimental.pallas import tpu as pltpu
from jax.sharding import PartitionSpec as P

EPS = 1e-6
ROPE_BASE = 10000.0
MESH_ID = pl.DeviceIdType.MESH
NY, NZ, NX = 4, 4, 4


def rope_angle(positions, head_dim):
    half_dim = head_dim // 2
    inv_freq = ROPE_BASE ** (-(jnp.arange(half_dim, dtype=jnp.float32) * 2.0) / head_dim)
    return positions.astype(jnp.float32)[:, None] * inv_freq[None, :]


def rotary(values_in, angles):
    half_dim = values_in.shape[-1] // 2
    cos_a = jnp.cos(angles)
    sin_a = jnp.sin(angles)
    first = values_in[..., :half_dim]
    second = values_in[..., half_dim:]
    return jnp.concatenate([first * cos_a - second * sin_a, second * cos_a + first * sin_a], axis=-1)


def sharded_norm(values_in, gain, width):
    stats = jnp.stack([jnp.sum(values_in, axis=-1), jnp.sum(values_in * values_in, axis=-1)])
    stats = lax.psum(stats, "xax")
    row_mean = stats[0] / width
    row_var = stats[1] / width - row_mean * row_mean
    return (values_in - row_mean[:, None]) * lax.rsqrt(row_var + EPS)[:, None] * gain


def attend_local(query, k_cache, v_cache, key_new, value_new, lengths):
    score_scale = query.shape[-1] ** -0.5
    scores = jnp.einsum("bhe,bse->bhs", query, k_cache, preferred_element_type=jnp.float32) * score_scale
    score_new = jnp.einsum("bhe,be->bh", query, key_new, preferred_element_type=jnp.float32) * score_scale
    valid = jnp.arange(k_cache.shape[1])[None, None, :] < lengths[:, None, None]
    row_max = jnp.maximum(jnp.max(jnp.where(valid, scores, -jnp.inf), axis=-1), score_new)
    weights = jnp.where(valid, jnp.exp(scores - row_max[..., None]), 0.0)
    weight_new = jnp.exp(score_new - row_max)
    denominator = jnp.sum(weights, axis=-1) + weight_new
    prob_all = (weights / denominator[..., None]).astype(jnp.bfloat16)
    prob_new = (weight_new / denominator).astype(jnp.bfloat16)
    attn_out = jnp.einsum("bhs,bse->bhe", prob_all, v_cache, preferred_element_type=jnp.float32)
    attn_out = attn_out + prob_new.astype(jnp.float32)[..., None] * value_new.astype(jnp.float32)[:, None, :]
    return attn_out.astype(jnp.bfloat16)


class Links:
    def __init__(self, send_sem, recv_sem):
        self.send_sem, self.recv_sem, self.count, self.sent = send_sem, recv_sem, 0, []
        self.y_idx = lax.axis_index("yax")
        self.x_idx = lax.axis_index("xax")
        self.z, self.y = self.y_idx // NY, self.y_idx % NY
        self.chip, self.core = self.x_idx // 2, self.x_idx % 2

    def at_plane(self, dz, dy):
        return {"yax": (self.z + dz) % NZ * NY + (self.y + dy) % NY, "xax": self.x_idx}

    def at_line(self, dx, other_core):
        core = 1 - self.core if other_core else self.core
        return {"yax": self.y_idx, "xax": (self.chip + dx) % NX * 2 + core}

    def send(self, src, dst, where):
        copy = pltpu.make_async_remote_copy(
            src_ref=src, dst_ref=dst, send_sem=self.send_sem.at[self.count], recv_sem=self.recv_sem.at[self.count],
            device_id=where, device_id_type=MESH_ID)
        self.count += 1
        copy.start()
        self.sent.append(copy)
        return copy

    def finish(self):
        for copy in self.sent:
            copy.wait_send()
        self.sent = []

    def barrier(self):
        barrier = pltpu.get_barrier_semaphore()
        peers = [self.at_line(dx, oc) for dx in range(NX) for oc in (0, 1) if (dx, oc) != (0, 0)]
        peers += [self.at_plane(dz, dy) for dz in range(NZ) for dy in range(NY) if (dz, dy) != (0, 0)]
        for peer in peers:
            pl.semaphore_signal(barrier, inc=1, device_id=peer, device_id_type=MESH_ID)
        pl.semaphore_wait(barrier, len(peers))


def plane_gather(links, buf):
    cols = buf.shape[-1]
    parts = []
    for part in range(2):
        lo = part * (cols // 2)
        mid = lo + cols // 4
        hi = lo + cols // 2

        def slot(du, dv, a, b, half=0, part=part):
            dz, dy = (dv, du) if part == 0 else (du, dv)
            return buf.at[half, (links.z + dz) % NZ, (links.y + dy) % NY, :, pl.ds(a, b - a)]

        def node(du, dv, part=part):
            return links.at_plane(dv, du) if part == 0 else links.at_plane(du, dv)

        parts.append((lo, mid, hi, slot, node))

    partner = links.at_line(0, True)
    crossing = []

    def give(p, du, dv):
        lo, mid, hi, slot, node = p
        crossing.append(links.send(slot(du, dv, lo, hi), slot(du, dv, lo, hi, half=1), partner))

    def push(p, du, dv, to_u, to_v, a=None, b=None):
        lo, mid, hi, slot, node = p
        a, b = (lo if a is None else a), (hi if b is None else b)
        return links.send(slot(du, dv, a, b), slot(du, dv, a, b), node(to_u, to_v))

    state = []
    for p in parts:
        s = {"u+": push(p, 0, 0, 1, 0), "u-": push(p, 0, 0, -1, 0)}
        s["v+", 0] = push(p, 0, 0, 0, 1)
        s["v-", 0] = push(p, 0, 0, 0, -1)
        state.append(s)
    for p in parts:
        give(p, 0, 0)
    for p, s in zip(parts, state):
        s["u+"].wait_recv()
        s["ur+"] = push(p, -1, 0, 1, 0, p[0], p[1])
        s["v+", 1] = push(p, -1, 0, 0, 1)
        s["v-", 1] = push(p, -1, 0, 0, -1)
        give(p, -1, 0)
    for p, s in zip(parts, state):
        s["u-"].wait_recv()
        s["ur-"] = push(p, 1, 0, -1, 0, p[1], p[2])
        s["v+", 2] = push(p, 1, 0, 0, 1)
        s["v-", 2] = push(p, 1, 0, 0, -1)
        give(p, 1, 0)
    offset = {0: 0, 1: -1, 2: 1, 3: 2}

    def arrive(p, s, k):
        s["v+", k].wait_recv()
        if k in (0, 3):
            s["vr+", k] = push(p, offset[k], -1, 0, 1)
        give(p, offset[k], -1)
        s["v-", k].wait_recv()
        if k in (1, 2):
            s["vr-", k] = push(p, offset[k], 1, 0, -1)
        give(p, offset[k], 1)

    for p, s in zip(parts, state):
        arrive(p, s, 0)
    for p, s in zip(parts, state):
        s["ur+"].wait_recv()
        s["ur-"].wait_recv()
        s["v+", 3] = push(p, 2, 0, 0, 1)
        s["v-", 3] = push(p, 2, 0, 0, -1)
        give(p, 2, 0)
    for k in (1, 2, 3):
        for p, s in zip(parts, state):
            arrive(p, s, k)
    for k, name in ((0, "vr+"), (1, "vr-"), (2, "vr-"), (3, "vr+")):
        for p, s in zip(parts, state):
            s[name, k].wait_recv()
            give(p, offset[k], 2)
    return crossing


def eye_mask():
    return lax.broadcasted_iota(jnp.int32, (128, 128), 0) == lax.broadcasted_iota(jnp.int32, (128, 128), 1)


def tail_kernel(vocab_own, part_ref, hid_ref, gain_ref, emb_ref, z_ref, norm_ref,
                ra1, rb1, ra2, rb2, acc_a, acc_b, xbuf, stat, f_buf, emb_buf, lse_x, lse_y,
                send_sem, recv_sem, local_sem):
    links = Links(send_sem, recv_sem)
    z, y = links.z, links.y
    half = part_ref.shape[-1] // 2
    rows = part_ref.shape[2]
    chunk = part_ref.shape[-1]
    take = emb_buf.shape[1]
    align = 16

    def emb_start(xid):
        first = vocab_own * xid // align * align
        return pl.multiple_of(first - xid // (2 * NX - 1) * align, align)

    def emb_piece(dx, other):
        core = 1 - links.core if other else links.core
        xid = (links.chip + dx) % NX * 2 + core
        return emb_ref.at[pl.ds(emb_start(xid), take), :]

    def emb_slot(dx, other):
        back = (NX - dx) % NX
        return emb_buf.at[int(other), :, pl.ds(back * chunk, chunk)]

    local = pltpu.make_async_copy(emb_piece(0, 0), emb_slot(0, 0), local_sem)
    local.start()
    links.barrier()

    low, high = pl.ds(0, half), pl.ds(half, half)
    first = []
    for d in (1, 3, 2):
        first.append((
            links.send(part_ref.at[:, (y + d) % NY, :, low], ra1.at[d - 1], links.at_plane(0, d)),
            links.send(part_ref.at[(z + d) % NZ, :, :, high], rb1.at[d - 1], links.at_plane(d, 0))))
    emb = [links.send(emb_piece(dx, oc), emb_slot(dx, oc), links.at_line(dx, oc))
           for dx, oc in ((0, 1), (1, 0), (3, 0), (1, 1), (3, 1))]
    for ca, cb in first:
        ca.wait_recv()
        cb.wait_recv()
    acc_a[...] = (part_ref[:, y, :, :half] + ra1[0]) + (ra1[1] + ra1[2])
    second_a = [links.send(acc_a.at[(z + d) % NZ], ra2.at[d - 1], links.at_plane(d, 0)) for d in (1, 3, 2)]
    acc_b[...] = (part_ref[z, :, :, half:] + rb1[0]) + (rb1[1] + rb1[2])
    second_b = [links.send(acc_b.at[(y + d) % NY], rb2.at[d - 1], links.at_plane(0, d)) for d in (1, 3, 2)]
    for c in second_a + second_b:
        c.wait_recv()
    res = hid_ref[z, y].astype(jnp.float32)
    xbuf[0, :rows, :half] = res[:, :half] + ((acc_a[z] + ra2[0]) + (ra2[1] + ra2[2]))
    xbuf[0, :rows, half:] = res[:, half:] + ((acc_b[y] + rb2[0]) + (rb2[1] + rb2[2]))
    xbuf[0, rows:, :] = jnp.broadcast_to(gain_ref[...], (8, chunk))

    line = [links.send(xbuf.at[0], xbuf.at[(NX - dx) % NX], links.at_line(dx, 0)) for dx in (1, 3, 2)]
    emb += [links.send(emb_piece(2, oc), emb_slot(2, oc), links.at_line(2, oc)) for oc in (0, 1)]
    for c in line:
        c.wait_recv()
    held = xbuf[:, :rows, :]
    count = NX * chunk
    mean = jnp.sum(jnp.sum(held, axis=0), axis=-1, keepdims=True) / count
    dev = held - mean[None]
    square = jnp.sum(jnp.sum(dev * dev, axis=0), axis=-1, keepdims=True)
    lane = lax.broadcasted_iota(jnp.int32, (rows, 128), 1)
    stat[0] = jnp.where(lane == 0, mean, square)
    links.send(stat.at[0], stat.at[1], links.at_line(0, True)).wait_recv()
    other_mean, other_square = stat[1, :, 0:1], stat[1, :, 1:2]
    both = (mean + other_mean) * 0.5
    gap = mean - other_mean
    var = (square + other_square + gap * gap * (count * 0.5)) / (2 * count)
    scale = lax.rsqrt(var + EPS)
    for e in range(NX):
        f_buf[0, z, y, :, e * chunk:(e + 1) * chunk] = (
            (xbuf[e, :rows, :] - both) * scale * xbuf[e, rows:rows + 1, :]).astype(jnp.bfloat16)

    crossing = plane_gather(links, f_buf)
    local.wait()
    for c in emb:
        c.wait_recv()
    for c in crossing:
        c.wait_recv()

    group = NY * rows
    for i in range(NZ):
        total = None
        for h in range(2):
            term = lax.dot_general(f_buf[h, i].reshape(group, NX * chunk), emb_buf[h],
                                   (((1,), (1,)), ((), ())), preferred_element_type=jnp.float32)
            total = term if total is None else total + term
        z_ref[i * group:(i + 1) * group, :] = total

    xid = links.x_idx
    shift = vocab_own * xid - emb_start(xid)
    eye = eye_mask()
    col = lax.broadcasted_iota(jnp.int32, (128, take), 1)
    own = (col >= shift) & (col < shift + vocab_own)
    blocks = z_ref.shape[0] // 128
    for b in range(blocks):
        zb = jnp.where(own, z_ref[b * 128:(b + 1) * 128, :], -jnp.inf)
        top = jnp.max(zb, axis=1, keepdims=True)
        mass = jnp.sum(jnp.exp(zb - top), axis=1, keepdims=True)
        lse_x[xid, b:b + 1, :] = jnp.sum(jnp.where(eye, top, 0.0), axis=0, keepdims=True)
        lse_x[xid, 8 + b:9 + b, :] = jnp.sum(jnp.where(eye, mass, 0.0), axis=0, keepdims=True)
    for b in range(blocks, 8):
        lse_x[xid, b:b + 1, :] = jnp.zeros((1, 128), jnp.float32)
        lse_x[xid, 8 + b:9 + b, :] = jnp.ones((1, 128), jnp.float32)

    def merge(ref):
        tops = ref[:, :8, :]
        top = jnp.max(tops, axis=0)
        return top, jnp.sum(ref[:, 8:, :] * jnp.exp(tops - top[None]), axis=0)

    got = [links.send(lse_x.at[xid], lse_x.at[xid], links.at_line(dx, oc))
           for dx in range(NX) for oc in (0, 1) if (dx, oc) != (0, 0)]
    for c in got:
        c.wait_recv()
    top, mass = merge(lse_x)
    yid = links.y_idx
    lse_y[yid, :8, :] = top
    lse_y[yid, 8:, :] = mass
    got = [links.send(lse_y.at[yid], lse_y.at[yid], links.at_plane(dz, dy))
           for dz in range(NZ) for dy in range(NY) if (dz, dy) != (0, 0)]
    for c in got:
        c.wait_recv()
    top, mass = merge(lse_y)
    norm_ref[...] = top + jnp.log(mass)
    links.finish()


def tail(part, hidden, g_final, embedding, vocab_own):
    total_rows, chunk = part.shape
    rows = total_rows // (NY * NZ)
    take = (vocab_own + 15 + 15) // 16 * 16
    half = chunk // 2
    f32, bf16 = jnp.float32, jnp.bfloat16
    copies = 100
    vmem = pl.BlockSpec(memory_space=pltpu.VMEM)
    hbm = pl.BlockSpec(memory_space=pl.ANY)
    return pl.pallas_call(
        lambda *refs: tail_kernel(vocab_own, *refs),
        out_shape=(jax.ShapeDtypeStruct((total_rows, take), f32), jax.ShapeDtypeStruct((8, 128), f32)),
        in_specs=[vmem, vmem, vmem, hbm],
        out_specs=(vmem, vmem),
        scratch_shapes=[
            pltpu.VMEM((3, NZ, rows, half), f32), pltpu.VMEM((3, NY, rows, half), f32),
            pltpu.VMEM((3, rows, half), f32), pltpu.VMEM((3, rows, half), f32),
            pltpu.VMEM((NZ, rows, half), f32), pltpu.VMEM((NY, rows, half), f32),
            pltpu.VMEM((NX, rows + 8, chunk), f32), pltpu.VMEM((2, rows, 128), f32),
            pltpu.VMEM((2, NZ, NY, rows, NX * chunk), bf16), pltpu.VMEM((2, take, NX * chunk), bf16),
            pltpu.VMEM((2 * NX, 16, 128), f32), pltpu.VMEM((NY * NZ, 16, 128), f32),
            pltpu.SemaphoreType.DMA((copies + 30,)), pltpu.SemaphoreType.DMA((copies + 30,)), pltpu.SemaphoreType.DMA,
        ],
        compiler_params=pltpu.CompilerParams(
            collective_id=1, has_side_effects=True, vmem_limit_bytes=56 * 1024 * 1024),
        name="tail",
    )(part.reshape(NZ, NY, rows, chunk), hidden.reshape(NZ, NY, rows, chunk), g_final[None, :], embedding)


def solution(mesh):
    y_size = mesh.shape["yax"]
    x_size = mesh.shape["xax"]
    row_spec = P(("dp", "yax", "xax"))

    def local_step(hidden, cache_len, k_cache, v_cache, g_attn, w_query, w_key, w_value,
                   w_gate, w_up, w_out, w_down, g_final, embedding):
        rows = hidden.shape[0]
        width = hidden.shape[1] * x_size
        own_rows = k_cache.shape[0]
        head_dim = k_cache.shape[2]
        q_cols = w_query.shape[1]
        kv_end = q_cols + 2 * head_dim
        ff_end = kv_end + w_gate.shape[1]
        y_idx = lax.axis_index("yax")
        x_idx = lax.axis_index("xax")
        own_start = (y_idx * x_size + x_idx) * own_rows

        residual = hidden.astype(jnp.float32)
        normed = sharded_norm(residual, g_attn, width).astype(jnp.bfloat16)
        proj_part = jnp.concatenate([
            jnp.dot(normed, w_query, preferred_element_type=jnp.float32),
            jnp.dot(normed, w_key, preferred_element_type=jnp.float32),
            jnp.dot(normed, w_value, preferred_element_type=jnp.float32),
            jnp.dot(normed, w_gate, preferred_element_type=jnp.float32),
            jnp.dot(normed, w_up, preferred_element_type=jnp.float32)], axis=1)
        projected = lax.psum(proj_part, "xax").astype(jnp.bfloat16)
        angles = rope_angle(cache_len, head_dim)
        query = projected[:, :q_cols].astype(jnp.float32).reshape(rows, q_cols // head_dim, head_dim)
        query = rotary(query, angles[:, None, :]).astype(jnp.bfloat16)
        key_new = rotary(projected[:, q_cols:q_cols + head_dim].astype(jnp.float32), angles).astype(jnp.bfloat16)
        value_new = projected[:, q_cols + head_dim:kv_end]
        gate = projected[:, kv_end:ff_end]
        up_val = projected[:, ff_end:]

        query_grp = lax.all_to_all(query, "yax", 0, 1, tiled=True)
        query_own = lax.dynamic_slice_in_dim(query_grp, x_idx * own_rows, own_rows, axis=0)
        key_own = lax.dynamic_slice_in_dim(key_new, own_start, own_rows, axis=0)
        value_own = lax.dynamic_slice_in_dim(value_new, own_start, own_rows, axis=0)
        len_own = lax.dynamic_slice_in_dim(cache_len, own_start, own_rows, axis=0)
        attn_own = attend_local(query_own, k_cache, v_cache, key_own, value_own, len_own)
        attn_grp = lax.all_gather(attn_own, "xax", axis=0, tiled=True)
        attn_heads = lax.all_to_all(attn_grp, "yax", 1, 0, tiled=True).reshape(rows, q_cols)

        mlp_act = (jax.nn.silu(gate.astype(jnp.float32)) * up_val.astype(jnp.float32)).astype(jnp.bfloat16)
        branch_sum = (jnp.dot(attn_heads, w_out, preferred_element_type=jnp.float32)
                      + jnp.dot(mlp_act, w_down, preferred_element_type=jnp.float32))

        vocab_own = embedding.shape[0] // x_size
        logits_wide, norm_tile = tail(branch_sum, hidden, g_final, embedding, vocab_own)
        log_norm = norm_tile[:rows // 128].reshape(rows)
        shift = vocab_own * x_idx - (vocab_own * x_idx // 16 * 16 - x_idx // (x_size - 1) * 16)
        logits = lax.dynamic_slice_in_dim(logits_wide, shift, vocab_own, axis=1)
        return key_own, value_own, logits - log_norm[:, None], log_norm

    in_specs = (P("dp", "xax"), P("dp"), row_spec, row_spec, P("xax"), P("xax", "yax"),
                P("xax", None), P("xax", None), P("xax", "yax"), P("xax", "yax"),
                P("yax", "xax"), P("yax", "xax"), P("xax"), P("yax", "xax"))
    out_specs = (row_spec, row_spec, P("dp", ("yax", "xax")), P("dp"))
    return jax.shard_map(local_step, mesh=mesh, in_specs=in_specs, out_specs=out_specs, check_vma=False)
```

```python
import jax
import jax.numpy as jnp
from jax import lax
from jax.experimental import pallas as pl
from jax.experimental.pallas import tpu as pltpu
from jax.sharding import PartitionSpec as P

EPS = 1e-6
ROPE_BASE = 10000.0
MESH_ID = pl.DeviceIdType.MESH
NY, NZ, NX = 4, 4, 4


def rope_angle(positions, head_dim):
    half_dim = head_dim // 2
    inv_freq = ROPE_BASE ** (-(jnp.arange(half_dim, dtype=jnp.float32) * 2.0) / head_dim)
    return positions.astype(jnp.float32)[:, None] * inv_freq[None, :]


class Links:
    def __init__(self, send_sem, recv_sem):
        self.send_sem, self.recv_sem, self.count, self.sent = send_sem, recv_sem, 0, []
        self.y_idx = lax.axis_index("yax")
        self.x_idx = lax.axis_index("xax")
        self.z, self.y = self.y_idx // NY, self.y_idx % NY
        self.chip, self.core = self.x_idx // 2, self.x_idx % 2

    def at_plane(self, dz, dy):
        return {"yax": (self.z + dz) % NZ * NY + (self.y + dy) % NY, "xax": self.x_idx}

    def at_line(self, dx, other_core):
        core = 1 - self.core if other_core else self.core
        return {"yax": self.y_idx, "xax": (self.chip + dx) % NX * 2 + core}

    def send(self, src, dst, where):
        copy = pltpu.make_async_remote_copy(
            src_ref=src, dst_ref=dst, send_sem=self.send_sem.at[self.count], recv_sem=self.recv_sem.at[self.count],
            device_id=where, device_id_type=MESH_ID)
        self.count += 1
        copy.start()
        self.sent.append(copy)
        return copy

    def finish(self):
        for copy in self.sent:
            copy.wait_send()
        self.sent = []

    def barrier(self):
        barrier = pltpu.get_barrier_semaphore()
        peers = [self.at_line(dx, oc) for dx in range(NX) for oc in (0, 1) if (dx, oc) != (0, 0)]
        peers += [self.at_plane(dz, dy) for dz in range(NZ) for dy in range(NY) if (dz, dy) != (0, 0)]
        for peer in peers:
            pl.semaphore_signal(barrier, inc=1, device_id=peer, device_id_type=MESH_ID)
        pl.semaphore_wait(barrier, len(peers))


def plane_gather(links, buf):
    cols = buf.shape[-1]
    parts = []
    for part in range(2):
        lo = part * (cols // 2)
        mid = lo + cols // 4
        hi = lo + cols // 2

        def slot(du, dv, a, b, half=0, part=part):
            dz, dy = (dv, du) if part == 0 else (du, dv)
            return buf.at[half, (links.z + dz) % NZ, (links.y + dy) % NY, :, pl.ds(a, b - a)]

        def node(du, dv, part=part):
            return links.at_plane(dv, du) if part == 0 else links.at_plane(du, dv)

        parts.append((lo, mid, hi, slot, node))

    partner = links.at_line(0, True)
    crossing = []

    def give(p, du, dv):
        lo, mid, hi, slot, node = p
        crossing.append(links.send(slot(du, dv, lo, hi), slot(du, dv, lo, hi, half=1), partner))

    def push(p, du, dv, to_u, to_v, a=None, b=None):
        lo, mid, hi, slot, node = p
        a, b = (lo if a is None else a), (hi if b is None else b)
        return links.send(slot(du, dv, a, b), slot(du, dv, a, b), node(to_u, to_v))

    state = []
    for p in parts:
        s = {"u+": push(p, 0, 0, 1, 0), "u-": push(p, 0, 0, -1, 0)}
        s["v+", 0] = push(p, 0, 0, 0, 1)
        s["v-", 0] = push(p, 0, 0, 0, -1)
        state.append(s)
    for p in parts:
        give(p, 0, 0)
    for p, s in zip(parts, state):
        s["u+"].wait_recv()
        s["ur+"] = push(p, -1, 0, 1, 0, p[0], p[1])
        s["v+", 1] = push(p, -1, 0, 0, 1)
        s["v-", 1] = push(p, -1, 0, 0, -1)
        give(p, -1, 0)
    for p, s in zip(parts, state):
        s["u-"].wait_recv()
        s["ur-"] = push(p, 1, 0, -1, 0, p[1], p[2])
        s["v+", 2] = push(p, 1, 0, 0, 1)
        s["v-", 2] = push(p, 1, 0, 0, -1)
        give(p, 1, 0)
    offset = {0: 0, 1: -1, 2: 1, 3: 2}

    def arrive(p, s, k):
        s["v+", k].wait_recv()
        if k in (0, 3):
            s["vr+", k] = push(p, offset[k], -1, 0, 1)
        give(p, offset[k], -1)
        s["v-", k].wait_recv()
        if k in (1, 2):
            s["vr-", k] = push(p, offset[k], 1, 0, -1)
        give(p, offset[k], 1)

    for p, s in zip(parts, state):
        arrive(p, s, 0)
    for p, s in zip(parts, state):
        s["ur+"].wait_recv()
        s["ur-"].wait_recv()
        s["v+", 3] = push(p, 2, 0, 0, 1)
        s["v-", 3] = push(p, 2, 0, 0, -1)
        give(p, 2, 0)
    for k in (1, 2, 3):
        for p, s in zip(parts, state):
            arrive(p, s, k)
    for k, name in ((0, "vr+"), (1, "vr-"), (2, "vr-"), (3, "vr+")):
        for p, s in zip(parts, state):
            s[name, k].wait_recv()
            give(p, offset[k], 2)
    return crossing


def eye_mask():
    return lax.broadcasted_iota(jnp.int32, (128, 128), 0) == lax.broadcasted_iota(jnp.int32, (128, 128), 1)


def norm_gather(links, rows_f32, gain_ref, xbuf, stat, out):
    rows, chunk = rows_f32.shape
    xbuf[0, :rows, :] = rows_f32
    xbuf[0, rows:, :] = jnp.broadcast_to(gain_ref[...], (8, chunk))
    line = [links.send(xbuf.at[0], xbuf.at[(NX - dx) % NX], links.at_line(dx, 0)) for dx in (1, 3, 2)]
    yield
    for c in line:
        c.wait_recv()
    held = xbuf[:, :rows, :]
    count = NX * chunk
    mean = jnp.sum(jnp.sum(held, axis=0), axis=-1, keepdims=True) / count
    dev = held - mean[None]
    square = jnp.sum(jnp.sum(dev * dev, axis=0), axis=-1, keepdims=True)
    lane = lax.broadcasted_iota(jnp.int32, (rows, 128), 1)
    stat[0] = jnp.where(lane == 0, mean, square)
    links.send(stat.at[0], stat.at[1], links.at_line(0, True)).wait_recv()
    other_mean, other_square = stat[1, :, 0:1], stat[1, :, 1:2]
    both = (mean + other_mean) * 0.5
    gap = mean - other_mean
    var = (square + other_square + gap * gap * (count * 0.5)) / (2 * count)
    scale = lax.rsqrt(var + EPS)
    for e in range(NX):
        out[0, links.z, links.y, :, e * chunk:(e + 1) * chunk] = (
            (xbuf[e, :rows, :] - both) * scale * xbuf[e, rows:rows + 1, :]).astype(jnp.bfloat16)
    for c in plane_gather(links, out):
        c.wait_recv()


def step_kernel(vocab_own, own_rows, hid_ref, gain_a, gain_f, cos_ref, sin_ref, len_ref, k_hbm, v_hbm,
                wq_ref, wk_ref, wv_ref, wg_ref, wu_ref, wo_hbm, wd_hbm, emb_ref,
                knew_ref, vnew_ref, z_ref, norm_ref,
                k_buf, v_buf, wo_buf, wd_buf, n_buf, w_buf, wq_t, wq_buf, sel, sel_t, qx, qr, qy, qf,
                kvp, kvr, o_buf, o_got, o_send, o_all, act,
                part, ra1, rb1, ra2, rb2, acc_a, acc_b, xbuf, stat, xbuf2, stat2, f_buf, emb_buf, lse_x, lse_y,
                send_sem, recv_sem, local_sem):
    links = Links(send_sem, recv_sem)
    f32, bf16 = jnp.float32, jnp.bfloat16
    z, y, xid, yid = links.z, links.y, links.x_idx, links.y_idx
    rows, chunk = hid_ref.shape[2], hid_ref.shape[3]
    half = chunk // 2
    nx2, nyz = 2 * NX, NY * NZ
    group = NY * rows
    head = 128
    pad = 8
    others = [(dx, oc) for dx, oc in ((0, 1), (1, 0), (3, 0), (1, 1), (3, 1), (2, 0), (2, 1))]

    def line_id(dx, oc):
        core = 1 - links.core if oc else links.core
        return (links.chip + dx) % NX * 2 + core

    local = []

    def fetch(src, dst):
        copy = pltpu.make_async_copy(src, dst, local_sem.at[len(local)])
        copy.start()
        local.append(copy)
        return copy

    ff = wg_ref.shape[1] // nx2

    def w_piece(ref, dx, oc):
        return ref.at[:, pl.ds(pl.multiple_of(line_id(dx, oc) * ff, ff), ff)]

    def w_slot(which, dx, oc):
        back = (NX - dx) % NX
        return w_buf.at[int(oc), pl.ds(back * chunk, chunk), pl.ds(which * ff, ff)]

    take = emb_buf.shape[1]

    def emb_start(xi):
        return pl.multiple_of(vocab_own * xi // 16 * 16 - xi // (nx2 - 1) * 16, 16)

    def emb_piece(dx, oc):
        return emb_ref.at[pl.ds(emb_start(line_id(dx, oc)), take), :]

    def emb_slot(dx, oc):
        return emb_buf.at[int(oc), :, pl.ds((NX - dx) % NX * chunk, chunk)]

    own_w = [fetch(w_piece(wg_ref, 0, 0), w_slot(0, 0, 0)), fetch(w_piece(wu_ref, 0, 0), w_slot(1, 0, 0))]
    got_kv = [fetch(k_hbm, k_buf), fetch(v_hbm, v_buf)]
    got_wo, got_wd = fetch(wo_hbm, wo_buf), fetch(wd_hbm, wd_buf)
    own_emb = fetch(emb_piece(0, 0), emb_slot(0, 0))

    qc = wq_ref.shape[1]
    qs = qc // nx2
    per = head // qs
    eye_q = (lax.broadcasted_iota(jnp.int32, (qc, qc), 0) == lax.broadcasted_iota(jnp.int32, (qc, qc), 1))
    wq_t[...] = lax.dot_general(eye_q.astype(bf16), wq_ref[...], (((1,), (1,)), ((), ())),
                                preferred_element_type=f32).astype(bf16)
    wq_buf[...] = jnp.zeros(wq_buf.shape, bf16)

    def q_rows(xi):
        return pl.ds(pl.multiple_of(xi % per * qs, qs), qs)

    wq_buf[0, q_rows(xid), 0:chunk] = wq_t[pl.ds(pl.multiple_of(xid * qs, qs), qs), :]
    links.barrier()

    front = norm_gather(links, hid_ref[z, y].astype(f32), gain_a, xbuf, stat, n_buf)
    next(front)
    wq_got, w_got = [], []
    for dx, oc in others:
        xi = line_id(dx, oc)
        wq_got.append(links.send(wq_t.at[pl.ds(pl.multiple_of(xi * qs, qs), qs), :],
                                 wq_buf.at[int(oc), q_rows(xi), pl.ds((NX - dx) % NX * chunk, chunk)],
                                 links.at_line(dx, oc)))
    for dx, oc in others:
        for which, ref in enumerate((wg_ref, wu_ref)):
            w_got.append(links.send(w_piece(ref, dx, oc), w_slot(which, dx, oc), links.at_line(dx, oc)))

    total_rows = nyz * rows
    r_id = lax.broadcasted_iota(jnp.int32, (nx2 * nyz * pad, 1), 0)
    r_j = r_id % pad
    r_src = jnp.where(r_j < own_rows, r_id // pad % nyz * rows + r_id // (pad * nyz) * own_rows + r_j, -1)
    s_id = lax.broadcasted_iota(jnp.int32, (1, total_rows), 1)
    sel[...] = jnp.where(r_src == s_id, 1.0, 0.0).astype(bf16)
    t_id = lax.broadcasted_iota(jnp.int32, (total_rows, 1), 0)
    t_in = t_id % rows
    t_src = t_in // own_rows * (nyz * pad) + t_id // rows * pad + t_in % own_rows
    u_id = lax.broadcasted_iota(jnp.int32, (1, nx2 * nyz * pad), 1)
    sel_t[...] = jnp.where(t_src == u_id, 1.0, 0.0).astype(bf16)
    k_id = lax.broadcasted_iota(jnp.int32, (nx2 * pad, rows), 0)
    k_src = jnp.where(k_id % pad < own_rows, k_id // pad * own_rows + k_id % pad, -1)
    sel_kv = jnp.where(k_src == lax.broadcasted_iota(jnp.int32, (nx2 * pad, rows), 1), 1.0, 0.0).astype(bf16)

    for _ in front:
        pass

    n_own = jnp.dot(sel_kv, n_buf[0, z, y, :, 0:chunk], preferred_element_type=f32).astype(bf16)
    kvp[:, :, :head] = jnp.dot(n_own, wk_ref[...], preferred_element_type=f32).reshape(nx2, pad, head)
    kvp[:, :, head:] = jnp.dot(n_own, wv_ref[...], preferred_element_type=f32).reshape(nx2, pad, head)
    kv_got = [links.send(kvp.at[line_id(dx, oc)], kvr.at[xid], links.at_line(dx, oc)) for dx, oc in others]
    kvr[xid] = kvp[xid]

    for c in wq_got:
        c.wait_recv()

    def wide(buf, i, h):
        return buf[h, i].reshape(group, NX * chunk)

    q_blocks = []
    for i in range(NZ):
        q_blocks.append((lax.dot_general(wide(n_buf, i, 0), wq_buf[0], (((1,), (1,)), ((), ())), preferred_element_type=f32)
                         + lax.dot_general(wide(n_buf, i, 1), wq_buf[1], (((1,), (1,)), ((), ())), preferred_element_type=f32)
                         ).astype(bf16))
    q_all = jnp.concatenate(q_blocks, axis=0)
    span = nyz * pad
    for i in range(nx2):
        qx[i] = jnp.dot(sel[i * span:(i + 1) * span, :], q_all, preferred_element_type=f32).astype(bf16)
    q_got = [links.send(qx.at[line_id(dx, oc)], qr.at[xid], links.at_line(dx, oc)) for dx, oc in others]
    qr[xid] = qx[xid]
    for c in q_got:
        c.wait_recv()
    for j in range(qc // head):
        piece = qr[j * per].astype(f32)
        for i in range(1, per):
            piece = piece + qr[j * per + i].astype(f32)
        qy[:, :, j * head:(j + 1) * head] = piece.reshape(nyz, pad, head)
    plane = [(dz, dy) for dz in range(NZ) for dy in range(NY) if (dz, dy) != (0, 0)]

    def plane_id(dz, dy):
        return (z + dz) % NZ * NY + (y + dy) % NY

    y_got = [links.send(qy.at[plane_id(dz, dy)], qf.at[yid], links.at_plane(dz, dy)) for dz, dy in plane]
    qf[yid] = qy[yid]

    for c in kv_got:
        c.wait_recv()
    kv_sum = kvr[0]
    for i in range(1, nx2):
        kv_sum = kv_sum + kvr[i]
    kv_new = kv_sum.astype(bf16).astype(f32)

    def turn(v, b=None):
        cos, sin = (cos_ref[...], sin_ref[...]) if b is None else (cos_ref[b:b + 1, :], sin_ref[b:b + 1, :])
        return (v * cos + pltpu.roll(v, head // 2, 1) * sin).astype(bf16)

    k_new = turn(kv_new[:, :head])
    knew_ref[...] = k_new
    vnew_ref[...] = kv_new[:, head:].astype(bf16)
    k_row, v_row = k_new.astype(f32), kv_new[:, head:]
    for c in got_kv:
        c.wait()
    for c in y_got:
        c.wait_recv()
    seq = k_buf.shape[1]
    score_scale = head ** -0.5
    position = lax.broadcasted_iota(jnp.int32, (1, seq), 1)
    o_buf[...] = jnp.zeros(o_buf.shape, f32)
    for b in range(own_rows):
        q_b = jnp.concatenate([turn(qf[:, b, j * head:(j + 1) * head], b) for j in range(qc // head)], axis=0)
        scores = lax.dot_general(q_b, k_buf[b], (((1,), (1,)), ((), ())), preferred_element_type=f32) * score_scale
        score_new = jnp.sum(q_b.astype(f32) * k_row[b:b + 1, :], axis=-1, keepdims=True) * score_scale
        valid = position < len_ref[b:b + 1, 0:1]
        top = jnp.maximum(jnp.max(jnp.where(valid, scores, -jnp.inf), axis=-1, keepdims=True), score_new)
        weights = jnp.where(valid, jnp.exp(scores - top), 0.0)
        weight_new = jnp.exp(score_new - top)
        denom = jnp.sum(weights, axis=-1, keepdims=True) + weight_new
        o_b = jnp.dot((weights / denom).astype(bf16), v_buf[b], preferred_element_type=f32)
        o_b = o_b + (weight_new / denom).astype(bf16).astype(f32) * v_row[b:b + 1, :]
        o_b = o_b.astype(bf16).astype(f32)
        for j in range(qc // head):
            o_buf[:, b, j * head:(j + 1) * head] = o_b[j * nyz:(j + 1) * nyz, :]
    o_back = [links.send(o_buf.at[plane_id(dz, dy)], o_got.at[yid], links.at_plane(dz, dy)) for dz, dy in plane]
    o_got[yid] = o_buf[yid]
    for c in o_back:
        c.wait_recv()
    o_all[xid] = o_got[...].reshape(span, qc).astype(bf16)
    o_line = [links.send(o_all.at[xid], o_all.at[xid], links.at_line(dx, oc)) for dx, oc in others]

    for c in own_w:
        c.wait()
    for c in w_got:
        c.wait_recv()
    own_cols = pl.ds(pl.multiple_of(xid * ff, ff), ff)
    a_got = []
    partner = links.at_line(0, True)
    for i in range(NZ):
        both = (jnp.dot(wide(n_buf, i, 0), w_buf[0], preferred_element_type=f32)
                + jnp.dot(wide(n_buf, i, 1), w_buf[1], preferred_element_type=f32)).astype(bf16).astype(f32)
        gate, up = both[:, :ff], both[:, ff:]
        act[i, :, own_cols] = (gate * jax.nn.sigmoid(gate) * up).astype(bf16)
        here = act.at[i, :, own_cols]
        a_got.append([links.send(here, here, links.at_line(dx, 0)) for dx in (1, 3, 2)]
                     + [links.send(here, here, partner)])

    emb = [links.send(emb_piece(dx, oc), emb_slot(dx, oc), links.at_line(dx, oc)) for dx, oc in others[:5]]

    for c in o_line:
        c.wait_recv()
    got_wo.wait()
    got_wd.wait()
    for i in range(NZ):
        o_nat = jnp.dot(sel_t[i * group:(i + 1) * group, :], o_all[...].reshape(nx2 * span, qc),
                        preferred_element_type=f32).astype(bf16)
        part[i] = jnp.dot(o_nat, wo_buf[...], preferred_element_type=f32).reshape(NY, rows, chunk)
    passed = []
    for i in range(NZ):
        for dx, c in zip((1, 3, 2), a_got[i]):
            c.wait_recv()
            came = pl.ds(pl.multiple_of(line_id((NX - dx) % NX, 0) * ff, ff), ff)
            passed.append(links.send(act.at[i, :, came], act.at[i, :, came], partner))
        a_got[i][3].wait_recv()
    for i in range(NZ):
        for c in passed[i * 3:i * 3 + 3]:
            c.wait_recv()
        part[i] = part[i] + jnp.dot(act[i], wd_buf[...], preferred_element_type=f32).reshape(NY, rows, chunk)

    low, high = pl.ds(0, half), pl.ds(half, half)
    first = []
    for d in (1, 3, 2):
        first.append((
            links.send(part.at[:, (y + d) % NY, :, low], ra1.at[d - 1], links.at_plane(0, d)),
            links.send(part.at[(z + d) % NZ, :, :, high], rb1.at[d - 1], links.at_plane(d, 0))))
    for ca, cb in first:
        ca.wait_recv()
        cb.wait_recv()
    acc_a[...] = (part[:, y, :, :half] + ra1[0]) + (ra1[1] + ra1[2])
    second_a = [links.send(acc_a.at[(z + d) % NZ], ra2.at[d - 1], links.at_plane(d, 0)) for d in (1, 3, 2)]
    acc_b[...] = (part[z, :, :, half:] + rb1[0]) + (rb1[1] + rb1[2])
    second_b = [links.send(acc_b.at[(y + d) % NY], rb2.at[d - 1], links.at_plane(0, d)) for d in (1, 3, 2)]
    for c in second_a + second_b:
        c.wait_recv()
    branch = jnp.concatenate([(acc_a[z] + ra2[0]) + (ra2[1] + ra2[2]), (acc_b[y] + rb2[0]) + (rb2[1] + rb2[2])], axis=1)
    back = norm_gather(links, hid_ref[z, y].astype(f32) + branch, gain_f, xbuf2, stat2, f_buf)
    next(back)
    emb += [links.send(emb_piece(dx, oc), emb_slot(dx, oc), links.at_line(dx, oc)) for dx, oc in others[5:]]
    for _ in back:
        pass
    own_emb.wait()
    for c in emb:
        c.wait_recv()

    for i in range(NZ):
        z_ref[i * group:(i + 1) * group, :] = (
            lax.dot_general(wide(f_buf, i, 0), emb_buf[0], (((1,), (1,)), ((), ())), preferred_element_type=f32)
            + lax.dot_general(wide(f_buf, i, 1), emb_buf[1], (((1,), (1,)), ((), ())), preferred_element_type=f32))

    shift = vocab_own * xid - emb_start(xid)
    eye = lax.broadcasted_iota(jnp.int32, (128, 128), 0) == lax.broadcasted_iota(jnp.int32, (128, 128), 1)
    col = lax.broadcasted_iota(jnp.int32, (128, take), 1)
    own = (col >= shift) & (col < shift + vocab_own)
    blocks = z_ref.shape[0] // 128
    for b in range(blocks):
        zb = jnp.where(own, z_ref[b * 128:(b + 1) * 128, :], -jnp.inf)
        top = jnp.max(zb, axis=1, keepdims=True)
        mass = jnp.sum(jnp.exp(zb - top), axis=1, keepdims=True)
        lse_x[xid, b:b + 1, :] = jnp.sum(jnp.where(eye, top, 0.0), axis=0, keepdims=True)
        lse_x[xid, 8 + b:9 + b, :] = jnp.sum(jnp.where(eye, mass, 0.0), axis=0, keepdims=True)
    for b in range(blocks, 8):
        lse_x[xid, b:b + 1, :] = jnp.zeros((1, 128), f32)
        lse_x[xid, 8 + b:9 + b, :] = jnp.ones((1, 128), f32)

    def merge(ref):
        tops = ref[:, :8, :]
        top = jnp.max(tops, axis=0)
        return top, jnp.sum(ref[:, 8:, :] * jnp.exp(tops - top[None]), axis=0)

    got = [links.send(lse_x.at[xid], lse_x.at[xid], links.at_line(dx, oc)) for dx, oc in others]
    for c in got:
        c.wait_recv()
    top, mass = merge(lse_x)
    lse_y[yid, :8, :] = top
    lse_y[yid, 8:, :] = mass
    got = [links.send(lse_y.at[yid], lse_y.at[yid], links.at_plane(dz, dy)) for dz, dy in plane]
    for c in got:
        c.wait_recv()
    top, mass = merge(lse_y)
    norm_ref[...] = top + jnp.log(mass)
    links.finish()


def whole_step(hidden, cos, sin, lens, k_cache, v_cache, g_attn, w_query, w_key, w_value,
               w_gate, w_up, w_out, w_down, g_final, embedding):
    total_rows, chunk = hidden.shape
    own_rows, seq, head = k_cache.shape
    rows = total_rows // (NY * NZ)
    vocab_own = embedding.shape[0] // (2 * NX)
    take = (vocab_own + 30) // 16 * 16
    half = chunk // 2
    qc = w_query.shape[1]
    ff = w_gate.shape[1] // (2 * NX)
    f32, bf16 = jnp.float32, jnp.bfloat16
    nyz, nx2, pad = NY * NZ, 2 * NX, 8
    copies = 360
    vmem = pl.BlockSpec(memory_space=pltpu.VMEM)
    hbm = pl.BlockSpec(memory_space=pl.ANY)
    V = pltpu.VMEM
    return pl.pallas_call(
        lambda *refs: step_kernel(vocab_own, own_rows, *refs),
        out_shape=(jax.ShapeDtypeStruct((pad, head), bf16), jax.ShapeDtypeStruct((pad, head), bf16),
                   jax.ShapeDtypeStruct((total_rows, take), f32), jax.ShapeDtypeStruct((8, 128), f32)),
        in_specs=[vmem] * 6 + [hbm] * 2 + [vmem] * 3 + [hbm] * 5,
        out_specs=(vmem,) * 4,
        scratch_shapes=[
            V((own_rows, seq, head), bf16), V((own_rows, seq, head), bf16), V((qc, chunk), bf16),
            V((nx2 * ff, chunk), bf16), V((2, NZ, NY, rows, NX * chunk), bf16), V((2, NX * chunk, 2 * ff), bf16),
            V((qc, chunk), bf16), V((2, head, NX * chunk), bf16),
            V((nx2 * nyz * pad, total_rows), bf16), V((total_rows, nx2 * nyz * pad), bf16),
            V((nx2, nyz * pad, head), bf16), V((nx2, nyz * pad, head), bf16),
            V((nyz, pad, qc), f32), V((nyz, pad, qc), f32),
            V((nx2, pad, 2 * head), f32), V((nx2, pad, 2 * head), f32),
            V((nyz, pad, qc), f32), V((nyz, pad, qc), f32), V((8, 128), f32), V((nx2, nyz * pad, qc), bf16),
            V((NZ, NY * rows, nx2 * ff), bf16),
            V((NZ, NY, rows, chunk), f32),
            V((3, NZ, rows, half), f32), V((3, NY, rows, half), f32), V((3, rows, half), f32), V((3, rows, half), f32),
            V((NZ, rows, half), f32), V((NY, rows, half), f32),
            V((NX, rows + 8, chunk), f32), V((2, rows, 128), f32), V((NX, rows + 8, chunk), f32), V((2, rows, 128), f32),
            V((2, NZ, NY, rows, NX * chunk), bf16), V((2, take, NX * chunk), bf16),
            V((nx2, 16, 128), f32), V((nyz, 16, 128), f32),
            pltpu.SemaphoreType.DMA((copies,)), pltpu.SemaphoreType.DMA((copies,)), pltpu.SemaphoreType.DMA((8,)),
        ],
        compiler_params=pltpu.CompilerParams(
            collective_id=1, has_side_effects=True, vmem_limit_bytes=60 * 1024 * 1024),
        name="decode_step",
    )(hidden.reshape(NZ, NY, rows, chunk), g_attn[None, :], g_final[None, :], cos, sin, lens, k_cache, v_cache,
      w_query, w_key, w_value, w_gate, w_up, w_out, w_down, embedding)


def solution(mesh):
    x_size = mesh.shape["xax"]
    row_spec = P(("dp", "yax", "xax"))

    def local_step(hidden, cache_len, k_cache, v_cache, g_attn, w_query, w_key, w_value,
                   w_gate, w_up, w_out, w_down, g_final, embedding):
        rows = hidden.shape[0]
        own_rows, _, head_dim = k_cache.shape
        y_idx = lax.axis_index("yax")
        x_idx = lax.axis_index("xax")
        own_start = (y_idx * x_size + x_idx) * own_rows
        len_own = jnp.pad(lax.dynamic_slice_in_dim(cache_len, own_start, own_rows, axis=0), (0, 8 - own_rows))
        angles = rope_angle(len_own, head_dim)
        cos_half, sin_half = jnp.cos(angles), jnp.sin(angles)
        cos = jnp.concatenate([cos_half, cos_half], axis=1)
        sin = jnp.concatenate([-sin_half, sin_half], axis=1)
        lens = jnp.broadcast_to(len_own[:, None], (8, 128))
        key_own, value_own, logits_wide, norm_tile = whole_step(
            hidden, cos, sin, lens, k_cache, v_cache, g_attn, w_query, w_key, w_value,
            w_gate, w_up, w_out, w_down, g_final, embedding)
        vocab_own = embedding.shape[0] // x_size
        log_norm = norm_tile[:rows // 128].reshape(rows)
        shift = vocab_own * x_idx - (vocab_own * x_idx // 16 * 16 - x_idx // (x_size - 1) * 16)
        logits = lax.dynamic_slice_in_dim(logits_wide, shift, vocab_own, axis=1)
        return key_own[:own_rows], value_own[:own_rows], logits - log_norm[:, None], log_norm

    in_specs = (P("dp", "xax"), P("dp"), row_spec, row_spec, P("xax"), P("xax", "yax"),
                P("xax", None), P("xax", None), P("xax", "yax"), P("xax", "yax"),
                P("yax", "xax"), P("yax", "xax"), P("xax"), P("yax", "xax"))
    out_specs = (row_spec, row_spec, P("dp", ("yax", "xax")), P("dp"))
    return jax.shard_map(local_step, mesh=mesh, in_specs=in_specs, out_specs=out_specs, check_vma=False)
```

```python
import jax
import jax.numpy as jnp
from jax import lax
from jax.experimental import pallas as pl
from jax.experimental.pallas import tpu as pltpu
from jax.sharding import PartitionSpec as P

EPS = 1e-6
ROPE_BASE = 10000.0
MESH_ID = pl.DeviceIdType.MESH
NY, NZ, NX = 4, 4, 4


def rope_angle(positions, head_dim):
    half_dim = head_dim // 2
    inv_freq = ROPE_BASE ** (-(jnp.arange(half_dim, dtype=jnp.float32) * 2.0) / head_dim)
    return positions.astype(jnp.float32)[:, None] * inv_freq[None, :]


class Phases:
    def __init__(self):
        self.open = None

    def __call__(self, name):
        self.close()
        self.open = jax.named_scope(name)
        self.open.__enter__()

    def close(self):
        if self.open is not None:
            self.open.__exit__(None, None, None)
        self.open = None


class Links:
    def __init__(self, send_sem, recv_sem):
        self.send_sem, self.recv_sem, self.count, self.sent = send_sem, recv_sem, 0, []
        self.y_idx = lax.axis_index("yax")
        self.x_idx = lax.axis_index("xax")
        self.z, self.y = self.y_idx // NY, self.y_idx % NY
        self.chip, self.core = self.x_idx // 2, self.x_idx % 2

    def at_plane(self, dz, dy):
        return {"yax": (self.z + dz) % NZ * NY + (self.y + dy) % NY, "xax": self.x_idx}

    def slot_rows(self, dz, dy, rows):
        slot = (self.z + dz) % NZ * NY + (self.y + dy) % NY
        return pl.ds(pl.multiple_of(slot * rows, rows), rows)

    def at_line(self, dx, other_core):
        core = 1 - self.core if other_core else self.core
        return {"yax": self.y_idx, "xax": (self.chip + dx) % NX * 2 + core}

    def send(self, src, dst, where):
        copy = pltpu.make_async_remote_copy(
            src_ref=src, dst_ref=dst, send_sem=self.send_sem.at[self.count], recv_sem=self.recv_sem.at[self.count],
            device_id=where, device_id_type=MESH_ID)
        self.count += 1
        copy.start()
        self.sent.append(copy)
        return copy

    def finish(self):
        for copy in self.sent:
            copy.wait_send()
        self.sent = []

    def barrier(self):
        barrier = pltpu.get_barrier_semaphore()
        peers = [self.at_line(dx, oc) for dx in range(NX) for oc in (0, 1) if (dx, oc) != (0, 0)]
        peers += [self.at_plane(dz, dy) for dz in range(NZ) for dy in range(NY) if (dz, dy) != (0, 0)]
        for peer in peers:
            pl.semaphore_signal(barrier, inc=1, device_id=peer, device_id_type=MESH_ID)
        pl.semaphore_wait(barrier, len(peers))


def plane_gather(links, buf):
    cols = buf.shape[-1]
    rows = buf.shape[1] // (NY * NZ)
    parts = []
    for part in range(2):
        lo = part * (cols // 2)
        mid = lo + cols // 4
        hi = lo + cols // 2

        def slot(du, dv, a, b, half=0, part=part):
            dz, dy = (dv, du) if part == 0 else (du, dv)
            return buf.at[half, links.slot_rows(dz, dy, rows), pl.ds(a, b - a)]

        def node(du, dv, part=part):
            return links.at_plane(dv, du) if part == 0 else links.at_plane(du, dv)

        parts.append((lo, mid, hi, slot, node))

    partner = links.at_line(0, True)
    crossing = []

    def give(p, du, dv):
        lo, mid, hi, slot, node = p
        crossing.append(links.send(slot(du, dv, lo, hi), slot(du, dv, lo, hi, half=1), partner))

    def push(p, du, dv, to_u, to_v, a=None, b=None):
        lo, mid, hi, slot, node = p
        a, b = (lo if a is None else a), (hi if b is None else b)
        return links.send(slot(du, dv, a, b), slot(du, dv, a, b), node(to_u, to_v))

    state = []
    for p in parts:
        s = {"u+": push(p, 0, 0, 1, 0), "u-": push(p, 0, 0, -1, 0)}
        s["v+", 0] = push(p, 0, 0, 0, 1)
        s["v-", 0] = push(p, 0, 0, 0, -1)
        state.append(s)
    for p in parts:
        give(p, 0, 0)
    for p, s in zip(parts, state):
        s["u+"].wait_recv()
        s["ur+"] = push(p, -1, 0, 1, 0, p[0], p[1])
        s["v+", 1] = push(p, -1, 0, 0, 1)
        s["v-", 1] = push(p, -1, 0, 0, -1)
        give(p, -1, 0)
    for p, s in zip(parts, state):
        s["u-"].wait_recv()
        s["ur-"] = push(p, 1, 0, -1, 0, p[1], p[2])
        s["v+", 2] = push(p, 1, 0, 0, 1)
        s["v-", 2] = push(p, 1, 0, 0, -1)
        give(p, 1, 0)
    offset = {0: 0, 1: -1, 2: 1, 3: 2}

    def arrive(p, s, k):
        s["v+", k].wait_recv()
        if k in (0, 3):
            s["vr+", k] = push(p, offset[k], -1, 0, 1)
        give(p, offset[k], -1)
        s["v-", k].wait_recv()
        if k in (1, 2):
            s["vr-", k] = push(p, offset[k], 1, 0, -1)
        give(p, offset[k], 1)

    for p, s in zip(parts, state):
        arrive(p, s, 0)
    for p, s in zip(parts, state):
        s["ur+"].wait_recv()
        s["ur-"].wait_recv()
        s["v+", 3] = push(p, 2, 0, 0, 1)
        s["v-", 3] = push(p, 2, 0, 0, -1)
        give(p, 2, 0)
    for k in (1, 2, 3):
        for p, s in zip(parts, state):
            arrive(p, s, k)
    for k, name in ((0, "vr+"), (1, "vr-"), (2, "vr-"), (3, "vr+")):
        for p, s in zip(parts, state):
            s[name, k].wait_recv()
            give(p, offset[k], 2)
    return crossing


def norm_gather(links, rows_f32, gain_ref, xbuf, stat, out):
    rows, chunk = rows_f32.shape
    xbuf[0, :rows, :] = rows_f32
    xbuf[0, rows:, :] = jnp.broadcast_to(gain_ref[...], (8, chunk))
    line = [links.send(xbuf.at[0], xbuf.at[(NX - dx) % NX], links.at_line(dx, 0)) for dx in (1, 3, 2)]
    yield
    phase = Phases()
    phase("ng_line")
    for c in line:
        c.wait_recv()
    phase("ng_stats")
    held = xbuf[:, :rows, :]
    count = NX * chunk
    mean = jnp.sum(jnp.sum(held, axis=0), axis=-1, keepdims=True) / count
    dev = held - mean[None]
    square = jnp.sum(jnp.sum(dev * dev, axis=0), axis=-1, keepdims=True)
    lane = lax.broadcasted_iota(jnp.int32, (rows, 128), 1)
    stat[0] = jnp.where(lane == 0, mean, square)
    links.send(stat.at[0], stat.at[1], links.at_line(0, True)).wait_recv()
    other_mean, other_square = stat[1, :, 0:1], stat[1, :, 1:2]
    both = (mean + other_mean) * 0.5
    gap = mean - other_mean
    var = (square + other_square + gap * gap * (count * 0.5)) / (2 * count)
    scale = lax.rsqrt(var + EPS)
    for e in range(NX):
        out[0, links.slot_rows(0, 0, rows), e * chunk:(e + 1) * chunk] = (
            (xbuf[e, :rows, :] - both) * scale * xbuf[e, rows:rows + 1, :]).astype(jnp.bfloat16)
    phase("ng_plane")
    crossing = plane_gather(links, out)
    phase("ng_cross")
    for c in crossing:
        c.wait_recv()
    phase.close()


def step_kernel(vocab_own, own_rows, hid_ref, gain_a, gain_f, cos_ref, sin_ref, len_ref, k_hbm, v_hbm,
                wq_ref, wk_ref, wv_ref, wg_ref, wu_ref, wo_hbm, wd_hbm, emb_ref,
                knew_ref, vnew_ref, z_ref, norm_ref,
                k_buf, v_buf, wo_buf, wd_buf, n_buf, w_buf, wq_t, wq_buf, sel, sel_t, qx, qr, qy, qf,
                kvp, kvr, o_buf, o_got, o_send, o_all, act,
                part, ra1, rb1, ra2, rb2, acc_a, acc_b, xbuf, stat, xbuf2, stat2, f_buf, emb_buf, lse_x, lse_y,
                send_sem, recv_sem, local_sem):
    links = Links(send_sem, recv_sem)
    phase = Phases()
    f32, bf16 = jnp.float32, jnp.bfloat16
    z, y, xid, yid = links.z, links.y, links.x_idx, links.y_idx
    rows, chunk = hid_ref.shape[2], hid_ref.shape[3]
    half = chunk // 2
    nx2, nyz = 2 * NX, NY * NZ
    group = NY * rows
    head = 128
    pad = 8
    others = [(dx, oc) for dx, oc in ((0, 1), (1, 0), (3, 0), (1, 1), (3, 1), (2, 0), (2, 1))]

    def line_id(dx, oc):
        core = 1 - links.core if oc else links.core
        return (links.chip + dx) % NX * 2 + core

    local = []

    def fetch(src, dst):
        copy = pltpu.make_async_copy(src, dst, local_sem.at[len(local)])
        copy.start()
        local.append(copy)
        return copy

    ff = wg_ref.shape[1] // nx2

    def w_piece(ref, dx, oc):
        return ref.at[:, pl.ds(pl.multiple_of(line_id(dx, oc) * ff, ff), ff)]

    def w_slot(which, dx, oc):
        back = (NX - dx) % NX
        return w_buf.at[int(oc), pl.ds(back * chunk, chunk), pl.ds(which * ff, ff)]

    take = emb_buf.shape[1]

    def emb_start(xi):
        return pl.multiple_of(vocab_own * xi // 16 * 16 - xi // (nx2 - 1) * 16, 16)

    def emb_piece(dx, oc):
        return emb_ref.at[pl.ds(emb_start(line_id(dx, oc)), take), :]

    def emb_slot(dx, oc):
        return emb_buf.at[int(oc), :, pl.ds((NX - dx) % NX * chunk, chunk)]

    phase("start")
    own_w = [fetch(w_piece(wg_ref, 0, 0), w_slot(0, 0, 0)), fetch(w_piece(wu_ref, 0, 0), w_slot(1, 0, 0))]
    got_kv = [fetch(k_hbm, k_buf), fetch(v_hbm, v_buf)]
    got_wo, got_wd = fetch(wo_hbm, wo_buf), fetch(wd_hbm, wd_buf)
    own_emb = fetch(emb_piece(0, 0), emb_slot(0, 0))

    qc = wq_ref.shape[1]
    qs = qc // nx2
    per = head // qs
    eye_q = (lax.broadcasted_iota(jnp.int32, (qc, qc), 0) == lax.broadcasted_iota(jnp.int32, (qc, qc), 1))
    wq_t[...] = lax.dot_general(eye_q.astype(bf16), wq_ref[...], (((1,), (1,)), ((), ())),
                                preferred_element_type=f32).astype(bf16)
    wq_buf[...] = jnp.zeros(wq_buf.shape, bf16)

    def q_rows(xi):
        return pl.ds(pl.multiple_of(xi % per * qs, qs), qs)

    wq_buf[0, q_rows(xid), 0:chunk] = wq_t[pl.ds(pl.multiple_of(xid * qs, qs), qs), :]
    phase("barrier")
    links.barrier()

    phase("front_send")
    front = norm_gather(links, hid_ref[z, y].astype(f32), gain_a, xbuf, stat, n_buf)
    next(front)
    wq_got, w_got = [], []
    for dx, oc in others:
        xi = line_id(dx, oc)
        wq_got.append(links.send(wq_t.at[pl.ds(pl.multiple_of(xi * qs, qs), qs), :],
                                 wq_buf.at[int(oc), q_rows(xi), pl.ds((NX - dx) % NX * chunk, chunk)],
                                 links.at_line(dx, oc)))
    for dx, oc in others:
        for which, ref in enumerate((wg_ref, wu_ref)):
            w_got.append(links.send(w_piece(ref, dx, oc), w_slot(which, dx, oc), links.at_line(dx, oc)))

    phase("selections")
    total_rows = nyz * rows
    r_id = lax.broadcasted_iota(jnp.int32, (nx2 * nyz * pad, 1), 0)
    r_j = r_id % pad
    r_src = jnp.where(r_j < own_rows, r_id // pad % nyz * rows + r_id // (pad * nyz) * own_rows + r_j, -1)
    s_id = lax.broadcasted_iota(jnp.int32, (1, total_rows), 1)
    sel[...] = jnp.where(r_src == s_id, 1.0, 0.0).astype(bf16)
    t_id = lax.broadcasted_iota(jnp.int32, (total_rows, 1), 0)
    t_in = t_id % rows
    t_src = t_in // own_rows * (nyz * pad) + t_id // rows * pad + t_in % own_rows
    u_id = lax.broadcasted_iota(jnp.int32, (1, nx2 * nyz * pad), 1)
    sel_t[...] = jnp.where(t_src == u_id, 1.0, 0.0).astype(bf16)
    k_id = lax.broadcasted_iota(jnp.int32, (nx2 * pad, rows), 0)
    k_src = jnp.where(k_id % pad < own_rows, k_id // pad * own_rows + k_id % pad, -1)
    sel_kv = jnp.where(k_src == lax.broadcasted_iota(jnp.int32, (nx2 * pad, rows), 1), 1.0, 0.0).astype(bf16)

    phase.close()
    for _ in front:
        pass
    phase("kv_part")

    n_own = jnp.dot(sel_kv, n_buf[0, links.slot_rows(0, 0, rows), 0:chunk], preferred_element_type=f32).astype(bf16)
    kvp[:, :, :head] = jnp.dot(n_own, wk_ref[...], preferred_element_type=f32).reshape(nx2, pad, head)
    kvp[:, :, head:] = jnp.dot(n_own, wv_ref[...], preferred_element_type=f32).reshape(nx2, pad, head)
    kv_got = [links.send(kvp.at[line_id(dx, oc)], kvr.at[xid], links.at_line(dx, oc)) for dx, oc in others]
    kvr[xid] = kvp[xid]

    phase("wait_wq")
    for c in wq_got:
        c.wait_recv()

    def wide(buf, i, h):
        return buf[h, i * group:(i + 1) * group, :]

    phase("q_mm")
    q_blocks = []
    for i in range(NZ):
        q_blocks.append((lax.dot_general(wide(n_buf, i, 0), wq_buf[0], (((1,), (1,)), ((), ())), preferred_element_type=f32)
                         + lax.dot_general(wide(n_buf, i, 1), wq_buf[1], (((1,), (1,)), ((), ())), preferred_element_type=f32)
                         ).astype(bf16))
    q_all = jnp.concatenate(q_blocks, axis=0)
    span = nyz * pad
    for i in range(nx2):
        qx[i] = jnp.dot(sel[i * span:(i + 1) * span, :], q_all, preferred_element_type=f32).astype(bf16)
    q_got = [links.send(qx.at[line_id(dx, oc)], qr.at[xid], links.at_line(dx, oc)) for dx, oc in others]
    qr[xid] = qx[xid]
    phase("wait_q")
    for c in q_got:
        c.wait_recv()
    phase("q_sum")
    for j in range(qc // head):
        piece = qr[j * per].astype(f32)
        for i in range(1, per):
            piece = piece + qr[j * per + i].astype(f32)
        qy[:, :, j * head:(j + 1) * head] = piece.reshape(nyz, pad, head)
    plane = [(dz, dy) for dz in range(NZ) for dy in range(NY) if (dz, dy) != (0, 0)]

    def plane_id(dz, dy):
        return (z + dz) % NZ * NY + (y + dy) % NY

    y_got = [links.send(qy.at[plane_id(dz, dy)], qf.at[yid], links.at_plane(dz, dy)) for dz, dy in plane]
    qf[yid] = qy[yid]

    phase("wait_kv")
    for c in kv_got:
        c.wait_recv()
    kv_sum = kvr[0]
    for i in range(1, nx2):
        kv_sum = kv_sum + kvr[i]
    kv_new = kv_sum.astype(bf16).astype(f32)

    def turn(v, b=None):
        cos, sin = (cos_ref[...], sin_ref[...]) if b is None else (cos_ref[b:b + 1, :], sin_ref[b:b + 1, :])
        return (v * cos + pltpu.roll(v, head // 2, 1) * sin).astype(bf16)

    k_new = turn(kv_new[:, :head])
    knew_ref[...] = k_new
    vnew_ref[...] = kv_new[:, head:].astype(bf16)
    k_row, v_row = k_new.astype(f32), kv_new[:, head:]
    phase("wait_qy")
    for c in got_kv:
        c.wait()
    for c in y_got:
        c.wait_recv()
    phase("attention")
    seq = k_buf.shape[1]
    score_scale = head ** -0.5
    position = lax.broadcasted_iota(jnp.int32, (1, seq), 1)
    o_buf[...] = jnp.zeros(o_buf.shape, f32)
    for b in range(own_rows):
        q_b = jnp.concatenate([turn(qf[:, b, j * head:(j + 1) * head], b) for j in range(qc // head)], axis=0)
        scores = lax.dot_general(q_b, k_buf[b], (((1,), (1,)), ((), ())), preferred_element_type=f32) * score_scale
        score_new = jnp.sum(q_b.astype(f32) * k_row[b:b + 1, :], axis=-1, keepdims=True) * score_scale
        valid = position < len_ref[b:b + 1, 0:1]
        top = jnp.maximum(jnp.max(jnp.where(valid, scores, -jnp.inf), axis=-1, keepdims=True), score_new)
        weights = jnp.where(valid, jnp.exp(scores - top), 0.0)
        weight_new = jnp.exp(score_new - top)
        denom = jnp.sum(weights, axis=-1, keepdims=True) + weight_new
        o_b = jnp.dot((weights / denom).astype(bf16), v_buf[b], preferred_element_type=f32)
        o_b = o_b + (weight_new / denom).astype(bf16).astype(f32) * v_row[b:b + 1, :]
        o_b = o_b.astype(bf16).astype(f32)
        for j in range(qc // head):
            o_buf[:, b, j * head:(j + 1) * head] = o_b[j * nyz:(j + 1) * nyz, :]
    phase("wait_oy")
    o_back = [links.send(o_buf.at[plane_id(dz, dy)], o_got.at[yid], links.at_plane(dz, dy)) for dz, dy in plane]
    o_got[yid] = o_buf[yid]
    for c in o_back:
        c.wait_recv()
    phase("o_send")
    o_all[xid] = o_got[...].reshape(span, qc).astype(bf16)
    o_line = [links.send(o_all.at[xid], o_all.at[xid], links.at_line(dx, oc)) for dx, oc in others]

    phase("wait_w")
    for c in own_w:
        c.wait()
    for c in w_got:
        c.wait_recv()
    phase("gate_up")
    own_cols = pl.ds(pl.multiple_of(xid * ff, ff), ff)
    a_got = []
    partner = links.at_line(0, True)
    for i in range(NZ):
        both = (jnp.dot(wide(n_buf, i, 0), w_buf[0], preferred_element_type=f32)
                + jnp.dot(wide(n_buf, i, 1), w_buf[1], preferred_element_type=f32)).astype(bf16).astype(f32)
        gate, up = both[:, :ff], both[:, ff:]
        act[i, :, own_cols] = (gate * jax.nn.sigmoid(gate) * up).astype(bf16)
        here = act.at[i, :, own_cols]
        a_got.append([links.send(here, here, links.at_line(dx, 0)) for dx in (1, 3, 2)]
                     + [links.send(here, here, partner)])

    phase("emb_send")
    emb = [links.send(emb_piece(dx, oc), emb_slot(dx, oc), links.at_line(dx, oc)) for dx, oc in others[:5]]

    phase("wait_o")
    for c in o_line:
        c.wait_recv()
    got_wo.wait()
    got_wd.wait()
    phase("out_mm")
    for i in range(NZ):
        o_nat = jnp.dot(sel_t[i * group:(i + 1) * group, :], o_all[...].reshape(nx2 * span, qc),
                        preferred_element_type=f32).astype(bf16)
        part[i] = jnp.dot(o_nat, wo_buf[...], preferred_element_type=f32).reshape(NY, rows, chunk)
    phase("wait_act")
    passed = []
    for i in range(NZ):
        for dx, c in zip((1, 3, 2), a_got[i]):
            c.wait_recv()
            came = pl.ds(pl.multiple_of(line_id((NX - dx) % NX, 0) * ff, ff), ff)
            passed.append(links.send(act.at[i, :, came], act.at[i, :, came], partner))
        a_got[i][3].wait_recv()
    phase("down_mm")
    for i in range(NZ):
        for c in passed[i * 3:i * 3 + 3]:
            c.wait_recv()
        part[i] = part[i] + jnp.dot(act[i], wd_buf[...], preferred_element_type=f32).reshape(NY, rows, chunk)

    phase("rs_send")
    low, high = pl.ds(0, half), pl.ds(half, half)
    first = []
    for d in (1, 3, 2):
        first.append((
            links.send(part.at[:, (y + d) % NY, :, low], ra1.at[d - 1], links.at_plane(0, d)),
            links.send(part.at[(z + d) % NZ, :, :, high], rb1.at[d - 1], links.at_plane(d, 0))))
    phase("wait_rs1")
    for ca, cb in first:
        ca.wait_recv()
        cb.wait_recv()
    phase("rs_sum1")
    acc_a[...] = (part[:, y, :, :half] + ra1[0]) + (ra1[1] + ra1[2])
    second_a = [links.send(acc_a.at[(z + d) % NZ], ra2.at[d - 1], links.at_plane(d, 0)) for d in (1, 3, 2)]
    acc_b[...] = (part[z, :, :, half:] + rb1[0]) + (rb1[1] + rb1[2])
    second_b = [links.send(acc_b.at[(y + d) % NY], rb2.at[d - 1], links.at_plane(0, d)) for d in (1, 3, 2)]
    phase("wait_rs2")
    for c in second_a + second_b:
        c.wait_recv()
    phase("rs_sum2")
    branch = jnp.concatenate([(acc_a[z] + ra2[0]) + (ra2[1] + ra2[2]), (acc_b[y] + rb2[0]) + (rb2[1] + rb2[2])], axis=1)
    back = norm_gather(links, hid_ref[z, y].astype(f32) + branch, gain_f, xbuf2, stat2, f_buf)
    next(back)
    emb += [links.send(emb_piece(dx, oc), emb_slot(dx, oc), links.at_line(dx, oc)) for dx, oc in others[5:]]
    phase.close()
    for _ in back:
        pass
    phase("wait_emb")
    own_emb.wait()
    for c in emb:
        c.wait_recv()

    phase("logits")
    wide_n = 256
    for i in range(total_rows // wide_n):
        cols = slice(i * wide_n, (i + 1) * wide_n)
        z_ref[:, cols] = (
            lax.dot_general(emb_buf[0], f_buf[0, cols, :], (((1,), (1,)), ((), ())), preferred_element_type=f32)
            + lax.dot_general(emb_buf[1], f_buf[1, cols, :], (((1,), (1,)), ((), ())), preferred_element_type=f32))

    phase("lse_own")
    shift = vocab_own * xid - emb_start(xid)
    vid = lax.broadcasted_iota(jnp.int32, (take, 1), 0)
    own = (vid >= shift) & (vid < shift + vocab_own)
    blocks = total_rows // 128
    for b in range(blocks):
        zb = jnp.where(own, z_ref[:, b * 128:(b + 1) * 128], -jnp.inf)
        top = jnp.max(zb, axis=0, keepdims=True)
        lse_x[xid, b:b + 1, :] = top
        lse_x[xid, 8 + b:9 + b, :] = jnp.sum(jnp.exp(zb - top), axis=0, keepdims=True)
    for b in range(blocks, 8):
        lse_x[xid, b:b + 1, :] = jnp.zeros((1, 128), f32)
        lse_x[xid, 8 + b:9 + b, :] = jnp.ones((1, 128), f32)

    def merge(ref):
        tops = ref[:, :8, :]
        top = jnp.max(tops, axis=0)
        return top, jnp.sum(ref[:, 8:, :] * jnp.exp(tops - top[None]), axis=0)

    phase("lse_line")
    got = [links.send(lse_x.at[xid], lse_x.at[xid], links.at_line(dx, oc)) for dx, oc in others]
    for c in got:
        c.wait_recv()
    top, mass = merge(lse_x)
    lse_y[yid, :8, :] = top
    lse_y[yid, 8:, :] = mass
    phase("lse_plane")
    got = [links.send(lse_y.at[yid], lse_y.at[yid], links.at_plane(dz, dy)) for dz, dy in plane]
    for c in got:
        c.wait_recv()
    top, mass = merge(lse_y)
    norm_ref[...] = top + jnp.log(mass)
    phase("finish")
    links.finish()
    phase.close()


def whole_step(hidden, cos, sin, lens, k_cache, v_cache, g_attn, w_query, w_key, w_value,
               w_gate, w_up, w_out, w_down, g_final, embedding):
    total_rows, chunk = hidden.shape
    own_rows, seq, head = k_cache.shape
    rows = total_rows // (NY * NZ)
    vocab_own = embedding.shape[0] // (2 * NX)
    take = (vocab_own + 30) // 16 * 16
    half = chunk // 2
    qc = w_query.shape[1]
    ff = w_gate.shape[1] // (2 * NX)
    f32, bf16 = jnp.float32, jnp.bfloat16
    nyz, nx2, pad = NY * NZ, 2 * NX, 8
    copies = 360
    vmem = pl.BlockSpec(memory_space=pltpu.VMEM)
    hbm = pl.BlockSpec(memory_space=pl.ANY)
    V = pltpu.VMEM
    return pl.pallas_call(
        lambda *refs: step_kernel(vocab_own, own_rows, *refs),
        out_shape=(jax.ShapeDtypeStruct((pad, head), bf16), jax.ShapeDtypeStruct((pad, head), bf16),
                   jax.ShapeDtypeStruct((take, total_rows), f32), jax.ShapeDtypeStruct((8, 128), f32)),
        in_specs=[vmem] * 6 + [hbm] * 2 + [vmem] * 3 + [hbm] * 5,
        out_specs=(vmem,) * 4,
        scratch_shapes=[
            V((own_rows, seq, head), bf16), V((own_rows, seq, head), bf16), V((qc, chunk), bf16),
            V((nx2 * ff, chunk), bf16), V((2, total_rows, NX * chunk), bf16), V((2, NX * chunk, 2 * ff), bf16),
            V((qc, chunk), bf16), V((2, head, NX * chunk), bf16),
            V((nx2 * nyz * pad, total_rows), bf16), V((total_rows, nx2 * nyz * pad), bf16),
            V((nx2, nyz * pad, head), bf16), V((nx2, nyz * pad, head), bf16),
            V((nyz, pad, qc), f32), V((nyz, pad, qc), f32),
            V((nx2, pad, 2 * head), f32), V((nx2, pad, 2 * head), f32),
            V((nyz, pad, qc), f32), V((nyz, pad, qc), f32), V((8, 128), f32), V((nx2, nyz * pad, qc), bf16),
            V((NZ, NY * rows, nx2 * ff), bf16),
            V((NZ, NY, rows, chunk), f32),
            V((3, NZ, rows, half), f32), V((3, NY, rows, half), f32), V((3, rows, half), f32), V((3, rows, half), f32),
            V((NZ, rows, half), f32), V((NY, rows, half), f32),
            V((NX, rows + 8, chunk), f32), V((2, rows, 128), f32), V((NX, rows + 8, chunk), f32), V((2, rows, 128), f32),
            V((2, total_rows, NX * chunk), bf16), V((2, take, NX * chunk), bf16),
            V((nx2, 16, 128), f32), V((nyz, 16, 128), f32),
            pltpu.SemaphoreType.DMA((copies,)), pltpu.SemaphoreType.DMA((copies,)), pltpu.SemaphoreType.DMA((8,)),
        ],
        compiler_params=pltpu.CompilerParams(
            collective_id=1, has_side_effects=True, vmem_limit_bytes=60 * 1024 * 1024),
        name="decode_step",
    )(hidden.reshape(NZ, NY, rows, chunk), g_attn[None, :], g_final[None, :], cos, sin, lens, k_cache, v_cache,
      w_query, w_key, w_value, w_gate, w_up, w_out, w_down, embedding)


def solution(mesh):
    x_size = mesh.shape["xax"]
    row_spec = P(("dp", "yax", "xax"))

    def local_step(hidden, cache_len, k_cache, v_cache, g_attn, w_query, w_key, w_value,
                   w_gate, w_up, w_out, w_down, g_final, embedding):
        rows = hidden.shape[0]
        own_rows, _, head_dim = k_cache.shape
        y_idx = lax.axis_index("yax")
        x_idx = lax.axis_index("xax")
        own_start = (y_idx * x_size + x_idx) * own_rows
        len_own = jnp.pad(lax.dynamic_slice_in_dim(cache_len, own_start, own_rows, axis=0), (0, 8 - own_rows))
        angles = rope_angle(len_own, head_dim)
        cos_half, sin_half = jnp.cos(angles), jnp.sin(angles)
        cos = jnp.concatenate([cos_half, cos_half], axis=1)
        sin = jnp.concatenate([-sin_half, sin_half], axis=1)
        lens = jnp.broadcast_to(len_own[:, None], (8, 128))
        key_own, value_own, logits_wide, norm_tile = whole_step(
            hidden, cos, sin, lens, k_cache, v_cache, g_attn, w_query, w_key, w_value,
            w_gate, w_up, w_out, w_down, g_final, embedding)
        vocab_own = embedding.shape[0] // x_size
        log_norm = norm_tile[:rows // 128].reshape(rows)
        shift = vocab_own * x_idx - (vocab_own * x_idx // 16 * 16 - x_idx // (x_size - 1) * 16)
        logits = lax.dynamic_slice_in_dim(logits_wide, shift, vocab_own, axis=0)
        return key_own[:own_rows], value_own[:own_rows], (logits - log_norm[None, :]).T, log_norm

    in_specs = (P("dp", "xax"), P("dp"), row_spec, row_spec, P("xax"), P("xax", "yax"),
                P("xax", None), P("xax", None), P("xax", "yax"), P("xax", "yax"),
                P("yax", "xax"), P("yax", "xax"), P("xax"), P("yax", "xax"))
    out_specs = (row_spec, row_spec, P("dp", ("yax", "xax")), P("dp"))
    return jax.shard_map(local_step, mesh=mesh, in_specs=in_specs, out_specs=out_specs, check_vma=False)
```

```python
import jax
import jax.numpy as jnp
from jax import lax
from jax.experimental import pallas as pl
from jax.experimental.pallas import tpu as pltpu
from jax.sharding import PartitionSpec as P

EPS = 1e-6
ROPE_BASE = 10000.0
MESH_ID = pl.DeviceIdType.MESH
NY, NZ, NX = 4, 4, 4


def rope_angle(positions, head_dim):
    half_dim = head_dim // 2
    inv_freq = ROPE_BASE ** (-(jnp.arange(half_dim, dtype=jnp.float32) * 2.0) / head_dim)
    return positions.astype(jnp.float32)[:, None] * inv_freq[None, :]


class Phases:
    def __init__(self):
        self.open = None

    def __call__(self, name):
        self.close()
        self.open = jax.named_scope(name)
        self.open.__enter__()

    def close(self):
        if self.open is not None:
            self.open.__exit__(None, None, None)
        self.open = None


class Links:
    def __init__(self, send_sem, recv_sem):
        self.send_sem, self.recv_sem, self.count, self.sent = send_sem, recv_sem, 0, []
        self.y_idx = lax.axis_index("yax")
        self.x_idx = lax.axis_index("xax")
        self.z, self.y = self.y_idx // NY, self.y_idx % NY
        self.chip, self.core = self.x_idx // 2, self.x_idx % 2

    def at_plane(self, dz, dy):
        return {"yax": (self.z + dz) % NZ * NY + (self.y + dy) % NY, "xax": self.x_idx}

    def slot_rows(self, dz, dy, rows):
        slot = (self.z + dz) % NZ * NY + (self.y + dy) % NY
        return pl.ds(pl.multiple_of(slot * rows, rows), rows)

    def at_line(self, dx, other_core):
        core = 1 - self.core if other_core else self.core
        return {"yax": self.y_idx, "xax": (self.chip + dx) % NX * 2 + core}

    def send(self, src, dst, where):
        copy = pltpu.make_async_remote_copy(
            src_ref=src, dst_ref=dst, send_sem=self.send_sem.at[self.count], recv_sem=self.recv_sem.at[self.count],
            device_id=where, device_id_type=MESH_ID)
        self.count += 1
        copy.start()
        self.sent.append(copy)
        return copy

    def finish(self):
        for copy in self.sent:
            copy.wait_send()
        self.sent = []

    def barrier(self):
        barrier = pltpu.get_barrier_semaphore()
        peers = [self.at_line(dx, oc) for dx in range(NX) for oc in (0, 1) if (dx, oc) != (0, 0)]
        peers += [self.at_plane(dz, dy) for dz in range(NZ) for dy in range(NY) if (dz, dy) != (0, 0)]
        for peer in peers:
            pl.semaphore_signal(barrier, inc=1, device_id=peer, device_id_type=MESH_ID)
        pl.semaphore_wait(barrier, len(peers))


def plane_gather(links, buf, hook=None):
    cols = buf.shape[-1]
    rows = buf.shape[1] // (NY * NZ)
    parts = []
    for part in range(2):
        lo = part * (cols // 2)
        mid = lo + cols // 4
        hi = lo + cols // 2

        def slot(du, dv, a, b, half=0, part=part):
            dz, dy = (dv, du) if part == 0 else (du, dv)
            return buf.at[half, links.slot_rows(dz, dy, rows), pl.ds(a, b - a)]

        def node(du, dv, part=part):
            return links.at_plane(dv, du) if part == 0 else links.at_plane(du, dv)

        parts.append((lo, mid, hi, slot, node))

    partner = links.at_line(0, True)
    crossing = []

    def give(p, du, dv):
        lo, mid, hi, slot, node = p
        crossing.append(links.send(slot(du, dv, lo, hi), slot(du, dv, lo, hi, half=1), partner))

    def push(p, du, dv, to_u, to_v, a=None, b=None):
        lo, mid, hi, slot, node = p
        a, b = (lo if a is None else a), (hi if b is None else b)
        return links.send(slot(du, dv, a, b), slot(du, dv, a, b), node(to_u, to_v))

    state = []
    for p in parts:
        s = {"u+": push(p, 0, 0, 1, 0), "u-": push(p, 0, 0, -1, 0)}
        s["v+", 0] = push(p, 0, 0, 0, 1)
        s["v-", 0] = push(p, 0, 0, 0, -1)
        state.append(s)
    for p in parts:
        give(p, 0, 0)
    for p, s in zip(parts, state):
        s["u+"].wait_recv()
        s["ur+"] = push(p, -1, 0, 1, 0, p[0], p[1])
        s["v+", 1] = push(p, -1, 0, 0, 1)
        s["v-", 1] = push(p, -1, 0, 0, -1)
        give(p, -1, 0)
    for p, s in zip(parts, state):
        s["u-"].wait_recv()
        s["ur-"] = push(p, 1, 0, -1, 0, p[1], p[2])
        s["v+", 2] = push(p, 1, 0, 0, 1)
        s["v-", 2] = push(p, 1, 0, 0, -1)
        give(p, 1, 0)
    if hook is not None:
        hook()
    offset = {0: 0, 1: -1, 2: 1, 3: 2}

    def arrive(p, s, k):
        s["v+", k].wait_recv()
        if k in (0, 3):
            s["vr+", k] = push(p, offset[k], -1, 0, 1)
        give(p, offset[k], -1)
        s["v-", k].wait_recv()
        if k in (1, 2):
            s["vr-", k] = push(p, offset[k], 1, 0, -1)
        give(p, offset[k], 1)

    for p, s in zip(parts, state):
        arrive(p, s, 0)
    for p, s in zip(parts, state):
        s["ur+"].wait_recv()
        s["ur-"].wait_recv()
        s["v+", 3] = push(p, 2, 0, 0, 1)
        s["v-", 3] = push(p, 2, 0, 0, -1)
        give(p, 2, 0)
    for k in (1, 2, 3):
        for p, s in zip(parts, state):
            arrive(p, s, k)
    for k, name in ((0, "vr+"), (1, "vr-"), (2, "vr-"), (3, "vr+")):
        for p, s in zip(parts, state):
            s[name, k].wait_recv()
            give(p, offset[k], 2)
    return crossing


def norm_gather(links, own_slot, gain_buf, which, xbuf, stat, out, hook=None):
    own_slot()
    rows, chunk = xbuf.shape[1:]
    line = [links.send(xbuf.at[0], xbuf.at[(NX - dx) % NX], links.at_line(dx, 0)) for dx in (1, 3, 2)]
    yield
    phase = Phases()
    for n, c in enumerate(line):
        phase(f"ng_line{which}_{n}")
        c.wait_recv()
    phase("ng_stats")
    held = xbuf[...].astype(jnp.float32)
    count = NX * chunk
    mean = jnp.sum(jnp.sum(held, axis=0), axis=-1, keepdims=True) / count
    dev = held - mean[None]
    square = jnp.sum(jnp.sum(dev * dev, axis=0), axis=-1, keepdims=True)
    lane = lax.broadcasted_iota(jnp.int32, (rows, 128), 1)
    stat[0] = jnp.where(lane == 0, mean, square)
    links.send(stat.at[0], stat.at[1], links.at_line(0, True)).wait_recv()
    other_mean, other_square = stat[1, :, 0:1], stat[1, :, 1:2]
    both = (mean + other_mean) * 0.5
    gap = mean - other_mean
    var = (square + other_square + gap * gap * (count * 0.5)) / (2 * count)
    scale = lax.rsqrt(var + EPS)
    for e in range(NX):
        out[0, links.slot_rows(0, 0, rows), e * chunk:(e + 1) * chunk] = (
            (xbuf[e].astype(jnp.float32) - both) * scale * gain_buf[e, which:which + 1, :]).astype(jnp.bfloat16)
    phase("ng_plane")
    crossing = plane_gather(links, out, hook)
    phase("ng_cross")
    for c in crossing:
        c.wait_recv()
    phase.close()


def step_kernel(vocab_own, own_rows, hid_ref, gain_a, gain_f, cos_ref, sin_ref, len_ref, k_hbm, v_hbm,
                wq_ref, wk_ref, wv_ref, wg_ref, wu_ref, wo_hbm, wd_hbm, emb_ref,
                knew_ref, vnew_ref, z_ref, norm_ref,
                k_buf, v_buf, wo_buf, wd_buf, n_buf, w_buf, wq_t, wq_buf, sel, sel_t, qx, qr, qy, qf,
                kvp, kvr, o_buf, o_got, o_all, act,
                part, ra1, rb1, ra2, rb2, acc_a, acc_b, xbuf, stat, xbuf2, stat2, gains, f_buf, emb_buf,
                w_relay, emb_relay, lse_x, lse_y, send_sem, recv_sem, local_sem):
    links = Links(send_sem, recv_sem)
    phase = Phases()
    f32, bf16 = jnp.float32, jnp.bfloat16
    z, y, xid, yid = links.z, links.y, links.x_idx, links.y_idx
    rows, chunk = hid_ref.shape[2], hid_ref.shape[3]
    half = chunk // 2
    nx2, nyz = 2 * NX, NY * NZ
    group = NY * rows
    head = 128
    pad = 8
    others = [(dx, oc) for dx, oc in ((0, 1), (1, 0), (3, 0), (1, 1), (3, 1), (2, 0), (2, 1))]
    near = [(1, 0), (3, 0), (1, 1), (3, 1)]
    partner = links.at_line(0, True)

    def line_id(dx, oc):
        core = 1 - links.core if oc else links.core
        return (links.chip + dx) % NX * 2 + core

    local = []

    def fetch(src, dst):
        copy = pltpu.make_async_copy(src, dst, local_sem.at[len(local)])
        copy.start()
        local.append(copy)
        return copy

    ff = wg_ref.shape[1] // nx2

    def w_piece(ref, dx, oc):
        return ref.at[:, pl.ds(pl.multiple_of(line_id(dx, oc) * ff, ff), ff)]

    def w_slot(which, dx, oc):
        back = (NX - dx) % NX
        return w_buf.at[int(oc), pl.ds(back * chunk, chunk), pl.ds(which * ff, ff)]

    take = emb_buf.shape[1]

    def emb_start(xi):
        return pl.multiple_of(vocab_own * xi // 16 * 16 - xi // (nx2 - 1) * 16, 16)

    def emb_piece(dx, oc):
        return emb_ref.at[pl.ds(emb_start(line_id(dx, oc)), take), :]

    def emb_slot(dx, oc):
        return emb_buf.at[int(oc), :, pl.ds((NX - dx) % NX * chunk, chunk)]

    def emb_half(oc, way):
        part_rows = take // 2
        return emb_ref.at[pl.ds(emb_start(line_id(2, oc)) + way * part_rows, part_rows), :]

    def emb_far_slot(oc, way):
        return emb_buf.at[int(oc), pl.ds(way * (take // 2), take // 2), pl.ds(2 * chunk, chunk)]

    phase("start")
    own_w = [fetch(w_piece(wg_ref, 0, 0), w_slot(0, 0, 0)), fetch(w_piece(wu_ref, 0, 0), w_slot(1, 0, 0))]
    got_kv = [fetch(k_hbm, k_buf), fetch(v_hbm, v_buf)]
    got_wo, got_wd = fetch(wo_hbm, wo_buf), fetch(wd_hbm, wd_buf)
    own_emb = fetch(emb_piece(0, 0), emb_slot(0, 0))

    qc = wq_ref.shape[1]
    qs = qc // nx2
    per = head // qs
    eye_q = (lax.broadcasted_iota(jnp.int32, (qc, qc), 0) == lax.broadcasted_iota(jnp.int32, (qc, qc), 1))
    wq_t[...] = lax.dot_general(eye_q.astype(bf16), wq_ref[...], (((1,), (1,)), ((), ())),
                                preferred_element_type=f32).astype(bf16)
    wq_buf[...] = jnp.zeros(wq_buf.shape, bf16)

    def q_rows(xi):
        return pl.ds(pl.multiple_of(xi % per * qs, qs), qs)

    wq_buf[0, q_rows(xid), 0:chunk] = wq_t[pl.ds(pl.multiple_of(xid * qs, qs), qs), :]
    phase("barrier")
    links.barrier()

    phase("front_send")
    gains[0, 0:1, :] = gain_a[...]
    gains[0, 1:2, :] = gain_f[...]
    gains[0, 2:, :] = jnp.zeros((6, chunk), f32)

    def own_input():
        xbuf[0] = hid_ref[z, y]

    w_far, wq_got, w_got, emb_far, emb_got = [], [], [], [], []
    ways = ((0, 1, 3), (1, 3, 1))

    def forward_weights():
        for way, hop, _ in ways:
            for oc in (0, 1):
                w_far[way * 2 + oc].wait_recv()
                w_got.append(links.send(w_relay.at[way, oc],
                                        w_buf.at[oc, pl.ds(2 * chunk, chunk), pl.ds(way * ff, ff)],
                                        links.at_line(hop, oc)))
        for way, hop, _ in ways:
            for oc in (0, 1):
                emb_far.append(links.send(emb_half(oc, way), emb_relay.at[way, oc], links.at_line(hop, 0)))

    front = norm_gather(links, own_input, gains, 0, xbuf, stat, n_buf, forward_weights)
    next(front)
    gain_got = [links.send(gains.at[0], gains.at[(NX - dx) % NX], links.at_line(dx, 0)) for dx in (1, 3, 2)]
    for way, hop, _ in ways:
        for oc in (0, 1):
            ref = (wg_ref, wu_ref)[way]
            w_far.append(links.send(w_piece(ref, 2, oc), w_relay.at[way, oc], links.at_line(hop, 0)))
    for dx, oc in others:
        xi = line_id(dx, oc)
        wq_got.append(links.send(wq_t.at[pl.ds(pl.multiple_of(xi * qs, qs), qs), :],
                                 wq_buf.at[int(oc), q_rows(xi), pl.ds((NX - dx) % NX * chunk, chunk)],
                                 links.at_line(dx, oc)))
    for dx, oc in [(0, 1)] + near:
        for which, ref in enumerate((wg_ref, wu_ref)):
            w_got.append(links.send(w_piece(ref, dx, oc), w_slot(which, dx, oc), links.at_line(dx, oc)))

    phase("selections")
    total_rows = nyz * rows
    r_id = lax.broadcasted_iota(jnp.int32, (nx2 * nyz * pad, 1), 0)
    r_j = r_id % pad
    r_src = jnp.where(r_j < own_rows, r_id // pad % nyz * rows + r_id // (pad * nyz) * own_rows + r_j, -1)
    s_id = lax.broadcasted_iota(jnp.int32, (1, total_rows), 1)
    sel[...] = jnp.where(r_src == s_id, 1.0, 0.0).astype(bf16)
    t_id = lax.broadcasted_iota(jnp.int32, (total_rows, 1), 0)
    t_in = t_id % rows
    t_src = t_in // own_rows * (nyz * pad) + t_id // rows * pad + t_in % own_rows
    u_id = lax.broadcasted_iota(jnp.int32, (1, nx2 * nyz * pad), 1)
    sel_t[...] = jnp.where(t_src == u_id, 1.0, 0.0).astype(bf16)
    k_id = lax.broadcasted_iota(jnp.int32, (nx2 * pad, rows), 0)
    k_src = jnp.where(k_id % pad < own_rows, k_id // pad * own_rows + k_id % pad, -1)
    sel_kv = jnp.where(k_src == lax.broadcasted_iota(jnp.int32, (nx2 * pad, rows), 1), 1.0, 0.0).astype(bf16)

    phase.close()
    for c in gain_got:
        c.wait_recv()
    for _ in front:
        pass
    phase("kv_part")

    n_own = jnp.dot(sel_kv, n_buf[0, links.slot_rows(0, 0, rows), 0:chunk], preferred_element_type=f32).astype(bf16)
    kvp[:, :, :head] = jnp.dot(n_own, wk_ref[...], preferred_element_type=f32).reshape(nx2, pad, head)
    kvp[:, :, head:] = jnp.dot(n_own, wv_ref[...], preferred_element_type=f32).reshape(nx2, pad, head)
    kv_got = [links.send(kvp.at[line_id(dx, oc)], kvr.at[xid], links.at_line(dx, oc)) for dx, oc in others]
    kvr[xid] = kvp[xid]

    phase("wait_wq")
    for c in wq_got:
        c.wait_recv()

    def wide(buf, i, h):
        return buf[h, i * group:(i + 1) * group, :]

    phase("q_mm")
    q_blocks = []
    for i in range(NZ):
        q_blocks.append((lax.dot_general(wide(n_buf, i, 0), wq_buf[0], (((1,), (1,)), ((), ())), preferred_element_type=f32)
                         + lax.dot_general(wide(n_buf, i, 1), wq_buf[1], (((1,), (1,)), ((), ())), preferred_element_type=f32)
                         ).astype(bf16))
    q_all = jnp.concatenate(q_blocks, axis=0)
    span = nyz * pad
    for i in range(nx2):
        qx[i] = jnp.dot(sel[i * span:(i + 1) * span, :], q_all, preferred_element_type=f32).astype(bf16)
    q_got = [links.send(qx.at[line_id(dx, oc)], qr.at[xid], links.at_line(dx, oc)) for dx, oc in others]
    qr[xid] = qx[xid]
    phase("wait_w")
    for c in own_w:
        c.wait()
    for c in w_got:
        c.wait_recv()
    phase("gate_up")
    own_cols = pl.ds(pl.multiple_of(xid * ff, ff), ff)
    a_got = []
    for i in range(NZ):
        both = (jnp.dot(wide(n_buf, i, 0), w_buf[0], preferred_element_type=f32)
                + jnp.dot(wide(n_buf, i, 1), w_buf[1], preferred_element_type=f32)).astype(bf16).astype(f32)
        gate, up = both[:, :ff], both[:, ff:]
        act[i, :, own_cols] = (gate * jax.nn.sigmoid(gate) * up).astype(bf16)
        here = act.at[i, :, own_cols]
        a_got.append([links.send(here, here, links.at_line(dx, 0)) for dx in (1, 3, 2)]
                     + [links.send(here, here, partner)])

    phase("wait_q")
    for c in q_got:
        c.wait_recv()
    phase("q_sum")
    for j in range(qc // head):
        piece = qr[j * per].astype(f32)
        for i in range(1, per):
            piece = piece + qr[j * per + i].astype(f32)
        qy[:, :, j * head:(j + 1) * head] = piece.reshape(nyz, pad, head)
    plane = [(dz, dy) for dz in range(NZ) for dy in range(NY) if (dz, dy) != (0, 0)]

    def plane_id(dz, dy):
        return (z + dz) % NZ * NY + (y + dy) % NY

    y_got = [links.send(qy.at[plane_id(dz, dy)], qf.at[yid], links.at_plane(dz, dy)) for dz, dy in plane]
    qf[yid] = qy[yid]

    phase("emb_forward")
    for way, hop, _ in ways:
        for oc in (0, 1):
            emb_far[way * 2 + oc].wait_recv()
            emb_got.append(links.send(emb_relay.at[way, oc], emb_far_slot(oc, way), links.at_line(hop, oc)))
    emb_got.append(links.send(emb_piece(0, 1), emb_slot(0, 1), partner))

    phase("wait_kv")
    for c in kv_got:
        c.wait_recv()
    kv_sum = kvr[0]
    for i in range(1, nx2):
        kv_sum = kv_sum + kvr[i]
    kv_new = kv_sum.astype(bf16).astype(f32)

    def turn(v, b=None):
        cos, sin = (cos_ref[...], sin_ref[...]) if b is None else (cos_ref[b:b + 1, :], sin_ref[b:b + 1, :])
        return (v * cos + pltpu.roll(v, head // 2, 1) * sin).astype(bf16)

    k_new = turn(kv_new[:, :head])
    knew_ref[...] = k_new
    vnew_ref[...] = kv_new[:, head:].astype(bf16)
    k_row, v_row = k_new.astype(f32), kv_new[:, head:]
    phase("wait_qy")
    for c in got_kv:
        c.wait()
    for c in y_got:
        c.wait_recv()
    phase("attention")
    seq = k_buf.shape[1]
    score_scale = head ** -0.5
    position = lax.broadcasted_iota(jnp.int32, (1, seq), 1)
    o_buf[...] = jnp.zeros(o_buf.shape, f32)
    for b in range(own_rows):
        q_b = jnp.concatenate([turn(qf[:, b, j * head:(j + 1) * head], b) for j in range(qc // head)], axis=0)
        scores = lax.dot_general(q_b, k_buf[b], (((1,), (1,)), ((), ())), preferred_element_type=f32) * score_scale
        score_new = jnp.sum(q_b.astype(f32) * k_row[b:b + 1, :], axis=-1, keepdims=True) * score_scale
        valid = position < len_ref[b:b + 1, 0:1]
        top = jnp.maximum(jnp.max(jnp.where(valid, scores, -jnp.inf), axis=-1, keepdims=True), score_new)
        weights = jnp.where(valid, jnp.exp(scores - top), 0.0)
        weight_new = jnp.exp(score_new - top)
        denom = jnp.sum(weights, axis=-1, keepdims=True) + weight_new
        o_b = jnp.dot((weights / denom).astype(bf16), v_buf[b], preferred_element_type=f32)
        o_b = o_b + (weight_new / denom).astype(bf16).astype(f32) * v_row[b:b + 1, :]
        o_b = o_b.astype(bf16).astype(f32)
        for j in range(qc // head):
            o_buf[:, b, j * head:(j + 1) * head] = o_b[j * nyz:(j + 1) * nyz, :]
    o_back = [links.send(o_buf.at[plane_id(dz, dy)], o_got.at[yid], links.at_plane(dz, dy)) for dz, dy in plane]
    o_got[yid] = o_buf[yid]
    phase("pass_act")
    passed = []
    for i in range(NZ):
        for dx, c in zip((1, 3, 2), a_got[i]):
            c.wait_recv()
            came = pl.ds(pl.multiple_of(line_id((NX - dx) % NX, 0) * ff, ff), ff)
            passed.append(links.send(act.at[i, :, came], act.at[i, :, came], partner))
    phase("wait_oy")
    for c in o_back:
        c.wait_recv()
    phase("o_send")
    o_all[xid] = o_got[...].reshape(span, qc).astype(bf16)
    o_line = [links.send(o_all.at[xid], o_all.at[xid], links.at_line(dx, 0)) for dx in (1, 3, 2)]
    o_cross = [links.send(o_all.at[xid], o_all.at[xid], partner)]
    emb_got += [links.send(emb_piece(dx, oc), emb_slot(dx, oc), links.at_line(dx, oc)) for dx, oc in near[:2]]
    phase("wait_act")
    got_wd.wait()
    for i in range(NZ):
        a_got[i][3].wait_recv()
        for c in passed[i * 3:i * 3 + 3]:
            c.wait_recv()
    phase("down_mm")
    for i in range(NZ):
        part[i] = jnp.dot(act[i], wd_buf[...], preferred_element_type=f32).reshape(NY, rows, chunk)
    phase("wait_o")
    got_wo.wait()
    for dx, c in zip((1, 3, 2), o_line):
        c.wait_recv()
        came = line_id((NX - dx) % NX, 0)
        o_cross.append(links.send(o_all.at[came], o_all.at[came], partner))
    for c in o_cross:
        c.wait_recv()

    phase("out_mm")
    low, high = pl.ds(0, half), pl.ds(half, half)
    first_a, first_b = [], []
    for k in (2, 1, 3, 0):
        g = (z + k) % NZ
        o_nat = jnp.dot(sel_t[pl.ds(pl.multiple_of(g * group, group), group), :], o_all[...].reshape(nx2 * span, qc),
                        preferred_element_type=f32).astype(bf16)
        part[g] = part[g] + jnp.dot(o_nat, wo_buf[...], preferred_element_type=f32).reshape(NY, rows, chunk)
        for d in (2, 1, 3):
            first_a.append(links.send(part.at[g, (y + d) % NY, :, low], ra1.at[d - 1, g], links.at_plane(0, d)))
        if k:
            first_b.append(links.send(part.at[g, :, :, high], rb1.at[k - 1], links.at_plane(k, 0)))
    phase("wait_rs1")
    for c in first_b:
        c.wait_recv()
    acc_b[...] = (part[z, :, :, half:] + rb1[0]) + (rb1[1] + rb1[2])
    second_b = [links.send(acc_b.at[(y + d) % NY], rb2.at[d - 1], links.at_plane(0, d)) for d in (2, 1, 3)]
    phase("wait_rs1a")
    for c in first_a:
        c.wait_recv()
    acc_a[...] = (part[:, y, :, :half] + ra1[0]) + (ra1[1] + ra1[2])
    second_a = [links.send(acc_a.at[(z + d) % NZ], ra2.at[d - 1], links.at_plane(d, 0)) for d in (2, 1, 3)]
    phase("wait_rs2")
    for c in second_a + second_b:
        c.wait_recv()
    phase("rs_sum2")
    def own_residual():
        res = hid_ref[z, y].astype(f32)
        xbuf2[0, :, :half] = res[:, :half] + ((acc_a[z] + ra2[0]) + (ra2[1] + ra2[2]))
        xbuf2[0, :, half:] = res[:, half:] + ((acc_b[y] + rb2[0]) + (rb2[1] + rb2[2]))

    back = norm_gather(links, own_residual, gains, 1, xbuf2, stat2, f_buf)
    next(back)
    emb_got += [links.send(emb_piece(dx, oc), emb_slot(dx, oc), links.at_line(dx, oc)) for dx, oc in near[2:]]
    phase.close()
    for _ in back:
        pass
    phase("wait_emb")
    own_emb.wait()
    for c in emb_got:
        c.wait_recv()

    phase("logits")
    wide_n = 256
    for i in range(total_rows // wide_n):
        cols = slice(i * wide_n, (i + 1) * wide_n)
        z_ref[:, cols] = (
            lax.dot_general(emb_buf[0], f_buf[0, cols, :], (((1,), (1,)), ((), ())), preferred_element_type=f32)
            + lax.dot_general(emb_buf[1], f_buf[1, cols, :], (((1,), (1,)), ((), ())), preferred_element_type=f32))

    phase("lse_own")
    shift = vocab_own * xid - emb_start(xid)
    vid = lax.broadcasted_iota(jnp.int32, (take, 1), 0)
    own = (vid >= shift) & (vid < shift + vocab_own)
    blocks = total_rows // 128
    for b in range(blocks):
        zb = jnp.where(own, z_ref[:, b * 128:(b + 1) * 128], -jnp.inf)
        top = jnp.max(zb, axis=0, keepdims=True)
        lse_x[xid, b:b + 1, :] = top
        lse_x[xid, 8 + b:9 + b, :] = jnp.sum(jnp.exp(zb - top), axis=0, keepdims=True)
    for b in range(blocks, 8):
        lse_x[xid, b:b + 1, :] = jnp.zeros((1, 128), f32)
        lse_x[xid, 8 + b:9 + b, :] = jnp.ones((1, 128), f32)

    def merge(ref):
        tops = ref[:, :8, :]
        top = jnp.max(tops, axis=0)
        return top, jnp.sum(ref[:, 8:, :] * jnp.exp(tops - top[None]), axis=0)

    phase("lse_line")
    got = [links.send(lse_x.at[xid], lse_x.at[xid], links.at_line(dx, oc)) for dx, oc in others]
    for c in got:
        c.wait_recv()
    top, mass = merge(lse_x)
    lse_y[yid, :8, :] = top
    lse_y[yid, 8:, :] = mass
    phase("lse_plane")
    got = [links.send(lse_y.at[yid], lse_y.at[yid], links.at_plane(dz, dy)) for dz, dy in plane]
    for c in got:
        c.wait_recv()
    top, mass = merge(lse_y)
    norm_ref[...] = top + jnp.log(mass)
    phase("finish")
    links.finish()
    phase.close()


def whole_step(hidden, cos, sin, lens, k_cache, v_cache, g_attn, w_query, w_key, w_value,
               w_gate, w_up, w_out, w_down, g_final, embedding):
    total_rows, chunk = hidden.shape
    own_rows, seq, head = k_cache.shape
    rows = total_rows // (NY * NZ)
    vocab_own = embedding.shape[0] // (2 * NX)
    take = (vocab_own + 30) // 16 * 16
    half = chunk // 2
    qc = w_query.shape[1]
    ff = w_gate.shape[1] // (2 * NX)
    f32, bf16 = jnp.float32, jnp.bfloat16
    nyz, nx2, pad = NY * NZ, 2 * NX, 8
    copies = 360
    vmem = pl.BlockSpec(memory_space=pltpu.VMEM)
    hbm = pl.BlockSpec(memory_space=pl.ANY)
    V = pltpu.VMEM
    return pl.pallas_call(
        lambda *refs: step_kernel(vocab_own, own_rows, *refs),
        out_shape=(jax.ShapeDtypeStruct((pad, head), bf16), jax.ShapeDtypeStruct((pad, head), bf16),
                   jax.ShapeDtypeStruct((take, total_rows), f32), jax.ShapeDtypeStruct((8, 128), f32)),
        in_specs=[vmem] * 6 + [hbm] * 2 + [vmem] * 3 + [hbm] * 5,
        out_specs=(vmem,) * 4,
        scratch_shapes=[
            V((own_rows, seq, head), bf16), V((own_rows, seq, head), bf16), V((qc, chunk), bf16),
            V((nx2 * ff, chunk), bf16), V((2, total_rows, NX * chunk), bf16), V((2, NX * chunk, 2 * ff), bf16),
            V((qc, chunk), bf16), V((2, head, NX * chunk), bf16),
            V((nx2 * nyz * pad, total_rows), bf16), V((total_rows, nx2 * nyz * pad), bf16),
            V((nx2, nyz * pad, head), bf16), V((nx2, nyz * pad, head), bf16),
            V((nyz, pad, qc), f32), V((nyz, pad, qc), f32),
            V((nx2, pad, 2 * head), f32), V((nx2, pad, 2 * head), f32),
            V((nyz, pad, qc), f32), V((nyz, pad, qc), f32), V((nx2, nyz * pad, qc), bf16),
            V((NZ, NY * rows, nx2 * ff), bf16),
            V((NZ, NY, rows, chunk), f32),
            V((3, NZ, rows, half), f32), V((3, NY, rows, half), f32), V((3, rows, half), f32), V((3, rows, half), f32),
            V((NZ, rows, half), f32), V((NY, rows, half), f32),
            V((NX, rows, chunk), bf16), V((2, rows, 128), f32), V((NX, rows, chunk), f32), V((2, rows, 128), f32),
            V((NX, 8, chunk), f32),
            V((2, total_rows, NX * chunk), bf16), V((2, take, NX * chunk), bf16),
            V((2, 2, chunk, ff), bf16), V((2, 2, take // 2, chunk), bf16),
            V((nx2, 16, 128), f32), V((nyz, 16, 128), f32),
            pltpu.SemaphoreType.DMA((copies,)), pltpu.SemaphoreType.DMA((copies,)), pltpu.SemaphoreType.DMA((8,)),
        ],
        compiler_params=pltpu.CompilerParams(
            collective_id=1, has_side_effects=True, vmem_limit_bytes=60 * 1024 * 1024),
        name="decode_step",
    )(hidden.reshape(NZ, NY, rows, chunk), g_attn[None, :], g_final[None, :], cos, sin, lens, k_cache, v_cache,
      w_query, w_key, w_value, w_gate, w_up, w_out, w_down, embedding)


def solution(mesh):
    x_size = mesh.shape["xax"]
    row_spec = P(("dp", "yax", "xax"))

    def local_step(hidden, cache_len, k_cache, v_cache, g_attn, w_query, w_key, w_value,
                   w_gate, w_up, w_out, w_down, g_final, embedding):
        rows = hidden.shape[0]
        own_rows, _, head_dim = k_cache.shape
        y_idx = lax.axis_index("yax")
        x_idx = lax.axis_index("xax")
        own_start = (y_idx * x_size + x_idx) * own_rows
        len_own = jnp.pad(lax.dynamic_slice_in_dim(cache_len, own_start, own_rows, axis=0), (0, 8 - own_rows))
        angles = rope_angle(len_own, head_dim)
        cos_half, sin_half = jnp.cos(angles), jnp.sin(angles)
        cos = jnp.concatenate([cos_half, cos_half], axis=1)
        sin = jnp.concatenate([-sin_half, sin_half], axis=1)
        lens = jnp.broadcast_to(len_own[:, None], (8, 128))
        key_own, value_own, logits_wide, norm_tile = whole_step(
            hidden, cos, sin, lens, k_cache, v_cache, g_attn, w_query, w_key, w_value,
            w_gate, w_up, w_out, w_down, g_final, embedding)
        vocab_own = embedding.shape[0] // x_size
        log_norm = norm_tile[:rows // 128].reshape(rows)
        shift = vocab_own * x_idx - (vocab_own * x_idx // 16 * 16 - x_idx // (x_size - 1) * 16)
        logits = lax.dynamic_slice_in_dim(logits_wide, shift, vocab_own, axis=0)
        return key_own[:own_rows], value_own[:own_rows], (logits - log_norm[None, :]).T, log_norm

    in_specs = (P("dp", "xax"), P("dp"), row_spec, row_spec, P("xax"), P("xax", "yax"),
                P("xax", None), P("xax", None), P("xax", "yax"), P("xax", "yax"),
                P("yax", "xax"), P("yax", "xax"), P("xax"), P("yax", "xax"))
    out_specs = (row_spec, row_spec, P("dp", ("yax", "xax")), P("dp"))
    return jax.shard_map(local_step, mesh=mesh, in_specs=in_specs, out_specs=out_specs, check_vma=False)
```

```python
import itertools

import jax
import jax.numpy as jnp
from jax import lax
from jax.experimental import pallas as pl
from jax.experimental.pallas import tpu as pltpu
from jax.sharding import PartitionSpec as P

EPS = 1e-6
ROPE_BASE = 10000.0
MESH_ID = pl.DeviceIdType.MESH
NY = NZ = NX = 4
CORES = 2
POOL = 48
HOPS = (1, 3, 2)
LINE = [(0, 1), (1, 0), (3, 0), (1, 1), (3, 1), (2, 0), (2, 1)]
NEAR = LINE[1:5]
NT = (((1,), (1,)), ((), ()))
PLANE = [(dz, dy) for dz in range(NZ) for dy in range(NY) if dz or dy]


def rope_angle(positions, head_dim):
    half_dim = head_dim // 2
    inv_freq = ROPE_BASE ** (-(jnp.arange(half_dim, dtype=jnp.float32) * 2.0) / head_dim)
    return positions.astype(jnp.float32)[:, None] * inv_freq[None, :]


class Phases:
    def __init__(self):
        self.open = None

    def __call__(self, name):
        self.close()
        self.open = jax.named_scope(name)
        self.open.__enter__()

    def close(self):
        if self.open is not None:
            self.open.__exit__(None, None, None)
        self.open = None


class Links:
    def __init__(self, send_sem, recv_sem):
        self.send_sem, self.recv_sem = send_sem, recv_sem
        self.tags, self.slow, self.fast = itertools.count(), itertools.count(POOL), []
        self.pending = []
        self.y_idx = lax.axis_index("yax")
        self.x_idx = lax.axis_index("xax")
        self.z, self.y = self.y_idx // NY, self.y_idx % NY
        self.chip, self.core = self.x_idx // CORES, self.x_idx % CORES

    def at_plane(self, dz, dy):
        return {"yax": (self.z + dz) % NZ * NY + (self.y + dy) % NY, "xax": self.x_idx}

    def slot_rows(self, dz, dy, rows):
        slot = (self.z + dz) % NZ * NY + (self.y + dy) % NY
        return pl.ds(pl.multiple_of(slot * rows, rows), rows)

    def line_id(self, dx, oc):
        core = 1 - self.core if oc else self.core
        return (self.chip + dx) % NX * CORES + core

    def at_line(self, dx, oc):
        return {"yax": self.y_idx, "xax": self.line_id(dx, oc)}

    def send(self, src, dst, where, tag=None, long=False):
        tag = next(self.tags) if tag is None else tag
        if long:
            sem = next(self.slow)
        else:
            sem = len(self.fast) % POOL
            if len(self.fast) >= POOL:
                self.fast[-POOL].wait_send()
        copy = pltpu.make_async_remote_copy(
            src_ref=src, dst_ref=dst, send_sem=self.send_sem.at[sem], recv_sem=self.recv_sem.at[tag],
            device_id=where, device_id_type=MESH_ID)
        copy.start()
        (self.pending if long else self.fast).append(copy)
        return copy

    def finish(self):
        for copy in self.pending + self.fast[-POOL:]:
            copy.wait_send()

    def barrier(self):
        barrier = pltpu.get_barrier_semaphore()
        peers = [self.at_line(*p) for p in LINE] + [self.at_plane(*p) for p in PLANE]
        for peer in peers:
            pl.semaphore_signal(barrier, inc=1, device_id=peer, device_id_type=MESH_ID)
        pl.semaphore_wait(barrier, len(peers))


def plane_gather(links, buf, tags, hook):
    cols = buf.shape[-1]
    rows = buf.shape[1] // (NY * NZ)
    span = cols // 2
    partner = links.at_line(0, 1)
    crossing = []

    class Part:
        def __init__(self, index):
            self.index, self.lo, self.got = index, index * span, {}

        def order(self, du, dv):
            return (du, dv) if self.index else (dv, du)

        def block(self, at, half=0, piece=None):
            width = span if piece is None else span // 2
            lo = self.lo if not piece else self.lo + width
            return buf.at[half, links.slot_rows(*self.order(*at), rows), pl.ds(lo, width)]

        def push(self, name, at, to, piece=None):
            ref = self.block(at, piece=piece)
            self.got[name] = links.send(ref, ref, links.at_plane(*self.order(*to)), next(tags))

        def spread(self, k, at):
            self.push(("v+", k), at, (0, 1))
            self.push(("v-", k), at, (0, -1))

        def give(self, at):
            crossing.append(links.send(self.block(at), self.block(at, half=1), partner, next(tags)))

        def wait(self, name):
            self.got[name].wait_recv()

    parts = [Part(index) for index in range(2)]
    offset = (0, -1, 1, 2)
    for p in parts:
        p.push("u+", (0, 0), (1, 0))
        p.push("u-", (0, 0), (-1, 0))
        p.spread(0, (0, 0))
    for p in parts:
        p.give((0, 0))
    for k, name in enumerate(("u+", "u-"), 1):
        for p in parts:
            p.wait(name)
            at = (offset[k], 0)
            p.push(("far", k), at, (-offset[k], 0), piece=k - 1)
            p.spread(k, at)
            p.give(at)
    hook()

    def arrive(p, k):
        for name, step in (("v+", -1), ("v-", 1)):
            p.wait((name, k))
            at = (offset[k], step)
            if (name == "v+") == (k in (0, 3)):
                p.push(("relay", k), at, (0, -step))
            p.give(at)

    for p in parts:
        arrive(p, 0)
    for p in parts:
        p.wait(("far", 1))
        p.wait(("far", 2))
        p.spread(3, (2, 0))
        p.give((2, 0))
    for k in range(1, len(offset)):
        for p in parts:
            arrive(p, k)
    for k in range(len(offset)):
        for p in parts:
            p.wait(("relay", k))
            p.give((offset[k], 2))
    return crossing


def norm_gather(links, own_slot, gain_buf, which, xbuf, stat, out, base, hook):
    own_slot()
    rows, chunk = xbuf.shape[1:]
    tags = itertools.count(base)
    line = [links.send(xbuf.at[0], xbuf.at[NX - dx], links.at_line(dx, 0), next(tags)) for dx in HOPS]
    yield
    phase = Phases()
    for n, c in enumerate(line):
        phase(f"ng_line{which}_{n}")
        c.wait_recv()
    phase("ng_stats")
    held = xbuf[...].astype(jnp.float32)
    count = NX * chunk
    mean = jnp.sum(jnp.sum(held, axis=0), axis=-1, keepdims=True) / count
    dev = held - mean[None]
    square = jnp.sum(jnp.sum(dev * dev, axis=0), axis=-1, keepdims=True)
    lane = lax.broadcasted_iota(jnp.int32, (rows, 128), 1)
    stat[0] = jnp.where(lane == 0, mean, square)
    links.send(stat.at[0], stat.at[1], links.at_line(0, 1), next(tags)).wait_recv()
    other_mean, other_square = stat[1, :, 0:1], stat[1, :, 1:2]
    both = (mean + other_mean) * 0.5
    gap = mean - other_mean
    var = (square + other_square + gap * gap * (count * 0.5)) / (2 * count)
    scale = lax.rsqrt(var + EPS)
    for e in range(NX):
        out[0, links.slot_rows(0, 0, rows), e * chunk:(e + 1) * chunk] = (
            (xbuf[e].astype(jnp.float32) - both) * scale * gain_buf[e, which:which + 1, :]).astype(jnp.bfloat16)
    phase("ng_plane")
    crossing = plane_gather(links, out, tags, hook)
    phase("ng_cross")
    for c in crossing:
        c.wait_recv()
    phase.close()


def step_kernel(vocab_own, own_rows, hid_ref, gain_a, gain_f, cos_ref, sin_ref, len_ref, k_hbm, v_hbm,
                wq_ref, wk_ref, wv_ref, wo_ref, wg_ref, wu_ref, wd_hbm, emb_ref,
                knew_ref, vnew_ref, z_ref, norm_ref,
                k_buf, v_buf, wd_buf, wo_all, att, rc, n_buf, w_buf, wq_t, wq_buf, sel, sel_t, qx, qr, qy, qf,
                kvp, kvr, o_buf, o_got, o_all, act,
                part, ra1, rb1, ra2, rb2, acc_a, acc_b, xbuf, stat, xbuf2, stat2, gains, f_buf, emb_buf,
                w_relay, emb_relay, lse_x, lse_y, send_sem, recv_sem, local_sem):
    links = Links(send_sem, recv_sem)
    phase = Phases()
    f32, bf16 = jnp.float32, jnp.bfloat16
    z, y, xid, yid = links.z, links.y, links.x_idx, links.y_idx
    rows, chunk = hid_ref.shape[2], hid_ref.shape[3]
    half = chunk // 2
    nx2, nyz = 2 * NX, NY * NZ
    group = NY * rows
    head = 128
    pad = 8
    partner = links.at_line(0, 1)
    line_id = links.line_id
    gather_tags = len(HOPS) + 1 + len(PLANE) * CORES * CORES + CORES * CORES
    gather_base = [next(links.tags) for _ in range(gather_tags)][0]

    def dot(a, b):
        return jnp.dot(a, b, preferred_element_type=f32)

    def dot_t(a, b):
        return lax.dot_general(a, b, NT, preferred_element_type=f32)

    def to_line(src, dst, where=LINE, **kw):
        return [links.send(src(dx, oc), dst(dx, oc), links.at_line(dx, oc), **kw) for dx, oc in where]

    local = []

    def fetch(src, dst):
        copy = pltpu.make_async_copy(src, dst, local_sem.at[len(local)])
        copy.start()
        local.append(copy)
        return copy

    ff = wg_ref.shape[1] // nx2

    def w_piece(ref, dx, oc):
        return ref.at[:, pl.ds(pl.multiple_of(line_id(dx, oc) * ff, ff), ff)]

    def w_slot(which, dx, oc):
        back = (NX - dx) % NX
        return w_buf.at[int(oc), pl.ds(back * chunk, chunk), pl.ds(which * ff, ff)]

    take = emb_buf.shape[1]

    def emb_start(xi):
        return pl.multiple_of(vocab_own * xi // 16 * 16 - xi // (nx2 - 1) * 16, 16)

    def emb_piece(dx, oc):
        return emb_ref.at[pl.ds(emb_start(line_id(dx, oc)), take), :]

    def emb_slot(dx, oc):
        return emb_buf.at[int(oc), :, pl.ds((NX - dx) % NX * chunk, chunk)]

    def emb_half(oc, way):
        part_rows = take // 2
        return emb_ref.at[pl.ds(emb_start(line_id(2, oc)) + way * part_rows, part_rows), :]

    def emb_far_slot(oc, way):
        return emb_buf.at[int(oc), pl.ds(way * (take // 2), take // 2), pl.ds(2 * chunk, chunk)]

    phase("start")
    own_w = [fetch(w_piece(wg_ref, 0, 0), w_slot(0, 0, 0)), fetch(w_piece(wu_ref, 0, 0), w_slot(1, 0, 0))]
    got_kv = [fetch(k_hbm, k_buf), fetch(v_hbm, v_buf)]
    got_wd = fetch(wd_hbm, wd_buf)
    own_emb = fetch(emb_piece(0, 0), emb_slot(0, 0))

    qc = wq_ref.shape[1]
    qs = qc // nx2
    per = head // qs
    eye_q = (lax.broadcasted_iota(jnp.int32, (qc, qc), 0) == lax.broadcasted_iota(jnp.int32, (qc, qc), 1))
    wq_t[...] = dot_t(eye_q.astype(bf16), wq_ref[...]).astype(bf16)
    wq_buf[...] = jnp.zeros(wq_buf.shape, bf16)

    def q_rows(xi):
        return pl.ds(pl.multiple_of(xi % per * qs, qs), qs)

    wq_buf[0, q_rows(xid), 0:chunk] = wq_t[pl.ds(pl.multiple_of(xid * qs, qs), qs), :]
    phase("barrier")
    links.barrier()

    phase("front_send")
    gains[0, 0:1, :] = gain_a[...]
    gains[0, 1:2, :] = gain_f[...]
    gains[0, 2:, :] = jnp.zeros((6, chunk), f32)

    def own_input():
        xbuf[0] = hid_ref[z, y]

    w_far, emb_far, emb_got = [], [], []
    ways = [(way, hop, oc) for oc in (0, 1) for way, hop in enumerate(HOPS[:2])]

    def forward_weights():
        for (way, hop, oc), c in zip(ways, w_far):
            c.wait_recv()
            w_got.append(links.send(w_relay.at[way, oc], w_buf.at[oc, pl.ds(2 * chunk, chunk), pl.ds(way * ff, ff)],
                                    links.at_line(hop, oc), long=True))

    def emb_out(some):
        for way, hop, oc in some:
            emb_far.append(links.send(emb_half(oc, way), emb_relay.at[way, oc], links.at_line(hop, 0), long=True))

    def emb_on(some, arrived):
        for (way, hop, oc), c in zip(some, arrived):
            c.wait_recv()
            emb_got.append(links.send(emb_relay.at[way, oc], emb_far_slot(oc, way), links.at_line(hop, oc), long=True))

    front = norm_gather(links, own_input, gains, 0, xbuf, stat, n_buf, gather_base, forward_weights)
    next(front)
    gain_got = [links.send(gains.at[0], gains.at[NX - dx], links.at_line(dx, 0)) for dx in HOPS]
    for way, hop, oc in ways:
        w_far.append(links.send(w_piece((wg_ref, wu_ref)[way], 2, oc), w_relay.at[way, oc], links.at_line(hop, 0),
                                long=True))

    def wq_rows(dx, oc):
        return wq_t.at[pl.ds(pl.multiple_of(line_id(dx, oc) * qs, qs), qs), :]

    def wq_slot(dx, oc):
        return wq_buf.at[oc, q_rows(line_id(dx, oc)), pl.ds((NX - dx) % NX * chunk, chunk)]

    wq_got = to_line(wq_rows, wq_slot, long=True)
    w_got = []
    for which, ref in enumerate((wg_ref, wu_ref)):
        w_got += to_line(lambda dx, oc: w_piece(ref, dx, oc), lambda dx, oc: w_slot(which, dx, oc),
                         LINE[:1] + NEAR, long=True)

    phase("selections")
    total_rows = nyz * rows
    r_id = lax.broadcasted_iota(jnp.int32, (nx2 * nyz * pad, 1), 0)
    r_j = r_id % pad
    r_src = jnp.where(r_j < own_rows, r_id // pad % nyz * rows + r_id // (pad * nyz) * own_rows + r_j, -1)
    s_id = lax.broadcasted_iota(jnp.int32, (1, total_rows), 1)
    sel[...] = jnp.where(r_src == s_id, 1.0, 0.0).astype(bf16)
    t_id = lax.broadcasted_iota(jnp.int32, (group, 1), 0)
    t_in = t_id % rows
    t_src = t_in // own_rows * (NY * pad) + t_id // rows * pad + t_in % own_rows
    u_id = lax.broadcasted_iota(jnp.int32, (1, nx2 * NY * pad), 1)
    sel_t[...] = jnp.where(t_src == u_id, 1.0, 0.0).astype(bf16)
    k_id = lax.broadcasted_iota(jnp.int32, (nx2 * pad, rows), 0)
    k_src = jnp.where(k_id % pad < own_rows, k_id // pad * own_rows + k_id % pad, -1)
    sel_kv = jnp.where(k_src == lax.broadcasted_iota(jnp.int32, (nx2 * pad, rows), 1), 1.0, 0.0).astype(bf16)

    phase.close()
    for c in gain_got:
        c.wait_recv()
    for _ in front:
        pass
    phase("kv_part")

    n_own = dot(sel_kv, n_buf[0, links.slot_rows(0, 0, rows), 0:chunk]).astype(bf16)
    kvp[:, :, :head] = dot(n_own, wk_ref[...]).reshape(nx2, pad, head)
    kvp[:, :, head:] = dot(n_own, wv_ref[...]).reshape(nx2, pad, head)
    kv_got = to_line(lambda dx, oc: kvp.at[line_id(dx, oc)], lambda dx, oc: kvr.at[xid])
    kvr[xid] = kvp[xid]

    phase("wait_wq")
    for c in wq_got:
        c.wait_recv()
    phase("q_mm")
    q_all = (dot_t(n_buf[0], wq_buf[0]) + dot_t(n_buf[1], wq_buf[1])).astype(bf16)
    span = nyz * pad
    for i in range(nx2):
        qx[i] = dot(sel[i * span:(i + 1) * span, :], q_all).astype(bf16)
    line_tags = [next(links.tags) for _ in LINE]
    plane_tags = [next(links.tags) for _ in PLANE]
    q_got = [links.send(qx.at[line_id(*p)], qr.at[xid], links.at_line(*p), t) for p, t in zip(LINE, line_tags)]
    qr[xid] = qx[xid]

    phase("wait_w")
    for c in own_w:
        c.wait()
    for c in w_got:
        c.wait_recv()
    phase("gate_up")

    def act_at(pair, dx):
        cols = pl.ds(pl.multiple_of(line_id(dx, 0) * ff, ff), ff)
        return act.at[pl.ds(pair * 2, 2), :, cols]

    a_got = []
    for pair in range(NZ // 2):
        these = slice(pair * 2 * group, (pair + 1) * 2 * group)
        both = (dot(n_buf[0, these, :], w_buf[0]) + dot(n_buf[1, these, :], w_buf[1])).astype(bf16).astype(f32)
        gate, up = both[:, :ff], both[:, ff:]
        act_at(pair, 0)[...] = (gate * jax.nn.sigmoid(gate) * up).astype(bf16).reshape(2, group, ff)
        here = act_at(pair, 0)
        a_got.append([links.send(here, here, links.at_line(dx, 0)) for dx in HOPS] + [links.send(here, here, partner)])
    emb_out(ways[:2])

    phase("wait_q")
    for c in q_got:
        c.wait_recv()
    phase("q_sum")
    for j in range(qc // head):
        piece = qr[j * per].astype(f32)
        for i in range(1, per):
            piece = piece + qr[j * per + i].astype(f32)
        qy[:, :, j * head:(j + 1) * head] = piece.reshape(nyz, pad, head)
    def plane_id(dz, dy):
        return (z + dz) % NZ * NY + (y + dy) % NY

    y_got = [links.send(qy.at[plane_id(*p)], qf.at[yid], links.at_plane(*p), t) for p, t in zip(PLANE, plane_tags)]
    qf[yid] = qy[yid]

    def wo_rows(dz):
        return wo_all.at[pl.ds(pl.multiple_of((z + dz) % NZ * qc, qc), qc), :]

    wo_got = [links.send(wo_ref, wo_rows(0), links.at_plane(d, 0), long=True) for d in HOPS]
    wo_rows(0)[...] = wo_ref[...]

    phase("wait_kv")
    for c in kv_got:
        c.wait_recv()
    kv_sum = kvr[0]
    for i in range(1, nx2):
        kv_sum = kv_sum + kvr[i]
    kv_new = kv_sum.astype(bf16).astype(f32)

    def turn(v, b=None):
        cos, sin = (cos_ref[...], sin_ref[...]) if b is None else (cos_ref[b:b + 1, :], sin_ref[b:b + 1, :])
        return (v * cos + pltpu.roll(v, head // 2, 1) * sin).astype(bf16)

    k_new = turn(kv_new[:, :head])
    knew_ref[...] = k_new
    vnew_ref[...] = kv_new[:, head:].astype(bf16)
    k_row, v_row = k_new.astype(f32), kv_new[:, head:]
    phase("wait_qy")
    for c in got_kv:
        c.wait()
    for c in y_got:
        c.wait_recv()
    phase("attention")
    seq = k_buf.shape[1]
    score_scale = head ** -0.5
    position = lax.broadcasted_iota(jnp.int32, (1, seq), 1)
    o_buf[...] = jnp.zeros(o_buf.shape, f32)
    for b in range(own_rows):
        q_b = jnp.concatenate([turn(qf[:, b, j * head:(j + 1) * head], b) for j in range(qc // head)], axis=0)
        scores = dot_t(q_b, k_buf[b]) * score_scale
        score_new = jnp.sum(q_b.astype(f32) * k_row[b:b + 1, :], axis=-1, keepdims=True) * score_scale
        valid = position < len_ref[b:b + 1, 0:1]
        top = jnp.maximum(jnp.max(jnp.where(valid, scores, -jnp.inf), axis=-1, keepdims=True), score_new)
        weights = jnp.where(valid, jnp.exp(scores - top), 0.0)
        weight_new = jnp.exp(score_new - top)
        denom = jnp.sum(weights, axis=-1, keepdims=True) + weight_new
        o_b = dot((weights / denom).astype(bf16), v_buf[b])
        o_b = o_b + (weight_new / denom).astype(bf16).astype(f32) * v_row[b:b + 1, :]
        o_b = o_b.astype(bf16).astype(f32)
        for j in range(qc // head):
            o_buf[:, :, b, j * head:(j + 1) * head] = o_b[j * nyz:(j + 1) * nyz, :].reshape(NZ, NY, head)
    o_back = [links.send(o_buf.at[:, (y + d) % NY], o_got.at[y], links.at_plane(0, d)) for d in HOPS]
    o_got[y] = o_buf[:, y]

    phase("pass_act")
    for pair, got in enumerate(a_got):
        for dx, c in zip(HOPS, got[:-1]):
            c.wait_recv()
            ref = act_at(pair, NX - dx)
            got.append(links.send(ref, ref, partner))
    phase("wait_act")
    got_wd.wait()
    for got in a_got:
        for c in got[len(HOPS):]:
            c.wait_recv()
    phase("down_mm")
    low, high = pl.ds(0, half), pl.ds(half, half)
    first_a, first_b = [], []
    for k in HOPS + (0,):
        g = (z + k) % NZ
        part[g] = dot(act[g], wd_buf[...]).reshape(NY, rows, chunk)
        for d in HOPS:
            first_a.append(links.send(part.at[g, (y + d) % NY, :, low], ra1.at[d - 1, g], links.at_plane(0, d)))
        if k:
            first_b.append(links.send(part.at[g, :, :, high], rb1.at[k - 1], links.at_plane(k, 0)))

    phase("wait_oy")
    for c in o_back:
        c.wait_recv()
    for i in range(NZ):
        o_all[xid, :, i * qc:(i + 1) * qc] = o_got[:, i].reshape(NY * pad, qc).astype(bf16)
    o_here = o_all.at[xid]
    o_line = [links.send(o_here, o_here, links.at_line(dx, 0)) for dx in HOPS]
    o_cross = [links.send(o_here, o_here, partner)]
    emb_out(ways[2:])
    emb_got += to_line(emb_piece, emb_slot, LINE[:1], long=True)
    phase("wait_o")
    for dx, c in zip(HOPS, o_line):
        c.wait_recv()
        came = o_all.at[line_id(NX - dx, 0)]
        o_cross.append(links.send(came, came, partner))
    for c in wo_got + o_cross:
        c.wait_recv()
    phase("out_mm")
    o_nat = dot(sel_t[...], o_all[...].reshape(nx2 * NY * pad, NZ * qc)).astype(bf16)
    att[...] = dot(o_nat, wo_all[...]).reshape(NY, rows, chunk)
    att_got = [links.send(att.at[(y + d) % NY], rc.at[d - 1], links.at_plane(0, d)) for d in HOPS]
    emb_on(ways[:2], emb_far[:2])

    phase("wait_rs1")
    for c in first_b:
        c.wait_recv()
    acc_b[...] = (part[z, :, :, half:] + rb1[0]) + (rb1[1] + rb1[2])
    second = [links.send(acc_b.at[(y + d) % NY], rb2.at[d - 1], links.at_plane(0, d)) for d in HOPS]
    phase("wait_rs1a")
    for c in first_a:
        c.wait_recv()
    acc_a[...] = (part[:, y, :, :half] + ra1[0]) + (ra1[1] + ra1[2])
    second += [links.send(acc_a.at[(z + d) % NZ], ra2.at[d - 1], links.at_plane(d, 0)) for d in HOPS]
    phase("wait_att")
    for c in att_got:
        c.wait_recv()
    phase("wait_rs2")
    for c in second:
        c.wait_recv()
    phase("rs_sum2")
    def own_residual():
        res = hid_ref[z, y].astype(f32) + ((att[y] + rc[0]) + (rc[1] + rc[2]))
        xbuf2[0, :, :half] = res[:, :half] + ((acc_a[z] + ra2[0]) + (ra2[1] + ra2[2]))
        xbuf2[0, :, half:] = res[:, half:] + ((acc_b[y] + rb2[0]) + (rb2[1] + rb2[2]))

    back = norm_gather(links, own_residual, gains, 1, xbuf2, stat2, f_buf, gather_base, lambda: None)
    next(back)
    emb_on(ways[2:], emb_far[2:])
    emb_got += to_line(emb_piece, emb_slot, NEAR, long=True)
    phase.close()
    for _ in back:
        pass
    phase("wait_emb")
    own_emb.wait()
    for c in emb_got:
        c.wait_recv()

    phase("logits")
    wide_n = 256
    for i in range(total_rows // wide_n):
        cols = slice(i * wide_n, (i + 1) * wide_n)
        z_ref[:, cols] = dot_t(emb_buf[0], f_buf[0, cols, :]) + dot_t(emb_buf[1], f_buf[1, cols, :])

    phase("lse_own")
    shift = vocab_own * xid - emb_start(xid)
    vid = lax.broadcasted_iota(jnp.int32, (take, 1), 0)
    own = (vid >= shift) & (vid < shift + vocab_own)
    blocks = total_rows // 128
    for b in range(blocks):
        zb = jnp.where(own, z_ref[:, b * 128:(b + 1) * 128], -jnp.inf)
        top = jnp.max(zb, axis=0, keepdims=True)
        lse_x[xid, b:b + 1, :] = top
        lse_x[xid, 8 + b:9 + b, :] = jnp.sum(jnp.exp(zb - top), axis=0, keepdims=True)
    for b in range(blocks, 8):
        lse_x[xid, b:b + 1, :] = jnp.zeros((1, 128), f32)
        lse_x[xid, 8 + b:9 + b, :] = jnp.ones((1, 128), f32)

    def merge(ref):
        tops = ref[:, :8, :]
        top = jnp.max(tops, axis=0)
        return top, jnp.sum(ref[:, 8:, :] * jnp.exp(tops - top[None]), axis=0)

    phase("lse_line")
    got = [links.send(lse_x.at[xid], lse_x.at[xid], links.at_line(*p), t) for p, t in zip(LINE, line_tags)]
    for c in got:
        c.wait_recv()
    top, mass = merge(lse_x)
    lse_y[yid, :8, :] = top
    lse_y[yid, 8:, :] = mass
    phase("lse_plane")
    got = [links.send(lse_y.at[yid], lse_y.at[yid], links.at_plane(*p), t) for p, t in zip(PLANE, plane_tags)]
    for c in got:
        c.wait_recv()
    top, mass = merge(lse_y)
    norm_ref[...] = top + jnp.log(mass)
    phase("finish")
    links.finish()
    phase.close()


def whole_step(hidden, cos, sin, lens, k_cache, v_cache, g_attn, w_query, w_key, w_value,
               w_gate, w_up, w_out, w_down, g_final, embedding):
    total_rows, chunk = hidden.shape
    own_rows, seq, head = k_cache.shape
    rows = total_rows // (NY * NZ)
    vocab_own = embedding.shape[0] // (2 * NX)
    take = (vocab_own + 30) // 16 * 16
    half = chunk // 2
    qc = w_query.shape[1]
    ff = w_gate.shape[1] // (2 * NX)
    f32, bf16 = jnp.float32, jnp.bfloat16
    nyz, nx2, pad = NY * NZ, 2 * NX, 8
    vmem = pl.BlockSpec(memory_space=pltpu.VMEM)
    hbm = pl.BlockSpec(memory_space=pl.ANY)
    V = pltpu.VMEM
    return pl.pallas_call(
        lambda *refs: step_kernel(vocab_own, own_rows, *refs),
        out_shape=(jax.ShapeDtypeStruct((pad, head), bf16), jax.ShapeDtypeStruct((pad, head), bf16),
                   jax.ShapeDtypeStruct((take, total_rows), f32), jax.ShapeDtypeStruct((8, 128), f32)),
        in_specs=[vmem] * 6 + [hbm] * 2 + [vmem] * 4 + [hbm] * 4,
        out_specs=(vmem,) * 4,
        scratch_shapes=[
            V((own_rows, seq, head), bf16), V((own_rows, seq, head), bf16),
            V((nx2 * ff, chunk), bf16), V((NZ * qc, chunk), bf16), V((NY, rows, chunk), f32), V((3, rows, chunk), f32), V((2, total_rows, NX * chunk), bf16), V((2, NX * chunk, 2 * ff), bf16),
            V((qc, chunk), bf16), V((2, head, NX * chunk), bf16),
            V((nx2 * nyz * pad, total_rows), bf16), V((NY * rows, nx2 * NY * pad), bf16),
            V((nx2, nyz * pad, head), bf16), V((nx2, nyz * pad, head), bf16),
            V((nyz, pad, qc), f32), V((nyz, pad, qc), f32),
            V((nx2, pad, 2 * head), f32), V((nx2, pad, 2 * head), f32),
            V((NZ, NY, pad, qc), f32), V((NY, NZ, pad, qc), f32), V((nx2, NY * pad, NZ * qc), bf16),
            V((NZ, NY * rows, nx2 * ff), bf16),
            V((NZ, NY, rows, chunk), f32),
            V((3, NZ, rows, half), f32), V((3, NY, rows, half), f32), V((3, rows, half), f32), V((3, rows, half), f32),
            V((NZ, rows, half), f32), V((NY, rows, half), f32),
            V((NX, rows, chunk), bf16), V((2, rows, 128), f32), V((NX, rows, chunk), f32), V((2, rows, 128), f32),
            V((NX, 8, chunk), f32),
            V((2, total_rows, NX * chunk), bf16), V((2, take, NX * chunk), bf16),
            V((2, 2, chunk, ff), bf16), V((2, 2, take // 2, chunk), bf16),
            V((nx2, 16, 128), f32), V((nyz, 16, 128), f32),
            pltpu.SemaphoreType.DMA((POOL + 41,)), pltpu.SemaphoreType.DMA((189,)), pltpu.SemaphoreType.DMA((6,)),
        ],
        compiler_params=pltpu.CompilerParams(
            collective_id=1, has_side_effects=True, vmem_limit_bytes=60 * 1024 * 1024),
        name="decode_step",
    )(hidden.reshape(NZ, NY, rows, chunk), g_attn[None, :], g_final[None, :], cos, sin, lens, k_cache, v_cache,
      w_query, w_key, w_value, w_out, w_gate, w_up, w_down, embedding)


def solution(mesh):
    x_size = mesh.shape["xax"]
    row_spec = P(("dp", "yax", "xax"))

    def local_step(hidden, cache_len, k_cache, v_cache, g_attn, w_query, w_key, w_value,
                   w_gate, w_up, w_out, w_down, g_final, embedding):
        rows = hidden.shape[0]
        own_rows, _, head_dim = k_cache.shape
        y_idx = lax.axis_index("yax")
        x_idx = lax.axis_index("xax")
        own_start = (y_idx * x_size + x_idx) * own_rows
        len_own = jnp.pad(lax.dynamic_slice_in_dim(cache_len, own_start, own_rows, axis=0), (0, 8 - own_rows))
        angles = rope_angle(len_own, head_dim)
        cos_half, sin_half = jnp.cos(angles), jnp.sin(angles)
        cos = jnp.concatenate([cos_half, cos_half], axis=1)
        sin = jnp.concatenate([-sin_half, sin_half], axis=1)
        lens = jnp.broadcast_to(len_own[:, None], (8, 128))
        key_own, value_own, logits_wide, norm_tile = whole_step(
            hidden, cos, sin, lens, k_cache, v_cache, g_attn, w_query, w_key, w_value,
            w_gate, w_up, w_out, w_down, g_final, embedding)
        vocab_own = embedding.shape[0] // x_size
        log_norm = norm_tile[:rows // 128].reshape(rows)
        shift = vocab_own * x_idx - (vocab_own * x_idx // 16 * 16 - x_idx // (x_size - 1) * 16)
        logits = lax.dynamic_slice_in_dim(logits_wide, shift, vocab_own, axis=0)
        return key_own[:own_rows], value_own[:own_rows], (logits - log_norm[None, :]).T, log_norm

    in_specs = (P("dp", "xax"), P("dp"), row_spec, row_spec, P("xax"), P("xax", "yax"),
                P("xax", None), P("xax", None), P("xax", "yax"), P("xax", "yax"),
                P("yax", "xax"), P("yax", "xax"), P("xax"), P("yax", "xax"))
    out_specs = (row_spec, row_spec, P("dp", ("yax", "xax")), P("dp"))
    return jax.shard_map(local_step, mesh=mesh, in_specs=in_specs, out_specs=out_specs, check_vma=False)
```

```python
import itertools

import jax
import jax.numpy as jnp
from jax import lax
from jax.experimental import pallas as pl
from jax.experimental.pallas import tpu as pltpu
from jax.sharding import PartitionSpec as P

EPS = 1e-6
ROPE_BASE = 10000.0
MESH_ID = pl.DeviceIdType.MESH
NY = NZ = NX = 4
CORES = 2
POOL = 48
HOPS = (1, 3, 2)
LINE = [(0, 1), (1, 0), (3, 0), (1, 1), (3, 1), (2, 0), (2, 1)]
NEAR = LINE[1:5]
NT = (((1,), (1,)), ((), ()))
PLANE = [(dz, dy) for dz in range(NZ) for dy in range(NY) if dz or dy]


def rope_angle(positions, head_dim):
    half_dim = head_dim // 2
    inv_freq = ROPE_BASE ** (-(jnp.arange(half_dim, dtype=jnp.float32) * 2.0) / head_dim)
    return positions.astype(jnp.float32)[:, None] * inv_freq[None, :]


class Phases:
    def __init__(self):
        self.open = None

    def __call__(self, name):
        self.close()
        self.open = jax.named_scope(name)
        self.open.__enter__()

    def close(self):
        if self.open is not None:
            self.open.__exit__(None, None, None)
        self.open = None


class Links:
    def __init__(self, send_sem, recv_sem):
        self.send_sem, self.recv_sem = send_sem, recv_sem
        self.tags, self.slow, self.fast = itertools.count(), itertools.count(POOL), []
        self.pending = []
        self.y_idx = lax.axis_index("yax")
        self.x_idx = lax.axis_index("xax")
        self.z, self.y = self.y_idx // NY, self.y_idx % NY
        self.chip, self.core = self.x_idx // CORES, self.x_idx % CORES

    def at_plane(self, dz, dy):
        return {"yax": (self.z + dz) % NZ * NY + (self.y + dy) % NY, "xax": self.x_idx}

    def slot_rows(self, dz, dy, rows):
        slot = (self.z + dz) % NZ * NY + (self.y + dy) % NY
        return pl.ds(pl.multiple_of(slot * rows, rows), rows)

    def line_id(self, dx, oc):
        core = 1 - self.core if oc else self.core
        return (self.chip + dx) % NX * CORES + core

    def at_line(self, dx, oc):
        return {"yax": self.y_idx, "xax": self.line_id(dx, oc)}

    def send(self, src, dst, where, tag=None, long=False):
        tag = next(self.tags) if tag is None else tag
        if long:
            sem = next(self.slow)
        else:
            sem = len(self.fast) % POOL
            if len(self.fast) >= POOL:
                self.fast[-POOL].wait_send()
        copy = pltpu.make_async_remote_copy(
            src_ref=src, dst_ref=dst, send_sem=self.send_sem.at[sem], recv_sem=self.recv_sem.at[tag],
            device_id=where, device_id_type=MESH_ID)
        copy.start()
        (self.pending if long else self.fast).append(copy)
        return copy

    def finish(self):
        for copy in self.pending + self.fast[-POOL:]:
            copy.wait_send()

    def barrier(self):
        barrier = pltpu.get_barrier_semaphore()
        peers = [self.at_line(*p) for p in LINE] + [self.at_plane(*p) for p in PLANE]
        for peer in peers:
            pl.semaphore_signal(barrier, inc=1, device_id=peer, device_id_type=MESH_ID)
        pl.semaphore_wait(barrier, len(peers))


def plane_gather(links, buf, tags, hook):
    cols = buf.shape[-1]
    rows = buf.shape[1] // (NY * NZ)
    span = cols // 2
    partner = links.at_line(0, 1)
    crossing = []

    class Part:
        def __init__(self, index):
            self.index, self.lo, self.got = index, index * span, {}

        def order(self, du, dv):
            return (du, dv) if self.index else (dv, du)

        def block(self, at, half=0, piece=None):
            width = span if piece is None else span // 2
            lo = self.lo if not piece else self.lo + width
            return buf.at[half, links.slot_rows(*self.order(*at), rows), pl.ds(lo, width)]

        def push(self, name, at, to, piece=None):
            ref = self.block(at, piece=piece)
            self.got[name] = links.send(ref, ref, links.at_plane(*self.order(*to)), next(tags))

        def spread(self, k, at):
            self.push(("v+", k), at, (0, 1))
            self.push(("v-", k), at, (0, -1))

        def give(self, at):
            crossing.append(links.send(self.block(at), self.block(at, half=1), partner, next(tags)))

        def wait(self, name):
            self.got[name].wait_recv()

    parts = [Part(index) for index in range(2)]
    offset = (0, -1, 1, 2)
    for p in parts:
        p.push("u+", (0, 0), (1, 0))
        p.push("u-", (0, 0), (-1, 0))
        p.spread(0, (0, 0))
    for p in parts:
        p.give((0, 0))
    for k, name in enumerate(("u+", "u-"), 1):
        for p in parts:
            p.wait(name)
            at = (offset[k], 0)
            p.push(("far", k), at, (-offset[k], 0), piece=k - 1)
            p.spread(k, at)
            p.give(at)
    hook()

    def arrive(p, k):
        for name, step in (("v+", -1), ("v-", 1)):
            p.wait((name, k))
            at = (offset[k], step)
            if (name == "v+") == (k in (0, 3)):
                p.push(("relay", k), at, (0, -step))
            p.give(at)

    for p in parts:
        arrive(p, 0)
    for p in parts:
        p.wait(("far", 1))
        p.wait(("far", 2))
        p.spread(3, (2, 0))
        p.give((2, 0))
    for k in range(1, len(offset)):
        for p in parts:
            arrive(p, k)
    for k in range(len(offset)):
        for p in parts:
            p.wait(("relay", k))
            p.give((offset[k], 2))
    return crossing


def norm_gather(links, own_slot, gain_buf, which, xbuf, stat, out, base, hook):
    own_slot()
    rows, chunk = xbuf.shape[1:]
    tags = itertools.count(base)
    line = [links.send(xbuf.at[0], xbuf.at[NX - dx], links.at_line(dx, 0), next(tags)) for dx in HOPS]
    yield
    phase = Phases()
    for n, c in enumerate(line):
        phase(f"ng_line{which}_{n}")
        c.wait_recv()
    phase("ng_stats")
    held = xbuf[...].astype(jnp.float32)
    count = NX * chunk
    mean = jnp.sum(jnp.sum(held, axis=0), axis=-1, keepdims=True) / count
    dev = held - mean[None]
    square = jnp.sum(jnp.sum(dev * dev, axis=0), axis=-1, keepdims=True)
    lane = lax.broadcasted_iota(jnp.int32, (rows, 128), 1)
    stat[0] = jnp.where(lane == 0, mean, square)
    links.send(stat.at[0], stat.at[1], links.at_line(0, 1), next(tags)).wait_recv()
    other_mean, other_square = stat[1, :, 0:1], stat[1, :, 1:2]
    both = (mean + other_mean) * 0.5
    gap = mean - other_mean
    var = (square + other_square + gap * gap * (count * 0.5)) / (2 * count)
    scale = lax.rsqrt(var + EPS)
    for e in range(NX):
        out[0, links.slot_rows(0, 0, rows), e * chunk:(e + 1) * chunk] = (
            (xbuf[e].astype(jnp.float32) - both) * scale * gain_buf[e, which:which + 1, :]).astype(jnp.bfloat16)
    phase("ng_plane")
    crossing = plane_gather(links, out, tags, hook)
    phase("ng_cross")
    for c in crossing:
        c.wait_recv()
    phase.close()


def step_kernel(vocab_own, own_rows, hid_ref, gain_a, gain_f, cos_ref, sin_ref, len_ref, k_hbm, v_hbm,
                wq_ref, wk_ref, wv_ref, wo_ref, wg_ref, wu_ref, wd_hbm, emb_ref,
                knew_ref, vnew_ref, z_ref, norm_ref,
                k_buf, v_buf, wd_buf, wo_all, att, rc, n_buf, w_buf, wq_t, wq_buf, sel, sel_t, qx, qr, qy, qf,
                kvp, kvr, o_buf, o_got, o_all, act,
                part, ra1, rb1, ra2, rb2, acc_a, acc_b, xbuf, stat, xbuf2, stat2, gains, f_buf, emb_buf,
                w_relay, emb_relay, lse_x, lse_y, send_sem, recv_sem, local_sem):
    links = Links(send_sem, recv_sem)
    phase = Phases()
    f32, bf16 = jnp.float32, jnp.bfloat16
    z, y, xid, yid = links.z, links.y, links.x_idx, links.y_idx
    rows, chunk = hid_ref.shape[2], hid_ref.shape[3]
    half = chunk // 2
    nx2, nyz = 2 * NX, NY * NZ
    group = NY * rows
    head = 128
    pad = 8
    partner = links.at_line(0, 1)
    line_id = links.line_id
    gather_tags = len(HOPS) + 1 + len(PLANE) * CORES * CORES + CORES * CORES
    gather_base = [next(links.tags) for _ in range(gather_tags)][0]

    def dot(a, b):
        return jnp.dot(a, b, preferred_element_type=f32)

    def dot_t(a, b):
        return lax.dot_general(a, b, NT, preferred_element_type=f32)

    def to_line(src, dst, where=LINE, **kw):
        return [links.send(src(dx, oc), dst(dx, oc), links.at_line(dx, oc), **kw) for dx, oc in where]

    local = []

    def fetch(src, dst):
        copy = pltpu.make_async_copy(src, dst, local_sem.at[len(local)])
        copy.start()
        local.append(copy)
        return copy

    ff = wg_ref.shape[1] // nx2

    def w_piece(ref, dx, oc):
        return ref.at[:, pl.ds(pl.multiple_of(line_id(dx, oc) * ff, ff), ff)]

    def w_slot(which, dx, oc):
        back = (NX - dx) % NX
        return w_buf.at[int(oc), pl.ds(back * chunk, chunk), pl.ds(which * ff, ff)]

    take = emb_buf.shape[1]

    def emb_start(xi):
        return pl.multiple_of(vocab_own * xi // 16 * 16 - xi // (nx2 - 1) * 16, 16)

    def emb_piece(dx, oc):
        return emb_ref.at[pl.ds(emb_start(line_id(dx, oc)), take), :]

    def emb_slot(dx, oc):
        return emb_buf.at[int(oc), :, pl.ds((NX - dx) % NX * chunk, chunk)]

    def emb_half(oc, way):
        part_rows = take // 2
        return emb_ref.at[pl.ds(emb_start(line_id(2, oc)) + way * part_rows, part_rows), :]

    def emb_far_slot(oc, way):
        return emb_buf.at[int(oc), pl.ds(way * (take // 2), take // 2), pl.ds(2 * chunk, chunk)]

    phase("start")
    own_w = [fetch(w_piece(wg_ref, 0, 0), w_slot(0, 0, 0)), fetch(w_piece(wu_ref, 0, 0), w_slot(1, 0, 0))]
    got_kv = [fetch(k_hbm, k_buf), fetch(v_hbm, v_buf)]
    got_wd = fetch(wd_hbm, wd_buf)
    own_emb = fetch(emb_piece(0, 0), emb_slot(0, 0))

    qc = wq_ref.shape[1]
    qs = qc // nx2
    per = head // qs
    eye_q = (lax.broadcasted_iota(jnp.int32, (qc, qc), 0) == lax.broadcasted_iota(jnp.int32, (qc, qc), 1))
    wq_t[...] = dot_t(eye_q.astype(bf16), wq_ref[...]).astype(bf16)
    wq_buf[...] = jnp.zeros(wq_buf.shape, bf16)

    def q_rows(xi):
        return pl.ds(pl.multiple_of(xi % per * qs, qs), qs)

    wq_buf[0, q_rows(xid), 0:chunk] = wq_t[pl.ds(pl.multiple_of(xid * qs, qs), qs), :]
    phase("barrier")
    links.barrier()

    phase("front_send")
    gains[0, 0:1, :] = gain_a[...]
    gains[0, 1:2, :] = gain_f[...]
    gains[0, 2:, :] = jnp.zeros((6, chunk), f32)

    def own_input():
        xbuf[0] = hid_ref[z, y]

    w_far, emb_far, emb_got = [], [], []
    ways = [(way, hop, oc) for oc in (0, 1) for way, hop in enumerate(HOPS[:2])]

    def forward_weights():
        for (way, hop, oc), c in zip(ways, w_far):
            c.wait_recv()
            w_got.append(links.send(w_relay.at[way, oc], w_buf.at[oc, pl.ds(2 * chunk, chunk), pl.ds(way * ff, ff)],
                                    links.at_line(hop, oc), long=True))
        emb_out(ways[:2])

    def emb_out(some):
        for way, hop, oc in some:
            emb_far.append(links.send(emb_half(oc, way), emb_relay.at[way, oc], links.at_line(hop, 0), long=True))

    def emb_on(some, arrived):
        for (way, hop, oc), c in zip(some, arrived):
            c.wait_recv()
            emb_got.append(links.send(emb_relay.at[way, oc], emb_far_slot(oc, way), links.at_line(hop, oc), long=True))

    front = norm_gather(links, own_input, gains, 0, xbuf, stat, n_buf, gather_base, forward_weights)
    next(front)
    gain_got = [links.send(gains.at[0], gains.at[NX - dx], links.at_line(dx, 0)) for dx in HOPS]
    for way, hop, oc in ways:
        w_far.append(links.send(w_piece((wg_ref, wu_ref)[way], 2, oc), w_relay.at[way, oc], links.at_line(hop, 0),
                                long=True))

    def wq_rows(dx, oc):
        return wq_t.at[pl.ds(pl.multiple_of(line_id(dx, oc) * qs, qs), qs), :]

    def wq_slot(dx, oc):
        return wq_buf.at[oc, q_rows(line_id(dx, oc)), pl.ds((NX - dx) % NX * chunk, chunk)]

    wq_got = to_line(wq_rows, wq_slot, long=True)
    w_got = []
    for which, ref in enumerate((wg_ref, wu_ref)):
        w_got += to_line(lambda dx, oc: w_piece(ref, dx, oc), lambda dx, oc: w_slot(which, dx, oc),
                         LINE[:1] + NEAR, long=True)

    phase("selections")
    total_rows = nyz * rows
    r_id = lax.broadcasted_iota(jnp.int32, (nx2 * nyz * pad, 1), 0)
    r_j = r_id % pad
    r_src = jnp.where(r_j < own_rows, r_id // pad % nyz * rows + r_id // (pad * nyz) * own_rows + r_j, -1)
    s_id = lax.broadcasted_iota(jnp.int32, (1, total_rows), 1)
    sel[...] = jnp.where(r_src == s_id, 1.0, 0.0).astype(bf16)
    t_id = lax.broadcasted_iota(jnp.int32, (group, 1), 0)
    t_in = t_id % rows
    t_src = t_in // own_rows * (NY * pad) + t_id // rows * pad + t_in % own_rows
    u_id = lax.broadcasted_iota(jnp.int32, (1, nx2 * NY * pad), 1)
    sel_t[...] = jnp.where(t_src == u_id, 1.0, 0.0).astype(bf16)
    k_id = lax.broadcasted_iota(jnp.int32, (nx2 * pad, rows), 0)
    k_src = jnp.where(k_id % pad < own_rows, k_id // pad * own_rows + k_id % pad, -1)
    sel_kv = jnp.where(k_src == lax.broadcasted_iota(jnp.int32, (nx2 * pad, rows), 1), 1.0, 0.0).astype(bf16)

    phase.close()
    for c in gain_got:
        c.wait_recv()
    for _ in front:
        pass
    phase("kv_part")

    n_own = dot(sel_kv, n_buf[0, links.slot_rows(0, 0, rows), 0:chunk]).astype(bf16)
    kvp[:, :, :head] = dot(n_own, wk_ref[...]).reshape(nx2, pad, head)
    kvp[:, :, head:] = dot(n_own, wv_ref[...]).reshape(nx2, pad, head)
    kv_got = to_line(lambda dx, oc: kvp.at[line_id(dx, oc)], lambda dx, oc: kvr.at[xid])
    kvr[xid] = kvp[xid]

    phase("wait_wq")
    for c in wq_got:
        c.wait_recv()
    phase("q_mm")
    q_all = jnp.concatenate([
        (dot_t(n_buf[0, i * group:(i + 1) * group, :], wq_buf[0])
         + dot_t(n_buf[1, i * group:(i + 1) * group, :], wq_buf[1])).astype(bf16) for i in range(NZ)], axis=0)
    span = nyz * pad
    for i in range(nx2):
        qx[i] = dot(sel[i * span:(i + 1) * span, :], q_all).astype(bf16)
    line_tags = [next(links.tags) for _ in LINE]
    plane_tags = [next(links.tags) for _ in PLANE]
    q_got = [links.send(qx.at[line_id(*p)], qr.at[xid], links.at_line(*p), t) for p, t in zip(LINE, line_tags)]
    qr[xid] = qx[xid]

    phase("wait_w")
    for c in own_w:
        c.wait()
    for c in w_got:
        c.wait_recv()
    phase("gate_up")

    def act_at(k, dx):
        return act.at[(z + k) % NZ, :, pl.ds(pl.multiple_of(line_id(dx, 0) * ff, ff), ff)]

    def act_out(k, dx, to_dx):
        return links.send(act_at(k, dx), act_at(k, dx), links.at_line(to_dx, 0))

    def act_give(k, dx):
        cross[k].append(links.send(act_at(k, dx), act_at(k, dx), partner))

    turns = (2, 1, 3, 0)
    early, late = turns[:2], turns[2:]
    near_act, far_act, cross = {}, {}, {k: [] for k in turns}
    for k in turns:
        these = pl.ds(pl.multiple_of((z + k) % NZ * group, group), group)
        both = (dot(n_buf[0, these, :], w_buf[0]) + dot(n_buf[1, these, :], w_buf[1])).astype(bf16).astype(f32)
        gate, up = both[:, :ff], both[:, ff:]
        act_at(k, 0)[...] = (gate * jax.nn.sigmoid(gate) * up).astype(bf16)
        near_act[k] = [(dx, act_out(k, 0, dx)) for dx in HOPS[:2]]
        act_give(k, 0)

    def act_pass(k):
        for dx, c in near_act[k]:
            c.wait_recv()
            if (k in early) == (dx == 1):
                far_act[k] = act_out(k, NX - dx, dx)
            act_give(k, NX - dx)

    low, high = pl.ds(0, half), pl.ds(half, half)
    first_a, first_b = [], []

    def act_use(k):
        for c in cross[k]:
            c.wait_recv()
        g = (z + k) % NZ
        part[g] = dot(act[g], wd_buf[...]).reshape(NY, rows, chunk)
        for d in turns[:-1]:
            first_a.append(links.send(part.at[g, (y + d) % NY, :, low], ra1.at[d - 1, g], links.at_plane(0, d)))
        if k:
            first_b.append(links.send(part.at[g, :, :, high], rb1.at[k - 1], links.at_plane(k, 0)))

    def act_far(ks):
        for k in ks:
            far_act[k].wait_recv()
            act_give(k, 2)

    phase("wait_q")
    for c in q_got:
        c.wait_recv()
    phase("q_sum")
    for j in range(qc // head):
        piece = qr[j * per].astype(f32)
        for i in range(1, per):
            piece = piece + qr[j * per + i].astype(f32)
        qy[:, :, j * head:(j + 1) * head] = piece.reshape(nyz, pad, head)
    def plane_id(dz, dy):
        return (z + dz) % NZ * NY + (y + dy) % NY

    y_got = [links.send(qy.at[plane_id(*p)], qf.at[yid], links.at_plane(*p), t) for p, t in zip(PLANE, plane_tags)]
    qf[yid] = qy[yid]

    def wo_rows(dz):
        return wo_all.at[pl.ds(pl.multiple_of((z + dz) % NZ * qc, qc), qc), :]

    wo_got = [links.send(wo_ref, wo_rows(0), links.at_plane(d, 0), long=True) for d in HOPS]
    wo_rows(0)[...] = wo_ref[...]

    phase("act_pass")
    for k in early:
        act_pass(k)
    phase("wait_kv")
    for c in kv_got:
        c.wait_recv()
    kv_sum = kvr[0]
    for i in range(1, nx2):
        kv_sum = kv_sum + kvr[i]
    kv_new = kv_sum.astype(bf16).astype(f32)

    def turn(v, b=None):
        cos, sin = (cos_ref[...], sin_ref[...]) if b is None else (cos_ref[b:b + 1, :], sin_ref[b:b + 1, :])
        return (v * cos + pltpu.roll(v, head // 2, 1) * sin).astype(bf16)

    k_new = turn(kv_new[:, :head])
    knew_ref[...] = k_new
    vnew_ref[...] = kv_new[:, head:].astype(bf16)
    k_row, v_row = k_new.astype(f32), kv_new[:, head:]
    phase("act_early")
    for k in late:
        act_pass(k)
    act_far(early)
    got_wd.wait()
    for k in early:
        act_use(k)
    phase("wait_qy")
    for c in got_kv:
        c.wait()
    for c in y_got:
        c.wait_recv()
    phase("attention")
    seq = k_buf.shape[1]
    score_scale = head ** -0.5
    position = lax.broadcasted_iota(jnp.int32, (1, seq), 1)
    o_buf[...] = jnp.zeros(o_buf.shape, f32)
    for b in range(own_rows):
        q_b = jnp.concatenate([turn(qf[:, b, j * head:(j + 1) * head], b) for j in range(qc // head)], axis=0)
        scores = dot_t(q_b, k_buf[b]) * score_scale
        score_new = jnp.sum(q_b.astype(f32) * k_row[b:b + 1, :], axis=-1, keepdims=True) * score_scale
        valid = position < len_ref[b:b + 1, 0:1]
        top = jnp.maximum(jnp.max(jnp.where(valid, scores, -jnp.inf), axis=-1, keepdims=True), score_new)
        weights = jnp.where(valid, jnp.exp(scores - top), 0.0)
        weight_new = jnp.exp(score_new - top)
        denom = jnp.sum(weights, axis=-1, keepdims=True) + weight_new
        o_b = dot((weights / denom).astype(bf16), v_buf[b])
        o_b = o_b + (weight_new / denom).astype(bf16).astype(f32) * v_row[b:b + 1, :]
        o_b = o_b.astype(bf16).astype(f32)
        for j in range(qc // head):
            o_buf[:, :, b, j * head:(j + 1) * head] = o_b[j * nyz:(j + 1) * nyz, :].reshape(NZ, NY, head)
    o_back = [links.send(o_buf.at[:, (y + d) % NY], o_got.at[y], links.at_plane(0, d)) for d in HOPS]
    o_got[y] = o_buf[:, y]

    phase("act_late")
    act_far(late)
    for k in late:
        act_use(k)

    phase("wait_oy")
    for c in o_back:
        c.wait_recv()
    for i in range(NZ):
        o_all[xid, :, i * qc:(i + 1) * qc] = o_got[:, i].reshape(NY * pad, qc).astype(bf16)
    o_here = o_all.at[xid]
    o_line = [links.send(o_here, o_here, links.at_line(dx, 0)) for dx in HOPS]
    o_cross = [links.send(o_here, o_here, partner)]
    emb_out(ways[2:])
    emb_got += to_line(emb_piece, emb_slot, LINE[:1], long=True)
    phase("wait_o")
    for dx, c in zip(HOPS, o_line):
        c.wait_recv()
        came = o_all.at[line_id(NX - dx, 0)]
        o_cross.append(links.send(came, came, partner))
    for c in wo_got + o_cross:
        c.wait_recv()
    phase("out_mm")
    o_nat = dot(sel_t[...], o_all[...].reshape(nx2 * NY * pad, NZ * qc)).astype(bf16)
    att[...] = dot(o_nat, wo_all[...]).reshape(NY, rows, chunk)
    att_got = [links.send(att.at[(y + d) % NY], rc.at[d - 1], links.at_plane(0, d)) for d in HOPS]
    emb_on(ways[:2], emb_far[:2])

    phase("wait_rs1")
    for c in first_b:
        c.wait_recv()
    acc_b[...] = (part[z, :, :, half:] + rb1[0]) + (rb1[1] + rb1[2])
    second = [links.send(acc_b.at[(y + d) % NY], rb2.at[d - 1], links.at_plane(0, d)) for d in HOPS]
    phase("wait_rs1a")
    for c in first_a:
        c.wait_recv()
    acc_a[...] = (part[:, y, :, :half] + ra1[0]) + (ra1[1] + ra1[2])
    second += [links.send(acc_a.at[(z + d) % NZ], ra2.at[d - 1], links.at_plane(d, 0)) for d in HOPS]
    phase("wait_att")
    for c in att_got:
        c.wait_recv()
    phase("wait_rs2")
    for c in second:
        c.wait_recv()
    phase("rs_sum2")
    def own_residual():
        res = hid_ref[z, y].astype(f32) + ((att[y] + rc[0]) + (rc[1] + rc[2]))
        xbuf2[0, :, :half] = res[:, :half] + ((acc_a[z] + ra2[0]) + (ra2[1] + ra2[2]))
        xbuf2[0, :, half:] = res[:, half:] + ((acc_b[y] + rb2[0]) + (rb2[1] + rb2[2]))

    back = norm_gather(links, own_residual, gains, 1, xbuf2, stat2, f_buf, gather_base, lambda: None)
    next(back)
    emb_on(ways[2:], emb_far[2:])
    emb_got += to_line(emb_piece, emb_slot, NEAR, long=True)
    phase.close()
    for _ in back:
        pass
    phase("wait_emb")
    own_emb.wait()
    for c in emb_got:
        c.wait_recv()

    phase("logits")
    wide_n = 256
    for i in range(total_rows // wide_n):
        cols = slice(i * wide_n, (i + 1) * wide_n)
        z_ref[:, cols] = dot_t(emb_buf[0], f_buf[0, cols, :]) + dot_t(emb_buf[1], f_buf[1, cols, :])

    phase("lse_own")
    shift = vocab_own * xid - emb_start(xid)
    vid = lax.broadcasted_iota(jnp.int32, (take, 1), 0)
    own = (vid >= shift) & (vid < shift + vocab_own)
    blocks = total_rows // 128
    for b in range(blocks):
        zb = jnp.where(own, z_ref[:, b * 128:(b + 1) * 128], -jnp.inf)
        top = jnp.max(zb, axis=0, keepdims=True)
        lse_x[xid, b:b + 1, :] = top
        lse_x[xid, 8 + b:9 + b, :] = jnp.sum(jnp.exp(zb - top), axis=0, keepdims=True)
    for b in range(blocks, 8):
        lse_x[xid, b:b + 1, :] = jnp.zeros((1, 128), f32)
        lse_x[xid, 8 + b:9 + b, :] = jnp.ones((1, 128), f32)

    def merge(ref):
        tops = ref[:, :8, :]
        top = jnp.max(tops, axis=0)
        return top, jnp.sum(ref[:, 8:, :] * jnp.exp(tops - top[None]), axis=0)

    phase("lse_line")
    got = [links.send(lse_x.at[xid], lse_x.at[xid], links.at_line(*p), t) for p, t in zip(LINE, line_tags)]
    for c in got:
        c.wait_recv()
    top, mass = merge(lse_x)
    lse_y[yid, :8, :] = top
    lse_y[yid, 8:, :] = mass
    phase("lse_plane")
    got = [links.send(lse_y.at[yid], lse_y.at[yid], links.at_plane(*p), t) for p, t in zip(PLANE, plane_tags)]
    for c in got:
        c.wait_recv()
    top, mass = merge(lse_y)
    norm_ref[...] = top + jnp.log(mass)
    phase("finish")
    links.finish()
    phase.close()


def whole_step(hidden, cos, sin, lens, k_cache, v_cache, g_attn, w_query, w_key, w_value,
               w_gate, w_up, w_out, w_down, g_final, embedding):
    total_rows, chunk = hidden.shape
    own_rows, seq, head = k_cache.shape
    rows = total_rows // (NY * NZ)
    vocab_own = embedding.shape[0] // (2 * NX)
    take = (vocab_own + 30) // 16 * 16
    half = chunk // 2
    qc = w_query.shape[1]
    ff = w_gate.shape[1] // (2 * NX)
    f32, bf16 = jnp.float32, jnp.bfloat16
    nyz, nx2, pad = NY * NZ, 2 * NX, 8
    vmem = pl.BlockSpec(memory_space=pltpu.VMEM)
    hbm = pl.BlockSpec(memory_space=pl.ANY)
    V = pltpu.VMEM
    return pl.pallas_call(
        lambda *refs: step_kernel(vocab_own, own_rows, *refs),
        out_shape=(jax.ShapeDtypeStruct((pad, head), bf16), jax.ShapeDtypeStruct((pad, head), bf16),
                   jax.ShapeDtypeStruct((take, total_rows), f32), jax.ShapeDtypeStruct((8, 128), f32)),
        in_specs=[vmem] * 6 + [hbm] * 2 + [vmem] * 4 + [hbm] * 4,
        out_specs=(vmem,) * 4,
        scratch_shapes=[
            V((own_rows, seq, head), bf16), V((own_rows, seq, head), bf16),
            V((nx2 * ff, chunk), bf16), V((NZ * qc, chunk), bf16), V((NY, rows, chunk), f32), V((3, rows, chunk), f32), V((2, total_rows, NX * chunk), bf16), V((2, NX * chunk, 2 * ff), bf16),
            V((qc, chunk), bf16), V((2, head, NX * chunk), bf16),
            V((nx2 * nyz * pad, total_rows), bf16), V((NY * rows, nx2 * NY * pad), bf16),
            V((nx2, nyz * pad, head), bf16), V((nx2, nyz * pad, head), bf16),
            V((nyz, pad, qc), f32), V((nyz, pad, qc), f32),
            V((nx2, pad, 2 * head), f32), V((nx2, pad, 2 * head), f32),
            V((NZ, NY, pad, qc), f32), V((NY, NZ, pad, qc), f32), V((nx2, NY * pad, NZ * qc), bf16),
            V((NZ, NY * rows, nx2 * ff), bf16),
            V((NZ, NY, rows, chunk), f32),
            V((3, NZ, rows, half), f32), V((3, NY, rows, half), f32), V((3, rows, half), f32), V((3, rows, half), f32),
            V((NZ, rows, half), f32), V((NY, rows, half), f32),
            V((NX, rows, chunk), bf16), V((2, rows, 128), f32), V((NX, rows, chunk), f32), V((2, rows, 128), f32),
            V((NX, 8, chunk), f32),
            V((2, total_rows, NX * chunk), bf16), V((2, take, NX * chunk), bf16),
            V((2, 2, chunk, ff), bf16), V((2, 2, take // 2, chunk), bf16),
            V((nx2, 16, 128), f32), V((nyz, 16, 128), f32),
            pltpu.SemaphoreType.DMA((POOL + 41,)), pltpu.SemaphoreType.DMA((203,)), pltpu.SemaphoreType.DMA((6,)),
        ],
        compiler_params=pltpu.CompilerParams(
            collective_id=1, has_side_effects=True, vmem_limit_bytes=60 * 1024 * 1024),
        name="decode_step",
    )(hidden.reshape(NZ, NY, rows, chunk), g_attn[None, :], g_final[None, :], cos, sin, lens, k_cache, v_cache,
      w_query, w_key, w_value, w_out, w_gate, w_up, w_down, embedding)


def solution(mesh):
    x_size = mesh.shape["xax"]
    row_spec = P(("dp", "yax", "xax"))

    def local_step(hidden, cache_len, k_cache, v_cache, g_attn, w_query, w_key, w_value,
                   w_gate, w_up, w_out, w_down, g_final, embedding):
        rows = hidden.shape[0]
        own_rows, _, head_dim = k_cache.shape
        y_idx = lax.axis_index("yax")
        x_idx = lax.axis_index("xax")
        own_start = (y_idx * x_size + x_idx) * own_rows
        len_own = jnp.pad(lax.dynamic_slice_in_dim(cache_len, own_start, own_rows, axis=0), (0, 8 - own_rows))
        angles = rope_angle(len_own, head_dim)
        cos_half, sin_half = jnp.cos(angles), jnp.sin(angles)
        cos = jnp.concatenate([cos_half, cos_half], axis=1)
        sin = jnp.concatenate([-sin_half, sin_half], axis=1)
        lens = jnp.broadcast_to(len_own[:, None], (8, 128))
        key_own, value_own, logits_wide, norm_tile = whole_step(
            hidden, cos, sin, lens, k_cache, v_cache, g_attn, w_query, w_key, w_value,
            w_gate, w_up, w_out, w_down, g_final, embedding)
        vocab_own = embedding.shape[0] // x_size
        log_norm = norm_tile[:rows // 128].reshape(rows)
        shift = vocab_own * x_idx - (vocab_own * x_idx // 16 * 16 - x_idx // (x_size - 1) * 16)
        logits = lax.dynamic_slice_in_dim(logits_wide, shift, vocab_own, axis=0)
        return key_own[:own_rows], value_own[:own_rows], (logits - log_norm[None, :]).T, log_norm

    in_specs = (P("dp", "xax"), P("dp"), row_spec, row_spec, P("xax"), P("xax", "yax"),
                P("xax", None), P("xax", None), P("xax", "yax"), P("xax", "yax"),
                P("yax", "xax"), P("yax", "xax"), P("xax"), P("yax", "xax"))
    out_specs = (row_spec, row_spec, P("dp", ("yax", "xax")), P("dp"))
    return jax.shard_map(local_step, mesh=mesh, in_specs=in_specs, out_specs=out_specs, check_vma=False)
```

```python
import itertools

import jax
import jax.numpy as jnp
from jax import lax
from jax.experimental import pallas as pl
from jax.experimental.pallas import tpu as pltpu
from jax.sharding import PartitionSpec as P

EPS = 1e-6
ROPE_BASE = 10000.0
MESH_ID = pl.DeviceIdType.MESH
NY = NZ = NX = 4
CORES = 2
POOL, SENDS, TAGS = 24, 57, 84
HOPS = (1, 3, 2)
LINE = [(0, 1), (1, 0), (3, 0), (1, 1), (3, 1), (2, 0), (2, 1)]
NEAR = LINE[1:5]
NT = (((1,), (1,)), ((), ()))
PLANE = [(dz, dy) for dz in range(NZ) for dy in range(NY) if dz or dy]


class Group:
    def __init__(self, links, whole):
        self.links, self.whole = links, whole
        self.tag, self.sem = next(links.tags), next(links.slow)
        links.groups.append(self)

    def send(self, src, dst, where):
        pltpu.make_async_remote_copy(
            src_ref=src, dst_ref=dst, send_sem=self.links.send_sem.at[self.sem],
            recv_sem=self.links.recv_sem.at[self.tag], device_id=where, device_id_type=MESH_ID).start()

    def wait(self):
        pltpu.make_async_copy(self.whole, self.whole, self.links.recv_sem.at[self.tag]).wait()

    def wait_sent(self):
        pltpu.make_async_copy(self.whole, self.whole, self.links.send_sem.at[self.sem]).wait()


class Phases:
    def __init__(self):
        self.open = None

    def __call__(self, name):
        self.close()
        self.open = jax.named_scope(name)
        self.open.__enter__()

    def close(self):
        if self.open is not None:
            self.open.__exit__(None, None, None)
        self.open = None


class Links:
    def __init__(self, send_sem, recv_sem):
        self.send_sem, self.recv_sem = send_sem, recv_sem
        self.tags, self.slow, self.fast = itertools.count(), itertools.count(POOL), []
        self.pending, self.groups = [], []
        self.y_idx = lax.axis_index("yax")
        self.x_idx = lax.axis_index("xax")
        self.z, self.y = self.y_idx // NY, self.y_idx % NY
        self.chip, self.core = self.x_idx // CORES, self.x_idx % CORES

    def at_plane(self, dz, dy):
        return {"yax": (self.z + dz) % NZ * NY + (self.y + dy) % NY, "xax": self.x_idx}

    def slot_rows(self, dz, dy, rows):
        slot = (self.z + dz) % NZ * NY + (self.y + dy) % NY
        return pl.ds(pl.multiple_of(slot * rows, rows), rows)

    def line_id(self, dx, oc):
        core = 1 - self.core if oc else self.core
        return (self.chip + dx) % NX * CORES + core

    def at_line(self, dx, oc):
        return {"yax": self.y_idx, "xax": self.line_id(dx, oc)}

    def send(self, src, dst, where, tag=None, long=False):
        tag = next(self.tags) if tag is None else tag
        if long:
            sem = next(self.slow)
        else:
            sem = len(self.fast) % POOL
            if len(self.fast) >= POOL:
                self.fast[-POOL].wait_send()
        copy = pltpu.make_async_remote_copy(
            src_ref=src, dst_ref=dst, send_sem=self.send_sem.at[sem], recv_sem=self.recv_sem.at[tag],
            device_id=where, device_id_type=MESH_ID)
        copy.start()
        (self.pending if long else self.fast).append(copy)
        return copy

    def finish(self):
        for copy in self.pending + self.fast[-POOL:]:
            copy.wait_send()
        for group in self.groups:
            group.wait_sent()

    def barrier(self):
        barrier = pltpu.get_barrier_semaphore()
        peers = [self.at_line(*p) for p in LINE] + [self.at_plane(*p) for p in PLANE]
        for peer in peers:
            pl.semaphore_signal(barrier, inc=1, device_id=peer, device_id_type=MESH_ID)
        pl.semaphore_wait(barrier, len(peers))


def plane_gather(links, buf, tags, hook, crossing):
    cols = buf.shape[-1]
    rows = buf.shape[1] // (NY * NZ)
    span = cols // 2
    partner = links.at_line(0, 1)

    class Part:
        def __init__(self, index):
            self.index, self.lo, self.got = index, index * span, {}

        def order(self, du, dv):
            return (du, dv) if self.index else (dv, du)

        def block(self, at, half=0, piece=None):
            width = span if piece is None else span // 2
            lo = self.lo if not piece else self.lo + width
            return buf.at[half, links.slot_rows(*self.order(*at), rows), pl.ds(lo, width)]

        def push(self, name, at, to, piece=None):
            ref = self.block(at, piece=piece)
            self.got[name] = links.send(ref, ref, links.at_plane(*self.order(*to)), next(tags))

        def spread(self, k, at):
            self.push(("v+", k), at, (0, 1))
            self.push(("v-", k), at, (0, -1))

        def give(self, at):
            crossing.send(self.block(at), self.block(at, half=1), partner)

        def wait(self, name):
            self.got[name].wait_recv()

    parts = [Part(index) for index in range(2)]
    offset = (0, -1, 1, 2)
    for p in parts:
        p.push("u+", (0, 0), (1, 0))
        p.push("u-", (0, 0), (-1, 0))
        p.spread(0, (0, 0))
    for p in parts:
        p.give((0, 0))
    for k, name in enumerate(("u+", "u-"), 1):
        for p in parts:
            p.wait(name)
            at = (offset[k], 0)
            p.push(("far", k), at, (-offset[k], 0), piece=k - 1)
            p.spread(k, at)
            p.give(at)
    hook()

    def arrive(p, k):
        for name, step in (("v+", -1), ("v-", 1)):
            p.wait((name, k))
            at = (offset[k], step)
            if (name == "v+") == (k in (0, 3)):
                p.push(("relay", k), at, (0, -step))
            p.give(at)

    for p in parts:
        arrive(p, 0)
    for p in parts:
        p.wait(("far", 1))
        p.wait(("far", 2))
        p.spread(3, (2, 0))
        p.give((2, 0))
    for k in range(1, len(offset)):
        for p in parts:
            arrive(p, k)
    for k in range(len(offset)):
        for p in parts:
            p.wait(("relay", k))
            p.give((offset[k], 2))


def norm_gather(links, own_slot, gain_buf, which, xbuf, stat, out, base, hook):
    own_slot()
    rows, chunk = xbuf.shape[1:]
    tags = itertools.count(base)
    line = [links.send(xbuf.at[0], xbuf.at[NX - dx], links.at_line(dx, 0), next(tags)) for dx in HOPS]
    yield
    phase = Phases()
    for n, c in enumerate(line):
        phase(f"ng_line{which}_{n}")
        c.wait_recv()
    phase("ng_stats")
    held = xbuf[...].astype(jnp.float32)
    count = NX * chunk
    mean = jnp.sum(jnp.sum(held, axis=0), axis=-1, keepdims=True) / count
    dev = held - mean[None]
    square = jnp.sum(jnp.sum(dev * dev, axis=0), axis=-1, keepdims=True)
    lane = lax.broadcasted_iota(jnp.int32, (rows, 128), 1)
    stat[0] = jnp.where(lane == 0, mean, square)
    links.send(stat.at[0], stat.at[1], links.at_line(0, 1), next(tags)).wait_recv()
    other_mean, other_square = stat[1, :, 0:1], stat[1, :, 1:2]
    both = (mean + other_mean) * 0.5
    gap = mean - other_mean
    var = (square + other_square + gap * gap * (count * 0.5)) / (2 * count)
    scale = lax.rsqrt(var + EPS)
    for e in range(NX):
        out[0, links.slot_rows(0, 0, rows), e * chunk:(e + 1) * chunk] = (
            (xbuf[e].astype(jnp.float32) - both) * scale * gain_buf[e, which:which + 1, :]).astype(jnp.bfloat16)
    phase("ng_plane")
    crossing = Group(links, out.at[1])
    plane_gather(links, out, tags, hook, crossing)
    phase("ng_cross")
    crossing.wait()
    phase.close()


def step_kernel(vocab_own, own_rows, hid_ref, gain_a, gain_f, freq_ref, len_ref, k_hbm, v_hbm,
                wq_hbm, wk_hbm, wv_hbm, wo_ref, wg_ref, wu_ref, wd_hbm, emb_ref,
                knew_ref, vnew_ref, out_ref, norm_ref,
                wq_ref, wk_ref, wv_ref, z_ref, k_buf, v_buf, wd_buf, wo_all, att, rc, n_buf, w_buf, wq_t, wq_buf, sel, sel_t, qx, qr, qy, qf,
                kvp, kvr, o_buf, o_got, o_all, act,
                part, ra1, rb1, ra2, rb2, acc_a, acc_b, xbuf, stat, xbuf2, stat2, gains, f_buf, emb_buf,
                w_relay, emb_relay, lse_x, lse_y, send_sem, recv_sem, local_sem):
    links = Links(send_sem, recv_sem)
    phase = Phases()
    f32, bf16 = jnp.float32, jnp.bfloat16
    z, y, xid, yid = links.z, links.y, links.x_idx, links.y_idx
    rows, chunk = hid_ref.shape[2], hid_ref.shape[3]
    half = chunk // 2
    nx2, nyz = 2 * NX, NY * NZ
    group = NY * rows
    head = 128
    pad = 8
    partner = links.at_line(0, 1)
    line_id = links.line_id
    gather_tags = len(HOPS) + 1 + len(PLANE) * CORES + CORES
    gather_base = [next(links.tags) for _ in range(gather_tags)][0]

    def dot(a, b):
        return jnp.dot(a, b, preferred_element_type=f32)

    def dot_t(a, b):
        return lax.dot_general(a, b, NT, preferred_element_type=f32)

    def rest(ref, n):
        return Group(links, ref.at[0:n - 1])

    local = []

    def fetch(src, dst):
        copy = pltpu.make_async_copy(src, dst, local_sem.at[len(local)])
        copy.start()
        local.append(copy)
        return copy

    ff = wg_ref.shape[1] // nx2

    def w_piece(ref, dx, oc):
        return ref.at[:, pl.ds(pl.multiple_of(line_id(dx, oc) * ff, ff), ff)]

    def w_slot(which, dx, oc):
        back = (NX - dx) % NX
        return w_buf.at[int(oc), pl.ds(back * chunk, chunk), pl.ds(which * ff, ff)]

    take = emb_buf.shape[1]

    def emb_start(xi):
        return pl.multiple_of(vocab_own * xi // 16 * 16 - xi // (nx2 - 1) * 16, 16)

    def emb_piece(dx, oc):
        return emb_ref.at[pl.ds(emb_start(line_id(dx, oc)), take), :]

    def emb_slot(dx, oc):
        return emb_buf.at[int(oc), :, pl.ds((NX - dx) % NX * chunk, chunk)]

    def emb_half(oc, way):
        part_rows = take // 2
        return emb_ref.at[pl.ds(emb_start(line_id(2, oc)) + way * part_rows, part_rows), :]

    def emb_far_slot(oc, way):
        return emb_buf.at[int(oc), pl.ds(way * (take // 2), take // 2), pl.ds(2 * chunk, chunk)]

    phase("start")
    got_wq = fetch(wq_hbm, wq_ref)
    own_w = [fetch(w_piece(wg_ref, 0, 0), w_slot(0, 0, 0)), fetch(w_piece(wu_ref, 0, 0), w_slot(1, 0, 0))]
    got_kv = [fetch(k_hbm, k_buf), fetch(v_hbm, v_buf)]
    got_wkv = [fetch(wk_hbm, wk_ref), fetch(wv_hbm, wv_ref)]
    got_wd = fetch(wd_hbm, wd_buf)
    own_emb = fetch(emb_piece(0, 0), emb_slot(0, 0))

    qc = wq_ref.shape[1]
    qs = qc // nx2
    per = head // qs
    wq_buf[...] = jnp.zeros(wq_buf.shape, bf16)

    def q_rows(xi):
        return pl.ds(pl.multiple_of(xi % per * qs, qs), qs)

    phase("barrier")
    links.barrier()

    phase("front_send")
    gains[0, 0:1, :] = gain_a[...]
    gains[0, 1:2, :] = gain_f[...]
    gains[0, 2:, :] = jnp.zeros((6, chunk), f32)

    def own_input():
        xbuf[0] = hid_ref[z, y]

    w_far, emb_far = [], []
    w_got = [Group(links, w_buf.at[0, 0:(NX - 1) * chunk]), Group(links, w_buf.at[1])]
    emb_got = [Group(links, emb_buf.at[0, :, 0:(NX - 1) * chunk]), Group(links, emb_buf.at[1])]
    ways = [(way, hop, oc) for oc in (0, 1) for way, hop in enumerate(HOPS[:2])]

    def forward_weights():
        for (way, hop, oc), c in zip(ways, w_far):
            c.wait_recv()
            w_got[oc].send(w_relay.at[way, oc], w_buf.at[oc, pl.ds(2 * chunk, chunk), pl.ds(way * ff, ff)],
                           links.at_line(hop, oc))

    def emb_out(some):
        for way, hop, oc in some:
            emb_far.append(links.send(emb_half(oc, way), emb_relay.at[way, oc], links.at_line(hop, 0), long=True))

    def emb_on(some, arrived):
        for (way, hop, oc), c in zip(some, arrived):
            c.wait_recv()
            emb_got[oc].send(emb_relay.at[way, oc], emb_far_slot(oc, way), links.at_line(hop, oc))

    front = norm_gather(links, own_input, gains, 0, xbuf, stat, n_buf, gather_base, forward_weights)
    next(front)
    gain_got = rest(gains, NX)
    for dx in HOPS:
        gain_got.send(gains.at[0], gains.at[NX - dx], links.at_line(dx, 0))
    for way, hop, oc in ways:
        w_far.append(links.send(w_piece((wg_ref, wu_ref)[way], 2, oc), w_relay.at[way, oc], links.at_line(hop, 0),
                                long=True))

    got_wq.wait()
    eye_q = (lax.broadcasted_iota(jnp.int32, (qc, qc), 0) == lax.broadcasted_iota(jnp.int32, (qc, qc), 1))
    wq_t[...] = dot_t(eye_q.astype(bf16), wq_ref[...]).astype(bf16)
    wq_buf[0, q_rows(xid), 0:chunk] = wq_t[pl.ds(pl.multiple_of(xid * qs, qs), qs), :]

    def wq_rows(dx, oc):
        return wq_t.at[pl.ds(pl.multiple_of(line_id(dx, oc) * qs, qs), qs), :]

    def wq_slot(dx, oc):
        return wq_buf.at[oc, q_rows(line_id(dx, oc)), pl.ds((NX - dx) % NX * chunk, chunk)]

    wq_got = Group(links, wq_t.at[0:qc - qs])
    for dx, oc in LINE:
        wq_got.send(wq_rows(dx, oc), wq_slot(dx, oc), links.at_line(dx, oc))
    for which, ref in enumerate((wg_ref, wu_ref)):
        for dx, oc in LINE[:1] + NEAR:
            w_got[oc].send(w_piece(ref, dx, oc), w_slot(which, dx, oc), links.at_line(dx, oc))

    phase("selections")
    total_rows = nyz * rows
    r_id = lax.broadcasted_iota(jnp.int32, (nx2 * nyz * pad, 1), 0)
    r_j = r_id % pad
    r_src = jnp.where(r_j < own_rows, r_id // pad % nyz * rows + r_id // (pad * nyz) * own_rows + r_j, -1)
    s_id = lax.broadcasted_iota(jnp.int32, (1, total_rows), 1)
    sel[...] = jnp.where(r_src == s_id, 1.0, 0.0).astype(bf16)
    t_id = lax.broadcasted_iota(jnp.int32, (group, 1), 0)
    t_in = t_id % rows
    t_src = t_in // own_rows * (NY * pad) + t_id // rows * pad + t_in % own_rows
    u_id = lax.broadcasted_iota(jnp.int32, (1, nx2 * NY * pad), 1)
    sel_t[...] = jnp.where(t_src == u_id, 1.0, 0.0).astype(bf16)
    k_id = lax.broadcasted_iota(jnp.int32, (nx2 * pad, rows), 0)
    k_src = jnp.where(k_id % pad < own_rows, k_id // pad * own_rows + k_id % pad, -1)
    sel_kv = jnp.where(k_src == lax.broadcasted_iota(jnp.int32, (nx2 * pad, rows), 1), 1.0, 0.0).astype(bf16)

    phase.close()
    gain_got.wait()
    lane = lax.broadcasted_iota(jnp.int32, (1, head), 1)
    lengths = []
    for b in range(own_rows):
        index = (yid * nx2 + xid) * own_rows + b
        row = len_ref[pl.ds(index // head, 1), :].astype(f32)
        lengths.append(jnp.sum(jnp.where(lane == index % head, row, 0.0), axis=-1, keepdims=True))
    lengths = jnp.concatenate(lengths + lengths[:pad - own_rows], axis=0)
    angles = lengths * freq_ref[...]
    cos_all = jnp.cos(angles)
    sin_all = jnp.sin(angles) * jnp.where(lane < head // 2, -1.0, 1.0)

    for _ in front:
        pass
    phase("kv_part")

    for c in got_wkv:
        c.wait()
    n_own = dot(sel_kv, n_buf[0, links.slot_rows(0, 0, rows), 0:chunk]).astype(bf16)
    kvp[:, :, :head] = dot(n_own, wk_ref[...]).reshape(nx2, pad, head)
    kvp[:, :, head:] = dot(n_own, wv_ref[...]).reshape(nx2, pad, head)
    kv_got = rest(kvr, nx2)
    for p in LINE:
        kv_got.send(kvp.at[line_id(*p)], kvr.at[xid], links.at_line(*p))
    kvr[xid] = kvp[xid]

    phase("wait_wq")
    wq_got.wait()
    phase("q_mm")
    q_all = jnp.concatenate([
        (dot_t(n_buf[0, i * group:(i + 1) * group, :], wq_buf[0])
         + dot_t(n_buf[1, i * group:(i + 1) * group, :], wq_buf[1])).astype(bf16) for i in range(NZ)], axis=0)
    span = nyz * pad
    for i in range(nx2):
        qx[i] = dot(sel[i * span:(i + 1) * span, :], q_all).astype(bf16)
    q_got = rest(qr, nx2)
    for p in LINE:
        q_got.send(qx.at[line_id(*p)], qr.at[xid], links.at_line(*p))
    qr[xid] = qx[xid]

    phase("wait_w")
    for c in own_w:
        c.wait()
    for c in w_got:
        c.wait()
    phase("gate_up")

    def act_at(k, dx):
        return act.at[(z + k) % NZ, :, pl.ds(pl.multiple_of(line_id(dx, 0) * ff, ff), ff)]

    def act_out(k, dx, to_dx):
        return links.send(act_at(k, dx), act_at(k, dx), links.at_line(to_dx, 0))

    def act_give(k, dx):
        cross[k].send(act_at(k, dx), act_at(k, dx), partner)

    turns = (2, 1, 3, 0)
    early, late = turns[:2], turns[2:]
    near_act, far_act = {}, {}
    cross = {k: Group(links, act.at[0, :, 0:NX * ff]) for k in turns}
    for k in turns:
        these = pl.ds(pl.multiple_of((z + k) % NZ * group, group), group)
        both = (dot(n_buf[0, these, :], w_buf[0]) + dot(n_buf[1, these, :], w_buf[1])).astype(bf16).astype(f32)
        gate, up = both[:, :ff], both[:, ff:]
        act_at(k, 0)[...] = (gate * jax.nn.sigmoid(gate) * up).astype(bf16)
        near_act[k] = [(dx, act_out(k, 0, dx)) for dx in HOPS[:2]]
        act_give(k, 0)

    def act_pass(k):
        for dx, c in near_act[k]:
            c.wait_recv()
            if (k in early) == (dx == 1):
                far_act[k] = act_out(k, NX - dx, dx)
            act_give(k, NX - dx)

    low, high = pl.ds(0, half), pl.ds(half, half)
    first_a, first_b = Group(links, ra1), Group(links, rb1)

    def act_use(k):
        cross[k].wait()
        g = (z + k) % NZ
        part[g] = dot(act[g], wd_buf[...]).reshape(NY, rows, chunk)
        if k:
            first_b.send(part.at[g, :, :, high], rb1.at[k - 1], links.at_plane(k, 0))

    def along_y(k):
        g = (z + k) % NZ
        for d in early + late[:1]:
            first_a.send(part.at[g, (y + d) % NY, :, low], ra1.at[d - 1, g], links.at_plane(0, d))

    def act_far(ks):
        for k in ks:
            far_act[k].wait_recv()
            act_give(k, 2)

    phase("wait_q")
    q_got.wait()
    phase("q_sum")
    for j in range(qc // head):
        piece = qr[j * per].astype(f32)
        for i in range(1, per):
            piece = piece + qr[j * per + i].astype(f32)
        qy[:, :, j * head:(j + 1) * head] = piece.reshape(nyz, pad, head)
    def plane_id(dz, dy):
        return (z + dz) % NZ * NY + (y + dy) % NY

    y_got = rest(qf, nyz)
    for p in PLANE:
        y_got.send(qy.at[plane_id(*p)], qf.at[yid], links.at_plane(*p))
    qf[yid] = qy[yid]

    def wo_rows(dz):
        return wo_all.at[pl.ds(pl.multiple_of((z + dz) % NZ * qc, qc), qc), :]

    wo_got = Group(links, wo_all.at[0:(NZ - 1) * qc])
    for d in HOPS:
        wo_got.send(wo_ref, wo_rows(0), links.at_plane(d, 0))
    own_wo = fetch(wo_ref, wo_rows(0))

    phase("act_pass")
    for k in early:
        act_pass(k)
    phase("wait_kv")
    kv_got.wait()
    kv_sum = kvr[0]
    for i in range(1, nx2):
        kv_sum = kv_sum + kvr[i]
    kv_new = kv_sum.astype(bf16).astype(f32)

    def turn(v, b=None):
        cos, sin = (cos_all, sin_all) if b is None else (cos_all[b:b + 1, :], sin_all[b:b + 1, :])
        return (v * cos + pltpu.roll(v, head // 2, 1) * sin).astype(bf16)

    k_new = turn(kv_new[:, :head])
    knew_ref[...] = k_new[:own_rows, :]
    vnew_ref[...] = kv_new[:own_rows, head:].astype(bf16)
    k_row, v_row = k_new.astype(f32), kv_new[:, head:]
    phase("act_early")
    for k in late:
        act_pass(k)
    act_far(early)
    emb_out(ways[:2])
    got_wd.wait()
    for k in early:
        act_use(k)
    phase("wait_qy")
    for c in got_kv:
        c.wait()
    y_got.wait()
    phase("attention")
    seq = k_buf.shape[1]
    score_scale = head ** -0.5
    position = lax.broadcasted_iota(jnp.int32, (1, seq), 1).astype(f32)
    o_buf[...] = jnp.zeros(o_buf.shape, f32)
    for b in range(own_rows):
        q_b = jnp.concatenate([turn(qf[:, b, j * head:(j + 1) * head], b) for j in range(qc // head)], axis=0)
        scores = dot_t(q_b, k_buf[b]) * score_scale
        score_new = jnp.sum(q_b.astype(f32) * k_row[b:b + 1, :], axis=-1, keepdims=True) * score_scale
        valid = position < lengths[b:b + 1, :]
        top = jnp.maximum(jnp.max(jnp.where(valid, scores, -jnp.inf), axis=-1, keepdims=True), score_new)
        weights = jnp.where(valid, jnp.exp(scores - top), 0.0)
        weight_new = jnp.exp(score_new - top)
        denom = jnp.sum(weights, axis=-1, keepdims=True) + weight_new
        o_b = dot((weights / denom).astype(bf16), v_buf[b])
        o_b = o_b + (weight_new / denom).astype(bf16).astype(f32) * v_row[b:b + 1, :]
        o_b = o_b.astype(bf16).astype(f32)
        for j in range(qc // head):
            o_buf[:, :, b, j * head:(j + 1) * head] = o_b[j * nyz:(j + 1) * nyz, :].reshape(NZ, NY, head)
    o_back = rest(o_got, NY)
    for d in HOPS:
        o_back.send(o_buf.at[:, (y + d) % NY], o_got.at[y], links.at_plane(0, d))
    for k in early:
        along_y(k)
    o_got[y] = o_buf[:, y]

    phase("act_late")
    act_far(late)
    for k in late:
        act_use(k)
        along_y(k)

    phase("wait_oy")
    o_back.wait()
    for i in range(NZ):
        o_all[xid, :, i * qc:(i + 1) * qc] = o_got[:, i].reshape(NY * pad, qc).astype(bf16)
    o_here = o_all.at[xid]
    o_line = [links.send(o_here, o_here, links.at_line(dx, 0)) for dx in HOPS]
    o_cross = rest(o_all, NX + 1)
    o_cross.send(o_here, o_here, partner)
    emb_out(ways[2:])
    emb_got[1].send(emb_piece(0, 1), emb_slot(0, 1), partner)
    phase("wait_o")
    for dx, c in zip(HOPS, o_line):
        c.wait_recv()
        came = o_all.at[line_id(NX - dx, 0)]
        o_cross.send(came, came, partner)
    wo_got.wait()
    own_wo.wait()
    o_cross.wait()
    phase("out_mm")
    o_nat = dot(sel_t[...], o_all[...].reshape(nx2 * NY * pad, NZ * qc)).astype(bf16)
    att[...] = dot(o_nat, wo_all[...]).reshape(NY, rows, chunk)
    att_got = Group(links, rc)
    for d in HOPS:
        att_got.send(att.at[(y + d) % NY], rc.at[d - 1], links.at_plane(0, d))
    emb_on(ways[:2], emb_far[:2])

    phase("wait_rs1")
    first_b.wait()
    acc_b[...] = (part[z, :, :, half:] + rb1[0]) + (rb1[1] + rb1[2])
    second = [Group(links, rb2), Group(links, ra2)]
    for d in HOPS:
        second[0].send(acc_b.at[(y + d) % NY], rb2.at[d - 1], links.at_plane(0, d))
    phase("wait_rs1a")
    first_a.wait()
    acc_a[...] = (part[:, y, :, :half] + ra1[0]) + (ra1[1] + ra1[2])
    for d in HOPS:
        second[1].send(acc_a.at[(z + d) % NZ], ra2.at[d - 1], links.at_plane(d, 0))
    phase("wait_att")
    att_got.wait()
    phase("wait_rs2")
    for c in second:
        c.wait()
    phase("rs_sum2")
    def own_residual():
        res = hid_ref[z, y].astype(f32) + ((att[y] + rc[0]) + (rc[1] + rc[2]))
        xbuf2[0, :, :half] = res[:, :half] + ((acc_a[z] + ra2[0]) + (ra2[1] + ra2[2]))
        xbuf2[0, :, half:] = res[:, half:] + ((acc_b[y] + rb2[0]) + (rb2[1] + rb2[2]))

    back = norm_gather(links, own_residual, gains, 1, xbuf2, stat2, f_buf, gather_base, lambda: None)
    next(back)
    emb_on(ways[2:], emb_far[2:])
    for dx, oc in NEAR:
        emb_got[oc].send(emb_piece(dx, oc), emb_slot(dx, oc), links.at_line(dx, oc))
    phase.close()
    for _ in back:
        pass
    phase("wait_emb")
    own_emb.wait()
    for c in emb_got:
        c.wait()

    phase("logits")
    wide_n = 256
    for i in range(total_rows // wide_n):
        cols = slice(i * wide_n, (i + 1) * wide_n)
        z_ref[:, cols] = dot_t(emb_buf[0], f_buf[0, cols, :]) + dot_t(emb_buf[1], f_buf[1, cols, :])

    phase("lse_own")
    shift = vocab_own * xid - emb_start(xid)
    vid = lax.broadcasted_iota(jnp.int32, (take, 1), 0)
    own = (vid >= shift) & (vid < shift + vocab_own)
    blocks = total_rows // 128
    for b in range(blocks):
        zb = jnp.where(own, z_ref[:, b * 128:(b + 1) * 128], -jnp.inf)
        top = jnp.max(zb, axis=0, keepdims=True)
        lse_x[xid, b:b + 1, :] = top
        lse_x[xid, 8 + b:9 + b, :] = jnp.sum(jnp.exp(zb - top), axis=0, keepdims=True)
    for b in range(blocks, 8):
        lse_x[xid, b:b + 1, :] = jnp.zeros((1, 128), f32)
        lse_x[xid, 8 + b:9 + b, :] = jnp.ones((1, 128), f32)

    def merge(ref):
        tops = ref[:, :8, :]
        top = jnp.max(tops, axis=0)
        return top, jnp.sum(ref[:, 8:, :] * jnp.exp(tops - top[None]), axis=0)

    phase("lse_line")
    got = rest(lse_x, nx2)
    for p in LINE:
        got.send(lse_x.at[xid], lse_x.at[xid], links.at_line(*p))
    got.wait()
    top, mass = merge(lse_x)
    lse_y[yid, :8, :] = top
    lse_y[yid, 8:, :] = mass
    phase("lse_plane")
    got = rest(lse_y, nyz)
    for p in PLANE:
        got.send(lse_y.at[yid], lse_y.at[yid], links.at_plane(*p))
    got.wait()
    top, mass = merge(lse_y)
    norm = top + jnp.log(mass)
    norm_ref[...] = norm[:blocks, :]
    phase("subtract")
    for b in range(blocks):
        cols = slice(b * head, (b + 1) * head)
        out_ref[:, cols] = pltpu.roll(z_ref[:, cols], (take - shift) % take, 0)[:vocab_own, :] - norm[b:b + 1, :]
    phase("finish")
    links.finish()
    phase.close()


def whole_step(hidden, freq, lens, k_cache, v_cache, g_attn, w_query, w_key, w_value,
               w_gate, w_up, w_out, w_down, g_final, embedding):
    total_rows, chunk = hidden.shape
    own_rows, seq, head = k_cache.shape
    rows = total_rows // (NY * NZ)
    vocab_own = embedding.shape[0] // (2 * NX)
    take = (vocab_own + 30) // 16 * 16
    half = chunk // 2
    qc = w_query.shape[1]
    ff = w_gate.shape[1] // (2 * NX)
    f32, bf16 = jnp.float32, jnp.bfloat16
    nyz, nx2, pad = NY * NZ, 2 * NX, 8
    vmem = pl.BlockSpec(memory_space=pltpu.VMEM)
    hbm = pl.BlockSpec(memory_space=pl.ANY)
    V = pltpu.VMEM
    return pl.pallas_call(
        lambda *refs: step_kernel(vocab_own, own_rows, *refs),
        out_shape=(jax.ShapeDtypeStruct((own_rows, head), bf16), jax.ShapeDtypeStruct((own_rows, head), bf16),
                   jax.ShapeDtypeStruct((vocab_own, total_rows), f32), jax.ShapeDtypeStruct((total_rows // head, head), f32)),
        in_specs=[vmem] * 5 + [hbm] * 10,
        out_specs=(vmem,) * 4,
        scratch_shapes=[
            V((chunk, qc), bf16), V((chunk, head), bf16), V((chunk, head), bf16), V((take, total_rows), f32),
            V((own_rows, seq, head), bf16), V((own_rows, seq, head), bf16),
            V((nx2 * ff, chunk), bf16), V((NZ * qc, chunk), bf16), V((NY, rows, chunk), f32), V((3, rows, chunk), f32), V((2, total_rows, NX * chunk), bf16), V((2, NX * chunk, 2 * ff), bf16),
            V((qc, chunk), bf16), V((2, head, NX * chunk), bf16),
            V((nx2 * nyz * pad, total_rows), bf16), V((NY * rows, nx2 * NY * pad), bf16),
            V((nx2, nyz * pad, head), bf16), V((nx2, nyz * pad, head), bf16),
            V((nyz, pad, qc), f32), V((nyz, pad, qc), f32),
            V((nx2, pad, 2 * head), f32), V((nx2, pad, 2 * head), f32),
            V((NZ, NY, pad, qc), f32), V((NY, NZ, pad, qc), f32), V((nx2, NY * pad, NZ * qc), bf16),
            V((NZ, NY * rows, nx2 * ff), bf16),
            V((NZ, NY, rows, chunk), f32),
            V((3, NZ, rows, half), f32), V((3, NY, rows, half), f32), V((3, rows, half), f32), V((3, rows, half), f32),
            V((NZ, rows, half), f32), V((NY, rows, half), f32),
            V((NX, rows, chunk), bf16), V((2, rows, 128), f32), V((NX, rows, chunk), f32), V((2, rows, 128), f32),
            V((NX, 8, chunk), f32),
            V((2, total_rows, NX * chunk), bf16), V((2, take, NX * chunk), bf16),
            V((2, 2, chunk, ff), bf16), V((2, 2, take // 2, chunk), bf16),
            V((nx2, 16, 128), f32), V((nyz, 16, 128), f32),
            pltpu.SemaphoreType.DMA((SENDS,)), pltpu.SemaphoreType.DMA((TAGS,)), pltpu.SemaphoreType.DMA((10,)),
        ],
        compiler_params=pltpu.CompilerParams(
            collective_id=1, has_side_effects=True, vmem_limit_bytes=60 * 1024 * 1024),
        name="decode_step",
    )(hidden.reshape(NZ, NY, rows, chunk), g_attn[None, :], g_final[None, :], freq, lens, k_cache, v_cache,
      w_query, w_key, w_value, w_out, w_gate, w_up, w_down, embedding)


def solution(mesh):
    row_spec = P(("dp", "yax", "xax"))

    def local_step(hidden, cache_len, k_cache, v_cache, g_attn, w_query, w_key, w_value,
                   w_gate, w_up, w_out, w_down, g_final, embedding):
        rows = hidden.shape[0]
        half_dim = k_cache.shape[2] // 2
        inv_freq = ROPE_BASE ** (-(jnp.arange(half_dim, dtype=jnp.float32) * 2.0) / (2 * half_dim))
        freq = jnp.concatenate([inv_freq, inv_freq])[None, :]
        key_own, value_own, log_probs, log_norm = whole_step(
            hidden, freq, cache_len.reshape(rows // 128, 128), k_cache, v_cache, g_attn, w_query, w_key, w_value,
            w_gate, w_up, w_out, w_down, g_final, embedding)
        return key_own, value_own, log_probs.T, log_norm.reshape(rows)

    in_specs = (P("dp", "xax"), P("dp"), row_spec, row_spec, P("xax"), P("xax", "yax"),
                P("xax", None), P("xax", None), P("xax", "yax"), P("xax", "yax"),
                P("yax", "xax"), P("yax", "xax"), P("xax"), P("yax", "xax"))
    out_specs = (row_spec, row_spec, P("dp", ("yax", "xax")), P("dp"))
    return jax.shard_map(local_step, mesh=mesh, in_specs=in_specs, out_specs=out_specs, check_vma=False)
```

```python
import itertools

import jax
import jax.numpy as jnp
from jax import lax
from jax.experimental import pallas as pl
from jax.experimental.pallas import tpu as pltpu
from jax.sharding import PartitionSpec as P

EPS = 1e-6
ROPE_BASE = 10000.0
MESH_ID = pl.DeviceIdType.MESH
NY = NZ = NX = 4
CORES = 2
POOL, SENDS, TAGS = 24, 57, 84
HOPS = (1, 3, 2)
LINE = [(0, 1), (1, 0), (3, 0), (1, 1), (3, 1), (2, 0), (2, 1)]
NEAR = LINE[1:5]
NT = (((1,), (1,)), ((), ()))
PLANE = [(dz, dy) for dz in range(NZ) for dy in range(NY) if dz or dy]


class Group:
    def __init__(self, links, whole):
        self.links, self.whole = links, whole
        self.tag, self.sem = next(links.tags), next(links.slow)
        links.groups.append(self)

    def send(self, src, dst, where):
        pltpu.make_async_remote_copy(
            src_ref=src, dst_ref=dst, send_sem=self.links.send_sem.at[self.sem],
            recv_sem=self.links.recv_sem.at[self.tag], device_id=where, device_id_type=MESH_ID).start()

    def wait(self):
        pltpu.make_async_copy(self.whole, self.whole, self.links.recv_sem.at[self.tag]).wait()

    def wait_sent(self):
        pltpu.make_async_copy(self.whole, self.whole, self.links.send_sem.at[self.sem]).wait()


class Phases:
    def __init__(self):
        self.open = None

    def __call__(self, name):
        self.close()
        self.open = jax.named_scope(name)
        self.open.__enter__()

    def close(self):
        if self.open is not None:
            self.open.__exit__(None, None, None)
        self.open = None


class Links:
    def __init__(self, send_sem, recv_sem):
        self.send_sem, self.recv_sem = send_sem, recv_sem
        self.tags, self.slow, self.fast = itertools.count(), itertools.count(POOL), []
        self.pending, self.groups = [], []
        self.y_idx = lax.axis_index("yax")
        self.x_idx = lax.axis_index("xax")
        self.z, self.y = self.y_idx // NY, self.y_idx % NY
        self.chip, self.core = self.x_idx // CORES, self.x_idx % CORES

    def at_plane(self, dz, dy):
        return {"yax": (self.z + dz) % NZ * NY + (self.y + dy) % NY, "xax": self.x_idx}

    def slot_rows(self, dz, dy, rows):
        slot = (self.z + dz) % NZ * NY + (self.y + dy) % NY
        return pl.ds(pl.multiple_of(slot * rows, rows), rows)

    def line_id(self, dx, oc):
        core = 1 - self.core if oc else self.core
        return (self.chip + dx) % NX * CORES + core

    def at_line(self, dx, oc):
        return {"yax": self.y_idx, "xax": self.line_id(dx, oc)}

    def send(self, src, dst, where, tag=None, long=False):
        tag = next(self.tags) if tag is None else tag
        if long:
            sem = next(self.slow)
        else:
            sem = len(self.fast) % POOL
            if len(self.fast) >= POOL:
                self.fast[-POOL].wait_send()
        copy = pltpu.make_async_remote_copy(
            src_ref=src, dst_ref=dst, send_sem=self.send_sem.at[sem], recv_sem=self.recv_sem.at[tag],
            device_id=where, device_id_type=MESH_ID)
        copy.start()
        (self.pending if long else self.fast).append(copy)
        return copy

    def finish(self):
        for copy in self.pending + self.fast[-POOL:]:
            copy.wait_send()
        for group in self.groups:
            group.wait_sent()

    def barrier(self):
        barrier = pltpu.get_barrier_semaphore()
        peers = [self.at_line(*p) for p in LINE] + [self.at_plane(*p) for p in PLANE]
        for peer in peers:
            pl.semaphore_signal(barrier, inc=1, device_id=peer, device_id_type=MESH_ID)
        pl.semaphore_wait(barrier, len(peers))


def plane_gather(links, buf, tags, hook, crossing):
    cols = buf.shape[-1]
    rows = buf.shape[1] // (NY * NZ)
    span = cols // 2
    partner = links.at_line(0, 1)

    class Part:
        def __init__(self, index):
            self.index, self.lo, self.got = index, index * span, {}

        def order(self, du, dv):
            return (du, dv) if self.index else (dv, du)

        def block(self, at, half=0, piece=None):
            width = span if piece is None else span // 2
            lo = self.lo if not piece else self.lo + width
            return buf.at[half, links.slot_rows(*self.order(*at), rows), pl.ds(lo, width)]

        def push(self, name, at, to, piece=None):
            ref = self.block(at, piece=piece)
            self.got[name] = links.send(ref, ref, links.at_plane(*self.order(*to)), next(tags))

        def spread(self, k, at):
            self.push(("v+", k), at, (0, 1))
            self.push(("v-", k), at, (0, -1))

        def give(self, at):
            crossing.send(self.block(at), self.block(at, half=1), partner)

        def wait(self, name):
            self.got[name].wait_recv()

    parts = [Part(index) for index in range(2)]
    offset = (0, -1, 1, 2)
    for p in parts:
        p.push("u+", (0, 0), (1, 0))
        p.push("u-", (0, 0), (-1, 0))
        p.spread(0, (0, 0))
    for p in parts:
        p.give((0, 0))
    for k, name in enumerate(("u+", "u-"), 1):
        for p in parts:
            p.wait(name)
            at = (offset[k], 0)
            p.push(("far", k), at, (-offset[k], 0), piece=k - 1)
            p.spread(k, at)
            p.give(at)
    hook()

    def arrive(p, k):
        for name, step in (("v+", -1), ("v-", 1)):
            p.wait((name, k))
            at = (offset[k], step)
            if (name == "v+") == (k in (0, 3)):
                p.push(("relay", k), at, (0, -step))
            p.give(at)

    for p in parts:
        arrive(p, 0)
    for p in parts:
        p.wait(("far", 1))
        p.wait(("far", 2))
        p.spread(3, (2, 0))
        p.give((2, 0))
    for k in range(1, len(offset)):
        for p in parts:
            arrive(p, k)
    for k in range(len(offset)):
        for p in parts:
            p.wait(("relay", k))
            p.give((offset[k], 2))


def norm_gather(links, own_slot, gain_buf, which, xbuf, stat, out, base, hook):
    own_slot()
    rows, chunk = xbuf.shape[1:]
    tags = itertools.count(base)
    line = [links.send(xbuf.at[0], xbuf.at[NX - dx], links.at_line(dx, 0), next(tags)) for dx in HOPS]
    yield
    phase = Phases()
    for n, c in enumerate(line):
        phase(f"ng_line{which}_{n}")
        c.wait_recv()
    phase("ng_stats")
    held = xbuf[...].astype(jnp.float32)
    count = NX * chunk
    mean = jnp.sum(jnp.sum(held, axis=0), axis=-1, keepdims=True) / count
    dev = held - mean[None]
    square = jnp.sum(jnp.sum(dev * dev, axis=0), axis=-1, keepdims=True)
    lane = lax.broadcasted_iota(jnp.int32, (rows, 128), 1)
    stat[0] = jnp.where(lane == 0, mean, square)
    links.send(stat.at[0], stat.at[1], links.at_line(0, 1), next(tags)).wait_recv()
    other_mean, other_square = stat[1, :, 0:1], stat[1, :, 1:2]
    both = (mean + other_mean) * 0.5
    gap = mean - other_mean
    var = (square + other_square + gap * gap * (count * 0.5)) / (2 * count)
    scale = lax.rsqrt(var + EPS)
    for e in range(NX):
        out[0, links.slot_rows(0, 0, rows), e * chunk:(e + 1) * chunk] = (
            (xbuf[e].astype(jnp.float32) - both) * scale * gain_buf[e, which:which + 1, :]).astype(jnp.bfloat16)
    phase("ng_plane")
    crossing = Group(links, out.at[1])
    plane_gather(links, out, tags, hook, crossing)
    phase.close()
    yield crossing


def step_kernel(vocab_own, own_rows, hid_ref, gain_a, gain_f, freq_ref, len_ref, k_hbm, v_hbm,
                wq_hbm, wk_hbm, wv_hbm, wo_ref, wg_ref, wu_ref, wd_hbm, emb_ref,
                knew_ref, vnew_ref, out_ref, norm_ref,
                wq_ref, wk_ref, wv_ref, z_ref, k_buf, v_buf, wd_buf, wo_all, att, rc, n_buf, w_buf, wq_t, wq_buf, sel, sel_t, qx, qr, qy, qf,
                kvp, kvr, o_buf, o_got, o_all, act,
                part, ra1, rb1, ra2, rb2, acc_a, acc_b, xbuf, stat, xbuf2, stat2, gains, f_buf, emb_buf,
                w_relay, emb_relay, lse_x, lse_y, send_sem, recv_sem, local_sem):
    links = Links(send_sem, recv_sem)
    phase = Phases()
    f32, bf16 = jnp.float32, jnp.bfloat16
    z, y, xid, yid = links.z, links.y, links.x_idx, links.y_idx
    rows, chunk = hid_ref.shape[2], hid_ref.shape[3]
    half = chunk // 2
    nx2, nyz = 2 * NX, NY * NZ
    group = NY * rows
    head = 128
    pad = 8
    partner = links.at_line(0, 1)
    line_id = links.line_id
    gather_tags = len(HOPS) + 1 + len(PLANE) * CORES + CORES
    gather_base = [next(links.tags) for _ in range(gather_tags)][0]

    def dot(a, b):
        return jnp.dot(a, b, preferred_element_type=f32)

    def dot_t(a, b):
        return lax.dot_general(a, b, NT, preferred_element_type=f32)

    def rest(ref, n):
        return Group(links, ref.at[0:n - 1])

    local = []

    def fetch(src, dst):
        copy = pltpu.make_async_copy(src, dst, local_sem.at[len(local)])
        copy.start()
        local.append(copy)
        return copy

    ff = wg_ref.shape[1] // nx2

    def w_piece(ref, dx, oc):
        return ref.at[:, pl.ds(pl.multiple_of(line_id(dx, oc) * ff, ff), ff)]

    def w_slot(which, dx, oc):
        back = (NX - dx) % NX
        return w_buf.at[int(oc), pl.ds(back * chunk, chunk), pl.ds(which * ff, ff)]

    take = emb_buf.shape[1]

    def emb_start(xi):
        return pl.multiple_of(vocab_own * xi // 16 * 16 - xi // (nx2 - 1) * 16, 16)

    def emb_piece(dx, oc):
        return emb_ref.at[pl.ds(emb_start(line_id(dx, oc)), take), :]

    def emb_slot(dx, oc):
        return emb_buf.at[int(oc), :, pl.ds((NX - dx) % NX * chunk, chunk)]

    def emb_half(oc, way):
        part_rows = take // 2
        return emb_ref.at[pl.ds(emb_start(line_id(2, oc)) + way * part_rows, part_rows), :]

    def emb_far_slot(oc, way):
        return emb_buf.at[int(oc), pl.ds(way * (take // 2), take // 2), pl.ds(2 * chunk, chunk)]

    phase("start")
    got_wq = fetch(wq_hbm, wq_ref)
    own_w = [fetch(w_piece(wg_ref, 0, 0), w_slot(0, 0, 0)), fetch(w_piece(wu_ref, 0, 0), w_slot(1, 0, 0))]
    got_kv = [fetch(k_hbm, k_buf), fetch(v_hbm, v_buf)]
    got_wkv = [fetch(wk_hbm, wk_ref), fetch(wv_hbm, wv_ref)]
    got_wd = fetch(wd_hbm, wd_buf)
    own_emb = fetch(emb_piece(0, 0), emb_slot(0, 0))

    qc = wq_ref.shape[1]
    qs = qc // nx2
    per = head // qs
    wq_buf[...] = jnp.zeros(wq_buf.shape, bf16)

    phase("barrier")
    links.barrier()

    phase("front_send")
    gains[0, 0:1, :] = gain_a[...]
    gains[0, 1:2, :] = gain_f[...]
    gains[0, 2:, :] = jnp.zeros((6, chunk), f32)

    def own_input():
        xbuf[0] = hid_ref[z, y]

    w_far, emb_far = [], []
    w_got = [Group(links, w_buf.at[0, 0:(NX - 1) * chunk]), Group(links, w_buf.at[1])]
    emb_got = [Group(links, emb_buf.at[0, :, 0:(NX - 1) * chunk]), Group(links, emb_buf.at[1])]
    ways = [(way, hop, oc) for oc in (0, 1) for way, hop in enumerate(HOPS[:2])]

    def forward_weights():
        for (way, hop, oc), c in zip(ways, w_far):
            c.wait_recv()
            w_got[oc].send(w_relay.at[way, oc], w_buf.at[oc, pl.ds(2 * chunk, chunk), pl.ds(way * ff, ff)],
                           links.at_line(hop, oc))

    def emb_out(some):
        for way, hop, oc in some:
            emb_far.append(links.send(emb_half(oc, way), emb_relay.at[way, oc], links.at_line(hop, 0), long=True))

    def emb_on(some, arrived):
        for (way, hop, oc), c in zip(some, arrived):
            c.wait_recv()
            emb_got[oc].send(emb_relay.at[way, oc], emb_far_slot(oc, way), links.at_line(hop, oc))

    front = norm_gather(links, own_input, gains, 0, xbuf, stat, n_buf, gather_base, forward_weights)
    next(front)
    gain_got = rest(gains, NX)
    for dx in HOPS:
        gain_got.send(gains.at[0], gains.at[NX - dx], links.at_line(dx, 0))
    for way, hop, oc in ways:
        w_far.append(links.send(w_piece((wg_ref, wu_ref)[way], 2, oc), w_relay.at[way, oc], links.at_line(hop, 0),
                                long=True))

    got_wq.wait()
    eye_q = (lax.broadcasted_iota(jnp.int32, (qc, qc), 0) == lax.broadcasted_iota(jnp.int32, (qc, qc), 1))
    wq_t[...] = dot_t(eye_q.astype(bf16), wq_ref[...]).astype(bf16)
    wq_buf[0, 0:qs, 0:chunk] = wq_t[pl.ds(pl.multiple_of(xid * qs, qs), qs), :]

    def wq_rows(dx, oc):
        return wq_t.at[pl.ds(pl.multiple_of(line_id(dx, oc) * qs, qs), qs), :]

    def wq_slot(dx, oc):
        return wq_buf.at[oc, pl.ds(0, qs), pl.ds((NX - dx) % NX * chunk, chunk)]

    wq_got = Group(links, wq_t.at[0:qc - qs])
    for dx, oc in LINE:
        wq_got.send(wq_rows(dx, oc), wq_slot(dx, oc), links.at_line(dx, oc))
    for which, ref in enumerate((wg_ref, wu_ref)):
        for dx, oc in LINE[:1] + NEAR:
            w_got[oc].send(w_piece(ref, dx, oc), w_slot(which, dx, oc), links.at_line(dx, oc))

    phase("selections")
    total_rows = nyz * rows
    r_id = lax.broadcasted_iota(jnp.int32, (nx2 * nyz * pad, 1), 0)
    r_j = r_id % pad
    r_src = jnp.where(r_j < own_rows, r_id // pad % nyz * rows + r_id // (pad * nyz) * own_rows + r_j, -1)
    s_id = lax.broadcasted_iota(jnp.int32, (1, total_rows), 1)
    sel[...] = jnp.where(r_src == s_id, 1.0, 0.0).astype(bf16)
    t_id = lax.broadcasted_iota(jnp.int32, (group, 1), 0)
    t_in = t_id % rows
    t_src = t_in // own_rows * (NY * pad) + t_id // rows * pad + t_in % own_rows
    u_id = lax.broadcasted_iota(jnp.int32, (1, nx2 * NY * pad), 1)
    sel_t[...] = jnp.where(t_src == u_id, 1.0, 0.0).astype(bf16)
    k_id = lax.broadcasted_iota(jnp.int32, (nx2 * pad, rows), 0)
    k_src = jnp.where(k_id % pad < own_rows, k_id // pad * own_rows + k_id % pad, -1)
    sel_kv = jnp.where(k_src == lax.broadcasted_iota(jnp.int32, (nx2 * pad, rows), 1), 1.0, 0.0).astype(bf16)

    phase.close()
    gain_got.wait()
    lane = lax.broadcasted_iota(jnp.int32, (1, head), 1)
    lengths = []
    for b in range(own_rows):
        index = (yid * nx2 + xid) * own_rows + b
        row = len_ref[pl.ds(index // head, 1), :].astype(f32)
        lengths.append(jnp.sum(jnp.where(lane == index % head, row, 0.0), axis=-1, keepdims=True))
    lengths = jnp.concatenate(lengths + lengths[:pad - own_rows], axis=0)
    angles = lengths * freq_ref[...]
    cos_all = jnp.cos(angles)
    sin_all = jnp.sin(angles) * jnp.where(lane < head // 2, -1.0, 1.0)

    crossing = next(front)
    phase("ng_cross")
    crossing.wait()
    phase("kv_part")

    for c in got_wkv:
        c.wait()
    n_own = dot(sel_kv, n_buf[0, links.slot_rows(0, 0, rows), 0:chunk]).astype(bf16)
    kvp[:, :, :head] = dot(n_own, wk_ref[...]).reshape(nx2, pad, head)
    kvp[:, :, head:] = dot(n_own, wv_ref[...]).reshape(nx2, pad, head)
    kv_got = rest(kvr, nx2)
    for p in LINE:
        kv_got.send(kvp.at[line_id(*p)], kvr.at[xid], links.at_line(*p))
    kvr[xid] = kvp[xid]

    phase("wait_wq")
    wq_got.wait()
    phase("q_mm")
    q_all = jnp.concatenate([
        (dot_t(n_buf[0, i * group:(i + 1) * group, :], wq_buf[0])
         + dot_t(n_buf[1, i * group:(i + 1) * group, :], wq_buf[1])).astype(bf16) for i in range(NZ)], axis=0)
    span = nyz * pad
    for i in range(nx2):
        chosen = dot(sel[i * span:(i + 1) * span, :], q_all)
        quarter = span // per
        packed = chosen[:quarter, :]
        for g in range(1, per):
            packed = packed + pltpu.roll(chosen[g * quarter:(g + 1) * quarter, :], g * qs, 1)
        qx[i] = packed.astype(bf16)
    q_got = rest(qr, nx2)
    for p in LINE:
        q_got.send(qx.at[line_id(*p)], qr.at[xid], links.at_line(*p))
    qr[xid] = qx[xid]

    phase("wait_w")
    for c in own_w:
        c.wait()
    for c in w_got:
        c.wait()
    phase("gate_up")

    def act_at(k, dx):
        return act.at[(z + k) % NZ, :, pl.ds(pl.multiple_of(line_id(dx, 0) * ff, ff), ff)]

    def act_out(k, dx, to_dx):
        return links.send(act_at(k, dx), act_at(k, dx), links.at_line(to_dx, 0))

    def act_give(k, dx):
        cross[k].send(act_at(k, dx), act_at(k, dx), partner)

    turns = (2, 1, 3, 0)
    early, late = turns[:2], turns[2:]
    near_act, far_act = {}, {}
    cross = {k: Group(links, act.at[0, :, 0:NX * ff]) for k in turns}
    for k in turns:
        these = pl.ds(pl.multiple_of((z + k) % NZ * group, group), group)
        both = (dot(n_buf[0, these, :], w_buf[0]) + dot(n_buf[1, these, :], w_buf[1])).astype(bf16).astype(f32)
        gate, up = both[:, :ff], both[:, ff:]
        act_at(k, 0)[...] = (gate * jax.nn.sigmoid(gate) * up).astype(bf16)
        near_act[k] = [(dx, act_out(k, 0, dx)) for dx in HOPS[:2]]
        act_give(k, 0)

    def act_pass(k):
        for dx, c in near_act[k]:
            c.wait_recv()
            if (k in early) == (dx == 1):
                far_act[k] = act_out(k, NX - dx, dx)
            act_give(k, NX - dx)

    low, high = pl.ds(0, half), pl.ds(half, half)
    first_a, first_b = Group(links, ra1), Group(links, rb1)

    def act_use(k):
        cross[k].wait()
        g = (z + k) % NZ
        part[g] = dot(act[g], wd_buf[...]).reshape(NY, rows, chunk)
        if k:
            first_b.send(part.at[g, :, :, high], rb1.at[k - 1], links.at_plane(k, 0))

    def along_y(k):
        g = (z + k) % NZ
        for d in early + late[:1]:
            first_a.send(part.at[g, (y + d) % NY, :, low], ra1.at[d - 1, g], links.at_plane(0, d))

    def act_far(ks):
        for k in ks:
            far_act[k].wait_recv()
            act_give(k, 2)

    phase("wait_q")
    q_got.wait()
    phase("q_sum")
    lane_group = lax.broadcasted_iota(jnp.int32, (1, head), 1) // qs
    for j in range(qc // head):
        came = [qr[j * per + i].astype(f32) for i in range(per)]
        for g in range(per):
            piece = jnp.zeros((span // per, head), f32)
            for i in range(per):
                piece = piece + jnp.where(lane_group == i, pltpu.roll(came[i], (i - g) % per * qs, 1), 0.0)
            qy[g * per:(g + 1) * per, :, j * head:(j + 1) * head] = piece.reshape(per, pad, head)

    def plane_id(dz, dy):
        return (z + dz) % NZ * NY + (y + dy) % NY

    y_got = rest(qf, nyz)
    for p in PLANE:
        y_got.send(qy.at[plane_id(*p)], qf.at[yid], links.at_plane(*p))
    qf[yid] = qy[yid]

    def wo_rows(dz):
        return wo_all.at[pl.ds(pl.multiple_of((z + dz) % NZ * qc, qc), qc), :]

    wo_got = Group(links, wo_all.at[0:(NZ - 1) * qc])
    for d in HOPS:
        wo_got.send(wo_ref, wo_rows(0), links.at_plane(d, 0))
    own_wo = fetch(wo_ref, wo_rows(0))

    phase("act_pass")
    for k in early:
        act_pass(k)
    phase("wait_kv")
    kv_got.wait()
    kv_sum = kvr[0]
    for i in range(1, nx2):
        kv_sum = kv_sum + kvr[i]
    kv_new = kv_sum.astype(bf16).astype(f32)

    def turn(v, b=None):
        cos, sin = (cos_all, sin_all) if b is None else (cos_all[b:b + 1, :], sin_all[b:b + 1, :])
        return (v * cos + pltpu.roll(v, head // 2, 1) * sin).astype(bf16)

    k_new = turn(kv_new[:, :head])
    knew_ref[...] = k_new[:own_rows, :]
    vnew_ref[...] = kv_new[:own_rows, head:].astype(bf16)
    k_row, v_row = k_new.astype(f32), kv_new[:, head:]
    phase("wait_qy")
    for c in got_kv:
        c.wait()
    y_got.wait()
    phase("attention")
    seq = k_buf.shape[1]
    score_scale = head ** -0.5
    position = lax.broadcasted_iota(jnp.int32, (1, seq), 1).astype(f32)
    o_buf[...] = jnp.zeros(o_buf.shape, f32)
    for b in range(own_rows):
        q_b = jnp.concatenate([turn(qf[:, b, j * head:(j + 1) * head], b) for j in range(qc // head)], axis=0)
        scores = dot_t(q_b, k_buf[b]) * score_scale
        score_new = jnp.sum(q_b.astype(f32) * k_row[b:b + 1, :], axis=-1, keepdims=True) * score_scale
        valid = position < lengths[b:b + 1, :]
        top = jnp.maximum(jnp.max(jnp.where(valid, scores, -jnp.inf), axis=-1, keepdims=True), score_new)
        weights = jnp.where(valid, jnp.exp(scores - top), 0.0)
        weight_new = jnp.exp(score_new - top)
        denom = jnp.sum(weights, axis=-1, keepdims=True) + weight_new
        o_b = dot((weights / denom).astype(bf16), v_buf[b])
        o_b = o_b + (weight_new / denom).astype(bf16).astype(f32) * v_row[b:b + 1, :]
        o_b = o_b.astype(bf16).astype(f32)
        for j in range(qc // head):
            o_buf[:, :, b, j * head:(j + 1) * head] = o_b[j * nyz:(j + 1) * nyz, :].reshape(NZ, NY, head)
    o_back = rest(o_got, NY)
    for d in HOPS:
        o_back.send(o_buf.at[:, (y + d) % NY], o_got.at[y], links.at_plane(0, d))
    phase("act_early")
    for k in late:
        act_pass(k)
    act_far(early)
    emb_out(ways[:2])
    got_wd.wait()
    for k in early:
        act_use(k)
        along_y(k)
    o_got[y] = o_buf[:, y]

    phase("act_late")
    act_far(late)
    for k in late:
        act_use(k)
        along_y(k)

    phase("wait_oy")
    o_back.wait()
    for i in range(NZ):
        o_all[xid, :, i * qc:(i + 1) * qc] = o_got[:, i].reshape(NY * pad, qc).astype(bf16)
    o_here = o_all.at[xid]
    o_line = [links.send(o_here, o_here, links.at_line(dx, 0)) for dx in HOPS]
    o_cross = rest(o_all, NX + 1)
    o_cross.send(o_here, o_here, partner)
    emb_out(ways[2:])
    emb_got[1].send(emb_piece(0, 1), emb_slot(0, 1), partner)
    phase("wait_o")
    for dx, c in zip(HOPS, o_line):
        c.wait_recv()
        came = o_all.at[line_id(NX - dx, 0)]
        o_cross.send(came, came, partner)
    wo_got.wait()
    own_wo.wait()
    o_cross.wait()
    phase("out_mm")
    o_nat = dot(sel_t[...], o_all[...].reshape(nx2 * NY * pad, NZ * qc)).astype(bf16)
    att[...] = dot(o_nat, wo_all[...]).reshape(NY, rows, chunk)
    att_got = Group(links, rc)
    for d in HOPS:
        att_got.send(att.at[(y + d) % NY], rc.at[d - 1], links.at_plane(0, d))
    emb_on(ways[:2], emb_far[:2])

    phase("wait_rs1")
    first_b.wait()
    acc_b[...] = (part[z, :, :, half:] + rb1[0]) + (rb1[1] + rb1[2])
    second = [Group(links, rb2), Group(links, ra2)]
    for d in HOPS:
        second[0].send(acc_b.at[(y + d) % NY], rb2.at[d - 1], links.at_plane(0, d))
    phase("wait_rs1a")
    first_a.wait()
    acc_a[...] = (part[:, y, :, :half] + ra1[0]) + (ra1[1] + ra1[2])
    for d in HOPS:
        second[1].send(acc_a.at[(z + d) % NZ], ra2.at[d - 1], links.at_plane(d, 0))
    phase("wait_att")
    att_got.wait()
    phase("wait_rs2")
    for c in second:
        c.wait()
    phase("rs_sum2")
    def own_residual():
        res = hid_ref[z, y].astype(f32) + ((att[y] + rc[0]) + (rc[1] + rc[2]))
        xbuf2[0, :, :half] = res[:, :half] + ((acc_a[z] + ra2[0]) + (ra2[1] + ra2[2]))
        xbuf2[0, :, half:] = res[:, half:] + ((acc_b[y] + rb2[0]) + (rb2[1] + rb2[2]))

    back = norm_gather(links, own_residual, gains, 1, xbuf2, stat2, f_buf, gather_base, lambda: None)
    next(back)
    emb_on(ways[2:], emb_far[2:])
    for dx, oc in NEAR:
        emb_got[oc].send(emb_piece(dx, oc), emb_slot(dx, oc), links.at_line(dx, oc))
    phase.close()
    crossing = next(back)
    phase("wait_emb")
    own_emb.wait()
    for c in emb_got:
        c.wait()

    phase("logits")
    wide_n = 256
    for h in range(CORES):
        if h:
            crossing.wait()
        for i in range(total_rows // wide_n):
            cols = slice(i * wide_n, (i + 1) * wide_n)
            term = dot_t(emb_buf[h], f_buf[h, cols, :])
            z_ref[:, cols] = z_ref[:, cols] + term if h else term

    phase("lse_own")
    shift = vocab_own * xid - emb_start(xid)
    vid = lax.broadcasted_iota(jnp.int32, (take, 1), 0)
    own = (vid >= shift) & (vid < shift + vocab_own)
    blocks = total_rows // 128
    for b in range(blocks):
        zb = jnp.where(own, z_ref[:, b * 128:(b + 1) * 128], -jnp.inf)
        top = jnp.max(zb, axis=0, keepdims=True)
        lse_x[xid, b:b + 1, :] = top
        lse_x[xid, 8 + b:9 + b, :] = jnp.sum(jnp.exp(zb - top), axis=0, keepdims=True)
    for b in range(blocks, 8):
        lse_x[xid, b:b + 1, :] = jnp.zeros((1, 128), f32)
        lse_x[xid, 8 + b:9 + b, :] = jnp.ones((1, 128), f32)

    def merge(ref):
        tops = ref[:, :8, :]
        top = jnp.max(tops, axis=0)
        return top, jnp.sum(ref[:, 8:, :] * jnp.exp(tops - top[None]), axis=0)

    phase("lse_line")
    got = rest(lse_x, nx2)
    for p in LINE:
        got.send(lse_x.at[xid], lse_x.at[xid], links.at_line(*p))
    got.wait()
    top, mass = merge(lse_x)
    lse_y[yid, :8, :] = top
    lse_y[yid, 8:, :] = mass
    phase("lse_plane")
    got = rest(lse_y, nyz)
    for p in PLANE:
        got.send(lse_y.at[yid], lse_y.at[yid], links.at_plane(*p))
    got.wait()
    top, mass = merge(lse_y)
    norm = top + jnp.log(mass)
    norm_ref[...] = norm[:blocks, :]
    phase("subtract")
    for b in range(blocks):
        cols = slice(b * head, (b + 1) * head)
        out_ref[:, cols] = pltpu.roll(z_ref[:, cols], (take - shift) % take, 0)[:vocab_own, :] - norm[b:b + 1, :]
    phase("finish")
    links.finish()
    phase.close()


def whole_step(hidden, freq, lens, k_cache, v_cache, g_attn, w_query, w_key, w_value,
               w_gate, w_up, w_out, w_down, g_final, embedding):
    total_rows, chunk = hidden.shape
    own_rows, seq, head = k_cache.shape
    rows = total_rows // (NY * NZ)
    vocab_own = embedding.shape[0] // (2 * NX)
    take = (vocab_own + 30) // 16 * 16
    half = chunk // 2
    qc = w_query.shape[1]
    ff = w_gate.shape[1] // (2 * NX)
    f32, bf16 = jnp.float32, jnp.bfloat16
    nyz, nx2, pad = NY * NZ, 2 * NX, 8
    vmem = pl.BlockSpec(memory_space=pltpu.VMEM)
    hbm = pl.BlockSpec(memory_space=pltpu.HBM)
    V = pltpu.VMEM
    return pl.pallas_call(
        lambda *refs: step_kernel(vocab_own, own_rows, *refs),
        out_shape=(jax.ShapeDtypeStruct((own_rows, head), bf16), jax.ShapeDtypeStruct((own_rows, head), bf16),
                   jax.ShapeDtypeStruct((vocab_own, total_rows), f32), jax.ShapeDtypeStruct((total_rows // head, head), f32)),
        in_specs=[vmem] * 5 + [hbm] * 10,
        out_specs=(vmem,) * 4,
        scratch_shapes=[
            V((chunk, qc), bf16), V((chunk, head), bf16), V((chunk, head), bf16), V((take, total_rows), f32),
            V((own_rows, seq, head), bf16), V((own_rows, seq, head), bf16),
            V((nx2 * ff, chunk), bf16), V((NZ * qc, chunk), bf16), V((NY, rows, chunk), f32), V((3, rows, chunk), f32), V((2, total_rows, NX * chunk), bf16), V((2, NX * chunk, 2 * ff), bf16),
            V((qc, chunk), bf16), V((2, head, NX * chunk), bf16),
            V((nx2 * nyz * pad, total_rows), bf16), V((NY * rows, nx2 * NY * pad), bf16),
            V((nx2, nyz * pad // 4, head), bf16), V((nx2, nyz * pad // 4, head), bf16),
            V((nyz, pad, qc), f32), V((nyz, pad, qc), f32),
            V((nx2, pad, 2 * head), f32), V((nx2, pad, 2 * head), f32),
            V((NZ, NY, pad, qc), f32), V((NY, NZ, pad, qc), f32), V((nx2, NY * pad, NZ * qc), bf16),
            V((NZ, NY * rows, nx2 * ff), bf16),
            V((NZ, NY, rows, chunk), f32),
            V((3, NZ, rows, half), f32), V((3, NY, rows, half), f32), V((3, rows, half), f32), V((3, rows, half), f32),
            V((NZ, rows, half), f32), V((NY, rows, half), f32),
            V((NX, rows, chunk), bf16), V((2, rows, 128), f32), V((NX, rows, chunk), f32), V((2, rows, 128), f32),
            V((NX, 8, chunk), f32),
            V((2, total_rows, NX * chunk), bf16), V((2, take, NX * chunk), bf16),
            V((2, 2, chunk, ff), bf16), V((2, 2, take // 2, chunk), bf16),
            V((nx2, 16, 128), f32), V((nyz, 16, 128), f32),
            pltpu.SemaphoreType.DMA((SENDS,)), pltpu.SemaphoreType.DMA((TAGS,)), pltpu.SemaphoreType.DMA((10,)),
        ],
        compiler_params=pltpu.CompilerParams(
            collective_id=1, has_side_effects=True, vmem_limit_bytes=54800 << 10),
        name="decode_step",
    )(hidden.reshape(NZ, NY, rows, chunk), g_attn[None, :], g_final[None, :], freq, lens, k_cache, v_cache,
      w_query, w_key, w_value, w_out, w_gate, w_up, w_down, embedding)


def solution(mesh):
    row_spec = P(("dp", "yax", "xax"))

    def local_step(hidden, cache_len, k_cache, v_cache, g_attn, w_query, w_key, w_value,
                   w_gate, w_up, w_out, w_down, g_final, embedding):
        rows = hidden.shape[0]
        half_dim = k_cache.shape[2] // 2
        inv_freq = ROPE_BASE ** (-(jnp.arange(half_dim, dtype=jnp.float32) * 2.0) / (2 * half_dim))
        freq = jnp.concatenate([inv_freq, inv_freq])[None, :]
        key_own, value_own, log_probs, log_norm = whole_step(
            hidden, freq, cache_len.reshape(rows // 128, 128), k_cache, v_cache, g_attn, w_query, w_key, w_value,
            w_gate, w_up, w_out, w_down, g_final, embedding)
        return key_own, value_own, log_probs.T, log_norm.reshape(rows)

    in_specs = (P("dp", "xax"), P("dp"), row_spec, row_spec, P("xax"), P("xax", "yax"),
                P("xax", None), P("xax", None), P("xax", "yax"), P("xax", "yax"),
                P("yax", "xax"), P("yax", "xax"), P("xax"), P("yax", "xax"))
    out_specs = (row_spec, row_spec, P("dp", ("yax", "xax")), P("dp"))
    return jax.shard_map(local_step, mesh=mesh, in_specs=in_specs, out_specs=out_specs, check_vma=False)
```

```python
import itertools

import jax
import jax.numpy as jnp
from jax import lax
from jax.experimental import pallas as pl
from jax.experimental.pallas import tpu as pltpu
from jax.sharding import PartitionSpec as P

EPS = 1e-6
ROPE_BASE = 10000.0
MESH_ID = pl.DeviceIdType.MESH
NY = NZ = NX = 4
CORES = 2
POOL, SENDS, TAGS = 24, 58, 85
HOPS = (1, 3, 2)
LINE = [(0, 1), (1, 0), (3, 0), (1, 1), (3, 1), (2, 0), (2, 1)]
NEAR = LINE[1:5]
NT = (((1,), (1,)), ((), ()))
PLANE = [(dz, dy) for dz in range(NZ) for dy in range(NY) if dz or dy]


class Group:
    def __init__(self, links, whole):
        self.links, self.whole = links, whole
        self.tag, self.sem = next(links.tags), next(links.slow)
        links.groups.append(self)

    def send(self, src, dst, where):
        pltpu.make_async_remote_copy(
            src_ref=src, dst_ref=dst, send_sem=self.links.send_sem.at[self.sem],
            recv_sem=self.links.recv_sem.at[self.tag], device_id=where, device_id_type=MESH_ID).start()

    def wait(self):
        pltpu.make_async_copy(self.whole, self.whole, self.links.recv_sem.at[self.tag]).wait()

    def wait_sent(self):
        pltpu.make_async_copy(self.whole, self.whole, self.links.send_sem.at[self.sem]).wait()


class Phases:
    def __init__(self):
        self.open = None

    def __call__(self, name):
        self.close()
        self.open = jax.named_scope(name)
        self.open.__enter__()

    def close(self):
        if self.open is not None:
            self.open.__exit__(None, None, None)
        self.open = None


class Links:
    def __init__(self, send_sem, recv_sem):
        self.send_sem, self.recv_sem = send_sem, recv_sem
        self.tags, self.slow, self.fast = itertools.count(), itertools.count(POOL), []
        self.pending, self.groups = [], []
        self.y_idx = lax.axis_index("yax")
        self.x_idx = lax.axis_index("xax")
        self.z, self.y = self.y_idx // NY, self.y_idx % NY
        self.chip, self.core = self.x_idx // CORES, self.x_idx % CORES

    def at_plane(self, dz, dy):
        return {"yax": (self.z + dz) % NZ * NY + (self.y + dy) % NY, "xax": self.x_idx}

    def slot_rows(self, dz, dy, rows):
        slot = (self.z + dz) % NZ * NY + (self.y + dy) % NY
        return pl.ds(pl.multiple_of(slot * rows, rows), rows)

    def line_id(self, dx, oc):
        core = 1 - self.core if oc else self.core
        return (self.chip + dx) % NX * CORES + core

    def at_line(self, dx, oc):
        return {"yax": self.y_idx, "xax": self.line_id(dx, oc)}

    def send(self, src, dst, where, tag=None, long=False):
        tag = next(self.tags) if tag is None else tag
        if long:
            sem = next(self.slow)
        else:
            sem = len(self.fast) % POOL
            if len(self.fast) >= POOL:
                self.fast[-POOL].wait_send()
        copy = pltpu.make_async_remote_copy(
            src_ref=src, dst_ref=dst, send_sem=self.send_sem.at[sem], recv_sem=self.recv_sem.at[tag],
            device_id=where, device_id_type=MESH_ID)
        copy.start()
        (self.pending if long else self.fast).append(copy)
        return copy

    def finish(self):
        for copy in self.pending + self.fast[-POOL:]:
            copy.wait_send()
        for group in self.groups:
            group.wait_sent()

    def barrier(self):
        barrier = pltpu.get_barrier_semaphore()
        peers = [self.at_line(*p) for p in LINE] + [self.at_plane(*p) for p in PLANE]
        for peer in peers:
            pl.semaphore_signal(barrier, inc=1, device_id=peer, device_id_type=MESH_ID)
        pl.semaphore_wait(barrier, len(peers))


def plane_gather(links, buf, tags, hook, crossing, start):
    cols = buf.shape[-1]
    rows = buf.shape[1] // (NY * NZ)
    span = (cols - start) // 2
    partner = links.at_line(0, 1)

    class Part:
        def __init__(self, index):
            self.index, self.lo, self.got = index, start + index * span, {}

        def order(self, du, dv):
            return (du, dv) if self.index else (dv, du)

        def block(self, at, half=0, piece=None):
            width = span if piece is None else span // 2
            lo = self.lo if not piece else self.lo + width
            return buf.at[half, links.slot_rows(*self.order(*at), rows), pl.ds(lo, width)]

        def push(self, name, at, to, piece=None):
            ref = self.block(at, piece=piece)
            self.got[name] = links.send(ref, ref, links.at_plane(*self.order(*to)), next(tags))

        def spread(self, k, at):
            self.push(("v+", k), at, (0, 1))
            self.push(("v-", k), at, (0, -1))

        def give(self, at):
            crossing.send(self.block(at), self.block(at, half=1), partner)

        def wait(self, name):
            self.got[name].wait_recv()

    parts = [Part(index) for index in range(2)]
    offset = (0, -1, 1, 2)
    for p in parts:
        p.push("u+", (0, 0), (1, 0))
        p.push("u-", (0, 0), (-1, 0))
        p.spread(0, (0, 0))
    for p in parts:
        p.give((0, 0))
    for k, name in enumerate(("u+", "u-"), 1):
        for p in parts:
            p.wait(name)
            at = (offset[k], 0)
            p.push(("far", k), at, (-offset[k], 0), piece=k - 1)
            p.spread(k, at)
            p.give(at)
    hook()

    def arrive(p, k):
        for name, step in (("v+", -1), ("v-", 1)):
            p.wait((name, k))
            at = (offset[k], step)
            if (name == "v+") == (k in (0, 3)):
                p.push(("relay", k), at, (0, -step))
            p.give(at)

    for p in parts:
        arrive(p, 0)
    for p in parts:
        p.wait(("far", 1))
        p.wait(("far", 2))
        p.spread(3, (2, 0))
        p.give((2, 0))
    for k in range(1, len(offset)):
        for p in parts:
            arrive(p, k)
    for k in range(len(offset)):
        for p in parts:
            p.wait(("relay", k))
            p.give((offset[k], 2))


def norm_gather(links, own_slot, gain_buf, which, xbuf, stat, out, base, hook, skip=0):
    own_slot()
    rows, chunk = xbuf.shape[1:]
    tags = itertools.count(base)
    line = [links.send(xbuf.at[0], xbuf.at[NX - dx], links.at_line(dx, 0), next(tags)) for dx in HOPS]
    yield
    phase = Phases()
    for n, c in enumerate(line):
        phase(f"ng_line{which}_{n}")
        c.wait_recv()
    phase("ng_stats")
    held = xbuf[...].astype(jnp.float32)
    count = NX * chunk
    mean = jnp.sum(jnp.sum(held, axis=0), axis=-1, keepdims=True) / count
    dev = held - mean[None]
    square = jnp.sum(jnp.sum(dev * dev, axis=0), axis=-1, keepdims=True)
    lane = lax.broadcasted_iota(jnp.int32, (rows, 128), 1)
    stat[0] = jnp.where(lane == 0, mean, square)
    links.send(stat.at[0], stat.at[1], links.at_line(0, 1), next(tags)).wait_recv()
    other_mean, other_square = stat[1, :, 0:1], stat[1, :, 1:2]
    both = (mean + other_mean) * 0.5
    gap = mean - other_mean
    var = (square + other_square + gap * gap * (count * 0.5)) / (2 * count)
    scale = lax.rsqrt(var + EPS)
    for e in range(skip, NX):
        out[0, links.slot_rows(0, 0, rows), e * chunk:(e + 1) * chunk] = (
            (xbuf[e].astype(jnp.float32) - both) * scale * gain_buf[e, which:which + 1, :]).astype(jnp.bfloat16)
    phase("ng_plane")
    crossing = Group(links, out.at[1])
    plane_gather(links, out, tags, lambda: hook(crossing), crossing, skip * chunk)
    phase.close()
    yield crossing


def step_kernel(vocab_own, own_rows, hid_ref, gain_a, gain_f, freq_ref, len_ref, k_hbm, v_hbm,
                wq_hbm, wk_hbm, wv_hbm, wo_ref, wg_ref, wu_ref, wd_hbm, emb_ref,
                knew_ref, vnew_ref, out_ref, norm_ref,
                wq_ref, wk_ref, wv_ref, z_ref, k_buf, v_buf, wd_buf, wo_all, att, rc, n_buf, w_buf, wq_t, wq_buf, sel, sel_t, qx, qr, qy, qf,
                kvp, kvr, o_buf, o_got, o_all, act,
                part, ra1, rb1, ra2, rb2, acc_a, acc_b, xbuf, stat, xbuf2, stat2, gains, f_buf, emb_buf,
                w_relay, emb_relay, row_stats, lse_x, lse_y, send_sem, recv_sem, local_sem):
    links = Links(send_sem, recv_sem)
    phase = Phases()
    f32, bf16 = jnp.float32, jnp.bfloat16
    z, y, xid, yid = links.z, links.y, links.x_idx, links.y_idx
    total_rows, chunk = hid_ref.shape
    rows = total_rows // (NY * NZ)
    here_rows = links.slot_rows(0, 0, rows)
    half = chunk // 2
    nx2, nyz = 2 * NX, NY * NZ
    group = NY * rows
    head = 128
    pad = 8
    partner = links.at_line(0, 1)
    line_id = links.line_id
    gather_tags = len(HOPS) + 1 + len(PLANE) * CORES + CORES
    gather_base = [next(links.tags) for _ in range(gather_tags)][0]

    def dot(a, b):
        return jnp.dot(a, b, preferred_element_type=f32)

    def dot_t(a, b):
        return lax.dot_general(a, b, NT, preferred_element_type=f32)

    def rest(ref, n):
        return Group(links, ref.at[0:n - 1])

    local = []

    def fetch(src, dst):
        copy = pltpu.make_async_copy(src, dst, local_sem.at[len(local)])
        copy.start()
        local.append(copy)
        return copy

    ff = wg_ref.shape[1] // nx2

    def w_piece(ref, dx, oc):
        return ref.at[:, pl.ds(pl.multiple_of(line_id(dx, oc) * ff, ff), ff)]

    def w_slot(which, dx, oc):
        back = (NX - dx) % NX
        return w_buf.at[int(oc), pl.ds(back * chunk, chunk), pl.ds(which * ff, ff)]

    take = emb_buf.shape[1]

    def emb_start(xi):
        return pl.multiple_of(vocab_own * xi // pad * pad, pad)

    def emb_piece(dx, oc):
        return emb_ref.at[pl.ds(emb_start(line_id(dx, oc)), take), :]

    def emb_slot(dx, oc):
        return emb_buf.at[int(oc), :, pl.ds((NX - dx) % NX * chunk, chunk)]

    near_part = (take // 2 + 15) // 16 * 16
    far_parts = ((0, near_part), (near_part, take - near_part))

    def emb_half(oc, way):
        first, size = far_parts[way]
        return emb_ref.at[pl.ds(pl.multiple_of(emb_start(line_id(2, oc)) + first, pad), size), :]

    def emb_mid(oc, way):
        return emb_relay.at[way, oc, pl.ds(0, far_parts[way][1])]

    def emb_far_slot(oc, way):
        return emb_buf.at[int(oc), pl.ds(*far_parts[way]), pl.ds(2 * chunk, chunk)]

    got_wq = fetch(wq_hbm, wq_ref)
    own_w = [fetch(w_piece(wg_ref, 0, 0), w_slot(0, 0, 0)), fetch(w_piece(wu_ref, 0, 0), w_slot(1, 0, 0))]
    got_kv = [fetch(k_hbm, k_buf), fetch(v_hbm, v_buf)]
    got_wkv = [fetch(wk_hbm, wk_ref), fetch(wv_hbm, wv_ref)]
    got_wd = fetch(wd_hbm, wd_buf)
    own_emb = fetch(emb_piece(0, 0), emb_slot(0, 0))

    qc = wq_ref.shape[1]
    qs = qc // nx2
    per = head // qs
    wq_buf[...] = jnp.zeros(wq_buf.shape, bf16)

    phase("row_stats")
    eye = lax.broadcasted_iota(jnp.int32, (head, head), 0) == lax.broadcasted_iota(jnp.int32, (head, head), 1)
    blocks = total_rows // head

    def block_rows(b):
        return slice(b * head, (b + 1) * head)

    def to_row(v):
        return jnp.sum(jnp.where(eye, v, 0.0), axis=0, keepdims=True)

    def to_col(v):
        return jnp.sum(jnp.where(eye, v, 0.0), axis=1, keepdims=True)

    row_stats[xid] = jnp.zeros((2 * pad, head), f32)
    for b in range(blocks):
        held = hid_ref[block_rows(b), :].astype(f32)
        mean = jnp.sum(held, axis=-1, keepdims=True) / chunk
        dev = held - mean
        row_stats[xid, b:b + 1, :] = to_row(mean)
        row_stats[xid, pad + b:pad + b + 1, :] = to_row(jnp.sum(dev * dev, axis=-1, keepdims=True))

    phase("barrier")
    links.barrier()

    phase("front_send")
    gains[0, 0:1, :] = gain_a[...]
    gains[0, 1:2, :] = gain_f[...]
    gains[0, 2:, :] = jnp.zeros((6, chunk), f32)

    def own_input():
        xbuf[0] = hid_ref[here_rows, :]

    w_far, emb_far = [], []
    w_got = [Group(links, w_buf.at[0, 0:(NX - 1) * chunk]), Group(links, w_buf.at[1])]
    emb_got = [Group(links, emb_buf.at[0, :, 0:(NX - 1) * chunk]), Group(links, emb_buf.at[1])]
    ways = [(way, hop, oc) for oc in (0, 1) for way, hop in enumerate(HOPS[:2])]

    def forward_weights():
        for (way, hop, oc), c in zip(ways, w_far):
            c.wait_recv()
            w_got[oc].send(w_relay.at[way, oc], w_buf.at[oc, pl.ds(2 * chunk, chunk), pl.ds(way * ff, ff)],
                           links.at_line(hop, oc))

    def emb_out(some):
        for way, hop, oc in some:
            emb_far.append(links.send(emb_half(oc, way), emb_mid(oc, way), links.at_line(hop, 0), long=True))

    def emb_on(some, arrived):
        for (way, hop, oc), c in zip(some, arrived):
            c.wait_recv()
            emb_got[oc].send(emb_mid(oc, way), emb_far_slot(oc, way), links.at_line(hop, oc))

    def amid(crossing):
        forward_weights()
        stats_got.wait()
        means = row_stats[:, :pad, :]
        mean = jnp.sum(means, axis=0) / nx2
        gap = means - mean[None]
        square = jnp.sum(row_stats[:, pad:, :], axis=0) + jnp.sum(gap * gap, axis=0) * chunk
        scale = lax.rsqrt(square / (nx2 * chunk) + EPS)
        for b in range(blocks):
            n_buf[0, block_rows(b), 0:chunk] = (
                (hid_ref[block_rows(b), :].astype(f32) - to_col(mean[b:b + 1, :])) * to_col(scale[b:b + 1, :])
                * gains[0, 0:1, :]).astype(bf16)
        own = n_buf.at[0, :, 0:chunk]
        crossing.send(own, n_buf.at[1, :, 0:chunk], partner)
        emb_out(ways[:2])

    front = norm_gather(links, own_input, gains, 0, xbuf, stat, n_buf, gather_base, amid, skip=1)
    next(front)
    gain_got = rest(gains, NX)
    for dx in HOPS:
        gain_got.send(gains.at[0], gains.at[NX - dx], links.at_line(dx, 0))
    stats_got = rest(row_stats, nx2)
    for p in LINE:
        stats_got.send(row_stats.at[xid], row_stats.at[xid], links.at_line(*p))
    for way, hop, oc in ways:
        w_far.append(links.send(w_piece((wg_ref, wu_ref)[way], 2, oc), w_relay.at[way, oc], links.at_line(hop, 0),
                                long=True))

    got_wq.wait()
    eye_q = (lax.broadcasted_iota(jnp.int32, (qc, qc), 0) == lax.broadcasted_iota(jnp.int32, (qc, qc), 1))
    wq_t[...] = dot_t(eye_q.astype(bf16), wq_ref[...]).astype(bf16)
    wq_buf[0, 0:qs, 0:chunk] = wq_t[pl.ds(pl.multiple_of(xid * qs, qs), qs), :]

    def wq_rows(dx, oc):
        return wq_t.at[pl.ds(pl.multiple_of(line_id(dx, oc) * qs, qs), qs), :]

    def wq_slot(dx, oc):
        return wq_buf.at[oc, pl.ds(0, qs), pl.ds((NX - dx) % NX * chunk, chunk)]

    wq_got = Group(links, wq_t.at[0:qc - qs])
    for dx, oc in LINE:
        wq_got.send(wq_rows(dx, oc), wq_slot(dx, oc), links.at_line(dx, oc))
    for which, ref in enumerate((wg_ref, wu_ref)):
        for dx, oc in LINE[:1] + NEAR:
            w_got[oc].send(w_piece(ref, dx, oc), w_slot(which, dx, oc), links.at_line(dx, oc))

    phase("selections")
    r_id = lax.broadcasted_iota(jnp.int32, (nx2 * nyz * pad, 1), 0)
    r_j = r_id % pad
    r_src = jnp.where(r_j < own_rows, r_id // pad % nyz * rows + r_id // (pad * nyz) * own_rows + r_j, -1)
    s_id = lax.broadcasted_iota(jnp.int32, (1, total_rows), 1)
    sel[...] = jnp.where(r_src == s_id, 1.0, 0.0).astype(bf16)
    t_id = lax.broadcasted_iota(jnp.int32, (group, 1), 0)
    t_in = t_id % rows
    t_src = t_in // own_rows * (NY * pad) + t_id // rows * pad + t_in % own_rows
    u_id = lax.broadcasted_iota(jnp.int32, (1, nx2 * NY * pad), 1)
    sel_t[...] = jnp.where(t_src == u_id, 1.0, 0.0).astype(bf16)
    k_id = lax.broadcasted_iota(jnp.int32, (nx2 * pad, rows), 0)
    k_src = jnp.where(k_id % pad < own_rows, k_id // pad * own_rows + k_id % pad, -1)
    sel_kv = jnp.where(k_src == lax.broadcasted_iota(jnp.int32, (nx2 * pad, rows), 1), 1.0, 0.0).astype(bf16)

    phase.close()
    gain_got.wait()
    lane = lax.broadcasted_iota(jnp.int32, (1, head), 1)
    lengths = []
    for b in range(own_rows):
        index = (yid * nx2 + xid) * own_rows + b
        row = len_ref[pl.ds(index // head, 1), :].astype(f32)
        lengths.append(jnp.sum(jnp.where(lane == index % head, row, 0.0), axis=-1, keepdims=True))
    lengths = jnp.concatenate(lengths + lengths[:pad - own_rows], axis=0)
    angles = lengths * freq_ref[...]
    cos_all = jnp.cos(angles)
    sin_all = jnp.sin(angles) * jnp.where(lane < head // 2, -1.0, 1.0)

    crossing = next(front)
    phase("ng_cross")
    crossing.wait()
    phase("kv_part")

    for c in got_wkv:
        c.wait()
    n_own = dot(sel_kv, n_buf[0, links.slot_rows(0, 0, rows), 0:chunk]).astype(bf16)
    kvp[:, :, :head] = dot(n_own, wk_ref[...]).reshape(nx2, pad, head)
    kvp[:, :, head:] = dot(n_own, wv_ref[...]).reshape(nx2, pad, head)
    kv_got = rest(kvr, nx2)
    for p in LINE:
        kv_got.send(kvp.at[line_id(*p)], kvr.at[xid], links.at_line(*p))
    kvr[xid] = kvp[xid]

    phase("wait_wq")
    wq_got.wait()
    phase("q_mm")
    q_all = jnp.concatenate([
        (dot_t(n_buf[0, i * group:(i + 1) * group, :], wq_buf[0])
         + dot_t(n_buf[1, i * group:(i + 1) * group, :], wq_buf[1])).astype(bf16) for i in range(NZ)], axis=0)
    span = nyz * pad
    for i in range(nx2):
        chosen = dot(sel[i * span:(i + 1) * span, :], q_all)
        quarter = span // per
        packed = chosen[:quarter, :]
        for g in range(1, per):
            packed = packed + pltpu.roll(chosen[g * quarter:(g + 1) * quarter, :], g * qs, 1)
        qx[i] = packed.astype(bf16)
    q_got = rest(qr, nx2)
    for p in LINE:
        q_got.send(qx.at[line_id(*p)], qr.at[xid], links.at_line(*p))
    qr[xid] = qx[xid]

    phase("wait_w")
    for c in own_w:
        c.wait()
    for c in w_got:
        c.wait()
    phase("gate_up")

    def act_at(k, dx):
        return act.at[(z + k) % NZ, :, pl.ds(pl.multiple_of(line_id(dx, 0) * ff, ff), ff)]

    def act_out(k, dx, to_dx):
        return links.send(act_at(k, dx), act_at(k, dx), links.at_line(to_dx, 0))

    def act_give(k, dx):
        cross[k].send(act_at(k, dx), act_at(k, dx), partner)

    turns = (2, 1, 3, 0)
    early, late = turns[:2], turns[2:]
    near_act, far_act = {}, {}
    cross = {k: Group(links, act.at[0, :, 0:NX * ff]) for k in turns}
    for k in turns:
        these = pl.ds(pl.multiple_of((z + k) % NZ * group, group), group)
        both = (dot(n_buf[0, these, :], w_buf[0]) + dot(n_buf[1, these, :], w_buf[1])).astype(bf16).astype(f32)
        gate, up = both[:, :ff], both[:, ff:]
        act_at(k, 0)[...] = (gate * jax.nn.sigmoid(gate) * up).astype(bf16)
        near_act[k] = [(dx, act_out(k, 0, dx)) for dx in HOPS[:2]]
        act_give(k, 0)

    def act_pass(k):
        for dx, c in near_act[k]:
            c.wait_recv()
            if (k in early) == (dx == 1):
                far_act[k] = act_out(k, NX - dx, dx)
            act_give(k, NX - dx)

    low, high = pl.ds(0, half), pl.ds(half, half)
    first_a, first_b = Group(links, ra1), Group(links, rb1)

    def act_use(k):
        cross[k].wait()
        g = (z + k) % NZ
        part[g] = dot(act[g], wd_buf[...]).reshape(NY, rows, chunk)
        if k:
            first_b.send(part.at[g, :, :, high], rb1.at[k - 1], links.at_plane(k, 0))

    def along_y(k):
        g = (z + k) % NZ
        for d in early + late[:1]:
            first_a.send(part.at[g, (y + d) % NY, :, low], ra1.at[d - 1, g], links.at_plane(0, d))

    def act_far(ks):
        for k in ks:
            far_act[k].wait_recv()
            act_give(k, 2)

    phase("wait_q")
    q_got.wait()
    phase("q_sum")
    lane_group = lax.broadcasted_iota(jnp.int32, (1, head), 1) // qs
    for j in range(qc // head):
        came = [qr[j * per + i].astype(f32) for i in range(per)]
        for g in range(per):
            piece = jnp.zeros((span // per, head), f32)
            for i in range(per):
                piece = piece + jnp.where(lane_group == i, pltpu.roll(came[i], (i - g) % per * qs, 1), 0.0)
            qy[g * per:(g + 1) * per, :, j * head:(j + 1) * head] = piece.reshape(per, pad, head)

    def plane_id(dz, dy):
        return (z + dz) % NZ * NY + (y + dy) % NY

    y_got = rest(qf, nyz)
    for p in PLANE:
        y_got.send(qy.at[plane_id(*p)], qf.at[yid], links.at_plane(*p))
    qf[yid] = qy[yid]

    def wo_rows(dz):
        return wo_all.at[pl.ds(pl.multiple_of((z + dz) % NZ * qc, qc), qc), :]

    wo_got = Group(links, wo_all.at[0:(NZ - 1) * qc])
    for d in HOPS:
        wo_got.send(wo_ref, wo_rows(0), links.at_plane(d, 0))
    own_wo = fetch(wo_ref, wo_rows(0))

    phase("act_pass")
    for k in early:
        act_pass(k)
    phase("wait_kv")
    kv_got.wait()
    kv_sum = kvr[0]
    for i in range(1, nx2):
        kv_sum = kv_sum + kvr[i]
    kv_new = kv_sum.astype(bf16).astype(f32)

    def turn(v, b=None):
        cos, sin = (cos_all, sin_all) if b is None else (cos_all[b:b + 1, :], sin_all[b:b + 1, :])
        return (v * cos + pltpu.roll(v, head // 2, 1) * sin).astype(bf16)

    k_new = turn(kv_new[:, :head])
    knew_ref[...] = k_new
    vnew_ref[...] = kv_new[:, head:].astype(bf16)
    k_row, v_row = k_new.astype(f32), kv_new[:, head:]
    phase("wait_qy")
    for c in got_kv:
        c.wait()
    y_got.wait()
    phase("attention")
    seq = k_buf.shape[1]
    score_scale = head ** -0.5
    position = lax.broadcasted_iota(jnp.int32, (1, seq), 1).astype(f32)
    o_buf[...] = jnp.zeros(o_buf.shape, f32)
    for b in range(own_rows):
        q_b = jnp.concatenate([turn(qf[:, b, j * head:(j + 1) * head], b) for j in range(qc // head)], axis=0)
        scores = dot_t(q_b, k_buf[b]) * score_scale
        score_new = jnp.sum(q_b.astype(f32) * k_row[b:b + 1, :], axis=-1, keepdims=True) * score_scale
        valid = position < lengths[b:b + 1, :]
        top = jnp.maximum(jnp.max(jnp.where(valid, scores, -jnp.inf), axis=-1, keepdims=True), score_new)
        weights = jnp.where(valid, jnp.exp(scores - top), 0.0)
        weight_new = jnp.exp(score_new - top)
        denom = jnp.sum(weights, axis=-1, keepdims=True) + weight_new
        o_b = dot((weights / denom).astype(bf16), v_buf[b])
        o_b = o_b + (weight_new / denom).astype(bf16).astype(f32) * v_row[b:b + 1, :]
        o_b = o_b.astype(bf16).astype(f32)
        for j in range(qc // head):
            o_buf[:, :, b, j * head:(j + 1) * head] = o_b[j * nyz:(j + 1) * nyz, :].reshape(NZ, NY, head)
    o_back = rest(o_got, NY)
    for d in HOPS:
        o_back.send(o_buf.at[:, (y + d) % NY], o_got.at[y], links.at_plane(0, d))
    phase("act_early")
    for k in late:
        act_pass(k)
    act_far(early)
    emb_on(ways[:2], emb_far[:2])
    got_wd.wait()
    for k in early:
        act_use(k)
        along_y(k)
    o_got[y] = o_buf[:, y]

    phase("act_late")
    act_far(late)
    for k in late:
        act_use(k)
        along_y(k)

    phase("wait_oy")
    o_back.wait()
    for i in range(NZ):
        o_all[xid, :, i * qc:(i + 1) * qc] = o_got[:, i].reshape(NY * pad, qc).astype(bf16)
    o_here = o_all.at[xid]
    o_line = [links.send(o_here, o_here, links.at_line(dx, 0)) for dx in HOPS]
    o_cross = rest(o_all, NX + 1)
    o_cross.send(o_here, o_here, partner)
    emb_out(ways[2:])
    emb_got[1].send(emb_piece(0, 1), emb_slot(0, 1), partner)
    phase("wait_o")
    for dx, c in zip(HOPS, o_line):
        c.wait_recv()
        came = o_all.at[line_id(NX - dx, 0)]
        o_cross.send(came, came, partner)
    wo_got.wait()
    own_wo.wait()
    o_cross.wait()
    phase("out_mm")
    o_nat = dot(sel_t[...], o_all[...].reshape(nx2 * NY * pad, NZ * qc)).astype(bf16)
    att[...] = dot(o_nat, wo_all[...]).reshape(NY, rows, chunk)
    att_got = Group(links, rc)
    for d in HOPS:
        att_got.send(att.at[(y + d) % NY], rc.at[d - 1], links.at_plane(0, d))

    phase("wait_rs1")
    first_b.wait()
    acc_b[...] = (part[z, :, :, half:] + rb1[0]) + (rb1[1] + rb1[2])
    second = [Group(links, rb2), Group(links, ra2)]
    for d in HOPS:
        second[0].send(acc_b.at[(y + d) % NY], rb2.at[d - 1], links.at_plane(0, d))
    phase("wait_rs1a")
    first_a.wait()
    acc_a[...] = (part[:, y, :, :half] + ra1[0]) + (ra1[1] + ra1[2])
    for d in HOPS:
        second[1].send(acc_a.at[(z + d) % NZ], ra2.at[d - 1], links.at_plane(d, 0))
    phase("wait_att")
    att_got.wait()
    phase("wait_rs2")
    for c in second:
        c.wait()
    phase("rs_sum2")
    def own_residual():
        res = hid_ref[here_rows, :].astype(f32) + ((att[y] + rc[0]) + (rc[1] + rc[2]))
        xbuf2[0, :, :half] = res[:, :half] + ((acc_a[z] + ra2[0]) + (ra2[1] + ra2[2]))
        xbuf2[0, :, half:] = res[:, half:] + ((acc_b[y] + rb2[0]) + (rb2[1] + rb2[2]))

    back = norm_gather(links, own_residual, gains, 1, xbuf2, stat2, f_buf, gather_base, lambda crossing: None)
    next(back)
    emb_on(ways[2:], emb_far[2:])
    for dx, oc in NEAR:
        emb_got[oc].send(emb_piece(dx, oc), emb_slot(dx, oc), links.at_line(dx, oc))
    phase.close()
    crossing = next(back)
    phase("wait_emb")
    own_emb.wait()
    for c in emb_got:
        c.wait()

    phase("logits")
    wide_n = 256
    for h in range(CORES):
        if h:
            crossing.wait()
        for i in range(total_rows // wide_n):
            cols = slice(i * wide_n, (i + 1) * wide_n)
            term = dot_t(emb_buf[h], f_buf[h, cols, :])
            z_ref[:, cols] = z_ref[:, cols] + term if h else term

    phase("lse_own")
    shift = vocab_own * xid - emb_start(xid)
    vid = lax.broadcasted_iota(jnp.int32, (take, 1), 0)
    own = (vid >= shift) & (vid < shift + vocab_own)
    for b in range(blocks):
        zb = jnp.where(own, z_ref[:, b * 128:(b + 1) * 128], -jnp.inf)
        top = jnp.max(zb, axis=0, keepdims=True)
        lse_x[xid, b:b + 1, :] = top
        lse_x[xid, 8 + b:9 + b, :] = jnp.sum(jnp.exp(zb - top), axis=0, keepdims=True)
    for b in range(blocks, 8):
        lse_x[xid, b:b + 1, :] = jnp.zeros((1, 128), f32)
        lse_x[xid, 8 + b:9 + b, :] = jnp.ones((1, 128), f32)

    def merge(ref):
        tops = ref[:, :8, :]
        top = jnp.max(tops, axis=0)
        return top, jnp.sum(ref[:, 8:, :] * jnp.exp(tops - top[None]), axis=0)

    phase("lse_line")
    got = rest(lse_x, nx2)
    for p in LINE:
        got.send(lse_x.at[xid], lse_x.at[xid], links.at_line(*p))
    got.wait()
    top, mass = merge(lse_x)
    lse_y[yid, :8, :] = top
    lse_y[yid, 8:, :] = mass
    phase("lse_plane")
    got = rest(lse_y, nyz)
    for p in PLANE:
        got.send(lse_y.at[yid], lse_y.at[yid], links.at_plane(*p))
    got.wait()
    top, mass = merge(lse_y)
    norm = top + jnp.log(mass)
    norm_ref[...] = norm[:blocks, :]
    phase("subtract")
    for b in range(blocks):
        cols = slice(b * head, (b + 1) * head)
        out_ref[:, cols] = pltpu.roll(z_ref[:, cols], (take - shift) % take, 0)[:vocab_own, :] - norm[b:b + 1, :]
    phase("finish")
    links.finish()
    phase.close()


def whole_step(hidden, freq, lens, k_cache, v_cache, g_attn, w_query, w_key, w_value,
               w_gate, w_up, w_out, w_down, g_final, embedding):
    total_rows, chunk = hidden.shape
    own_rows, seq, head = k_cache.shape
    rows = total_rows // (NY * NZ)
    vocab_own = embedding.shape[0] // (2 * NX)
    take = (vocab_own + 6 + 15) // 16 * 16
    half = chunk // 2
    qc = w_query.shape[1]
    ff = w_gate.shape[1] // (2 * NX)
    f32, bf16 = jnp.float32, jnp.bfloat16
    nyz, nx2, pad = NY * NZ, 2 * NX, 8
    vmem = pl.BlockSpec(memory_space=pltpu.VMEM)
    hbm = pl.BlockSpec(memory_space=pl.ANY)
    V = pltpu.VMEM
    return pl.pallas_call(
        lambda *refs: step_kernel(vocab_own, own_rows, *refs),
        out_shape=(jax.ShapeDtypeStruct((pad, head), bf16), jax.ShapeDtypeStruct((pad, head), bf16),
                   jax.ShapeDtypeStruct((vocab_own, total_rows), f32), jax.ShapeDtypeStruct((total_rows // head, head), f32)),
        in_specs=[vmem] * 5 + [hbm] * 10,
        out_specs=(vmem,) * 4,
        scratch_shapes=[
            V((chunk, qc), bf16), V((chunk, head), bf16), V((chunk, head), bf16), V((take, total_rows), f32),
            V((own_rows, seq, head), bf16), V((own_rows, seq, head), bf16),
            V((nx2 * ff, chunk), bf16), V((NZ * qc, chunk), bf16), V((NY, rows, chunk), f32), V((3, rows, chunk), f32), V((2, total_rows, NX * chunk), bf16), V((2, NX * chunk, 2 * ff), bf16),
            V((qc, chunk), bf16), V((2, head, NX * chunk), bf16),
            V((nx2 * nyz * pad, total_rows), bf16), V((NY * rows, nx2 * NY * pad), bf16),
            V((nx2, nyz * pad // 4, head), bf16), V((nx2, nyz * pad // 4, head), bf16),
            V((nyz, pad, qc), f32), V((nyz, pad, qc), f32),
            V((nx2, pad, 2 * head), f32), V((nx2, pad, 2 * head), f32),
            V((NZ, NY, pad, qc), f32), V((NY, NZ, pad, qc), f32), V((nx2, NY * pad, NZ * qc), bf16),
            V((NZ, NY * rows, nx2 * ff), bf16),
            V((NZ, NY, rows, chunk), f32),
            V((3, NZ, rows, half), f32), V((3, NY, rows, half), f32), V((3, rows, half), f32), V((3, rows, half), f32),
            V((NZ, rows, half), f32), V((NY, rows, half), f32),
            V((NX, rows, chunk), bf16), V((2, rows, 128), f32), V((NX, rows, chunk), f32), V((2, rows, 128), f32),
            V((NX, 8, chunk), f32),
            V((2, total_rows, NX * chunk), bf16), V((2, take, NX * chunk), bf16),
            V((2, 2, chunk, ff), bf16), V((2, 2, (take // 2 + 15) // 16 * 16, chunk), bf16),
            V((nx2, 16, 128), f32), V((nx2, 16, 128), f32), V((nyz, 16, 128), f32),
            pltpu.SemaphoreType.DMA((SENDS,)), pltpu.SemaphoreType.DMA((TAGS,)), pltpu.SemaphoreType.DMA((10,)),
        ],
        compiler_params=pltpu.CompilerParams(
            collective_id=1, has_side_effects=True, vmem_limit_bytes=60 << 20),
        name="decode_step",
    )(hidden, g_attn[None, :], g_final[None, :], freq, lens, k_cache, v_cache,
      w_query, w_key, w_value, w_out, w_gate, w_up, w_down, embedding)


def solution(mesh):
    row_spec = P(("dp", "yax", "xax"))

    def local_step(hidden, cache_len, k_cache, v_cache, g_attn, w_query, w_key, w_value,
                   w_gate, w_up, w_out, w_down, g_final, embedding):
        rows = hidden.shape[0]
        half_dim = k_cache.shape[2] // 2
        inv_freq = ROPE_BASE ** (-(jnp.arange(half_dim, dtype=jnp.float32) * 2.0) / (2 * half_dim))
        freq = jnp.concatenate([inv_freq, inv_freq])[None, :]
        key_own, value_own, log_probs, log_norm = whole_step(
            hidden, freq, cache_len.reshape(rows // 128, 128), k_cache, v_cache, g_attn, w_query, w_key, w_value,
            w_gate, w_up, w_out, w_down, g_final, embedding)
        own_rows = k_cache.shape[0]
        return key_own[:own_rows], value_own[:own_rows], log_probs.T, log_norm.reshape(rows)

    in_specs = (P("dp", "xax"), P("dp"), row_spec, row_spec, P("xax"), P("xax", "yax"),
                P("xax", None), P("xax", None), P("xax", "yax"), P("xax", "yax"),
                P("yax", "xax"), P("yax", "xax"), P("xax"), P("yax", "xax"))
    out_specs = (row_spec, row_spec, P("dp", ("yax", "xax")), P("dp"))
    return jax.shard_map(local_step, mesh=mesh, in_specs=in_specs, out_specs=out_specs, check_vma=False)
```

```python
import itertools

import jax
import jax.numpy as jnp
import numpy as np
from jax import lax
from jax.experimental import pallas as pl
from jax.experimental.pallas import tpu as pltpu
from jax.sharding import PartitionSpec as P

EPS = 1e-6
ROPE_BASE = 10000.0
MESH_ID = pl.DeviceIdType.MESH
NY = NZ = NX = 4
CORES = 2
POOL, SENDS, TAGS = 24, 58, 85
HOPS = (1, 3, 2)
LINE = [(0, 1), (1, 0), (3, 0), (1, 1), (3, 1), (2, 0), (2, 1)]
NEAR = LINE[1:5]
NT = (((1,), (1,)), ((), ()))
PLANE = [(dz, dy) for dz in range(NZ) for dy in range(NY) if dz or dy]


class Group:
    def __init__(self, links, whole):
        self.links, self.whole = links, whole
        self.tag, self.sem = next(links.tags), next(links.slow)
        links.groups.append(self)

    def send(self, src, dst, where):
        pltpu.make_async_remote_copy(
            src_ref=src, dst_ref=dst, send_sem=self.links.send_sem.at[self.sem],
            recv_sem=self.links.recv_sem.at[self.tag], device_id=where, device_id_type=MESH_ID).start()

    def wait(self):
        pltpu.make_async_copy(self.whole, self.whole, self.links.recv_sem.at[self.tag]).wait()

    def wait_sent(self):
        pltpu.make_async_copy(self.whole, self.whole, self.links.send_sem.at[self.sem]).wait()


class Phases:
    def __init__(self):
        self.open = None

    def __call__(self, name):
        self.close()
        self.open = jax.named_scope(name)
        self.open.__enter__()

    def close(self):
        if self.open is not None:
            self.open.__exit__(None, None, None)
        self.open = None


class Links:
    def __init__(self, send_sem, recv_sem):
        self.send_sem, self.recv_sem = send_sem, recv_sem
        self.tags, self.slow, self.fast = itertools.count(), itertools.count(POOL), []
        self.pending, self.groups = [], []
        self.y_idx = lax.axis_index("yax")
        self.x_idx = lax.axis_index("xax")
        self.z, self.y = self.y_idx // NY, self.y_idx % NY
        self.chip, self.core = self.x_idx // CORES, self.x_idx % CORES

    def at_plane(self, dz, dy):
        return {"yax": (self.z + dz) % NZ * NY + (self.y + dy) % NY, "xax": self.x_idx}

    def slot_rows(self, dz, dy, rows):
        slot = (self.z + dz) % NZ * NY + (self.y + dy) % NY
        return pl.ds(pl.multiple_of(slot * rows, rows), rows)

    def line_id(self, dx, oc):
        core = 1 - self.core if oc else self.core
        return (self.chip + dx) % NX * CORES + core

    def at_line(self, dx, oc):
        return {"yax": self.y_idx, "xax": self.line_id(dx, oc)}

    def send(self, src, dst, where, tag=None, long=False):
        tag = next(self.tags) if tag is None else tag
        if long:
            sem = next(self.slow)
        else:
            sem = len(self.fast) % POOL
            if len(self.fast) >= POOL:
                self.fast[-POOL].wait_send()
        copy = pltpu.make_async_remote_copy(
            src_ref=src, dst_ref=dst, send_sem=self.send_sem.at[sem], recv_sem=self.recv_sem.at[tag],
            device_id=where, device_id_type=MESH_ID)
        copy.start()
        (self.pending if long else self.fast).append(copy)
        return copy

    def finish(self):
        for copy in self.pending + self.fast[-POOL:]:
            copy.wait_send()
        for group in self.groups:
            group.wait_sent()

    def barrier(self):
        barrier = pltpu.get_barrier_semaphore()
        peers = [self.at_line(*p) for p in LINE] + [self.at_plane(*p) for p in PLANE]
        for peer in peers:
            pl.semaphore_signal(barrier, inc=1, device_id=peer, device_id_type=MESH_ID)
        pl.semaphore_wait(barrier, len(peers))


def plane_gather(links, buf, tags, hook, crossing, start):
    cols = buf.shape[-1]
    rows = buf.shape[1] // (NY * NZ)
    span = (cols - start) // 2
    partner = links.at_line(0, 1)

    class Part:
        def __init__(self, index):
            self.index, self.lo, self.got = index, start + index * span, {}

        def order(self, du, dv):
            return (du, dv) if self.index else (dv, du)

        def block(self, at, half=0, piece=None):
            width = span if piece is None else span // 2
            lo = self.lo if not piece else self.lo + width
            return buf.at[half, links.slot_rows(*self.order(*at), rows), pl.ds(lo, width)]

        def push(self, name, at, to, piece=None):
            ref = self.block(at, piece=piece)
            self.got[name] = links.send(ref, ref, links.at_plane(*self.order(*to)), next(tags))

        def spread(self, k, at):
            self.push(("v+", k), at, (0, 1))
            self.push(("v-", k), at, (0, -1))

        def give(self, at):
            crossing.send(self.block(at), self.block(at, half=1), partner)

        def wait(self, name):
            self.got[name].wait_recv()

    parts = [Part(index) for index in range(2)]
    offset = (0, -1, 1, 2)
    for p in parts:
        p.push("u+", (0, 0), (1, 0))
        p.push("u-", (0, 0), (-1, 0))
        p.spread(0, (0, 0))
    for p in parts:
        p.give((0, 0))
    for k, name in enumerate(("u+", "u-"), 1):
        for p in parts:
            p.wait(name)
            at = (offset[k], 0)
            p.push(("far", k), at, (-offset[k], 0), piece=k - 1)
            p.spread(k, at)
            p.give(at)
    hook()

    def arrive(p, k):
        for name, step in (("v+", -1), ("v-", 1)):
            p.wait((name, k))
            at = (offset[k], step)
            if (name == "v+") == (k in (0, 3)):
                p.push(("relay", k), at, (0, -step))
            p.give(at)

    for p in parts:
        arrive(p, 0)
    for p in parts:
        p.wait(("far", 1))
        p.wait(("far", 2))
        p.spread(3, (2, 0))
        p.give((2, 0))
    for k in range(1, len(offset)):
        for p in parts:
            arrive(p, k)
    for k in range(len(offset)):
        for p in parts:
            p.wait(("relay", k))
            p.give((offset[k], 2))


def norm_gather(links, own_slot, gain_buf, which, xbuf, stat, out, base, hook, skip=0):
    own_slot()
    rows, chunk = xbuf.shape[1:]
    tags = itertools.count(base)
    line = [links.send(xbuf.at[0], xbuf.at[NX - dx], links.at_line(dx, 0), next(tags)) for dx in HOPS]
    yield
    phase = Phases()
    for n, c in enumerate(line):
        phase(f"ng_line{which}_{n}")
        c.wait_recv()
    phase("ng_stats")
    held = xbuf[...].astype(jnp.float32)
    count = NX * chunk
    mean = jnp.sum(jnp.sum(held, axis=0), axis=-1, keepdims=True) / count
    dev = held - mean[None]
    square = jnp.sum(jnp.sum(dev * dev, axis=0), axis=-1, keepdims=True)
    lane = lax.broadcasted_iota(jnp.int32, (rows, 128), 1)
    stat[0] = jnp.where(lane == 0, mean, square)
    links.send(stat.at[0], stat.at[1], links.at_line(0, 1), next(tags)).wait_recv()
    other_mean, other_square = stat[1, :, 0:1], stat[1, :, 1:2]
    both = (mean + other_mean) * 0.5
    gap = mean - other_mean
    var = (square + other_square + gap * gap * (count * 0.5)) / (2 * count)
    scale = lax.rsqrt(var + EPS)
    for e in range(skip, NX):
        out[0, links.slot_rows(0, 0, rows), e * chunk:(e + 1) * chunk] = (
            (xbuf[e].astype(jnp.float32) - both) * scale * gain_buf[e, which:which + 1, :]).astype(jnp.bfloat16)
    phase("ng_plane")
    crossing = Group(links, out.at[1])
    plane_gather(links, out, tags, lambda: hook(crossing), crossing, skip * chunk)
    phase.close()
    yield crossing


def step_kernel(vocab_own, own_rows, hid_ref, gain_a, gain_f, freq_ref, len_ref, k_hbm, v_hbm,
                wq_hbm, wk_hbm, wv_hbm, wo_ref, wg_ref, wu_ref, wd_hbm, emb_ref,
                knew_ref, vnew_ref, z_ref, norm_ref,
                wq_ref, wk_ref, wv_ref, k_buf, v_buf, wd_buf, wo_all, att, rc, n_buf, w_buf, wq_t, wq_buf, sel, sel_t, qx, qr, qy, qf,
                kvp, kvr, o_buf, o_got, o_all, act,
                part, ra1, rb1, ra2, rb2, acc_a, acc_b, xbuf, stat, xbuf2, stat2, gains, f_buf, emb_buf,
                w_relay, emb_relay, row_stats, lse_x, lse_y, send_sem, recv_sem, local_sem):
    links = Links(send_sem, recv_sem)
    phase = Phases()
    f32, bf16 = jnp.float32, jnp.bfloat16
    z, y, xid, yid = links.z, links.y, links.x_idx, links.y_idx
    total_rows, chunk = hid_ref.shape
    rows = total_rows // (NY * NZ)
    here_rows = links.slot_rows(0, 0, rows)
    half = chunk // 2
    nx2, nyz = 2 * NX, NY * NZ
    group = NY * rows
    head = 128
    pad = 8
    partner = links.at_line(0, 1)
    line_id = links.line_id
    gather_tags = len(HOPS) + 1 + len(PLANE) * CORES + CORES
    gather_base = [next(links.tags) for _ in range(gather_tags)][0]

    def dot(a, b):
        return jnp.dot(a, b, preferred_element_type=f32)

    def dot_t(a, b):
        return lax.dot_general(a, b, NT, preferred_element_type=f32)

    def rest(ref, n):
        return Group(links, ref.at[0:n - 1])

    local = []

    def fetch(src, dst):
        copy = pltpu.make_async_copy(src, dst, local_sem.at[len(local)])
        copy.start()
        local.append(copy)
        return copy

    ff = wg_ref.shape[1] // nx2

    def w_piece(ref, dx, oc):
        return ref.at[:, pl.ds(pl.multiple_of(line_id(dx, oc) * ff, ff), ff)]

    def w_slot(which, dx, oc):
        back = (NX - dx) % NX
        return w_buf.at[int(oc), pl.ds(back * chunk, chunk), pl.ds(which * ff, ff)]

    take = emb_buf.shape[1]

    def emb_start(xi):
        return pl.multiple_of(vocab_own * xi // pad * pad, pad)

    def emb_piece(dx, oc):
        return emb_ref.at[pl.ds(emb_start(line_id(dx, oc)), take), :]

    def emb_slot(dx, oc):
        return emb_buf.at[int(oc), :, pl.ds((NX - dx) % NX * chunk, chunk)]

    near_part = (take // 2 + 15) // 16 * 16
    far_parts = ((0, near_part), (near_part, take - near_part))

    def emb_half(oc, way):
        first, size = far_parts[way]
        return emb_ref.at[pl.ds(pl.multiple_of(emb_start(line_id(2, oc)) + first, pad), size), :]

    def emb_mid(oc, way):
        return emb_relay.at[way, oc, pl.ds(0, far_parts[way][1])]

    def emb_far_slot(oc, way):
        return emb_buf.at[int(oc), pl.ds(*far_parts[way]), pl.ds(2 * chunk, chunk)]

    got_wq = fetch(wq_hbm, wq_ref)
    own_w = [fetch(w_piece(wg_ref, 0, 0), w_slot(0, 0, 0)), fetch(w_piece(wu_ref, 0, 0), w_slot(1, 0, 0))]
    got_kv = [fetch(k_hbm, k_buf), fetch(v_hbm, v_buf)]
    got_wkv = [fetch(wk_hbm, wk_ref), fetch(wv_hbm, wv_ref)]
    got_wd = fetch(wd_hbm, wd_buf)
    own_emb = fetch(emb_piece(0, 0), emb_slot(0, 0))

    qc = wq_ref.shape[1]
    qs = qc // nx2
    per = head // qs
    wq_buf[...] = jnp.zeros(wq_buf.shape, bf16)

    phase("row_stats")
    eye = lax.broadcasted_iota(jnp.int32, (head, head), 0) == lax.broadcasted_iota(jnp.int32, (head, head), 1)
    blocks = total_rows // head

    def block_rows(b):
        return slice(b * head, (b + 1) * head)

    def to_row(v):
        return jnp.sum(jnp.where(eye, v, 0.0), axis=0, keepdims=True)

    def to_col(v):
        return jnp.sum(jnp.where(eye, v, 0.0), axis=1, keepdims=True)

    row_stats[xid] = jnp.zeros((2 * pad, head), f32)
    for b in range(blocks):
        held = hid_ref[block_rows(b), :].astype(f32)
        mean = jnp.sum(held, axis=-1, keepdims=True) / chunk
        dev = held - mean
        row_stats[xid, b:b + 1, :] = to_row(mean)
        row_stats[xid, pad + b:pad + b + 1, :] = to_row(jnp.sum(dev * dev, axis=-1, keepdims=True))

    phase("barrier")
    links.barrier()

    phase("front_send")
    gains[0, 0:1, :] = gain_a[...]
    gains[0, 1:2, :] = gain_f[...]
    gains[0, 2:, :] = jnp.zeros((6, chunk), f32)

    def own_input():
        xbuf[0] = hid_ref[here_rows, :]

    w_far, emb_far = [], []
    w_got = [Group(links, w_buf.at[0, 0:(NX - 1) * chunk]), Group(links, w_buf.at[1])]
    emb_got = [Group(links, emb_buf.at[0, :, 0:(NX - 1) * chunk]), Group(links, emb_buf.at[1])]
    ways = [(way, hop, oc) for oc in (0, 1) for way, hop in enumerate(HOPS[:2])]

    def forward_weights():
        for (way, hop, oc), c in zip(ways, w_far):
            c.wait_recv()
            w_got[oc].send(w_relay.at[way, oc], w_buf.at[oc, pl.ds(2 * chunk, chunk), pl.ds(way * ff, ff)],
                           links.at_line(hop, oc))

    def emb_out(some):
        for way, hop, oc in some:
            emb_far.append(links.send(emb_half(oc, way), emb_mid(oc, way), links.at_line(hop, 0), long=True))

    def emb_on(some, arrived):
        for (way, hop, oc), c in zip(some, arrived):
            c.wait_recv()
            emb_got[oc].send(emb_mid(oc, way), emb_far_slot(oc, way), links.at_line(hop, oc))

    def amid(crossing):
        forward_weights()
        stats_got.wait()
        means = row_stats[:, :pad, :]
        mean = jnp.sum(means, axis=0) / nx2
        gap = means - mean[None]
        square = jnp.sum(row_stats[:, pad:, :], axis=0) + jnp.sum(gap * gap, axis=0) * chunk
        scale = lax.rsqrt(square / (nx2 * chunk) + EPS)
        for b in range(blocks):
            n_buf[0, block_rows(b), 0:chunk] = (
                (hid_ref[block_rows(b), :].astype(f32) - to_col(mean[b:b + 1, :])) * to_col(scale[b:b + 1, :])
                * gains[0, 0:1, :]).astype(bf16)
        own = n_buf.at[0, :, 0:chunk]
        crossing.send(own, n_buf.at[1, :, 0:chunk], partner)

    front = norm_gather(links, own_input, gains, 0, xbuf, stat, n_buf, gather_base, amid, skip=1)
    next(front)
    gain_got = rest(gains, NX)
    for dx in HOPS:
        gain_got.send(gains.at[0], gains.at[NX - dx], links.at_line(dx, 0))
    stats_got = rest(row_stats, nx2)
    for p in LINE:
        stats_got.send(row_stats.at[xid], row_stats.at[xid], links.at_line(*p))
    for way, hop, oc in ways:
        w_far.append(links.send(w_piece((wg_ref, wu_ref)[way], 2, oc), w_relay.at[way, oc], links.at_line(hop, 0),
                                long=True))

    got_wq.wait()
    eye_q = (lax.broadcasted_iota(jnp.int32, (qc, qc), 0) == lax.broadcasted_iota(jnp.int32, (qc, qc), 1))
    wq_t[...] = dot_t(eye_q.astype(bf16), wq_ref[...]).astype(bf16)
    wq_buf[0, 0:qs, 0:chunk] = wq_t[pl.ds(pl.multiple_of(xid * qs, qs), qs), :]

    def wq_rows(dx, oc):
        return wq_t.at[pl.ds(pl.multiple_of(line_id(dx, oc) * qs, qs), qs), :]

    def wq_slot(dx, oc):
        return wq_buf.at[oc, pl.ds(0, qs), pl.ds((NX - dx) % NX * chunk, chunk)]

    wq_got = Group(links, wq_t.at[0:qc - qs])
    for dx, oc in LINE:
        wq_got.send(wq_rows(dx, oc), wq_slot(dx, oc), links.at_line(dx, oc))
    for which, ref in enumerate((wg_ref, wu_ref)):
        for dx, oc in LINE[:1] + NEAR:
            w_got[oc].send(w_piece(ref, dx, oc), w_slot(which, dx, oc), links.at_line(dx, oc))

    phase("selections")
    r_id = lax.broadcasted_iota(jnp.int32, (nx2 * nyz * pad, 1), 0)
    r_j = r_id % pad
    r_src = jnp.where(r_j < own_rows, r_id // pad % nyz * rows + r_id // (pad * nyz) * own_rows + r_j, -1)
    s_id = lax.broadcasted_iota(jnp.int32, (1, total_rows), 1)
    sel[...] = jnp.where(r_src == s_id, 1.0, 0.0).astype(bf16)
    t_id = lax.broadcasted_iota(jnp.int32, (group, 1), 0)
    t_in = t_id % rows
    t_src = t_in // own_rows * (NY * pad) + t_id // rows * pad + t_in % own_rows
    u_id = lax.broadcasted_iota(jnp.int32, (1, nx2 * NY * pad), 1)
    sel_t[...] = jnp.where(t_src == u_id, 1.0, 0.0).astype(bf16)
    k_id = lax.broadcasted_iota(jnp.int32, (nx2 * pad, rows), 0)
    k_src = jnp.where(k_id % pad < own_rows, k_id // pad * own_rows + k_id % pad, -1)
    sel_kv = jnp.where(k_src == lax.broadcasted_iota(jnp.int32, (nx2 * pad, rows), 1), 1.0, 0.0).astype(bf16)

    phase.close()
    gain_got.wait()
    lane = lax.broadcasted_iota(jnp.int32, (1, head), 1)
    lengths = []
    for b in range(own_rows):
        index = (yid * nx2 + xid) * own_rows + b
        row = len_ref[pl.ds(index // head, 1), :].astype(f32)
        lengths.append(jnp.sum(jnp.where(lane == index % head, row, 0.0), axis=-1, keepdims=True))
    lengths = jnp.concatenate(lengths + lengths[:pad - own_rows], axis=0)
    angles = lengths * freq_ref[...]
    cos_all = jnp.cos(angles)
    sin_all = jnp.sin(angles) * jnp.where(lane < head // 2, -1.0, 1.0)

    crossing = next(front)
    phase("ng_cross")
    crossing.wait()
    phase("kv_part")

    for c in got_wkv:
        c.wait()
    n_own = dot(sel_kv, n_buf[0, links.slot_rows(0, 0, rows), 0:chunk]).astype(bf16)
    kvp[:, :, :head] = dot(n_own, wk_ref[...]).reshape(nx2, pad, head)
    kvp[:, :, head:] = dot(n_own, wv_ref[...]).reshape(nx2, pad, head)
    kv_got = rest(kvr, nx2)
    for p in LINE:
        kv_got.send(kvp.at[line_id(*p)], kvr.at[xid], links.at_line(*p))
    kvr[xid] = kvp[xid]

    phase("wait_wq")
    wq_got.wait()
    phase("q_mm")
    q_all = jnp.concatenate([
        (dot_t(n_buf[0, i * group:(i + 1) * group, :], wq_buf[0])
         + dot_t(n_buf[1, i * group:(i + 1) * group, :], wq_buf[1])).astype(bf16) for i in range(NZ)], axis=0)
    span = nyz * pad
    for i in range(nx2):
        chosen = dot(sel[i * span:(i + 1) * span, :], q_all)
        quarter = span // per
        packed = chosen[:quarter, :]
        for g in range(1, per):
            packed = packed + pltpu.roll(chosen[g * quarter:(g + 1) * quarter, :], g * qs, 1)
        qx[i] = packed.astype(bf16)
    q_got = rest(qr, nx2)
    for p in LINE:
        q_got.send(qx.at[line_id(*p)], qr.at[xid], links.at_line(*p))
    qr[xid] = qx[xid]

    phase("wait_w")
    for c in own_w:
        c.wait()
    for c in w_got:
        c.wait()
    phase("gate_up")

    def act_at(k, dx):
        return act.at[(z + k) % NZ, :, pl.ds(pl.multiple_of(line_id(dx, 0) * ff, ff), ff)]

    def act_out(k, dx, to_dx):
        return links.send(act_at(k, dx), act_at(k, dx), links.at_line(to_dx, 0))

    def act_give(k, dx):
        cross[k].send(act_at(k, dx), act_at(k, dx), partner)

    turns = (2, 1, 3, 0)
    early, late = turns[:2], turns[2:]
    near_act, far_act = {}, {}
    cross = {k: Group(links, act.at[0, :, 0:NX * ff]) for k in turns}
    for k in turns:
        these = pl.ds(pl.multiple_of((z + k) % NZ * group, group), group)
        both = (dot(n_buf[0, these, :], w_buf[0]) + dot(n_buf[1, these, :], w_buf[1])).astype(bf16).astype(f32)
        gate, up = both[:, :ff], both[:, ff:]
        act_at(k, 0)[...] = (gate * jax.nn.sigmoid(gate) * up).astype(bf16)
        near_act[k] = [(dx, act_out(k, 0, dx)) for dx in HOPS[:2]]
        act_give(k, 0)

    def act_pass(k):
        for dx, c in near_act[k]:
            c.wait_recv()
            if (k in early) == (dx == 1):
                far_act[k] = act_out(k, NX - dx, dx)
            act_give(k, NX - dx)

    low, high = pl.ds(0, half), pl.ds(half, half)
    first_a, first_b = Group(links, ra1), Group(links, rb1)

    def act_use(k):
        cross[k].wait()
        g = (z + k) % NZ
        part[g] = dot(act[g], wd_buf[...]).reshape(NY, rows, chunk)
        if k:
            first_b.send(part.at[g, :, :, high], rb1.at[k - 1], links.at_plane(k, 0))

    def along_y(k):
        g = (z + k) % NZ
        for d in early + late[:1]:
            first_a.send(part.at[g, (y + d) % NY, :, low], ra1.at[d - 1, g], links.at_plane(0, d))

    def act_far(ks):
        for k in ks:
            far_act[k].wait_recv()
            act_give(k, 2)

    phase("wait_q")
    q_got.wait()
    phase("q_sum")
    lane_group = lax.broadcasted_iota(jnp.int32, (1, head), 1) // qs
    for j in range(qc // head):
        came = [qr[j * per + i].astype(f32) for i in range(per)]
        for g in range(per):
            piece = jnp.zeros((span // per, head), f32)
            for i in range(per):
                piece = piece + jnp.where(lane_group == i, pltpu.roll(came[i], (i - g) % per * qs, 1), 0.0)
            qy[g * per:(g + 1) * per, :, j * head:(j + 1) * head] = piece.reshape(per, pad, head)

    def plane_id(dz, dy):
        return (z + dz) % NZ * NY + (y + dy) % NY

    y_got = rest(qf, nyz)
    for p in PLANE:
        y_got.send(qy.at[plane_id(*p)], qf.at[yid], links.at_plane(*p))
    qf[yid] = qy[yid]

    def wo_rows(dz):
        return wo_all.at[pl.ds(pl.multiple_of((z + dz) % NZ * qc, qc), qc), :]

    wo_got = Group(links, wo_all.at[0:(NZ - 1) * qc])
    for d in HOPS:
        wo_got.send(wo_ref, wo_rows(0), links.at_plane(d, 0))
    own_wo = fetch(wo_ref, wo_rows(0))

    phase("act_pass")
    for k in early:
        act_pass(k)
    emb_out(ways[:2])
    phase("wait_kv")
    kv_got.wait()
    kv_sum = kvr[0]
    for i in range(1, nx2):
        kv_sum = kv_sum + kvr[i]
    kv_new = kv_sum.astype(bf16).astype(f32)

    def turn(v, b=None):
        cos, sin = (cos_all, sin_all) if b is None else (cos_all[b:b + 1, :], sin_all[b:b + 1, :])
        return (v * cos + pltpu.roll(v, head // 2, 1) * sin).astype(bf16)

    k_new = turn(kv_new[:, :head])
    knew_ref[...] = k_new
    vnew_ref[...] = kv_new[:, head:].astype(bf16)
    k_row, v_row = k_new.astype(f32), kv_new[:, head:]
    phase("act_pass2")
    for k in late:
        act_pass(k)
    phase("wait_qy")
    for c in got_kv:
        c.wait()
    y_got.wait()
    phase("attention")
    seq = k_buf.shape[1]
    score_scale = head ** -0.5
    position = lax.broadcasted_iota(jnp.int32, (1, seq), 1).astype(f32)
    o_buf[...] = jnp.zeros(o_buf.shape, f32)
    for b in range(own_rows):
        q_b = jnp.concatenate([turn(qf[:, b, j * head:(j + 1) * head], b) for j in range(qc // head)], axis=0)
        scores = dot_t(q_b, k_buf[b]) * score_scale
        score_new = jnp.sum(q_b.astype(f32) * k_row[b:b + 1, :], axis=-1, keepdims=True) * score_scale
        valid = position < lengths[b:b + 1, :]
        top = jnp.maximum(jnp.max(jnp.where(valid, scores, -jnp.inf), axis=-1, keepdims=True), score_new)
        weights = jnp.where(valid, jnp.exp(scores - top), 0.0)
        weight_new = jnp.exp(score_new - top)
        denom = jnp.sum(weights, axis=-1, keepdims=True) + weight_new
        o_b = dot((weights / denom).astype(bf16), v_buf[b])
        o_b = o_b + (weight_new / denom).astype(bf16).astype(f32) * v_row[b:b + 1, :]
        o_b = o_b.astype(bf16).astype(f32)
        for j in range(qc // head):
            o_buf[:, :, b, j * head:(j + 1) * head] = o_b[j * nyz:(j + 1) * nyz, :].reshape(NZ, NY, head)
    o_back = rest(o_got, NY)
    for d in HOPS:
        o_back.send(o_buf.at[:, (y + d) % NY], o_got.at[y], links.at_plane(0, d))
    phase("act_early")
    act_far(early)
    emb_on(ways[:2], emb_far[:2])
    got_wd.wait()
    for k in early:
        act_use(k)
        along_y(k)
    o_got[y] = o_buf[:, y]

    phase("act_late")
    act_far(late)
    for k in late:
        act_use(k)
        along_y(k)

    phase("wait_oy")
    o_back.wait()
    for i in range(NZ):
        o_all[xid, :, i * qc:(i + 1) * qc] = o_got[:, i].reshape(NY * pad, qc).astype(bf16)
    o_here = o_all.at[xid]
    o_line = [links.send(o_here, o_here, links.at_line(dx, 0)) for dx in HOPS]
    o_cross = rest(o_all, NX + 1)
    o_cross.send(o_here, o_here, partner)
    emb_out(ways[2:])
    emb_got[1].send(emb_piece(0, 1), emb_slot(0, 1), partner)
    phase("wait_o")
    for dx, c in zip(HOPS, o_line):
        c.wait_recv()
        came = o_all.at[line_id(NX - dx, 0)]
        o_cross.send(came, came, partner)
    wo_got.wait()
    own_wo.wait()
    o_cross.wait()
    phase("out_mm")
    o_nat = dot(sel_t[...], o_all[...].reshape(nx2 * NY * pad, NZ * qc)).astype(bf16)
    att[...] = dot(o_nat, wo_all[...]).reshape(NY, rows, chunk)
    att_got = Group(links, rc)
    for d in HOPS:
        att_got.send(att.at[(y + d) % NY], rc.at[d - 1], links.at_plane(0, d))

    phase("wait_rs1")
    first_b.wait()
    acc_b[...] = (part[z, :, :, half:] + rb1[0]) + (rb1[1] + rb1[2])
    second = [Group(links, rb2), Group(links, ra2)]
    for d in HOPS:
        second[0].send(acc_b.at[(y + d) % NY], rb2.at[d - 1], links.at_plane(0, d))
    phase("wait_rs1a")
    first_a.wait()
    acc_a[...] = (part[:, y, :, :half] + ra1[0]) + (ra1[1] + ra1[2])
    for d in HOPS:
        second[1].send(acc_a.at[(z + d) % NZ], ra2.at[d - 1], links.at_plane(d, 0))
    emb_on(ways[2:], emb_far[2:])
    phase("wait_att")
    att_got.wait()
    phase("wait_rs2")
    for c in second:
        c.wait()
    phase("rs_sum2")
    def own_residual():
        res = hid_ref[here_rows, :].astype(f32) + ((att[y] + rc[0]) + (rc[1] + rc[2]))
        xbuf2[0, :, :half] = res[:, :half] + ((acc_a[z] + ra2[0]) + (ra2[1] + ra2[2]))
        xbuf2[0, :, half:] = res[:, half:] + ((acc_b[y] + rb2[0]) + (rb2[1] + rb2[2]))

    back = norm_gather(links, own_residual, gains, 1, xbuf2, stat2, f_buf, gather_base, lambda crossing: None)
    next(back)
    for dx, oc in NEAR:
        emb_got[oc].send(emb_piece(dx, oc), emb_slot(dx, oc), links.at_line(dx, oc))
    phase.close()
    crossing = next(back)
    phase("wait_emb")
    own_emb.wait()
    for c in emb_got:
        c.wait()

    phase("logits")
    wide_n = 256
    for h in range(CORES):
        if h:
            crossing.wait()
        for i in range(total_rows // wide_n):
            cols = slice(i * wide_n, (i + 1) * wide_n)
            term = dot_t(emb_buf[h], f_buf[h, cols, :])
            z_ref[:, cols] = z_ref[:, cols] + term if h else term

    phase("lse_own")
    shift = vocab_own * xid - emb_start(xid)
    vid = lax.broadcasted_iota(jnp.int32, (take, 1), 0)
    own = (vid >= shift) & (vid < shift + vocab_own)
    for b in range(blocks):
        zb = jnp.where(own, z_ref[:, b * 128:(b + 1) * 128], -jnp.inf)
        top = jnp.max(zb, axis=0, keepdims=True)
        lse_x[xid, b:b + 1, :] = top
        lse_x[xid, 8 + b:9 + b, :] = jnp.sum(jnp.exp(zb - top), axis=0, keepdims=True)
    for b in range(blocks, 8):
        lse_x[xid, b:b + 1, :] = jnp.zeros((1, 128), f32)
        lse_x[xid, 8 + b:9 + b, :] = jnp.ones((1, 128), f32)

    def merge(ref):
        tops = ref[:, :8, :]
        top = jnp.max(tops, axis=0)
        return top, jnp.sum(ref[:, 8:, :] * jnp.exp(tops - top[None]), axis=0)

    phase("lse_line")
    got = rest(lse_x, nx2)
    for p in LINE:
        got.send(lse_x.at[xid], lse_x.at[xid], links.at_line(*p))
    got.wait()
    top, mass = merge(lse_x)
    lse_y[yid, :8, :] = top
    lse_y[yid, 8:, :] = mass
    phase("lse_plane")
    got = rest(lse_y, nyz)
    for p in PLANE:
        got.send(lse_y.at[yid], lse_y.at[yid], links.at_plane(*p))
    got.wait()
    top, mass = merge(lse_y)
    norm_ref[...] = top + jnp.log(mass)
    phase("finish")
    links.finish()
    phase.close()


def whole_step(hidden, freq, lens, k_cache, v_cache, g_attn, w_query, w_key, w_value,
               w_gate, w_up, w_out, w_down, g_final, embedding):
    total_rows, chunk = hidden.shape
    own_rows, seq, head = k_cache.shape
    rows = total_rows // (NY * NZ)
    vocab_own = embedding.shape[0] // (2 * NX)
    take = (vocab_own + 6 + 15) // 16 * 16
    half = chunk // 2
    qc = w_query.shape[1]
    ff = w_gate.shape[1] // (2 * NX)
    f32, bf16 = jnp.float32, jnp.bfloat16
    nyz, nx2, pad = NY * NZ, 2 * NX, 8
    vmem = pl.BlockSpec(memory_space=pltpu.VMEM)
    hbm = pl.BlockSpec(memory_space=pl.ANY)
    V = pltpu.VMEM
    return pl.pallas_call(
        lambda *refs: step_kernel(vocab_own, own_rows, *refs),
        out_shape=(jax.ShapeDtypeStruct((pad, head), bf16), jax.ShapeDtypeStruct((pad, head), bf16),
                   jax.ShapeDtypeStruct((take, total_rows), f32), jax.ShapeDtypeStruct((pad, head), f32)),
        in_specs=[vmem] * 5 + [hbm] * 10,
        out_specs=(vmem,) * 4,
        scratch_shapes=[
            V((chunk, qc), bf16), V((chunk, head), bf16), V((chunk, head), bf16),
            V((own_rows, seq, head), bf16), V((own_rows, seq, head), bf16),
            V((nx2 * ff, chunk), bf16), V((NZ * qc, chunk), bf16), V((NY, rows, chunk), f32), V((3, rows, chunk), f32), V((2, total_rows, NX * chunk), bf16), V((2, NX * chunk, 2 * ff), bf16),
            V((qc, chunk), bf16), V((2, head, NX * chunk), bf16),
            V((nx2 * nyz * pad, total_rows), bf16), V((NY * rows, nx2 * NY * pad), bf16),
            V((nx2, nyz * pad // 4, head), bf16), V((nx2, nyz * pad // 4, head), bf16),
            V((nyz, pad, qc), f32), V((nyz, pad, qc), f32),
            V((nx2, pad, 2 * head), f32), V((nx2, pad, 2 * head), f32),
            V((NZ, NY, pad, qc), f32), V((NY, NZ, pad, qc), f32), V((nx2, NY * pad, NZ * qc), bf16),
            V((NZ, NY * rows, nx2 * ff), bf16),
            V((NZ, NY, rows, chunk), f32),
            V((3, NZ, rows, half), f32), V((3, NY, rows, half), f32), V((3, rows, half), f32), V((3, rows, half), f32),
            V((NZ, rows, half), f32), V((NY, rows, half), f32),
            V((NX, rows, chunk), bf16), V((2, rows, 128), f32), V((NX, rows, chunk), f32), V((2, rows, 128), f32),
            V((NX, 8, chunk), f32),
            V((2, total_rows, NX * chunk), bf16), V((2, take, NX * chunk), bf16),
            V((2, 2, chunk, ff), bf16), V((2, 2, (take // 2 + 15) // 16 * 16, chunk), bf16),
            V((nx2, 16, 128), f32), V((nx2, 16, 128), f32), V((nyz, 16, 128), f32),
            pltpu.SemaphoreType.DMA((SENDS,)), pltpu.SemaphoreType.DMA((TAGS,)), pltpu.SemaphoreType.DMA((10,)),
        ],
        compiler_params=pltpu.CompilerParams(
            collective_id=1, has_side_effects=True, vmem_limit_bytes=60 << 20),
        name="decode_step",
    )(hidden, g_attn[None, :], g_final[None, :], freq, lens, k_cache, v_cache,
      w_query, w_key, w_value, w_out, w_gate, w_up, w_down, embedding)


def solution(mesh):
    row_spec = P(("dp", "yax", "xax"))

    def local_step(hidden, cache_len, k_cache, v_cache, g_attn, w_query, w_key, w_value,
                   w_gate, w_up, w_out, w_down, g_final, embedding):
        rows = hidden.shape[0]
        half_dim = k_cache.shape[2] // 2
        inv_freq = ROPE_BASE ** (-(np.arange(half_dim, dtype=np.float64) * 2.0) / (2 * half_dim))
        freq = np.concatenate([inv_freq, inv_freq])[None, :].astype(np.float32)
        key_own, value_own, logits_wide, norm_tile = whole_step(
            hidden, freq, cache_len.reshape(rows // 128, 128), k_cache, v_cache, g_attn, w_query, w_key, w_value,
            w_gate, w_up, w_out, w_down, g_final, embedding)
        own_rows = k_cache.shape[0]
        vocab_own = embedding.shape[0] // (CORES * NX)
        first = vocab_own * lax.axis_index("xax")
        logits = lax.dynamic_slice_in_dim(logits_wide, first - first // 8 * 8, vocab_own, axis=0)
        log_norm = norm_tile[:rows // 128].reshape(rows)
        return key_own[:own_rows], value_own[:own_rows], (logits - log_norm).T, log_norm

    in_specs = (P("dp", "xax"), P("dp"), row_spec, row_spec, P("xax"), P("xax", "yax"),
                P("xax", None), P("xax", None), P("xax", "yax"), P("xax", "yax"),
                P("yax", "xax"), P("yax", "xax"), P("xax"), P("yax", "xax"))
    out_specs = (row_spec, row_spec, P("dp", ("yax", "xax")), P("dp"))
    return jax.shard_map(local_step, mesh=mesh, in_specs=in_specs, out_specs=out_specs, check_vma=False)
```

```python
import itertools

import jax
import jax.numpy as jnp
import numpy as np
from jax import lax
from jax.experimental import pallas as pl
from jax.experimental.pallas import tpu as pltpu
from jax.sharding import PartitionSpec as P

EPS = 1e-6
ROPE_BASE = 10000.0
MESH_ID = pl.DeviceIdType.MESH
NY = NZ = NX = 4
CORES = 2
POOL, SENDS, TAGS = 24, 59, 86
HOPS = (1, 3, 2)
FAR_FIRST = (2, 1, 3)
LINE = [(0, 1), (1, 0), (3, 0), (1, 1), (3, 1), (2, 0), (2, 1)]
NEAR = LINE[1:5]
NT = (((1,), (1,)), ((), ()))
PLANE = [(dz, dy) for dz in range(NZ) for dy in range(NY) if dz or dy]


class Group:
    def __init__(self, links, whole):
        self.links, self.whole = links, whole
        self.tag, self.sem = next(links.tags), next(links.slow)
        links.groups.append(self)

    def send(self, src, dst, where):
        pltpu.make_async_remote_copy(
            src_ref=src, dst_ref=dst, send_sem=self.links.send_sem.at[self.sem],
            recv_sem=self.links.recv_sem.at[self.tag], device_id=where, device_id_type=MESH_ID).start()

    def wait(self):
        pltpu.make_async_copy(self.whole, self.whole, self.links.recv_sem.at[self.tag]).wait()

    def wait_sent(self):
        pltpu.make_async_copy(self.whole, self.whole, self.links.send_sem.at[self.sem]).wait()


class Phases:
    def __init__(self):
        self.open = None

    def __call__(self, name):
        self.close()
        self.open = jax.named_scope(name)
        self.open.__enter__()

    def close(self):
        if self.open is not None:
            self.open.__exit__(None, None, None)
        self.open = None


class Links:
    def __init__(self, send_sem, recv_sem):
        self.send_sem, self.recv_sem = send_sem, recv_sem
        self.tags, self.slow, self.fast = itertools.count(), itertools.count(POOL), []
        self.pending, self.groups = [], []
        self.y_idx = lax.axis_index("yax")
        self.x_idx = lax.axis_index("xax")
        self.z, self.y = self.y_idx // NY, self.y_idx % NY
        self.chip, self.core = self.x_idx // CORES, self.x_idx % CORES

    def at_plane(self, dz, dy):
        return {"yax": (self.z + dz) % NZ * NY + (self.y + dy) % NY, "xax": self.x_idx}

    def slot_rows(self, dz, dy, rows):
        slot = (self.z + dz) % NZ * NY + (self.y + dy) % NY
        return pl.ds(pl.multiple_of(slot * rows, rows), rows)

    def line_id(self, dx, oc):
        core = 1 - self.core if oc else self.core
        return (self.chip + dx) % NX * CORES + core

    def at_line(self, dx, oc):
        return {"yax": self.y_idx, "xax": self.line_id(dx, oc)}

    def send(self, src, dst, where, tag=None, long=False):
        tag = next(self.tags) if tag is None else tag
        if long:
            sem = next(self.slow)
        else:
            sem = len(self.fast) % POOL
            if len(self.fast) >= POOL:
                self.fast[-POOL].wait_send()
        copy = pltpu.make_async_remote_copy(
            src_ref=src, dst_ref=dst, send_sem=self.send_sem.at[sem], recv_sem=self.recv_sem.at[tag],
            device_id=where, device_id_type=MESH_ID)
        copy.start()
        (self.pending if long else self.fast).append(copy)
        return copy

    def finish(self):
        for copy in self.pending + self.fast[-POOL:]:
            copy.wait_send()
        for group in self.groups:
            group.wait_sent()

    def barrier(self):
        barrier = pltpu.get_barrier_semaphore()
        peers = [self.at_line(*p) for p in LINE] + [self.at_plane(*p) for p in PLANE]
        for peer in peers:
            pl.semaphore_signal(barrier, inc=1, device_id=peer, device_id_type=MESH_ID)
        pl.semaphore_wait(barrier, len(peers))


def lane_sum(v):
    return jnp.sum(v, axis=-1, keepdims=True)


def plane_gather(links, buf, tags, hook, crossing, start):
    cols = buf.shape[-1]
    rows = buf.shape[1] // (NY * NZ)
    span = (cols - start) // 2
    partner = links.at_line(0, 1)

    class Part:
        def __init__(self, index):
            self.index, self.lo, self.got = index, start + index * span, {}

        def order(self, du, dv):
            return (du, dv) if self.index else (dv, du)

        def block(self, at, half=0, piece=None):
            width = span if piece is None else span // 2
            lo = self.lo if not piece else self.lo + width
            return buf.at[half, links.slot_rows(*self.order(*at), rows), pl.ds(lo, width)]

        def push(self, name, at, to, piece=None):
            ref = self.block(at, piece=piece)
            self.got[name] = links.send(ref, ref, links.at_plane(*self.order(*to)), next(tags))

        def spread(self, k, at):
            self.push(("v+", k), at, (0, 1))
            self.push(("v-", k), at, (0, -1))

        def give(self, at):
            crossing.send(self.block(at), self.block(at, half=1), partner)

        def wait(self, name):
            self.got[name].wait_recv()

    parts = [Part(index) for index in range(2)]
    offset = (0, -1, 1, 2)
    for p in parts:
        p.push("u+", (0, 0), (1, 0))
        p.push("u-", (0, 0), (-1, 0))
        p.spread(0, (0, 0))
    for p in parts:
        p.give((0, 0))
    for k, name in enumerate(("u+", "u-"), 1):
        for p in parts:
            p.wait(name)
            at = (offset[k], 0)
            p.push(("far", k), at, (-offset[k], 0), piece=k - 1)
            p.spread(k, at)
            p.give(at)
    hook()

    def arrive(p, k):
        for name, step in (("v+", -1), ("v-", 1)):
            p.wait((name, k))
            at = (offset[k], step)
            if (name == "v+") == (k in (0, 3)):
                p.push(("relay", k), at, (0, -step))
            p.give(at)

    for p in parts:
        arrive(p, 0)
    for p in parts:
        p.wait(("far", 1))
        p.wait(("far", 2))
        p.spread(3, (2, 0))
        p.give((2, 0))
    for k in range(1, len(offset)):
        for p in parts:
            arrive(p, k)
    for k in range(len(offset)):
        for p in parts:
            p.wait(("relay", k))
            p.give((offset[k], 2))


def norm_gather(links, own_slot, gain_buf, which, xbuf, stat, out, base, hook, skip=0):
    own_slot()
    rows, chunk = xbuf.shape[1:]
    tags = itertools.count(base)
    line = [links.send(xbuf.at[0], xbuf.at[NX - dx], links.at_line(dx, 0), next(tags)) for dx in FAR_FIRST]
    yield
    phase = Phases()
    for n, c in enumerate(line):
        phase(f"ng_line{which}_{n}")
        c.wait_recv()
    phase("ng_stats")
    held = xbuf[...].astype(jnp.float32)
    count = NX * chunk
    mean = lane_sum(jnp.sum(held, axis=0)) / count
    dev = held - mean[None]
    square = lane_sum(jnp.sum(dev * dev, axis=0))
    lane = lax.broadcasted_iota(jnp.int32, (rows, 128), 1)
    stat[0] = jnp.where(lane == 0, mean, square)
    links.send(stat.at[0], stat.at[1], links.at_line(0, 1), next(tags)).wait_recv()
    other_mean, other_square = stat[1, :, 0:1], stat[1, :, 1:2]
    both = (mean + other_mean) * 0.5
    gap = mean - other_mean
    var = (square + other_square + gap * gap * (count * 0.5)) / (2 * count)
    scale = lax.rsqrt(var + EPS)
    for e in range(skip, NX):
        out[0, links.slot_rows(0, 0, rows), e * chunk:(e + 1) * chunk] = (
            (xbuf[e].astype(jnp.float32) - both) * scale * gain_buf[e, which:which + 1, :]).astype(jnp.bfloat16)
    phase("ng_plane")
    crossing = Group(links, out.at[1])
    plane_gather(links, out, tags, lambda: hook(crossing), crossing, skip * chunk)
    phase.close()
    yield crossing


def step_kernel(vocab_own, own_rows, hid_ref, gain_a, gain_f, freq_ref, len_ref, k_hbm, v_hbm,
                wq_hbm, wk_hbm, wv_hbm, wo_ref, wg_ref, wu_ref, wd_hbm, emb_ref,
                knew_ref, vnew_ref, z_ref, norm_ref,
                wq_ref, wk_ref, wv_ref, k_buf, v_buf, wd_buf, wo_all, att, rc, gu_acc, n_buf, w_buf, wq_t, wq_buf, sel, sel_t, qx, qr, qy, qf,
                kvp, kvr, o_buf, o_got, o_all, act,
                part, ra1, rb1, ra2, rb2, acc_a, acc_b, xbuf, stat, xbuf2, stat2, gains, f_buf, emb_buf,
                w_relay, emb_relay, row_stats, lse_x, lse_y, send_sem, recv_sem, local_sem):
    links = Links(send_sem, recv_sem)
    phase = Phases()
    f32, bf16 = jnp.float32, jnp.bfloat16
    z, y, xid, yid = links.z, links.y, links.x_idx, links.y_idx
    total_rows, chunk = hid_ref.shape
    rows = total_rows // (NY * NZ)
    here_rows = links.slot_rows(0, 0, rows)
    half = chunk // 2
    nx2, nyz = 2 * NX, NY * NZ
    group = NY * rows
    head = 128
    pad = 8
    partner = links.at_line(0, 1)
    line_id = links.line_id
    gather_tags = len(HOPS) + 1 + len(PLANE) * CORES + CORES
    gather_base = [next(links.tags) for _ in range(gather_tags)][0]

    def dot(a, b):
        return jnp.dot(a, b, preferred_element_type=f32)

    def dot_t(a, b):
        return lax.dot_general(a, b, NT, preferred_element_type=f32)

    def rest(ref, n):
        return Group(links, ref.at[0:n - 1])

    local = []

    def fetch(src, dst):
        copy = pltpu.make_async_copy(src, dst, local_sem.at[len(local)])
        copy.start()
        local.append(copy)
        return copy

    ff = wg_ref.shape[1] // nx2

    def w_piece(ref, dx, oc):
        return ref.at[:, pl.ds(pl.multiple_of(line_id(dx, oc) * ff, ff), ff)]

    def w_slot(which, dx, oc):
        back = (NX - dx) % NX
        return w_buf.at[int(oc), pl.ds(back * chunk, chunk), pl.ds(which * ff, ff)]

    take = emb_buf.shape[1]

    def emb_start(xi):
        return pl.multiple_of(vocab_own * xi // pad * pad, pad)

    def emb_piece(dx, oc):
        return emb_ref.at[pl.ds(emb_start(line_id(dx, oc)), take), :]

    def emb_slot(dx, oc):
        return emb_buf.at[int(oc), :, pl.ds((NX - dx) % NX * chunk, chunk)]

    near_part = (take // 2 + 15) // 16 * 16
    far_parts = ((0, near_part), (near_part, take - near_part))

    def emb_half(oc, way):
        first, size = far_parts[way]
        return emb_ref.at[pl.ds(pl.multiple_of(emb_start(line_id(2, oc)) + first, pad), size), :]

    def emb_mid(oc, way):
        return emb_relay.at[way, oc, pl.ds(0, far_parts[way][1])]

    def emb_far_slot(oc, way):
        return emb_buf.at[int(oc), pl.ds(*far_parts[way]), pl.ds(2 * chunk, chunk)]

    got_wq = fetch(wq_hbm, wq_ref)
    own_w = [fetch(w_piece(wg_ref, 0, 0), w_slot(0, 0, 0)), fetch(w_piece(wu_ref, 0, 0), w_slot(1, 0, 0))]
    got_kv = [fetch(k_hbm, k_buf), fetch(v_hbm, v_buf)]
    got_wkv = [fetch(wk_hbm, wk_ref), fetch(wv_hbm, wv_ref)]
    got_wd = fetch(wd_hbm, wd_buf)
    own_emb = fetch(emb_piece(0, 0), emb_slot(0, 0))

    qc = wq_ref.shape[1]
    qs = qc // nx2
    per = head // qs
    wq_buf[...] = jnp.zeros(wq_buf.shape, bf16)

    phase("row_stats")
    eye = lax.broadcasted_iota(jnp.int32, (head, head), 0) == lax.broadcasted_iota(jnp.int32, (head, head), 1)
    blocks = total_rows // head

    def block_rows(b):
        return slice(b * head, (b + 1) * head)

    def to_row(v):
        return jnp.sum(jnp.where(eye, v, 0.0), axis=0, keepdims=True)

    def to_col(v):
        return lane_sum(jnp.where(eye, v, 0.0))

    row_stats[xid] = jnp.zeros((2 * pad, head), f32)
    for b in range(blocks):
        held = hid_ref[block_rows(b), :].astype(f32)
        mean = lane_sum(held) / chunk
        dev = held - mean
        row_stats[xid, b:b + 1, :] = to_row(mean)
        row_stats[xid, pad + b:pad + b + 1, :] = to_row(lane_sum(dev * dev))

    phase("barrier")
    links.barrier()

    phase("front_send")
    gains[0, 0:1, :] = gain_a[...]
    gains[0, 1:2, :] = gain_f[...]
    gains[0, 2:, :] = jnp.zeros((6, chunk), f32)

    def own_input():
        xbuf[0] = hid_ref[here_rows, :]

    w_far, emb_far = [], []
    w_got = [Group(links, w_buf.at[0, 0:2 * chunk]), Group(links, w_buf.at[1, 0:(NX - 1) * chunk])]
    w_last = Group(links, w_buf.at[0, 0:2 * chunk])
    emb_got = [Group(links, emb_buf.at[0, :, 0:(NX - 1) * chunk]), Group(links, emb_buf.at[1])]
    ways = [(way, hop, oc) for oc in (0, 1) for way, hop in enumerate(HOPS[:2])]

    def forward_weights():
        for (way, hop, oc), c in zip(ways, w_far):
            c.wait_recv()
            w_last.send(w_relay.at[way, oc], w_buf.at[oc, pl.ds(2 * chunk, chunk), pl.ds(way * ff, ff)],
                        links.at_line(hop, oc))

    def emb_out(some):
        for way, hop, oc in some:
            emb_far.append(links.send(emb_half(oc, way), emb_mid(oc, way), links.at_line(hop, 0), long=True))

    def emb_on(some, arrived):
        for (way, hop, oc), c in zip(some, arrived):
            c.wait_recv()
            emb_got[oc].send(emb_mid(oc, way), emb_far_slot(oc, way), links.at_line(hop, oc))

    def amid(crossing):
        forward_weights()
        stats_got.wait()
        means = row_stats[:, :pad, :]
        mean = jnp.sum(means, axis=0) / nx2
        gap = means - mean[None]
        square = jnp.sum(row_stats[:, pad:, :], axis=0) + jnp.sum(gap * gap, axis=0) * chunk
        scale = lax.rsqrt(square / (nx2 * chunk) + EPS)
        for b in range(blocks):
            n_buf[0, block_rows(b), 0:chunk] = (
                (hid_ref[block_rows(b), :].astype(f32) - to_col(mean[b:b + 1, :])) * to_col(scale[b:b + 1, :])
                * gains[0, 0:1, :]).astype(bf16)
        own = n_buf.at[0, :, 0:chunk]
        crossing.send(own, n_buf.at[1, :, 0:chunk], partner)

    front = norm_gather(links, own_input, gains, 0, xbuf, stat, n_buf, gather_base, amid, skip=1)
    next(front)
    gain_got = rest(gains, NX)
    for dx in HOPS:
        gain_got.send(gains.at[0], gains.at[NX - dx], links.at_line(dx, 0))
    stats_got = rest(row_stats, nx2)
    for p in LINE:
        stats_got.send(row_stats.at[xid], row_stats.at[xid], links.at_line(*p))
    for way, hop, oc in ways:
        w_far.append(links.send(w_piece((wg_ref, wu_ref)[way], 2, oc), w_relay.at[way, oc], links.at_line(hop, 0),
                                long=True))

    got_wq.wait()
    eye_q = (lax.broadcasted_iota(jnp.int32, (qc, qc), 0) == lax.broadcasted_iota(jnp.int32, (qc, qc), 1))
    wq_t[...] = dot_t(eye_q.astype(bf16), wq_ref[...]).astype(bf16)
    wq_buf[0, 0:qs, 0:chunk] = wq_t[pl.ds(pl.multiple_of(xid * qs, qs), qs), :]

    def wq_rows(dx, oc):
        return wq_t.at[pl.ds(pl.multiple_of(line_id(dx, oc) * qs, qs), qs), :]

    def wq_slot(dx, oc):
        return wq_buf.at[oc, pl.ds(0, qs), pl.ds((NX - dx) % NX * chunk, chunk)]

    wq_got = Group(links, wq_t.at[0:qc - qs])
    for dx, oc in LINE:
        wq_got.send(wq_rows(dx, oc), wq_slot(dx, oc), links.at_line(dx, oc))
    for which, ref in enumerate((wg_ref, wu_ref)):
        for dx, oc in LINE[:1] + NEAR:
            w_got[oc].send(w_piece(ref, dx, oc), w_slot(which, dx, oc), links.at_line(dx, oc))

    phase("selections")
    r_id = lax.broadcasted_iota(jnp.int32, (nx2 * nyz * pad, 1), 0)
    r_j = r_id % pad
    r_src = jnp.where(r_j < own_rows, r_id // pad % nyz * rows + r_id // (pad * nyz) * own_rows + r_j, -1)
    s_id = lax.broadcasted_iota(jnp.int32, (1, total_rows), 1)
    sel[...] = jnp.where(r_src == s_id, 1.0, 0.0).astype(bf16)
    t_id = lax.broadcasted_iota(jnp.int32, (group, 1), 0)
    t_in = t_id % rows
    t_src = t_in // own_rows * (NY * pad) + t_id // rows * pad + t_in % own_rows
    u_id = lax.broadcasted_iota(jnp.int32, (1, nx2 * NY * pad), 1)
    sel_t[...] = jnp.where(t_src == u_id, 1.0, 0.0).astype(bf16)
    k_id = lax.broadcasted_iota(jnp.int32, (nx2 * pad, rows), 0)
    k_src = jnp.where(k_id % pad < own_rows, k_id // pad * own_rows + k_id % pad, -1)
    sel_kv = jnp.where(k_src == lax.broadcasted_iota(jnp.int32, (nx2 * pad, rows), 1), 1.0, 0.0).astype(bf16)

    phase.close()
    gain_got.wait()
    lane = lax.broadcasted_iota(jnp.int32, (1, head), 1)
    lengths = []
    for b in range(own_rows):
        index = (yid * nx2 + xid) * own_rows + b
        row = len_ref[pl.ds(index // head, 1), :].astype(f32)
        lengths.append(lane_sum(jnp.where(lane == index % head, row, 0.0)))
    lengths = jnp.concatenate(lengths + lengths[:pad - own_rows], axis=0)
    angles = lengths * freq_ref[...]
    cos_all = jnp.cos(angles)
    sin_all = jnp.sin(angles) * jnp.where(lane < head // 2, -1.0, 1.0)

    crossing = next(front)
    phase("ng_cross")
    crossing.wait()
    phase("kv_part")

    for c in got_wkv:
        c.wait()
    n_own = dot(sel_kv, n_buf[0, links.slot_rows(0, 0, rows), 0:chunk]).astype(bf16)
    kvp[:, :, :head] = dot(n_own, wk_ref[...]).reshape(nx2, pad, head)
    kvp[:, :, head:] = dot(n_own, wv_ref[...]).reshape(nx2, pad, head)
    kv_got = rest(kvr, nx2)
    for p in LINE:
        kv_got.send(kvp.at[line_id(*p)], kvr.at[xid], links.at_line(*p))
    kvr[xid] = kvp[xid]

    phase("wait_wq")
    wq_got.wait()
    phase("q_mm")
    q_all = jnp.concatenate([
        (dot_t(n_buf[0, i * group:(i + 1) * group, :], wq_buf[0])
         + dot_t(n_buf[1, i * group:(i + 1) * group, :], wq_buf[1])).astype(bf16) for i in range(NZ)], axis=0)
    span = nyz * pad
    for i in range(nx2):
        chosen = dot(sel[i * span:(i + 1) * span, :], q_all)
        quarter = span // per
        packed = chosen[:quarter, :]
        for g in range(1, per):
            packed = packed + pltpu.roll(chosen[g * quarter:(g + 1) * quarter, :], g * qs, 1)
        qx[i] = packed.astype(bf16)
    q_got = rest(qr, nx2)
    for p in LINE:
        q_got.send(qx.at[line_id(*p)], qr.at[xid], links.at_line(*p))
    qr[xid] = qx[xid]

    phase("wait_w")
    for c in own_w:
        c.wait()
    for c in w_got:
        c.wait()
    phase("gate_up")

    def act_at(k, dx):
        return act.at[(z + k) % NZ, :, pl.ds(pl.multiple_of(line_id(dx, 0) * ff, ff), ff)]

    def act_out(k, dx, to_dx):
        return links.send(act_at(k, dx), act_at(k, dx), links.at_line(to_dx, 0))

    def act_give(k, dx):
        cross[k].send(act_at(k, dx), act_at(k, dx), partner)

    turns = (2, 1, 3, 0)
    early, late = turns[:2], turns[2:]
    near_act, far_act = {}, {}
    cross = {k: Group(links, act.at[0, :, 0:NX * ff]) for k in turns}
    def group_rows(k):
        return pl.ds(pl.multiple_of((z + k) % NZ * group, group), group)

    far = slice(2 * chunk, (NX - 1) * chunk)

    def over(k, part_cols):
        return dot(n_buf[0, group_rows(k), part_cols], w_buf[0, part_cols, :]) + dot(
            n_buf[1, group_rows(k), part_cols], w_buf[1, part_cols, :])

    for k in turns:
        gu_acc[k] = over(k, slice(0, far.start)) + over(k, slice(far.stop, NX * chunk))
    phase("wait_w_far")
    w_last.wait()
    phase("gate_up_far")
    for k in turns:
        both = (gu_acc[k] + over(k, far)).astype(bf16).astype(f32)
        gate, up = both[:, :ff], both[:, ff:]
        act_at(k, 0)[...] = (gate * jax.nn.sigmoid(gate) * up).astype(bf16)
        near_act[k] = [(dx, act_out(k, 0, dx)) for dx in HOPS[:2]]
        act_give(k, 0)

    def act_pass(k):
        for dx, c in near_act[k]:
            c.wait_recv()
            if (k in early) == (dx == 1):
                far_act[k] = act_out(k, NX - dx, dx)
            act_give(k, NX - dx)

    low, high = pl.ds(0, half), pl.ds(half, half)
    first_a, first_b = Group(links, ra1), Group(links, rb1)

    def act_use(k):
        cross[k].wait()
        g = (z + k) % NZ
        part[g] = dot(act[g], wd_buf[...]).reshape(NY, rows, chunk)
        if k:
            first_b.send(part.at[g, :, :, high], rb1.at[k - 1], links.at_plane(k, 0))

    def along_y(k):
        g = (z + k) % NZ
        for d in early + late[:1]:
            first_a.send(part.at[g, (y + d) % NY, :, low], ra1.at[d - 1, g], links.at_plane(0, d))

    def act_far(ks):
        for k in ks:
            far_act[k].wait_recv()
            act_give(k, 2)

    phase("wait_q")
    q_got.wait()
    phase("q_sum")
    lane_group = lax.broadcasted_iota(jnp.int32, (1, head), 1) // qs
    for j in range(qc // head):
        came = [qr[j * per + i].astype(f32) for i in range(per)]
        for g in range(per):
            piece = jnp.zeros((span // per, head), f32)
            for i in range(per):
                piece = piece + jnp.where(lane_group == i, pltpu.roll(came[i], (i - g) % per * qs, 1), 0.0)
            qy[g * per:(g + 1) * per, :, j * head:(j + 1) * head] = piece.reshape(per, pad, head)

    def plane_id(dz, dy):
        return (z + dz) % NZ * NY + (y + dy) % NY

    y_got = rest(qf, nyz)
    for p in PLANE:
        y_got.send(qy.at[plane_id(*p)], qf.at[yid], links.at_plane(*p))
    qf[yid] = qy[yid]

    def wo_rows(dz):
        return wo_all.at[pl.ds(pl.multiple_of((z + dz) % NZ * qc, qc), qc), :]

    wo_got = Group(links, wo_all.at[0:(NZ - 1) * qc])
    for d in HOPS:
        wo_got.send(wo_ref, wo_rows(0), links.at_plane(d, 0))
    own_wo = fetch(wo_ref, wo_rows(0))

    phase("act_pass")
    for k in early:
        act_pass(k)
    emb_out(ways[:2])
    phase("wait_kv")
    kv_got.wait()
    kv_sum = kvr[0]
    for i in range(1, nx2):
        kv_sum = kv_sum + kvr[i]
    kv_new = kv_sum.astype(bf16).astype(f32)

    def turn(v, b=None):
        cos, sin = (cos_all, sin_all) if b is None else (cos_all[b:b + 1, :], sin_all[b:b + 1, :])
        return (v * cos + pltpu.roll(v, head // 2, 1) * sin).astype(bf16)

    k_new = turn(kv_new[:, :head])
    knew_ref[...] = k_new
    vnew_ref[...] = kv_new[:, head:].astype(bf16)
    k_row, v_row = k_new.astype(f32), kv_new[:, head:]
    phase("act_pass2")
    for k in late:
        act_pass(k)
    phase("wait_qy")
    for c in got_kv:
        c.wait()
    y_got.wait()
    phase("attention")
    seq = k_buf.shape[1]
    score_scale = head ** -0.5
    position = lax.broadcasted_iota(jnp.int32, (1, seq), 1).astype(f32)
    o_buf[...] = jnp.zeros(o_buf.shape, f32)
    for b in range(own_rows):
        q_b = jnp.concatenate([turn(qf[:, b, j * head:(j + 1) * head], b) for j in range(qc // head)], axis=0)
        scores = dot_t(q_b, k_buf[b]) * score_scale
        score_new = lane_sum(q_b.astype(f32) * k_row[b:b + 1, :]) * score_scale
        valid = position < lengths[b:b + 1, :]
        top = jnp.maximum(jnp.max(jnp.where(valid, scores, -jnp.inf), axis=-1, keepdims=True), score_new)
        weights = jnp.where(valid, jnp.exp(scores - top), 0.0)
        weight_new = jnp.exp(score_new - top)
        denom = lane_sum(weights) + weight_new
        o_b = dot((weights / denom).astype(bf16), v_buf[b])
        o_b = o_b + (weight_new / denom).astype(bf16).astype(f32) * v_row[b:b + 1, :]
        o_b = o_b.astype(bf16).astype(f32)
        for j in range(qc // head):
            o_buf[:, :, b, j * head:(j + 1) * head] = o_b[j * nyz:(j + 1) * nyz, :].reshape(NZ, NY, head)
    o_back = rest(o_got, NY)
    for d in HOPS:
        o_back.send(o_buf.at[:, (y + d) % NY], o_got.at[y], links.at_plane(0, d))
    phase("act_early")
    act_far(early)
    got_wd.wait()
    for k in early:
        act_use(k)
        along_y(k)
    o_got[y] = o_buf[:, y]

    phase("wait_oy")
    o_back.wait()
    for i in range(NZ):
        o_all[xid, :, i * qc:(i + 1) * qc] = o_got[:, i].reshape(NY * pad, qc).astype(bf16)
    o_here = o_all.at[xid]
    o_line = [links.send(o_here, o_here, links.at_line(dx, 0)) for dx in HOPS]
    o_cross = rest(o_all, NX + 1)
    o_cross.send(o_here, o_here, partner)
    emb_out(ways[2:])
    emb_got[1].send(emb_piece(0, 1), emb_slot(0, 1), partner)
    phase("act_late")
    act_far(late)
    for k in late:
        act_use(k)
        along_y(k)
    emb_on(ways[:2], emb_far[:2])
    phase("wait_o")
    for dx, c in zip(HOPS, o_line):
        c.wait_recv()
        came = o_all.at[line_id(NX - dx, 0)]
        o_cross.send(came, came, partner)
    wo_got.wait()
    own_wo.wait()
    o_cross.wait()
    phase("out_mm")
    o_nat = dot(sel_t[...], o_all[...].reshape(nx2 * NY * pad, NZ * qc)).astype(bf16)
    att[...] = dot(o_nat, wo_all[...]).reshape(NY, rows, chunk)
    att_got = Group(links, rc)
    for d in HOPS:
        att_got.send(att.at[(y + d) % NY], rc.at[d - 1], links.at_plane(0, d))

    phase("wait_rs1")
    first_b.wait()
    acc_b[...] = (part[z, :, :, half:] + rb1[0]) + (rb1[1] + rb1[2])
    second = [Group(links, rb2), Group(links, ra2)]
    for d in HOPS:
        second[0].send(acc_b.at[(y + d) % NY], rb2.at[d - 1], links.at_plane(0, d))
    phase("wait_rs1a")
    first_a.wait()
    acc_a[...] = (part[:, y, :, :half] + ra1[0]) + (ra1[1] + ra1[2])
    for d in HOPS:
        second[1].send(acc_a.at[(z + d) % NZ], ra2.at[d - 1], links.at_plane(d, 0))
    phase("wait_att")
    att_got.wait()
    phase("wait_rs2")
    for c in second:
        c.wait()
    phase("rs_sum2")
    def own_residual():
        res = hid_ref[here_rows, :].astype(f32) + ((att[y] + rc[0]) + (rc[1] + rc[2]))
        xbuf2[0, :, :half] = res[:, :half] + ((acc_a[z] + ra2[0]) + (ra2[1] + ra2[2]))
        xbuf2[0, :, half:] = res[:, half:] + ((acc_b[y] + rb2[0]) + (rb2[1] + rb2[2]))

    back = norm_gather(links, own_residual, gains, 1, xbuf2, stat2, f_buf, gather_base, lambda crossing: None)
    next(back)
    emb_on(ways[2:], emb_far[2:])
    for dx, oc in NEAR:
        emb_got[oc].send(emb_piece(dx, oc), emb_slot(dx, oc), links.at_line(dx, oc))
    phase.close()
    crossing = next(back)
    phase("wait_emb")
    own_emb.wait()
    for c in emb_got:
        c.wait()

    phase("logits")
    wide_n = 256
    for h in range(CORES):
        if h:
            crossing.wait()
        for i in range(total_rows // wide_n):
            cols = slice(i * wide_n, (i + 1) * wide_n)
            term = dot_t(emb_buf[h], f_buf[h, cols, :])
            z_ref[:, cols] = z_ref[:, cols] + term if h else term

    phase("lse_own")
    shift = vocab_own * xid - emb_start(xid)
    vid = lax.broadcasted_iota(jnp.int32, (take, 1), 0)
    own = (vid >= shift) & (vid < shift + vocab_own)
    for b in range(blocks):
        zb = jnp.where(own, z_ref[:, b * 128:(b + 1) * 128], -jnp.inf)
        top = jnp.max(zb, axis=0, keepdims=True)
        lse_x[xid, b:b + 1, :] = top
        lse_x[xid, 8 + b:9 + b, :] = jnp.sum(jnp.exp(zb - top), axis=0, keepdims=True)
    for b in range(blocks, 8):
        lse_x[xid, b:b + 1, :] = jnp.zeros((1, 128), f32)
        lse_x[xid, 8 + b:9 + b, :] = jnp.ones((1, 128), f32)

    def merge(ref):
        tops = ref[:, :8, :]
        top = jnp.max(tops, axis=0)
        return top, jnp.sum(ref[:, 8:, :] * jnp.exp(tops - top[None]), axis=0)

    phase("lse_line")
    got = rest(lse_x, nx2)
    for p in LINE:
        got.send(lse_x.at[xid], lse_x.at[xid], links.at_line(*p))
    got.wait()
    top, mass = merge(lse_x)
    lse_y[yid, :8, :] = top
    lse_y[yid, 8:, :] = mass
    phase("lse_plane")
    got = rest(lse_y, nyz)
    for p in PLANE:
        got.send(lse_y.at[yid], lse_y.at[yid], links.at_plane(*p))
    got.wait()
    top, mass = merge(lse_y)
    norm_ref[...] = top + jnp.log(mass)
    phase("finish")
    links.finish()
    phase.close()


def whole_step(hidden, freq, lens, k_cache, v_cache, g_attn, w_query, w_key, w_value,
               w_gate, w_up, w_out, w_down, g_final, embedding):
    total_rows, chunk = hidden.shape
    own_rows, seq, head = k_cache.shape
    rows = total_rows // (NY * NZ)
    vocab_own = embedding.shape[0] // (2 * NX)
    take = (vocab_own + 6 + 15) // 16 * 16
    half = chunk // 2
    qc = w_query.shape[1]
    ff = w_gate.shape[1] // (2 * NX)
    f32, bf16 = jnp.float32, jnp.bfloat16
    nyz, nx2, pad = NY * NZ, 2 * NX, 8
    vmem = pl.BlockSpec(memory_space=pltpu.VMEM)
    hbm = pl.BlockSpec(memory_space=pl.ANY)
    V = pltpu.VMEM
    return pl.pallas_call(
        lambda *refs: step_kernel(vocab_own, own_rows, *refs),
        out_shape=(jax.ShapeDtypeStruct((pad, head), bf16), jax.ShapeDtypeStruct((pad, head), bf16),
                   jax.ShapeDtypeStruct((take, total_rows), f32), jax.ShapeDtypeStruct((pad, head), f32)),
        in_specs=[vmem] * 5 + [hbm] * 10,
        out_specs=(vmem,) * 4,
        scratch_shapes=[
            V((chunk, qc), bf16), V((chunk, head), bf16), V((chunk, head), bf16),
            V((own_rows, seq, head), bf16), V((own_rows, seq, head), bf16),
            V((nx2 * ff, chunk), bf16), V((NZ * qc, chunk), bf16), V((NY, rows, chunk), f32), V((3, rows, chunk), f32),
            V((NZ, NY * rows, 2 * ff), f32), V((2, total_rows, NX * chunk), bf16), V((2, NX * chunk, 2 * ff), bf16),
            V((qc, chunk), bf16), V((2, head, NX * chunk), bf16),
            V((nx2 * nyz * pad, total_rows), bf16), V((NY * rows, nx2 * NY * pad), bf16),
            V((nx2, nyz * pad // 4, head), bf16), V((nx2, nyz * pad // 4, head), bf16),
            V((nyz, pad, qc), f32), V((nyz, pad, qc), f32),
            V((nx2, pad, 2 * head), f32), V((nx2, pad, 2 * head), f32),
            V((NZ, NY, pad, qc), f32), V((NY, NZ, pad, qc), f32), V((nx2, NY * pad, NZ * qc), bf16),
            V((NZ, NY * rows, nx2 * ff), bf16),
            V((NZ, NY, rows, chunk), f32),
            V((3, NZ, rows, half), f32), V((3, NY, rows, half), f32), V((3, rows, half), f32), V((3, rows, half), f32),
            V((NZ, rows, half), f32), V((NY, rows, half), f32),
            V((NX, rows, chunk), bf16), V((2, rows, 128), f32), V((NX, rows, chunk), f32), V((2, rows, 128), f32),
            V((NX, 8, chunk), f32),
            V((2, total_rows, NX * chunk), bf16), V((2, take, NX * chunk), bf16),
            V((2, 2, chunk, ff), bf16), V((2, 2, (take // 2 + 15) // 16 * 16, chunk), bf16),
            V((nx2, 16, 128), f32), V((nx2, 16, 128), f32), V((nyz, 16, 128), f32),
            pltpu.SemaphoreType.DMA((SENDS,)), pltpu.SemaphoreType.DMA((TAGS,)), pltpu.SemaphoreType.DMA((10,)),
        ],
        compiler_params=pltpu.CompilerParams(
            collective_id=1, has_side_effects=True, vmem_limit_bytes=60 << 20),
        name="decode_step",
    )(hidden, g_attn[None, :], g_final[None, :], freq, lens, k_cache, v_cache,
      w_query, w_key, w_value, w_out, w_gate, w_up, w_down, embedding)


def solution(mesh):
    row_spec = P(("dp", "yax", "xax"))

    def local_step(hidden, cache_len, k_cache, v_cache, g_attn, w_query, w_key, w_value,
                   w_gate, w_up, w_out, w_down, g_final, embedding):
        rows = hidden.shape[0]
        half_dim = k_cache.shape[2] // 2
        inv_freq = ROPE_BASE ** (-(np.arange(half_dim, dtype=np.float64) * 2.0) / (2 * half_dim))
        freq = np.concatenate([inv_freq, inv_freq])[None, :].astype(np.float32)
        key_own, value_own, logits_wide, norm_tile = whole_step(
            hidden, freq, cache_len.reshape(rows // 128, 128), k_cache, v_cache, g_attn, w_query, w_key, w_value,
            w_gate, w_up, w_out, w_down, g_final, embedding)
        own_rows = k_cache.shape[0]
        vocab_own = embedding.shape[0] // (CORES * NX)
        first = vocab_own * lax.axis_index("xax")
        logits = lax.dynamic_slice_in_dim(logits_wide, first - first // 8 * 8, vocab_own, axis=0)
        log_norm = norm_tile[:rows // 128].reshape(rows)
        return key_own[:own_rows], value_own[:own_rows], (logits - log_norm).T, log_norm

    in_specs = (P("dp", "xax"), P("dp"), row_spec, row_spec, P("xax"), P("xax", "yax"),
                P("xax", None), P("xax", None), P("xax", "yax"), P("xax", "yax"),
                P("yax", "xax"), P("yax", "xax"), P("xax"), P("yax", "xax"))
    out_specs = (row_spec, row_spec, P("dp", ("yax", "xax")), P("dp"))
    return jax.shard_map(local_step, mesh=mesh, in_specs=in_specs, out_specs=out_specs, check_vma=False)
```

```python
import contextlib
import itertools

import jax
import jax.numpy as jnp
import numpy as np
from jax import lax
from jax.experimental import pallas as pl
from jax.experimental.pallas import tpu as pltpu
from jax.sharding import PartitionSpec as P

EPS = 1e-6
ROPE_BASE = 10000.0
MESH_ID = pl.DeviceIdType.MESH
NY = NZ = NX = 4
CORES = 2
POOL, SENDS, TAGS = 24, 59, 86
HOPS = (1, 3, 2)
FAR_FIRST = (2, 1, 3)
LINE = [(0, 1), (1, 0), (3, 0), (1, 1), (3, 1), (2, 0), (2, 1)]
NEAR = LINE[1:5]
NT = (((1,), (1,)), ((), ()))
PLANE = [(dz, dy) for dz in range(NZ) for dy in range(NY) if dz or dy]


class Group:
    def __init__(self, links, whole):
        self.links, self.whole = links, whole
        self.tag, self.sem = next(links.tags), next(links.slow)
        links.groups.append(self)

    def send(self, src, dst, where):
        pltpu.make_async_remote_copy(
            src_ref=src, dst_ref=dst, send_sem=self.links.send_sem.at[self.sem],
            recv_sem=self.links.recv_sem.at[self.tag], device_id=where, device_id_type=MESH_ID).start()

    def wait(self):
        pltpu.make_async_copy(self.whole, self.whole, self.links.recv_sem.at[self.tag]).wait()

    def wait_sent(self):
        pltpu.make_async_copy(self.whole, self.whole, self.links.send_sem.at[self.sem]).wait()


class Phases:
    def __init__(self):
        self.stack = contextlib.ExitStack()

    def __call__(self, name):
        self.close()
        self.stack.enter_context(jax.named_scope(name))

    def close(self):
        self.stack.close()


class Links:
    def __init__(self, send_sem, recv_sem):
        self.send_sem, self.recv_sem = send_sem, recv_sem
        self.tags, self.slow, self.fast = itertools.count(), itertools.count(POOL), []
        self.pending, self.groups = [], []
        self.y_idx = lax.axis_index("yax")
        self.x_idx = lax.axis_index("xax")
        self.z, self.y = self.y_idx // NY, self.y_idx % NY
        self.chip, self.core = self.x_idx // CORES, self.x_idx % CORES

    def at_plane(self, dz, dy):
        return {"yax": (self.z + dz) % NZ * NY + (self.y + dy) % NY, "xax": self.x_idx}

    def slot_rows(self, dz, dy, rows):
        slot = (self.z + dz) % NZ * NY + (self.y + dy) % NY
        return pl.ds(pl.multiple_of(slot * rows, rows), rows)

    def line_id(self, dx, oc):
        core = 1 - self.core if oc else self.core
        return (self.chip + dx) % NX * CORES + core

    def at_line(self, dx, oc):
        return {"yax": self.y_idx, "xax": self.line_id(dx, oc)}

    def send(self, src, dst, where, tag=None, long=False):
        tag = next(self.tags) if tag is None else tag
        if long:
            sem = next(self.slow)
        else:
            sem = len(self.fast) % POOL
            if len(self.fast) >= POOL:
                self.fast[-POOL].wait_send()
        copy = pltpu.make_async_remote_copy(
            src_ref=src, dst_ref=dst, send_sem=self.send_sem.at[sem], recv_sem=self.recv_sem.at[tag],
            device_id=where, device_id_type=MESH_ID)
        copy.start()
        (self.pending if long else self.fast).append(copy)
        return copy

    def finish(self):
        for copy in self.pending + self.fast[-POOL:]:
            copy.wait_send()
        for group in self.groups:
            group.wait_sent()

    def barrier(self):
        barrier = pltpu.get_barrier_semaphore()
        peers = [self.at_line(*p) for p in LINE] + [self.at_plane(*p) for p in PLANE]
        for peer in peers:
            pl.semaphore_signal(barrier, inc=1, device_id=peer, device_id_type=MESH_ID)
        pl.semaphore_wait(barrier, len(peers))


def lane_sum(v):
    return jnp.sum(v, axis=-1, keepdims=True)


def plane_gather(links, buf, tags, hook, crossing, start):
    cols = buf.shape[-1]
    rows = buf.shape[1] // (NY * NZ)
    span = (cols - start) // 2
    partner = links.at_line(0, 1)

    class Part:
        def __init__(self, index):
            self.index, self.lo, self.got = index, start + index * span, {}

        def order(self, du, dv):
            return (du, dv) if self.index else (dv, du)

        def block(self, at, half=0, piece=None):
            width = span if piece is None else span // 2
            lo = self.lo if not piece else self.lo + width
            return buf.at[half, links.slot_rows(*self.order(*at), rows), pl.ds(lo, width)]

        def push(self, name, at, to, piece=None):
            ref = self.block(at, piece=piece)
            self.got[name] = links.send(ref, ref, links.at_plane(*self.order(*to)), next(tags))

        def spread(self, k, at):
            self.push(("v+", k), at, (0, 1))
            self.push(("v-", k), at, (0, -1))

        def give(self, at):
            crossing.send(self.block(at), self.block(at, half=1), partner)

        def wait(self, name):
            self.got[name].wait_recv()

    parts = [Part(index) for index in range(2)]
    offset = (0, -1, 1, 2)
    for p in parts:
        p.push("u+", (0, 0), (1, 0))
        p.push("u-", (0, 0), (-1, 0))
        p.spread(0, (0, 0))
    for p in parts:
        p.give((0, 0))
    for k, name in enumerate(("u+", "u-"), 1):
        for p in parts:
            p.wait(name)
            at = (offset[k], 0)
            p.push(("far", k), at, (-offset[k], 0), piece=k - 1)
            p.spread(k, at)
            p.give(at)
    hook()

    def arrive(p, k):
        for name, step in (("v+", -1), ("v-", 1)):
            p.wait((name, k))
            at = (offset[k], step)
            if (name == "v+") == (k in (0, 3)):
                p.push(("relay", k), at, (0, -step))
            p.give(at)

    for p in parts:
        arrive(p, 0)
    for p in parts:
        p.wait(("far", 1))
        p.wait(("far", 2))
        p.spread(3, (2, 0))
        p.give((2, 0))
    for k in range(1, len(offset)):
        for p in parts:
            arrive(p, k)
    for k in range(len(offset)):
        for p in parts:
            p.wait(("relay", k))
            p.give((offset[k], 2))


def norm_gather(links, own_slot, gain_buf, which, xbuf, stat, out, base, hook, skip=0, known=None):
    own_slot()
    rows, chunk = xbuf.shape[1:]
    tags = itertools.count(base)
    line = [links.send(xbuf.at[0], xbuf.at[NX - dx], links.at_line(dx, 0), next(tags)) for dx in FAR_FIRST]
    yield
    phase = Phases()
    for n, c in enumerate(line):
        phase(f"ng_line{which}_{n}")
        c.wait_recv()
    phase("ng_stats")
    stat_tag = next(tags)
    if known is not None:
        both, scale = known()
    else:
        held = xbuf[...].astype(jnp.float32)
        count = NX * chunk
        mean = lane_sum(jnp.sum(held, axis=0)) / count
        dev = held - mean[None]
        square = lane_sum(jnp.sum(dev * dev, axis=0))
        lane = lax.broadcasted_iota(jnp.int32, (rows, 128), 1)
        stat[0] = jnp.where(lane == 0, mean, square)
        links.send(stat.at[0], stat.at[1], links.at_line(0, 1), stat_tag).wait_recv()
        other_mean, other_square = stat[1, :, 0:1], stat[1, :, 1:2]
        both = (mean + other_mean) * 0.5
        gap = mean - other_mean
        var = (square + other_square + gap * gap * (count * 0.5)) / (2 * count)
        scale = lax.rsqrt(var + EPS)
    for e in range(skip, NX):
        out[0, links.slot_rows(0, 0, rows), e * chunk:(e + 1) * chunk] = (
            (xbuf[e].astype(jnp.float32) - both) * scale * gain_buf[e, which:which + 1, :]).astype(jnp.bfloat16)
    phase("ng_plane")
    crossing = Group(links, out.at[1])
    plane_gather(links, out, tags, lambda: hook(crossing), crossing, skip * chunk)
    phase.close()
    yield crossing


def step_kernel(vocab_own, own_rows, hid_ref, gain_a, gain_f, freq_ref, len_ref, k_hbm, v_hbm,
                wq_hbm, wk_hbm, wv_hbm, wo_ref, wg_ref, wu_ref, wd_hbm, emb_ref,
                knew_ref, vnew_ref, z_ref, norm_ref,
                wq_ref, wk_ref, wv_ref, k_buf, v_buf, wd_buf, wo_all, att, rc, gu_acc, n_buf, w_buf, wq_t, wq_buf, sel, sel_t, qx, qr, qy, qf,
                kvp, kvr, o_buf, o_got, o_all, act,
                part, ra1, rb1, ra2, rb2, acc_a, acc_b, xbuf, xbuf2, stat2, gains, f_buf, emb_buf,
                w_relay, emb_relay, row_stats, lse_x, lse_y, send_sem, recv_sem, local_sem):
    links = Links(send_sem, recv_sem)
    phase = Phases()
    f32, bf16 = jnp.float32, jnp.bfloat16
    z, y, xid, yid = links.z, links.y, links.x_idx, links.y_idx
    total_rows, chunk = hid_ref.shape
    rows = total_rows // (NY * NZ)
    here_rows = links.slot_rows(0, 0, rows)
    half = chunk // 2
    nx2, nyz = 2 * NX, NY * NZ
    group = NY * rows
    head = 128
    pad = 8
    partner = links.at_line(0, 1)
    line_id = links.line_id
    gather_tags = len(HOPS) + 1 + len(PLANE) * CORES + CORES
    gather_base = [next(links.tags) for _ in range(gather_tags)][0]

    def dot(a, b):
        return jnp.dot(a, b, preferred_element_type=f32)

    def dot_t(a, b):
        return lax.dot_general(a, b, NT, preferred_element_type=f32)

    def rest(ref, n):
        return Group(links, ref.at[0:n - 1])

    local = []

    def fetch(src, dst):
        copy = pltpu.make_async_copy(src, dst, local_sem.at[len(local)])
        copy.start()
        local.append(copy)
        return copy

    ff = wg_ref.shape[1] // nx2

    def w_piece(ref, dx, oc):
        return ref.at[:, pl.ds(pl.multiple_of(line_id(dx, oc) * ff, ff), ff)]

    def w_slot(which, dx, oc):
        back = (NX - dx) % NX
        return w_buf.at[int(oc), pl.ds(back * chunk, chunk), pl.ds(which * ff, ff)]

    take = emb_buf.shape[1]

    def emb_start(xi):
        return pl.multiple_of(vocab_own * xi // pad * pad, pad)

    def emb_piece(dx, oc):
        return emb_ref.at[pl.ds(emb_start(line_id(dx, oc)), take), :]

    def emb_slot(dx, oc):
        return emb_buf.at[int(oc), :, pl.ds((NX - dx) % NX * chunk, chunk)]

    near_part = (take // 2 + 15) // 16 * 16
    far_parts = ((0, near_part), (near_part, take - near_part))

    def emb_half(oc, way):
        first, size = far_parts[way]
        return emb_ref.at[pl.ds(pl.multiple_of(emb_start(line_id(2, oc)) + first, pad), size), :]

    def emb_mid(oc, way):
        return emb_relay.at[way, oc, pl.ds(0, far_parts[way][1])]

    def emb_far_slot(oc, way):
        return emb_buf.at[int(oc), pl.ds(*far_parts[way]), pl.ds(2 * chunk, chunk)]

    got_wq = fetch(wq_hbm, wq_ref)
    own_w = [fetch(w_piece(wg_ref, 0, 0), w_slot(0, 0, 0)), fetch(w_piece(wu_ref, 0, 0), w_slot(1, 0, 0))]
    got_kv = [fetch(k_hbm, k_buf), fetch(v_hbm, v_buf)]
    got_wkv = [fetch(wk_hbm, wk_ref), fetch(wv_hbm, wv_ref)]
    got_wd = fetch(wd_hbm, wd_buf)
    own_emb = fetch(emb_piece(0, 0), emb_slot(0, 0))

    qc = wq_ref.shape[1]
    qs = qc // nx2
    per = head // qs
    wq_buf[...] = jnp.zeros(wq_buf.shape, bf16)

    phase("row_stats")
    eye = lax.broadcasted_iota(jnp.int32, (head, head), 0) == lax.broadcasted_iota(jnp.int32, (head, head), 1)
    blocks = total_rows // head

    def block_rows(b):
        return slice(b * head, (b + 1) * head)

    def to_row(v):
        return jnp.sum(jnp.where(eye, v, 0.0), axis=0, keepdims=True)

    def to_col(v):
        return lane_sum(jnp.where(eye, v, 0.0))

    row_stats[xid] = jnp.zeros((2 * pad, head), f32)
    for b in range(blocks):
        held = hid_ref[block_rows(b), :].astype(f32)
        mean = lane_sum(held) / chunk
        dev = held - mean
        row_stats[xid, b:b + 1, :] = to_row(mean)
        row_stats[xid, pad + b:pad + b + 1, :] = to_row(lane_sum(dev * dev))

    phase("barrier")
    links.barrier()

    phase("front_send")
    gains[0, 0:1, :] = gain_a[...]
    gains[0, 1:2, :] = gain_f[...]
    gains[0, 2:, :] = jnp.zeros((6, chunk), f32)

    def own_input():
        xbuf[0] = hid_ref[here_rows, :]

    w_far, emb_far = [], []
    w_got = [Group(links, w_buf.at[0, 0:2 * chunk]), Group(links, w_buf.at[1, 0:(NX - 1) * chunk])]
    w_last = Group(links, w_buf.at[0, 0:2 * chunk])
    emb_got = [Group(links, emb_buf.at[0, :, 0:(NX - 1) * chunk]), Group(links, emb_buf.at[1])]
    ways = [(way, hop, oc) for oc in (0, 1) for way, hop in enumerate(HOPS[:2])]

    def forward_weights():
        for (way, hop, oc), c in zip(ways, w_far):
            c.wait_recv()
            w_last.send(w_relay.at[way, oc], w_buf.at[oc, pl.ds(2 * chunk, chunk), pl.ds(way * ff, ff)],
                        links.at_line(hop, oc))

    def emb_out(some):
        for way, hop, oc in some:
            emb_far.append(links.send(emb_half(oc, way), emb_mid(oc, way), links.at_line(hop, 0), long=True))

    def emb_on(some, arrived):
        for (way, hop, oc), c in zip(some, arrived):
            c.wait_recv()
            emb_got[oc].send(emb_mid(oc, way), emb_far_slot(oc, way), links.at_line(hop, oc))

    def col_of_slot(v):
        here = (z * NY + y) * rows + lax.broadcasted_iota(jnp.int32, (rows, 1), 0)
        lane_id = lax.broadcasted_iota(jnp.int32, (1, head), 1)
        return sum(lane_sum(jnp.where(lane_id + b * head == here, v[b:b + 1, :], 0.0)) for b in range(blocks))

    all_rows = []

    def slot_stats():
        stats_got.wait()
        means = row_stats[:, :pad, :]
        mean = jnp.sum(means, axis=0) / nx2
        gap = means - mean[None]
        square = jnp.sum(row_stats[:, pad:, :], axis=0) + jnp.sum(gap * gap, axis=0) * chunk
        all_rows.extend((mean, lax.rsqrt(square / (nx2 * chunk) + EPS)))
        return [col_of_slot(v) for v in all_rows]

    def amid(crossing):
        forward_weights()
        mean, scale = all_rows
        for b in range(blocks):
            n_buf[0, block_rows(b), 0:chunk] = (
                (hid_ref[block_rows(b), :].astype(f32) - to_col(mean[b:b + 1, :])) * to_col(scale[b:b + 1, :])
                * gains[0, 0:1, :]).astype(bf16)
        own = n_buf.at[0, :, 0:chunk]
        crossing.send(own, n_buf.at[1, :, 0:chunk], partner)

    front = norm_gather(links, own_input, gains, 0, xbuf, None, n_buf, gather_base, amid, skip=1, known=slot_stats)
    stats_got = rest(row_stats, nx2)
    for p in LINE:
        stats_got.send(row_stats.at[xid], row_stats.at[xid], links.at_line(*p))
    next(front)
    gain_got = rest(gains, NX)
    for dx in HOPS:
        gain_got.send(gains.at[0], gains.at[NX - dx], links.at_line(dx, 0))
    for way, hop, oc in ways:
        w_far.append(links.send(w_piece((wg_ref, wu_ref)[way], 2, oc), w_relay.at[way, oc], links.at_line(hop, 0),
                                long=True))

    got_wq.wait()
    eye_q = (lax.broadcasted_iota(jnp.int32, (qc, qc), 0) == lax.broadcasted_iota(jnp.int32, (qc, qc), 1))
    wq_t[...] = dot_t(eye_q.astype(bf16), wq_ref[...]).astype(bf16)
    wq_buf[0, 0:qs, 0:chunk] = wq_t[pl.ds(pl.multiple_of(xid * qs, qs), qs), :]

    def wq_rows(dx, oc):
        return wq_t.at[pl.ds(pl.multiple_of(line_id(dx, oc) * qs, qs), qs), :]

    def wq_slot(dx, oc):
        return wq_buf.at[oc, pl.ds(0, qs), pl.ds((NX - dx) % NX * chunk, chunk)]

    wq_got = Group(links, wq_t.at[0:qc - qs])
    for dx, oc in LINE:
        wq_got.send(wq_rows(dx, oc), wq_slot(dx, oc), links.at_line(dx, oc))
    for which, ref in enumerate((wg_ref, wu_ref)):
        for dx, oc in LINE[:1] + NEAR:
            w_got[oc].send(w_piece(ref, dx, oc), w_slot(which, dx, oc), links.at_line(dx, oc))

    phase("selections")
    r_id = lax.broadcasted_iota(jnp.int32, (nx2 * nyz * pad, 1), 0)
    r_j = r_id % pad
    r_src = jnp.where(r_j < own_rows, r_id // pad % nyz * rows + r_id // (pad * nyz) * own_rows + r_j, -1)
    s_id = lax.broadcasted_iota(jnp.int32, (1, total_rows), 1)
    sel[...] = jnp.where(r_src == s_id, 1.0, 0.0).astype(bf16)
    t_id = lax.broadcasted_iota(jnp.int32, (group, 1), 0)
    t_in = t_id % rows
    t_src = t_in // own_rows * (NY * pad) + t_id // rows * pad + t_in % own_rows
    u_id = lax.broadcasted_iota(jnp.int32, (1, nx2 * NY * pad), 1)
    sel_t[...] = jnp.where(t_src == u_id, 1.0, 0.0).astype(bf16)
    k_id = lax.broadcasted_iota(jnp.int32, (nx2 * pad, rows), 0)
    k_src = jnp.where(k_id % pad < own_rows, k_id // pad * own_rows + k_id % pad, -1)
    sel_kv = jnp.where(k_src == lax.broadcasted_iota(jnp.int32, (nx2 * pad, rows), 1), 1.0, 0.0).astype(bf16)

    phase.close()
    gain_got.wait()
    lane = lax.broadcasted_iota(jnp.int32, (1, head), 1)
    lengths = []
    for b in range(own_rows):
        index = (yid * nx2 + xid) * own_rows + b
        row = len_ref[pl.ds(index // head, 1), :].astype(f32)
        lengths.append(lane_sum(jnp.where(lane == index % head, row, 0.0)))
    lengths = jnp.concatenate(lengths + lengths[:pad - own_rows], axis=0)
    angles = lengths * freq_ref[...]
    cos_all = jnp.cos(angles)
    sin_all = jnp.sin(angles) * jnp.where(lane < head // 2, -1.0, 1.0)

    crossing = next(front)
    phase("ng_cross")
    crossing.wait()
    phase("kv_part")

    for c in got_wkv:
        c.wait()
    n_own = dot(sel_kv, n_buf[0, links.slot_rows(0, 0, rows), 0:chunk]).astype(bf16)
    kvp[:, :, :head] = dot(n_own, wk_ref[...]).reshape(nx2, pad, head)
    kvp[:, :, head:] = dot(n_own, wv_ref[...]).reshape(nx2, pad, head)
    kv_got = rest(kvr, nx2)
    for p in LINE:
        kv_got.send(kvp.at[line_id(*p)], kvr.at[xid], links.at_line(*p))
    kvr[xid] = kvp[xid]

    phase("wait_wq")
    wq_got.wait()
    phase("q_mm")
    q_all = jnp.concatenate([
        (dot_t(n_buf[0, i * group:(i + 1) * group, :], wq_buf[0])
         + dot_t(n_buf[1, i * group:(i + 1) * group, :], wq_buf[1])).astype(bf16) for i in range(NZ)], axis=0)
    span = nyz * pad
    for i in range(nx2):
        chosen = dot(sel[i * span:(i + 1) * span, :], q_all)
        quarter = span // per
        packed = chosen[:quarter, :]
        for g in range(1, per):
            packed = packed + pltpu.roll(chosen[g * quarter:(g + 1) * quarter, :], g * qs, 1)
        qx[i] = packed.astype(bf16)
    q_got = rest(qr, nx2)
    for p in LINE:
        q_got.send(qx.at[line_id(*p)], qr.at[xid], links.at_line(*p))
    qr[xid] = qx[xid]

    phase("wait_w")
    for c in own_w:
        c.wait()
    for c in w_got:
        c.wait()
    phase("gate_up")

    def act_at(k, dx):
        return act.at[(z + k) % NZ, :, pl.ds(pl.multiple_of(line_id(dx, 0) * ff, ff), ff)]

    def act_out(k, dx, to_dx):
        return links.send(act_at(k, dx), act_at(k, dx), links.at_line(to_dx, 0))

    def act_give(k, dx):
        cross[k].send(act_at(k, dx), act_at(k, dx), partner)

    turns = (2, 1, 3, 0)
    early, late = turns[:2], turns[2:]
    near_act, far_act = {}, {}
    cross = {k: Group(links, act.at[0, :, 0:NX * ff]) for k in turns}
    def group_rows(k):
        return pl.ds(pl.multiple_of((z + k) % NZ * group, group), group)

    far = slice(2 * chunk, (NX - 1) * chunk)

    def over(k, part_cols):
        return dot(n_buf[0, group_rows(k), part_cols], w_buf[0, part_cols, :]) + dot(
            n_buf[1, group_rows(k), part_cols], w_buf[1, part_cols, :])

    for k in turns:
        gu_acc[k] = over(k, slice(0, far.start)) + over(k, slice(far.stop, NX * chunk))
    phase("wait_w_far")
    w_last.wait()
    phase("gate_up_far")
    for k in turns:
        both = (gu_acc[k] + over(k, far)).astype(bf16).astype(f32)
        gate, up = both[:, :ff], both[:, ff:]
        act_at(k, 0)[...] = (gate * jax.nn.sigmoid(gate) * up).astype(bf16)
        near_act[k] = [(dx, act_out(k, 0, dx)) for dx in HOPS[:2]]
        act_give(k, 0)

    def act_pass(k):
        for dx, c in near_act[k]:
            c.wait_recv()
            if (k in early) == (dx == 1):
                far_act[k] = act_out(k, NX - dx, dx)
            act_give(k, NX - dx)

    low, high = pl.ds(0, half), pl.ds(half, half)
    first_a, first_b = Group(links, ra1), Group(links, rb1)

    def act_use(k):
        cross[k].wait()
        g = (z + k) % NZ
        part[g] = dot(act[g], wd_buf[...]).reshape(NY, rows, chunk)
        if k:
            first_b.send(part.at[g, :, :, high], rb1.at[k - 1], links.at_plane(k, 0))

    def along_y(k):
        g = (z + k) % NZ
        for d in early + late[:1]:
            first_a.send(part.at[g, (y + d) % NY, :, low], ra1.at[d - 1, g], links.at_plane(0, d))

    def act_far(ks):
        for k in ks:
            far_act[k].wait_recv()
            act_give(k, 2)

    phase("wait_q")
    q_got.wait()
    phase("q_sum")
    lane_group = lax.broadcasted_iota(jnp.int32, (1, head), 1) // qs
    for j in range(qc // head):
        came = [qr[j * per + i].astype(f32) for i in range(per)]
        for g in range(per):
            piece = jnp.zeros((span // per, head), f32)
            for i in range(per):
                piece = piece + jnp.where(lane_group == i, pltpu.roll(came[i], (i - g) % per * qs, 1), 0.0)
            qy[g * per:(g + 1) * per, :, j * head:(j + 1) * head] = piece.reshape(per, pad, head)

    def plane_id(dz, dy):
        return (z + dz) % NZ * NY + (y + dy) % NY

    y_got = rest(qf, nyz)
    for p in PLANE:
        y_got.send(qy.at[plane_id(*p)], qf.at[yid], links.at_plane(*p))
    qf[yid] = qy[yid]

    def wo_rows(dz):
        return wo_all.at[pl.ds(pl.multiple_of((z + dz) % NZ * qc, qc), qc), :]

    wo_got = Group(links, wo_all.at[0:(NZ - 1) * qc])
    for d in HOPS:
        wo_got.send(wo_ref, wo_rows(0), links.at_plane(d, 0))
    own_wo = fetch(wo_ref, wo_rows(0))

    phase("act_pass")
    for k in early:
        act_pass(k)
    emb_out(ways[:2])
    phase("wait_kv")
    kv_got.wait()
    kv_sum = kvr[0]
    for i in range(1, nx2):
        kv_sum = kv_sum + kvr[i]
    kv_new = kv_sum.astype(bf16).astype(f32)

    def turn(v, b=None):
        cos, sin = (cos_all, sin_all) if b is None else (cos_all[b:b + 1, :], sin_all[b:b + 1, :])
        return (v * cos + pltpu.roll(v, head // 2, 1) * sin).astype(bf16)

    k_new = turn(kv_new[:, :head])
    knew_ref[...] = k_new
    vnew_ref[...] = kv_new[:, head:].astype(bf16)
    k_row, v_row = k_new.astype(f32), kv_new[:, head:]
    phase("act_pass2")
    for k in late:
        act_pass(k)
    phase("wait_qy")
    for c in got_kv:
        c.wait()
    y_got.wait()
    phase("attention")
    seq = k_buf.shape[1]
    score_scale = head ** -0.5
    position = lax.broadcasted_iota(jnp.int32, (1, seq), 1).astype(f32)
    o_buf[...] = jnp.zeros(o_buf.shape, f32)
    for b in range(own_rows):
        q_b = jnp.concatenate([turn(qf[:, b, j * head:(j + 1) * head], b) for j in range(qc // head)], axis=0)
        scores = dot_t(q_b, k_buf[b]) * score_scale
        score_new = lane_sum(q_b.astype(f32) * k_row[b:b + 1, :]) * score_scale
        valid = position < lengths[b:b + 1, :]
        top = jnp.maximum(jnp.max(jnp.where(valid, scores, -jnp.inf), axis=-1, keepdims=True), score_new)
        weights = jnp.where(valid, jnp.exp(scores - top), 0.0)
        weight_new = jnp.exp(score_new - top)
        denom = lane_sum(weights) + weight_new
        o_b = dot((weights / denom).astype(bf16), v_buf[b])
        o_b = o_b + (weight_new / denom).astype(bf16).astype(f32) * v_row[b:b + 1, :]
        o_b = o_b.astype(bf16).astype(f32)
        for j in range(qc // head):
            o_buf[:, :, b, j * head:(j + 1) * head] = o_b[j * nyz:(j + 1) * nyz, :].reshape(NZ, NY, head)
    o_back = rest(o_got, NY)
    for d in HOPS:
        o_back.send(o_buf.at[:, (y + d) % NY], o_got.at[y], links.at_plane(0, d))
    phase("act_early")
    act_far(turns)
    got_wd.wait()
    for k in turns:
        act_use(k)
        along_y(k)
    o_got[y] = o_buf[:, y]

    phase("wait_oy")
    o_back.wait()
    for i in range(NZ):
        o_all[xid, :, i * qc:(i + 1) * qc] = o_got[:, i].reshape(NY * pad, qc).astype(bf16)
    o_here = o_all.at[xid]
    o_line = [links.send(o_here, o_here, links.at_line(dx, 0)) for dx in HOPS]
    o_cross = rest(o_all, NX + 1)
    o_cross.send(o_here, o_here, partner)
    emb_out(ways[2:])
    emb_got[1].send(emb_piece(0, 1), emb_slot(0, 1), partner)
    emb_on(ways[:2], emb_far[:2])
    phase("wait_o")
    for dx, c in zip(HOPS, o_line):
        c.wait_recv()
        came = o_all.at[line_id(NX - dx, 0)]
        o_cross.send(came, came, partner)
    wo_got.wait()
    own_wo.wait()
    o_cross.wait()
    phase("out_mm")
    o_nat = dot(sel_t[...], o_all[...].reshape(nx2 * NY * pad, NZ * qc)).astype(bf16)
    att[...] = dot(o_nat, wo_all[...]).reshape(NY, rows, chunk)
    att_got = Group(links, rc)
    for d in HOPS:
        att_got.send(att.at[(y + d) % NY], rc.at[d - 1], links.at_plane(0, d))

    phase("wait_rs1")
    first_b.wait()
    acc_b[...] = (part[z, :, :, half:] + rb1[0]) + (rb1[1] + rb1[2])
    second = [Group(links, rb2), Group(links, ra2)]
    for d in HOPS:
        second[0].send(acc_b.at[(y + d) % NY], rb2.at[d - 1], links.at_plane(0, d))
    phase("wait_rs1a")
    first_a.wait()
    acc_a[...] = (part[:, y, :, :half] + ra1[0]) + (ra1[1] + ra1[2])
    for d in HOPS:
        second[1].send(acc_a.at[(z + d) % NZ], ra2.at[d - 1], links.at_plane(d, 0))
    phase("wait_att")
    att_got.wait()
    phase("wait_rs2")
    for c in second:
        c.wait()
    phase("rs_sum2")
    def own_residual():
        res = hid_ref[here_rows, :].astype(f32) + ((att[y] + rc[0]) + (rc[1] + rc[2]))
        xbuf2[0, :, :half] = res[:, :half] + ((acc_a[z] + ra2[0]) + (ra2[1] + ra2[2]))
        xbuf2[0, :, half:] = res[:, half:] + ((acc_b[y] + rb2[0]) + (rb2[1] + rb2[2]))

    back = norm_gather(links, own_residual, gains, 1, xbuf2, stat2, f_buf, gather_base, lambda crossing: None)
    next(back)
    emb_on(ways[2:], emb_far[2:])
    for dx, oc in NEAR:
        emb_got[oc].send(emb_piece(dx, oc), emb_slot(dx, oc), links.at_line(dx, oc))
    phase.close()
    crossing = next(back)
    phase("wait_emb")
    own_emb.wait()
    for c in emb_got:
        c.wait()

    phase("logits")
    wide_n = 256
    for h in range(CORES):
        if h:
            crossing.wait()
        for i in range(total_rows // wide_n):
            cols = slice(i * wide_n, (i + 1) * wide_n)
            term = dot_t(emb_buf[h], f_buf[h, cols, :])
            z_ref[:, cols] = z_ref[:, cols] + term if h else term

    phase("lse_own")
    shift = vocab_own * xid - emb_start(xid)
    vid = lax.broadcasted_iota(jnp.int32, (take, 1), 0)
    own = (vid >= shift) & (vid < shift + vocab_own)
    for b in range(blocks):
        zb = jnp.where(own, z_ref[:, b * 128:(b + 1) * 128], -jnp.inf)
        top = jnp.max(zb, axis=0, keepdims=True)
        lse_x[xid, b:b + 1, :] = top
        lse_x[xid, 8 + b:9 + b, :] = jnp.sum(jnp.exp(zb - top), axis=0, keepdims=True)
    for b in range(blocks, 8):
        lse_x[xid, b:b + 1, :] = jnp.zeros((1, 128), f32)
        lse_x[xid, 8 + b:9 + b, :] = jnp.ones((1, 128), f32)

    def merge(ref):
        tops = ref[:, :8, :]
        top = jnp.max(tops, axis=0)
        return top, jnp.sum(ref[:, 8:, :] * jnp.exp(tops - top[None]), axis=0)

    phase("lse_line")
    got = rest(lse_x, nx2)
    for p in LINE:
        got.send(lse_x.at[xid], lse_x.at[xid], links.at_line(*p))
    got.wait()
    top, mass = merge(lse_x)
    lse_y[yid, :8, :] = top
    lse_y[yid, 8:, :] = mass
    phase("lse_plane")
    got = rest(lse_y, nyz)
    for p in PLANE:
        got.send(lse_y.at[yid], lse_y.at[yid], links.at_plane(*p))
    got.wait()
    top, mass = merge(lse_y)
    norm_ref[...] = top + jnp.log(mass)
    phase("finish")
    links.finish()
    phase.close()


def whole_step(hidden, freq, lens, k_cache, v_cache, g_attn, w_query, w_key, w_value,
               w_gate, w_up, w_out, w_down, g_final, embedding):
    total_rows, chunk = hidden.shape
    own_rows, seq, head = k_cache.shape
    rows = total_rows // (NY * NZ)
    vocab_own = embedding.shape[0] // (2 * NX)
    take = (vocab_own + 6 + 15) // 16 * 16
    half = chunk // 2
    qc = w_query.shape[1]
    ff = w_gate.shape[1] // (2 * NX)
    f32, bf16 = jnp.float32, jnp.bfloat16
    nyz, nx2, pad = NY * NZ, 2 * NX, 8
    vmem = pl.BlockSpec(memory_space=pltpu.VMEM)
    hbm = pl.BlockSpec(memory_space=pl.ANY)
    V = pltpu.VMEM
    return pl.pallas_call(
        lambda *refs: step_kernel(vocab_own, own_rows, *refs),
        out_shape=(jax.ShapeDtypeStruct((pad, head), bf16), jax.ShapeDtypeStruct((pad, head), bf16),
                   jax.ShapeDtypeStruct((take, total_rows), f32), jax.ShapeDtypeStruct((pad, head), f32)),
        in_specs=[vmem] * 5 + [hbm] * 10,
        out_specs=(vmem,) * 4,
        scratch_shapes=[
            V((chunk, qc), bf16), V((chunk, head), bf16), V((chunk, head), bf16),
            V((own_rows, seq, head), bf16), V((own_rows, seq, head), bf16),
            V((nx2 * ff, chunk), bf16), V((NZ * qc, chunk), bf16), V((NY, rows, chunk), f32), V((3, rows, chunk), f32),
            V((NZ, NY * rows, 2 * ff), f32), V((2, total_rows, NX * chunk), bf16), V((2, NX * chunk, 2 * ff), bf16),
            V((qc, chunk), bf16), V((2, head, NX * chunk), bf16),
            V((nx2 * nyz * pad, total_rows), bf16), V((NY * rows, nx2 * NY * pad), bf16),
            V((nx2, nyz * pad // 4, head), bf16), V((nx2, nyz * pad // 4, head), bf16),
            V((nyz, pad, qc), f32), V((nyz, pad, qc), f32),
            V((nx2, pad, 2 * head), f32), V((nx2, pad, 2 * head), f32),
            V((NZ, NY, pad, qc), f32), V((NY, NZ, pad, qc), f32), V((nx2, NY * pad, NZ * qc), bf16),
            V((NZ, NY * rows, nx2 * ff), bf16),
            V((NZ, NY, rows, chunk), f32),
            V((3, NZ, rows, half), f32), V((3, NY, rows, half), f32), V((3, rows, half), f32), V((3, rows, half), f32),
            V((NZ, rows, half), f32), V((NY, rows, half), f32),
            V((NX, rows, chunk), bf16), V((NX, rows, chunk), f32), V((2, rows, 128), f32),
            V((NX, 8, chunk), f32),
            V((2, total_rows, NX * chunk), bf16), V((2, take, NX * chunk), bf16),
            V((2, 2, chunk, ff), bf16), V((2, 2, (take // 2 + 15) // 16 * 16, chunk), bf16),
            V((nx2, 16, 128), f32), V((nx2, 16, 128), f32), V((nyz, 16, 128), f32),
            pltpu.SemaphoreType.DMA((SENDS,)), pltpu.SemaphoreType.DMA((TAGS,)), pltpu.SemaphoreType.DMA((10,)),
        ],
        compiler_params=pltpu.CompilerParams(
            collective_id=1, has_side_effects=True, vmem_limit_bytes=60 << 20),
        name="decode_step",
    )(hidden, g_attn[None, :], g_final[None, :], freq, lens, k_cache, v_cache,
      w_query, w_key, w_value, w_out, w_gate, w_up, w_down, embedding)


def solution(mesh):
    row_spec = P(("dp", "yax", "xax"))

    def local_step(hidden, cache_len, k_cache, v_cache, g_attn, w_query, w_key, w_value,
                   w_gate, w_up, w_out, w_down, g_final, embedding):
        rows = hidden.shape[0]
        half_dim = k_cache.shape[2] // 2
        inv_freq = ROPE_BASE ** (-(np.arange(half_dim, dtype=np.float64) * 2.0) / (2 * half_dim))
        freq = np.concatenate([inv_freq, inv_freq])[None, :].astype(np.float32)
        key_own, value_own, logits_wide, norm_tile = whole_step(
            hidden, freq, cache_len.reshape(rows // 128, 128), k_cache, v_cache, g_attn, w_query, w_key, w_value,
            w_gate, w_up, w_out, w_down, g_final, embedding)
        own_rows = k_cache.shape[0]
        vocab_own = embedding.shape[0] // (CORES * NX)
        first = vocab_own * lax.axis_index("xax")
        logits = lax.dynamic_slice_in_dim(logits_wide, first - first // 8 * 8, vocab_own, axis=0)
        log_norm = norm_tile[:rows // 128].reshape(rows)
        return key_own[:own_rows], value_own[:own_rows], (logits - log_norm).T, log_norm

    in_specs = (P("dp", "xax"), P("dp"), row_spec, row_spec, P("xax"), P("xax", "yax"),
                P("xax"), P("xax"), P("xax", "yax"), P("xax", "yax"),
                P("yax", "xax"), P("yax", "xax"), P("xax"), P("yax", "xax"))
    out_specs = (row_spec, row_spec, P("dp", ("yax", "xax")), P("dp"))
    return jax.shard_map(local_step, mesh=mesh, in_specs=in_specs, out_specs=out_specs, check_vma=False)
```

```python
import contextlib
import itertools

import jax
import jax.numpy as jnp
import numpy as np
from jax import lax
from jax.experimental import pallas as pl
from jax.experimental.pallas import tpu as pltpu
from jax.sharding import PartitionSpec as P

EPS = 1e-6
ROPE_BASE = 10000.0
MESH_ID = pl.DeviceIdType.MESH
NY = NZ = NX = 4
CORES = 2
POOL, SENDS, TAGS = 24, 59, 86
HOPS = (1, 3, 2)
FAR_FIRST = (2, 1, 3)
LINE = [(0, 1), (1, 0), (3, 0), (1, 1), (3, 1), (2, 0), (2, 1)]
NEAR = LINE[1:5]
NT = (((1,), (1,)), ((), ()))
PLANE = [(dz, dy) for dz in range(NZ) for dy in range(NY) if dz or dy]


class Group:
    def __init__(self, links, whole):
        self.links, self.whole = links, whole
        self.tag, self.sem = next(links.tags), next(links.slow)
        links.groups.append(self)

    def send(self, src, dst, where):
        pltpu.make_async_remote_copy(
            src_ref=src, dst_ref=dst, send_sem=self.links.send_sem.at[self.sem],
            recv_sem=self.links.recv_sem.at[self.tag], device_id=where, device_id_type=MESH_ID).start()

    def wait(self):
        pltpu.make_async_copy(self.whole, self.whole, self.links.recv_sem.at[self.tag]).wait()

    def wait_sent(self):
        pltpu.make_async_copy(self.whole, self.whole, self.links.send_sem.at[self.sem]).wait()


class Phases:
    def __init__(self):
        self.stack = contextlib.ExitStack()

    def __call__(self, name):
        self.close()
        self.stack.enter_context(jax.named_scope(name))

    def close(self):
        self.stack.close()


class Links:
    def __init__(self, send_sem, recv_sem):
        self.send_sem, self.recv_sem = send_sem, recv_sem
        self.tags, self.slow, self.fast = itertools.count(), itertools.count(POOL), []
        self.pending, self.groups = [], []
        self.y_idx = lax.axis_index("yax")
        self.x_idx = lax.axis_index("xax")
        self.z, self.y = self.y_idx // NY, self.y_idx % NY
        self.chip, self.core = self.x_idx // CORES, self.x_idx % CORES

    def at_plane(self, dz, dy):
        return {"yax": (self.z + dz) % NZ * NY + (self.y + dy) % NY, "xax": self.x_idx}

    def slot_rows(self, dz, dy, rows):
        slot = (self.z + dz) % NZ * NY + (self.y + dy) % NY
        return pl.ds(pl.multiple_of(slot * rows, rows), rows)

    def line_id(self, dx, oc):
        core = 1 - self.core if oc else self.core
        return (self.chip + dx) % NX * CORES + core

    def at_line(self, dx, oc):
        return {"yax": self.y_idx, "xax": self.line_id(dx, oc)}

    def send(self, src, dst, where, tag=None, long=False):
        tag = next(self.tags) if tag is None else tag
        if long:
            sem = next(self.slow)
        else:
            sem = len(self.fast) % POOL
            if len(self.fast) >= POOL:
                self.fast[-POOL].wait_send()
        copy = pltpu.make_async_remote_copy(
            src_ref=src, dst_ref=dst, send_sem=self.send_sem.at[sem], recv_sem=self.recv_sem.at[tag],
            device_id=where, device_id_type=MESH_ID)
        copy.start()
        (self.pending if long else self.fast).append(copy)
        return copy

    def finish(self):
        for copy in self.pending + self.fast[-POOL:]:
            copy.wait_send()
        for group in self.groups:
            group.wait_sent()

    def barrier(self):
        barrier = pltpu.get_barrier_semaphore()
        peers = [self.at_line(*p) for p in LINE] + [self.at_plane(*p) for p in PLANE]
        for peer in peers:
            pl.semaphore_signal(barrier, inc=1, device_id=peer, device_id_type=MESH_ID)
        pl.semaphore_wait(barrier, len(peers))


def lane_sum(v):
    return jnp.sum(v, axis=-1, keepdims=True)


def plane_gather(links, buf, tags, hook, crossing, start):
    cols = buf.shape[-1]
    rows = buf.shape[1] // (NY * NZ)
    span = (cols - start) // 2
    partner = links.at_line(0, 1)

    class Part:
        def __init__(self, index):
            self.index, self.lo, self.got = index, start + index * span, {}

        def order(self, du, dv):
            return (du, dv) if self.index else (dv, du)

        def block(self, at, half=0, piece=None):
            width = span if piece is None else span // 2
            lo = self.lo if not piece else self.lo + width
            return buf.at[half, links.slot_rows(*self.order(*at), rows), pl.ds(lo, width)]

        def push(self, name, at, to, piece=None):
            ref = self.block(at, piece=piece)
            self.got[name] = links.send(ref, ref, links.at_plane(*self.order(*to)), next(tags))

        def spread(self, k, at):
            self.push(("v+", k), at, (0, 1))
            self.push(("v-", k), at, (0, -1))

        def give(self, at):
            crossing.send(self.block(at), self.block(at, half=1), partner)

        def wait(self, name):
            self.got[name].wait_recv()

    parts = [Part(index) for index in range(2)]
    offset = (0, -1, 1, 2)
    for p in parts:
        p.push("u+", (0, 0), (1, 0))
        p.push("u-", (0, 0), (-1, 0))
        p.spread(0, (0, 0))
    for p in parts:
        p.give((0, 0))
    for k, name in enumerate(("u+", "u-"), 1):
        for p in parts:
            p.wait(name)
            at = (offset[k], 0)
            p.push(("far", k), at, (-offset[k], 0), piece=k - 1)
            p.spread(k, at)
            p.give(at)
    hook()

    def arrive(p, k):
        for name, step in (("v+", -1), ("v-", 1)):
            p.wait((name, k))
            at = (offset[k], step)
            if (name == "v+") == (k in (0, 3)):
                p.push(("relay", k), at, (0, -step))
            p.give(at)

    for p in parts:
        arrive(p, 0)
    for p in parts:
        p.wait(("far", 1))
        p.wait(("far", 2))
        p.spread(3, (2, 0))
        p.give((2, 0))
    for k in range(1, len(offset)):
        for p in parts:
            arrive(p, k)
    for k in range(len(offset)):
        for p in parts:
            p.wait(("relay", k))
            p.give((offset[k], 2))


def norm_gather(links, own_slot, gain_buf, which, xbuf, stat, out, base, hook, skip=0):
    own_slot()
    rows, chunk = xbuf.shape[1:]
    tags = itertools.count(base)
    line = [links.send(xbuf.at[0], xbuf.at[NX - dx], links.at_line(dx, 0), next(tags)) for dx in FAR_FIRST]
    yield
    phase = Phases()
    for n, c in enumerate(line):
        phase(f"ng_line{which}_{n}")
        c.wait_recv()
    phase("ng_stats")
    held = xbuf[...].astype(jnp.float32)
    count = NX * chunk
    mean = lane_sum(jnp.sum(held, axis=0)) / count
    dev = held - mean[None]
    square = lane_sum(jnp.sum(dev * dev, axis=0))
    lane = lax.broadcasted_iota(jnp.int32, (rows, 128), 1)
    stat[0] = jnp.where(lane == 0, mean, square)
    links.send(stat.at[0], stat.at[1], links.at_line(0, 1), next(tags)).wait_recv()
    other_mean, other_square = stat[1, :, 0:1], stat[1, :, 1:2]
    both = (mean + other_mean) * 0.5
    gap = mean - other_mean
    var = (square + other_square + gap * gap * (count * 0.5)) / (2 * count)
    scale = lax.rsqrt(var + EPS)
    for e in range(skip, NX):
        out[0, links.slot_rows(0, 0, rows), e * chunk:(e + 1) * chunk] = (
            (xbuf[e].astype(jnp.float32) - both) * scale * gain_buf[e, which:which + 1, :]).astype(jnp.bfloat16)
    phase("ng_plane")
    crossing = Group(links, out.at[1])
    plane_gather(links, out, tags, lambda: hook(crossing), crossing, skip * chunk)
    phase.close()
    yield crossing


def step_kernel(vocab_own, own_rows, hid_ref, gain_a, gain_f, freq_ref, len_ref, k_hbm, v_hbm,
                wq_hbm, wk_hbm, wv_hbm, wo_ref, wg_ref, wu_ref, wd_hbm, emb_ref,
                knew_ref, vnew_ref, z_ref, norm_ref,
                wq_ref, wk_ref, wv_ref, k_buf, v_buf, wd_buf, wo_all, att, rc, gu_acc, n_buf, w_buf, wq_t, wq_buf, sel, sel_t, qx, qr, qy, qf,
                kvp, kvr, o_buf, o_got, o_all, act,
                part, ra1, rb1, ra2, rb2, acc_a, acc_b, xbuf, stat, xbuf2, stat2, gains, f_buf, emb_buf,
                w_relay, emb_relay, row_stats, lse_x, lse_y, send_sem, recv_sem, local_sem):
    links = Links(send_sem, recv_sem)
    phase = Phases()
    f32, bf16 = jnp.float32, jnp.bfloat16
    z, y, xid, yid = links.z, links.y, links.x_idx, links.y_idx
    total_rows, chunk = hid_ref.shape
    rows = total_rows // (NY * NZ)
    here_rows = links.slot_rows(0, 0, rows)
    half = chunk // 2
    nx2, nyz = 2 * NX, NY * NZ
    group = NY * rows
    head = 128
    pad = 8
    partner = links.at_line(0, 1)
    line_id = links.line_id
    gather_tags = len(HOPS) + 1 + len(PLANE) * CORES + CORES
    gather_base = [next(links.tags) for _ in range(gather_tags)][0]

    def dot(a, b):
        return jnp.dot(a, b, preferred_element_type=f32)

    def dot_t(a, b):
        return lax.dot_general(a, b, NT, preferred_element_type=f32)

    def rest(ref, n):
        return Group(links, ref.at[0:n - 1])

    local = []

    def fetch(src, dst):
        copy = pltpu.make_async_copy(src, dst, local_sem.at[len(local)])
        copy.start()
        local.append(copy)
        return copy

    ff = wg_ref.shape[1] // nx2

    def w_piece(ref, dx, oc):
        return ref.at[:, pl.ds(pl.multiple_of(line_id(dx, oc) * ff, ff), ff)]

    def w_slot(which, dx, oc):
        back = (NX - dx) % NX
        return w_buf.at[int(oc), pl.ds(back * chunk, chunk), pl.ds(which * ff, ff)]

    take = emb_buf.shape[1]

    def emb_start(xi):
        return pl.multiple_of(vocab_own * xi // pad * pad, pad)

    def emb_piece(dx, oc):
        return emb_ref.at[pl.ds(emb_start(line_id(dx, oc)), take), :]

    def emb_slot(dx, oc):
        return emb_buf.at[int(oc), :, pl.ds((NX - dx) % NX * chunk, chunk)]

    near_part = (take // 2 + 15) // 16 * 16
    far_parts = ((0, near_part), (near_part, take - near_part))

    def emb_half(oc, way):
        first, size = far_parts[way]
        return emb_ref.at[pl.ds(pl.multiple_of(emb_start(line_id(2, oc)) + first, pad), size), :]

    def emb_mid(oc, way):
        return emb_relay.at[way, oc, pl.ds(0, far_parts[way][1])]

    def emb_far_slot(oc, way):
        return emb_buf.at[int(oc), pl.ds(*far_parts[way]), pl.ds(2 * chunk, chunk)]

    got_wq = fetch(wq_hbm, wq_ref)
    own_w = [fetch(w_piece(wg_ref, 0, 0), w_slot(0, 0, 0)), fetch(w_piece(wu_ref, 0, 0), w_slot(1, 0, 0))]
    got_kv = [fetch(k_hbm, k_buf), fetch(v_hbm, v_buf)]
    got_wkv = [fetch(wk_hbm, wk_ref), fetch(wv_hbm, wv_ref)]
    got_wd = fetch(wd_hbm, wd_buf)
    own_emb = fetch(emb_piece(0, 0), emb_slot(0, 0))

    qc = wq_ref.shape[1]
    qs = qc // nx2
    per = head // qs
    wq_buf[...] = jnp.zeros(wq_buf.shape, bf16)

    phase("row_stats")
    eye = lax.broadcasted_iota(jnp.int32, (head, head), 0) == lax.broadcasted_iota(jnp.int32, (head, head), 1)
    blocks = total_rows // head

    def block_rows(b):
        return slice(b * head, (b + 1) * head)

    def to_row(v):
        return jnp.sum(jnp.where(eye, v, 0.0), axis=0, keepdims=True)

    def to_col(v):
        return lane_sum(jnp.where(eye, v, 0.0))

    row_stats[xid] = jnp.zeros((2 * pad, head), f32)
    for b in range(blocks):
        held = hid_ref[block_rows(b), :].astype(f32)
        mean = lane_sum(held) / chunk
        dev = held - mean
        row_stats[xid, b:b + 1, :] = to_row(mean)
        row_stats[xid, pad + b:pad + b + 1, :] = to_row(lane_sum(dev * dev))

    phase("barrier")
    links.barrier()

    phase("front_send")
    gains[0, 0:1, :] = gain_a[...]
    gains[0, 1:2, :] = gain_f[...]
    gains[0, 2:, :] = jnp.zeros((6, chunk), f32)

    def own_input():
        xbuf[0] = hid_ref[here_rows, :]

    w_far, emb_far = [], []
    w_got = [Group(links, w_buf.at[0, 0:2 * chunk]), Group(links, w_buf.at[1, 0:(NX - 1) * chunk])]
    w_last = Group(links, w_buf.at[0, 0:2 * chunk])
    emb_got = [Group(links, emb_buf.at[0, :, 0:(NX - 1) * chunk]), Group(links, emb_buf.at[1])]
    ways = [(way, hop, oc) for oc in (0, 1) for way, hop in enumerate(HOPS[:2])]

    def forward_weights():
        for (way, hop, oc), c in zip(ways, w_far):
            c.wait_recv()
            w_last.send(w_relay.at[way, oc], w_buf.at[oc, pl.ds(2 * chunk, chunk), pl.ds(way * ff, ff)],
                        links.at_line(hop, oc))

    def emb_out(some):
        for way, hop, oc in some:
            emb_far.append(links.send(emb_half(oc, way), emb_mid(oc, way), links.at_line(hop, 0), long=True))

    def emb_on(some, arrived):
        for (way, hop, oc), c in zip(some, arrived):
            c.wait_recv()
            emb_got[oc].send(emb_mid(oc, way), emb_far_slot(oc, way), links.at_line(hop, oc))

    def amid(crossing):
        forward_weights()
        stats_got.wait()
        means = row_stats[:, :pad, :]
        mean = jnp.sum(means, axis=0) / nx2
        gap = means - mean[None]
        square = jnp.sum(row_stats[:, pad:, :], axis=0) + jnp.sum(gap * gap, axis=0) * chunk
        scale = lax.rsqrt(square / (nx2 * chunk) + EPS)
        for b in range(blocks):
            n_buf[0, block_rows(b), 0:chunk] = (
                (hid_ref[block_rows(b), :].astype(f32) - to_col(mean[b:b + 1, :])) * to_col(scale[b:b + 1, :])
                * gains[0, 0:1, :]).astype(bf16)
        own = n_buf.at[0, :, 0:chunk]
        crossing.send(own, n_buf.at[1, :, 0:chunk], partner)

    front = norm_gather(links, own_input, gains, 0, xbuf, stat, n_buf, gather_base, amid, skip=1)
    next(front)
    gain_got = rest(gains, NX)
    for dx in HOPS:
        gain_got.send(gains.at[0], gains.at[NX - dx], links.at_line(dx, 0))
    stats_got = rest(row_stats, nx2)
    for p in LINE:
        stats_got.send(row_stats.at[xid], row_stats.at[xid], links.at_line(*p))
    for way, hop, oc in ways:
        w_far.append(links.send(w_piece((wg_ref, wu_ref)[way], 2, oc), w_relay.at[way, oc], links.at_line(hop, 0),
                                long=True))

    got_wq.wait()
    eye_q = (lax.broadcasted_iota(jnp.int32, (qc, qc), 0) == lax.broadcasted_iota(jnp.int32, (qc, qc), 1))
    wq_t[...] = dot_t(eye_q.astype(bf16), wq_ref[...]).astype(bf16)
    wq_buf[0, 0:qs, 0:chunk] = wq_t[pl.ds(pl.multiple_of(xid * qs, qs), qs), :]

    def wq_rows(dx, oc):
        return wq_t.at[pl.ds(pl.multiple_of(line_id(dx, oc) * qs, qs), qs), :]

    def wq_slot(dx, oc):
        return wq_buf.at[oc, pl.ds(0, qs), pl.ds((NX - dx) % NX * chunk, chunk)]

    wq_got = Group(links, wq_t.at[0:qc - qs])
    for dx, oc in LINE:
        wq_got.send(wq_rows(dx, oc), wq_slot(dx, oc), links.at_line(dx, oc))
    for which, ref in enumerate((wg_ref, wu_ref)):
        for dx, oc in LINE[:1] + NEAR:
            w_got[oc].send(w_piece(ref, dx, oc), w_slot(which, dx, oc), links.at_line(dx, oc))

    phase("selections")
    r_id = lax.broadcasted_iota(jnp.int32, (nx2 * nyz * pad, 1), 0)
    r_j = r_id % pad
    r_src = jnp.where(r_j < own_rows, r_id // pad % nyz * rows + r_id // (pad * nyz) * own_rows + r_j, -1)
    s_id = lax.broadcasted_iota(jnp.int32, (1, total_rows), 1)
    sel[...] = jnp.where(r_src == s_id, 1.0, 0.0).astype(bf16)
    t_id = lax.broadcasted_iota(jnp.int32, (group, 1), 0)
    t_in = t_id % rows
    t_src = t_in // own_rows * (NY * pad) + t_id // rows * pad + t_in % own_rows
    u_id = lax.broadcasted_iota(jnp.int32, (1, nx2 * NY * pad), 1)
    sel_t[...] = jnp.where(t_src == u_id, 1.0, 0.0).astype(bf16)
    k_id = lax.broadcasted_iota(jnp.int32, (nx2 * pad, rows), 0)
    k_src = jnp.where(k_id % pad < own_rows, k_id // pad * own_rows + k_id % pad, -1)
    sel_kv = jnp.where(k_src == lax.broadcasted_iota(jnp.int32, (nx2 * pad, rows), 1), 1.0, 0.0).astype(bf16)

    phase.close()
    gain_got.wait()
    lane = lax.broadcasted_iota(jnp.int32, (1, head), 1)
    lengths = []
    for b in range(own_rows):
        index = (yid * nx2 + xid) * own_rows + b
        row = len_ref[pl.ds(index // head, 1), :].astype(f32)
        lengths.append(lane_sum(jnp.where(lane == index % head, row, 0.0)))
    lengths = jnp.concatenate(lengths + lengths[:pad - own_rows], axis=0)
    angles = lengths * freq_ref[...]
    cos_all = jnp.cos(angles)
    sin_all = jnp.sin(angles) * jnp.where(lane < head // 2, -1.0, 1.0)

    crossing = next(front)
    phase("ng_cross")
    crossing.wait()
    phase("kv_part")

    for c in got_wkv:
        c.wait()
    n_own = dot(sel_kv, n_buf[0, links.slot_rows(0, 0, rows), 0:chunk]).astype(bf16)
    kvp[:, :, :head] = dot(n_own, wk_ref[...]).reshape(nx2, pad, head)
    kvp[:, :, head:] = dot(n_own, wv_ref[...]).reshape(nx2, pad, head)
    kv_got = rest(kvr, nx2)
    for p in LINE:
        kv_got.send(kvp.at[line_id(*p)], kvr.at[xid], links.at_line(*p))
    kvr[xid] = kvp[xid]

    phase("wait_wq")
    wq_got.wait()
    phase("q_mm")
    q_all = jnp.concatenate([
        (dot_t(n_buf[0, i * group:(i + 1) * group, :], wq_buf[0])
         + dot_t(n_buf[1, i * group:(i + 1) * group, :], wq_buf[1])).astype(bf16) for i in range(NZ)], axis=0)
    span = nyz * pad
    for i in range(nx2):
        chosen = dot(sel[i * span:(i + 1) * span, :], q_all)
        quarter = span // per
        packed = chosen[:quarter, :]
        for g in range(1, per):
            packed = packed + pltpu.roll(chosen[g * quarter:(g + 1) * quarter, :], g * qs, 1)
        qx[i] = packed.astype(bf16)
    q_got = rest(qr, nx2)
    for p in LINE:
        q_got.send(qx.at[line_id(*p)], qr.at[xid], links.at_line(*p))
    qr[xid] = qx[xid]

    phase("wait_w")
    for c in own_w:
        c.wait()
    for c in w_got:
        c.wait()
    phase("gate_up")

    def act_at(k, dx):
        return act.at[(z + k) % NZ, :, pl.ds(pl.multiple_of(line_id(dx, 0) * ff, ff), ff)]

    def act_out(k, dx, to_dx):
        return links.send(act_at(k, dx), act_at(k, dx), links.at_line(to_dx, 0))

    def act_give(k, dx):
        cross[k].send(act_at(k, dx), act_at(k, dx), partner)

    turns = (2, 1, 3, 0)
    early, late = turns[:2], turns[2:]
    near_act, far_act = {}, {}
    cross = {k: Group(links, act.at[0, :, 0:NX * ff]) for k in turns}
    def group_rows(k):
        return pl.ds(pl.multiple_of((z + k) % NZ * group, group), group)

    far = slice(2 * chunk, (NX - 1) * chunk)

    def over(k, part_cols):
        return dot(n_buf[0, group_rows(k), part_cols], w_buf[0, part_cols, :]) + dot(
            n_buf[1, group_rows(k), part_cols], w_buf[1, part_cols, :])

    for k in turns:
        gu_acc[k] = over(k, slice(0, far.start)) + over(k, slice(far.stop, NX * chunk))
    phase("wait_w_far")
    w_last.wait()
    phase("gate_up_far")
    for k in turns:
        both = (gu_acc[k] + over(k, far)).astype(bf16).astype(f32)
        gate, up = both[:, :ff], both[:, ff:]
        act_at(k, 0)[...] = (gate * jax.nn.sigmoid(gate) * up).astype(bf16)
        near_act[k] = [(dx, act_out(k, 0, dx)) for dx in HOPS[:2]]
        act_give(k, 0)

    def act_pass(k):
        for dx, c in near_act[k]:
            c.wait_recv()
            if (k in early) == (dx == 1):
                far_act[k] = act_out(k, NX - dx, dx)
            act_give(k, NX - dx)

    low, high = pl.ds(0, half), pl.ds(half, half)
    first_a, first_b = Group(links, ra1), Group(links, rb1)

    def act_use(k):
        cross[k].wait()
        g = (z + k) % NZ
        part[g] = dot(act[g], wd_buf[...]).reshape(NY, rows, chunk)
        if k:
            first_b.send(part.at[g, :, :, high], rb1.at[k - 1], links.at_plane(k, 0))

    def along_y(k):
        g = (z + k) % NZ
        for d in early + late[:1]:
            first_a.send(part.at[g, (y + d) % NY, :, low], ra1.at[d - 1, g], links.at_plane(0, d))

    def act_far(ks):
        for k in ks:
            far_act[k].wait_recv()
            act_give(k, 2)

    phase("wait_q")
    q_got.wait()
    phase("q_sum")
    lane_group = lax.broadcasted_iota(jnp.int32, (1, head), 1) // qs
    for j in range(qc // head):
        came = [qr[j * per + i].astype(f32) for i in range(per)]
        for g in range(per):
            piece = jnp.zeros((span // per, head), f32)
            for i in range(per):
                piece = piece + jnp.where(lane_group == i, pltpu.roll(came[i], (i - g) % per * qs, 1), 0.0)
            qy[g * per:(g + 1) * per, :, j * head:(j + 1) * head] = piece.reshape(per, pad, head)

    def plane_id(dz, dy):
        return (z + dz) % NZ * NY + (y + dy) % NY

    y_got = rest(qf, nyz)
    for p in PLANE:
        y_got.send(qy.at[plane_id(*p)], qf.at[yid], links.at_plane(*p))
    qf[yid] = qy[yid]

    def wo_rows(dz):
        return wo_all.at[pl.ds(pl.multiple_of((z + dz) % NZ * qc, qc), qc), :]

    wo_got = Group(links, wo_all.at[0:(NZ - 1) * qc])
    for d in HOPS:
        wo_got.send(wo_ref, wo_rows(0), links.at_plane(d, 0))
    own_wo = fetch(wo_ref, wo_rows(0))

    phase("act_pass")
    for k in early:
        act_pass(k)
    phase("wait_kv")
    kv_got.wait()
    kv_sum = kvr[0]
    for i in range(1, nx2):
        kv_sum = kv_sum + kvr[i]
    kv_new = kv_sum.astype(bf16).astype(f32)

    def turn(v, b=None):
        cos, sin = (cos_all, sin_all) if b is None else (cos_all[b:b + 1, :], sin_all[b:b + 1, :])
        return (v * cos + pltpu.roll(v, head // 2, 1) * sin).astype(bf16)

    k_new = turn(kv_new[:, :head])
    knew_ref[...] = k_new
    vnew_ref[...] = kv_new[:, head:].astype(bf16)
    k_row, v_row = k_new.astype(f32), kv_new[:, head:]
    phase("act_pass2")
    for k in late:
        act_pass(k)
    emb_out(ways[:2])
    phase("wait_qy")
    for c in got_kv:
        c.wait()
    y_got.wait()
    phase("attention")
    seq = k_buf.shape[1]
    score_scale = head ** -0.5
    position = lax.broadcasted_iota(jnp.int32, (1, seq), 1).astype(f32)
    o_buf[...] = jnp.zeros(o_buf.shape, f32)
    for b in range(own_rows):
        q_b = jnp.concatenate([turn(qf[:, b, j * head:(j + 1) * head], b) for j in range(qc // head)], axis=0)
        scores = dot_t(q_b, k_buf[b]) * score_scale
        score_new = lane_sum(q_b.astype(f32) * k_row[b:b + 1, :]) * score_scale
        valid = position < lengths[b:b + 1, :]
        top = jnp.maximum(jnp.max(jnp.where(valid, scores, -jnp.inf), axis=-1, keepdims=True), score_new)
        weights = jnp.where(valid, jnp.exp(scores - top), 0.0)
        weight_new = jnp.exp(score_new - top)
        denom = lane_sum(weights) + weight_new
        o_b = dot((weights / denom).astype(bf16), v_buf[b])
        o_b = o_b + (weight_new / denom).astype(bf16).astype(f32) * v_row[b:b + 1, :]
        o_b = o_b.astype(bf16).astype(f32)
        for j in range(qc // head):
            o_buf[:, :, b, j * head:(j + 1) * head] = o_b[j * nyz:(j + 1) * nyz, :].reshape(NZ, NY, head)
    o_back = rest(o_got, NY)
    for d in HOPS:
        o_back.send(o_buf.at[:, (y + d) % NY], o_got.at[y], links.at_plane(0, d))
    phase("act_early")
    act_far(turns)
    got_wd.wait()
    for k in turns:
        act_use(k)
        along_y(k)
    o_got[y] = o_buf[:, y]

    phase("wait_oy")
    o_back.wait()
    for i in range(NZ):
        o_all[xid, :, i * qc:(i + 1) * qc] = o_got[:, i].reshape(NY * pad, qc).astype(bf16)
    o_here = o_all.at[xid]
    o_line = [links.send(o_here, o_here, links.at_line(dx, 0)) for dx in HOPS]
    o_cross = rest(o_all, NX + 1)
    o_cross.send(o_here, o_here, partner)
    emb_out(ways[2:])
    emb_got[1].send(emb_piece(0, 1), emb_slot(0, 1), partner)
    emb_on(ways[:2], emb_far[:2])
    phase("wait_o")
    for dx, c in zip(HOPS, o_line):
        c.wait_recv()
        came = o_all.at[line_id(NX - dx, 0)]
        o_cross.send(came, came, partner)
    wo_got.wait()
    own_wo.wait()
    o_cross.wait()
    phase("out_mm")
    o_nat = dot(sel_t[...], o_all[...].reshape(nx2 * NY * pad, NZ * qc)).astype(bf16)
    att[...] = dot(o_nat, wo_all[...]).reshape(NY, rows, chunk)
    att_got = Group(links, rc)
    for d in HOPS:
        att_got.send(att.at[(y + d) % NY], rc.at[d - 1], links.at_plane(0, d))

    phase("wait_rs1")
    first_b.wait()
    acc_b[...] = (part[z, :, :, half:] + rb1[0]) + (rb1[1] + rb1[2])
    second = [Group(links, rb2), Group(links, ra2)]
    for d in HOPS:
        second[0].send(acc_b.at[(y + d) % NY], rb2.at[d - 1], links.at_plane(0, d))
    phase("wait_rs1a")
    first_a.wait()
    acc_a[...] = (part[:, y, :, :half] + ra1[0]) + (ra1[1] + ra1[2])
    for d in HOPS:
        second[1].send(acc_a.at[(z + d) % NZ], ra2.at[d - 1], links.at_plane(d, 0))
    phase("wait_att")
    att_got.wait()
    phase("wait_rs2")
    for c in second:
        c.wait()
    phase("rs_sum2")
    def own_residual():
        res = hid_ref[here_rows, :].astype(f32) + ((att[y] + rc[0]) + (rc[1] + rc[2]))
        xbuf2[0, :, :half] = res[:, :half] + ((acc_a[z] + ra2[0]) + (ra2[1] + ra2[2]))
        xbuf2[0, :, half:] = res[:, half:] + ((acc_b[y] + rb2[0]) + (rb2[1] + rb2[2]))

    back = norm_gather(links, own_residual, gains, 1, xbuf2, stat2, f_buf, gather_base, lambda crossing: None)
    next(back)
    emb_on(ways[2:], emb_far[2:])
    for dx, oc in NEAR:
        emb_got[oc].send(emb_piece(dx, oc), emb_slot(dx, oc), links.at_line(dx, oc))
    phase.close()
    crossing = next(back)
    phase("wait_emb")
    own_emb.wait()
    for c in emb_got:
        c.wait()

    phase("logits")
    wide_n = 256
    for h in range(CORES):
        if h:
            crossing.wait()
        for i in range(total_rows // wide_n):
            cols = slice(i * wide_n, (i + 1) * wide_n)
            term = dot_t(emb_buf[h], f_buf[h, cols, :])
            z_ref[:, cols] = z_ref[:, cols] + term if h else term

    phase("lse_own")
    shift = vocab_own * xid - emb_start(xid)
    vid = lax.broadcasted_iota(jnp.int32, (take, 1), 0)
    own = (vid >= shift) & (vid < shift + vocab_own)
    for b in range(blocks):
        zb = jnp.where(own, z_ref[:, b * 128:(b + 1) * 128], -jnp.inf)
        top = jnp.max(zb, axis=0, keepdims=True)
        lse_x[xid, b:b + 1, :] = top
        lse_x[xid, 8 + b:9 + b, :] = jnp.sum(jnp.exp(zb - top), axis=0, keepdims=True)
    for b in range(blocks, 8):
        lse_x[xid, b:b + 1, :] = jnp.zeros((1, 128), f32)
        lse_x[xid, 8 + b:9 + b, :] = jnp.ones((1, 128), f32)

    def merge(ref):
        tops = ref[:, :8, :]
        top = jnp.max(tops, axis=0)
        return top, jnp.sum(ref[:, 8:, :] * jnp.exp(tops - top[None]), axis=0)

    phase("lse_line")
    got = rest(lse_x, nx2)
    for p in LINE:
        got.send(lse_x.at[xid], lse_x.at[xid], links.at_line(*p))
    got.wait()
    top, mass = merge(lse_x)
    lse_y[yid, :8, :] = top
    lse_y[yid, 8:, :] = mass
    phase("lse_plane")
    got = rest(lse_y, nyz)
    for p in PLANE:
        got.send(lse_y.at[yid], lse_y.at[yid], links.at_plane(*p))
    got.wait()
    top, mass = merge(lse_y)
    norm_ref[...] = top + jnp.log(mass)
    phase("finish")
    links.finish()
    phase.close()


def whole_step(hidden, freq, lens, k_cache, v_cache, g_attn, w_query, w_key, w_value,
               w_gate, w_up, w_out, w_down, g_final, embedding):
    total_rows, chunk = hidden.shape
    own_rows, seq, head = k_cache.shape
    rows = total_rows // (NY * NZ)
    vocab_own = embedding.shape[0] // (2 * NX)
    take = (vocab_own + 6 + 15) // 16 * 16
    half = chunk // 2
    qc = w_query.shape[1]
    ff = w_gate.shape[1] // (2 * NX)
    f32, bf16 = jnp.float32, jnp.bfloat16
    nyz, nx2, pad = NY * NZ, 2 * NX, 8
    vmem = pl.BlockSpec(memory_space=pltpu.VMEM)
    hbm = pl.BlockSpec(memory_space=pl.ANY)
    V = pltpu.VMEM
    return pl.pallas_call(
        lambda *refs: step_kernel(vocab_own, own_rows, *refs),
        out_shape=(jax.ShapeDtypeStruct((pad, head), bf16), jax.ShapeDtypeStruct((pad, head), bf16),
                   jax.ShapeDtypeStruct((take, total_rows), f32), jax.ShapeDtypeStruct((pad, head), f32)),
        in_specs=[vmem] * 5 + [hbm] * 10,
        out_specs=(vmem,) * 4,
        scratch_shapes=[
            V((chunk, qc), bf16), V((chunk, head), bf16), V((chunk, head), bf16),
            V((own_rows, seq, head), bf16), V((own_rows, seq, head), bf16),
            V((nx2 * ff, chunk), bf16), V((NZ * qc, chunk), bf16), V((NY, rows, chunk), f32), V((3, rows, chunk), f32),
            V((NZ, NY * rows, 2 * ff), f32), V((2, total_rows, NX * chunk), bf16), V((2, NX * chunk, 2 * ff), bf16),
            V((qc, chunk), bf16), V((2, head, NX * chunk), bf16),
            V((nx2 * nyz * pad, total_rows), bf16), V((NY * rows, nx2 * NY * pad), bf16),
            V((nx2, nyz * pad // 4, head), bf16), V((nx2, nyz * pad // 4, head), bf16),
            V((nyz, pad, qc), f32), V((nyz, pad, qc), f32),
            V((nx2, pad, 2 * head), f32), V((nx2, pad, 2 * head), f32),
            V((NZ, NY, pad, qc), f32), V((NY, NZ, pad, qc), f32), V((nx2, NY * pad, NZ * qc), bf16),
            V((NZ, NY * rows, nx2 * ff), bf16),
            V((NZ, NY, rows, chunk), f32),
            V((3, NZ, rows, half), f32), V((3, NY, rows, half), f32), V((3, rows, half), f32), V((3, rows, half), f32),
            V((NZ, rows, half), f32), V((NY, rows, half), f32),
            V((NX, rows, chunk), bf16), V((2, rows, 128), f32), V((NX, rows, chunk), f32), V((2, rows, 128), f32),
            V((NX, 8, chunk), f32),
            V((2, total_rows, NX * chunk), bf16), V((2, take, NX * chunk), bf16),
            V((2, 2, chunk, ff), bf16), V((2, 2, (take // 2 + 15) // 16 * 16, chunk), bf16),
            V((nx2, 16, 128), f32), V((nx2, 16, 128), f32), V((nyz, 16, 128), f32),
            pltpu.SemaphoreType.DMA((SENDS,)), pltpu.SemaphoreType.DMA((TAGS,)), pltpu.SemaphoreType.DMA((10,)),
        ],
        compiler_params=pltpu.CompilerParams(
            collective_id=1, has_side_effects=True, vmem_limit_bytes=60 << 20),
        name="decode_step",
    )(hidden, g_attn[None, :], g_final[None, :], freq, lens, k_cache, v_cache,
      w_query, w_key, w_value, w_out, w_gate, w_up, w_down, embedding)


def solution(mesh):
    row_spec = P(("dp", "yax", "xax"))

    def local_step(hidden, cache_len, k_cache, v_cache, g_attn, w_query, w_key, w_value,
                   w_gate, w_up, w_out, w_down, g_final, embedding):
        rows = hidden.shape[0]
        half_dim = k_cache.shape[2] // 2
        inv_freq = ROPE_BASE ** (-(np.arange(half_dim, dtype=np.float64) * 2.0) / (2 * half_dim))
        freq = np.concatenate([inv_freq, inv_freq])[None, :].astype(np.float32)
        key_own, value_own, logits_wide, norm_tile = whole_step(
            hidden, freq, cache_len.reshape(rows // 128, 128), k_cache, v_cache, g_attn, w_query, w_key, w_value,
            w_gate, w_up, w_out, w_down, g_final, embedding)
        own_rows = k_cache.shape[0]
        vocab_own = embedding.shape[0] // (CORES * NX)
        first = vocab_own * lax.axis_index("xax")
        logits = lax.dynamic_slice_in_dim(logits_wide, first - first // 8 * 8, vocab_own, axis=0)
        log_norm = norm_tile[:rows // 128].reshape(rows)
        return key_own[:own_rows], value_own[:own_rows], (logits - log_norm).T, log_norm

    in_specs = (P("dp", "xax"), P("dp"), row_spec, row_spec, P("xax"), P("xax", "yax"),
                P("xax"), P("xax"), P("xax", "yax"), P("xax", "yax"),
                P("yax", "xax"), P("yax", "xax"), P("xax"), P("yax", "xax"))
    out_specs = (row_spec, row_spec, P("dp", ("yax", "xax")), P("dp"))
    return jax.shard_map(local_step, mesh=mesh, in_specs=in_specs, out_specs=out_specs, check_vma=False)
```

```python
import contextlib
import itertools

import jax
import jax.numpy as jnp
import numpy as np
from jax import lax
from jax.experimental import pallas as pl
from jax.experimental.pallas import tpu as pltpu
from jax.sharding import PartitionSpec as P

EPS = 1e-6
ROPE_BASE = 10000.0
MESH_ID = pl.DeviceIdType.MESH
NY = NZ = NX = 4
CORES = 2
POOL, SENDS, TAGS = 24, 59, 89
HOPS = (1, 3, 2)
FAR_FIRST = (2, 1, 3)
LINE = [(0, 1), (1, 0), (3, 0), (1, 1), (3, 1), (2, 0), (2, 1)]
NEAR = LINE[1:5]
NT = (((1,), (1,)), ((), ()))
PLANE = [(dz, dy) for dz in range(NZ) for dy in range(NY) if dz or dy]


class Group:
    def __init__(self, links, whole):
        self.links, self.whole = links, whole
        self.tag, self.sem = next(links.tags), next(links.slow)
        links.groups.append(self)

    def send(self, src, dst, where):
        pltpu.make_async_remote_copy(
            src_ref=src, dst_ref=dst, send_sem=self.links.send_sem.at[self.sem],
            recv_sem=self.links.recv_sem.at[self.tag], device_id=where, device_id_type=MESH_ID).start()

    def wait(self):
        pltpu.make_async_copy(self.whole, self.whole, self.links.recv_sem.at[self.tag]).wait()

    def wait_sent(self):
        pltpu.make_async_copy(self.whole, self.whole, self.links.send_sem.at[self.sem]).wait()


class Phases:
    def __init__(self):
        self.stack = contextlib.ExitStack()

    def __call__(self, name):
        self.close()
        self.stack.enter_context(jax.named_scope(name))

    def close(self):
        self.stack.close()


class Links:
    def __init__(self, send_sem, recv_sem):
        self.send_sem, self.recv_sem = send_sem, recv_sem
        self.tags, self.slow, self.fast = itertools.count(), itertools.count(POOL), []
        self.pending, self.groups = [], []
        self.y_idx = lax.axis_index("yax")
        self.x_idx = lax.axis_index("xax")
        self.z, self.y = self.y_idx // NY, self.y_idx % NY
        self.chip, self.core = self.x_idx // CORES, self.x_idx % CORES

    def at_plane(self, dz, dy):
        return {"yax": (self.z + dz) % NZ * NY + (self.y + dy) % NY, "xax": self.x_idx}

    def slot_rows(self, dz, dy, rows):
        slot = (self.z + dz) % NZ * NY + (self.y + dy) % NY
        return pl.ds(pl.multiple_of(slot * rows, rows), rows)

    def line_id(self, dx, oc):
        core = 1 - self.core if oc else self.core
        return (self.chip + dx) % NX * CORES + core

    def at_line(self, dx, oc):
        return {"yax": self.y_idx, "xax": self.line_id(dx, oc)}

    def send(self, src, dst, where, tag=None, long=False):
        tag = next(self.tags) if tag is None else tag
        if long:
            sem = next(self.slow)
        else:
            sem = len(self.fast) % POOL
            if len(self.fast) >= POOL:
                self.fast[-POOL].wait_send()
        copy = pltpu.make_async_remote_copy(
            src_ref=src, dst_ref=dst, send_sem=self.send_sem.at[sem], recv_sem=self.recv_sem.at[tag],
            device_id=where, device_id_type=MESH_ID)
        copy.start()
        (self.pending if long else self.fast).append(copy)
        return copy

    def finish(self):
        for copy in self.pending + self.fast[-POOL:]:
            copy.wait_send()
        for group in self.groups:
            group.wait_sent()

    def barrier(self):
        barrier = pltpu.get_barrier_semaphore()
        peers = [self.at_line(*p) for p in LINE] + [self.at_plane(*p) for p in PLANE]
        for peer in peers:
            pl.semaphore_signal(barrier, inc=1, device_id=peer, device_id_type=MESH_ID)
        pl.semaphore_wait(barrier, len(peers))


def lane_sum(v):
    return jnp.sum(v, axis=-1, keepdims=True)


def plane_gather(links, buf, tags, hooks, crossing, start):
    cols = buf.shape[-1]
    rows = buf.shape[1] // (NY * NZ)
    span = (cols - start) // 2
    partner = links.at_line(0, 1)

    class Part:
        def __init__(self, index):
            self.index, self.lo, self.got = index, start + index * span, {}

        def order(self, du, dv):
            return (du, dv) if self.index else (dv, du)

        def block(self, at, half=0, piece=None):
            width = span if piece is None else span // 2
            lo = self.lo if not piece else self.lo + width
            return buf.at[half, links.slot_rows(*self.order(*at), rows), pl.ds(lo, width)]

        def push(self, name, at, to, piece=None):
            ref = self.block(at, piece=piece)
            self.got[name] = links.send(ref, ref, links.at_plane(*self.order(*to)), next(tags))

        def spread(self, k, at):
            self.push(("v+", k), at, (0, 1))
            self.push(("v-", k), at, (0, -1))

        def give(self, at):
            crossing.send(self.block(at), self.block(at, half=1), partner)

        def wait(self, name):
            self.got[name].wait_recv()

    parts = [Part(index) for index in range(2)]
    offset = (0, -1, 1, 2)
    for p in parts:
        p.push("u+", (0, 0), (1, 0))
        p.push("u-", (0, 0), (-1, 0))
        p.spread(0, (0, 0))
    for p in parts:
        p.give((0, 0))
    hooks[0](crossing)
    for k, name in enumerate(("u+", "u-"), 1):
        for p in parts:
            p.wait(name)
            at = (offset[k], 0)
            p.push(("far", k), at, (-offset[k], 0), piece=k - 1)
            p.spread(k, at)
            p.give(at)
    hooks[1]()

    def arrive(p, k):
        for name, step in (("v+", -1), ("v-", 1)):
            p.wait((name, k))
            at = (offset[k], step)
            if (name == "v+") == (k in (0, 3)):
                p.push(("relay", k), at, (0, -step))
            p.give(at)

    for p in parts:
        arrive(p, 0)
    for p in parts:
        p.wait(("far", 1))
        p.wait(("far", 2))
        p.spread(3, (2, 0))
        p.give((2, 0))
    for k in range(1, len(offset)):
        for p in parts:
            arrive(p, k)
    for k in range(len(offset)):
        for p in parts:
            p.wait(("relay", k))
            p.give((offset[k], 2))


def norm_gather(links, own_slot, gain_buf, which, xbuf, stat, out, base, hooks, skip=0):
    rows, chunk = xbuf.shape[1:]
    tags = itertools.count(base)
    line = []
    for cols in own_slot():
        line += [links.send(xbuf.at[0, :, cols], xbuf.at[NX - dx, :, cols], links.at_line(dx, 0), next(tags))
                 for dx in FAR_FIRST]
    yield
    phase = Phases()
    for n, c in enumerate(line):
        phase(f"ng_line{which}_{n}")
        c.wait_recv()
    phase("ng_stats")
    held = xbuf[...].astype(jnp.float32)
    count = NX * chunk
    mean = lane_sum(jnp.sum(held, axis=0)) / count
    dev = held - mean[None]
    square = lane_sum(jnp.sum(dev * dev, axis=0))
    lane = lax.broadcasted_iota(jnp.int32, (rows, 128), 1)
    stat[0] = jnp.where(lane == 0, mean, square)
    links.send(stat.at[0], stat.at[1], links.at_line(0, 1), next(tags)).wait_recv()
    other_mean, other_square = stat[1, :, 0:1], stat[1, :, 1:2]
    both = (mean + other_mean) * 0.5
    gap = mean - other_mean
    var = (square + other_square + gap * gap * (count * 0.5)) / (2 * count)
    scale = lax.rsqrt(var + EPS)
    for e in range(skip, NX):
        out[0, links.slot_rows(0, 0, rows), e * chunk:(e + 1) * chunk] = (
            (xbuf[e].astype(jnp.float32) - both) * scale * gain_buf[e, which:which + 1, :]).astype(jnp.bfloat16)
    phase("ng_plane")
    crossing = Group(links, out.at[1])
    plane_gather(links, out, tags, hooks, crossing, skip * chunk)
    phase.close()
    yield crossing


def step_kernel(vocab_own, own_rows, hid_ref, gain_a, gain_f, freq_ref, len_ref, k_hbm, v_hbm,
                wq_hbm, wk_hbm, wv_hbm, wo_ref, wg_ref, wu_ref, wd_hbm, emb_ref,
                knew_ref, vnew_ref, z_hbm, norm_ref,
                z_ref, wq_ref, wk_ref, wv_ref, k_buf, v_buf, wd_buf, wo_all, att, rc, gu_acc, n_buf, w_buf, wq_t, wq_buf, sel, sel_t, qx, qr, qy, qf,
                kvp, kvr, o_buf, o_got, o_all, act,
                part, ra1, rb1, ra2, rb2, acc_a, acc_b, xbuf, stat, xbuf2, stat2, gains, f_buf, emb_buf,
                w_relay, emb_relay, row_stats, lse_x, lse_y, send_sem, recv_sem, local_sem):
    links = Links(send_sem, recv_sem)
    phase = Phases()
    f32, bf16 = jnp.float32, jnp.bfloat16
    z, y, xid, yid = links.z, links.y, links.x_idx, links.y_idx
    total_rows, chunk = hid_ref.shape
    rows = total_rows // (NY * NZ)
    here_rows = links.slot_rows(0, 0, rows)
    half = chunk // 2
    nx2, nyz = 2 * NX, NY * NZ
    group = NY * rows
    head = 128
    pad = 8
    partner = links.at_line(0, 1)
    line_id = links.line_id
    gather_tags = 2 * len(HOPS) + 1 + len(PLANE) * CORES + CORES
    gather_base = [next(links.tags) for _ in range(gather_tags)][0]

    def dot(a, b):
        return jnp.dot(a, b, preferred_element_type=f32)

    def dot_t(a, b):
        return lax.dot_general(a, b, NT, preferred_element_type=f32)

    def rest(ref, n):
        return Group(links, ref.at[0:n - 1])

    local = []

    def fetch(src, dst):
        copy = pltpu.make_async_copy(src, dst, local_sem.at[len(local)])
        copy.start()
        local.append(copy)
        return copy

    ff = wg_ref.shape[1] // nx2

    def w_piece(ref, dx, oc):
        return ref.at[:, pl.ds(pl.multiple_of(line_id(dx, oc) * ff, ff), ff)]

    def w_slot(which, dx, oc):
        back = (NX - dx) % NX
        return w_buf.at[int(oc), pl.ds(back * chunk, chunk), pl.ds(which * ff, ff)]

    take = emb_buf.shape[1]

    def emb_start(xi):
        return pl.multiple_of(vocab_own * xi // pad * pad, pad)

    def emb_piece(dx, oc):
        return emb_ref.at[pl.ds(emb_start(line_id(dx, oc)), take), :]

    def emb_slot(dx, oc):
        return emb_buf.at[int(oc), :, pl.ds((NX - dx) % NX * chunk, chunk)]

    near_part = (take // 2 + 15) // 16 * 16
    far_parts = ((0, near_part), (near_part, take - near_part))

    def emb_half(oc, way):
        first, size = far_parts[way]
        return emb_ref.at[pl.ds(pl.multiple_of(emb_start(line_id(2, oc)) + first, pad), size), :]

    def emb_mid(oc, way):
        return emb_relay.at[way, oc, pl.ds(0, far_parts[way][1])]

    def emb_far_slot(oc, way):
        return emb_buf.at[int(oc), pl.ds(*far_parts[way]), pl.ds(2 * chunk, chunk)]

    got_wq = fetch(wq_hbm, wq_ref)
    own_w = [fetch(w_piece(wg_ref, 0, 0), w_slot(0, 0, 0)), fetch(w_piece(wu_ref, 0, 0), w_slot(1, 0, 0))]
    got_kv = [fetch(k_hbm, k_buf), fetch(v_hbm, v_buf)]
    got_wkv = [fetch(wk_hbm, wk_ref), fetch(wv_hbm, wv_ref)]
    got_wd = fetch(wd_hbm, wd_buf)
    own_emb = fetch(emb_piece(0, 0), emb_slot(0, 0))

    qc = wq_ref.shape[1]
    qs = qc // nx2
    per = head // qs
    wq_buf[...] = jnp.zeros(wq_buf.shape, bf16)

    phase("row_stats")
    eye = lax.broadcasted_iota(jnp.int32, (head, head), 0) == lax.broadcasted_iota(jnp.int32, (head, head), 1)
    blocks = total_rows // head

    def block_rows(b):
        return slice(b * head, (b + 1) * head)

    def to_row(v):
        return jnp.sum(jnp.where(eye, v, 0.0), axis=0, keepdims=True)

    def to_col(v):
        return lane_sum(jnp.where(eye, v, 0.0))

    row_stats[xid] = jnp.zeros((2 * pad, head), f32)
    for b in range(blocks):
        held = hid_ref[block_rows(b), :].astype(f32)
        mean = lane_sum(held) / chunk
        dev = held - mean
        row_stats[xid, b:b + 1, :] = to_row(mean)
        row_stats[xid, pad + b:pad + b + 1, :] = to_row(lane_sum(dev * dev))

    phase("barrier")
    links.barrier()

    phase("front_send")
    gains[0, 0:1, :] = gain_a[...]
    gains[0, 1:2, :] = gain_f[...]
    gains[0, 2:, :] = jnp.zeros((6, chunk), f32)

    def own_input():
        xbuf[0] = hid_ref[here_rows, :]
        yield pl.ds(0, chunk)

    w_far, emb_far = [], []
    w_got = [Group(links, w_buf.at[0, 0:2 * chunk]), Group(links, w_buf.at[1, 0:(NX - 1) * chunk])]
    w_last = Group(links, w_buf.at[0, 0:2 * chunk])
    emb_got = [Group(links, emb_buf.at[0, :, 0:(NX - 1) * chunk]), Group(links, emb_buf.at[1])]
    ways = [(way, hop, oc) for oc in (0, 1) for way, hop in enumerate(HOPS[:2])]

    def forward_weights():
        for (way, hop, oc), c in zip(ways, w_far):
            c.wait_recv()
            w_last.send(w_relay.at[way, oc], w_buf.at[oc, pl.ds(2 * chunk, chunk), pl.ds(way * ff, ff)],
                        links.at_line(hop, oc))

    def emb_out(some):
        for way, hop, oc in some:
            emb_far.append(links.send(emb_half(oc, way), emb_mid(oc, way), links.at_line(hop, 0), long=True))

    def emb_on(some, arrived):
        for (way, hop, oc), c in zip(some, arrived):
            c.wait_recv()
            emb_got[oc].send(emb_mid(oc, way), emb_far_slot(oc, way), links.at_line(hop, oc))

    def amid(crossing):
        stats_got.wait()
        means = row_stats[:, :pad, :]
        mean = jnp.sum(means, axis=0) / nx2
        gap = means - mean[None]
        square = jnp.sum(row_stats[:, pad:, :], axis=0) + jnp.sum(gap * gap, axis=0) * chunk
        scale = lax.rsqrt(square / (nx2 * chunk) + EPS)
        for b in range(blocks):
            n_buf[0, block_rows(b), 0:chunk] = (
                (hid_ref[block_rows(b), :].astype(f32) - to_col(mean[b:b + 1, :])) * to_col(scale[b:b + 1, :])
                * gains[0, 0:1, :]).astype(bf16)
        own = n_buf.at[0, :, 0:chunk]
        crossing.send(own, n_buf.at[1, :, 0:chunk], partner)

    front = norm_gather(links, own_input, gains, 0, xbuf, stat, n_buf, gather_base, (amid, forward_weights), skip=1)
    next(front)
    gain_got = rest(gains, NX)
    for dx in HOPS:
        gain_got.send(gains.at[0], gains.at[NX - dx], links.at_line(dx, 0))
    stats_got = rest(row_stats, nx2)
    for p in LINE:
        stats_got.send(row_stats.at[xid], row_stats.at[xid], links.at_line(*p))
    for way, hop, oc in ways:
        w_far.append(links.send(w_piece((wg_ref, wu_ref)[way], 2, oc), w_relay.at[way, oc], links.at_line(hop, 0),
                                long=True))

    got_wq.wait()
    eye_q = (lax.broadcasted_iota(jnp.int32, (qc, qc), 0) == lax.broadcasted_iota(jnp.int32, (qc, qc), 1))
    wq_t[...] = dot_t(eye_q.astype(bf16), wq_ref[...]).astype(bf16)
    wq_buf[0, 0:qs, 0:chunk] = wq_t[pl.ds(pl.multiple_of(xid * qs, qs), qs), :]

    def wq_rows(dx, oc):
        return wq_t.at[pl.ds(pl.multiple_of(line_id(dx, oc) * qs, qs), qs), :]

    def wq_slot(dx, oc):
        return wq_buf.at[oc, pl.ds(0, qs), pl.ds((NX - dx) % NX * chunk, chunk)]

    wq_got = Group(links, wq_t.at[0:qc - qs])
    for dx, oc in LINE:
        wq_got.send(wq_rows(dx, oc), wq_slot(dx, oc), links.at_line(dx, oc))
    for which, ref in enumerate((wg_ref, wu_ref)):
        for dx, oc in LINE[:1] + NEAR:
            w_got[oc].send(w_piece(ref, dx, oc), w_slot(which, dx, oc), links.at_line(dx, oc))

    phase("selections")
    r_id = lax.broadcasted_iota(jnp.int32, (nx2 * nyz * pad, 1), 0)
    r_j = r_id % pad
    r_src = jnp.where(r_j < own_rows, r_id // pad % nyz * rows + r_id // (pad * nyz) * own_rows + r_j, -1)
    s_id = lax.broadcasted_iota(jnp.int32, (1, total_rows), 1)
    sel[...] = jnp.where(r_src == s_id, 1.0, 0.0).astype(bf16)
    t_id = lax.broadcasted_iota(jnp.int32, (group, 1), 0)
    t_in = t_id % rows
    t_src = t_in // own_rows * (NY * pad) + t_id // rows * pad + t_in % own_rows
    u_id = lax.broadcasted_iota(jnp.int32, (1, nx2 * NY * pad), 1)
    sel_t[...] = jnp.where(t_src == u_id, 1.0, 0.0).astype(bf16)
    k_id = lax.broadcasted_iota(jnp.int32, (nx2 * pad, rows), 0)
    k_src = jnp.where(k_id % pad < own_rows, k_id // pad * own_rows + k_id % pad, -1)
    sel_kv = jnp.where(k_src == lax.broadcasted_iota(jnp.int32, (nx2 * pad, rows), 1), 1.0, 0.0).astype(bf16)

    phase.close()
    gain_got.wait()
    lane = lax.broadcasted_iota(jnp.int32, (1, head), 1)
    lengths = []
    for b in range(own_rows):
        index = (yid * nx2 + xid) * own_rows + b
        row = len_ref[pl.ds(index // head, 1), :].astype(f32)
        lengths.append(lane_sum(jnp.where(lane == index % head, row, 0.0)))
    lengths = jnp.concatenate(lengths + lengths[:pad - own_rows], axis=0)
    angles = lengths * freq_ref[...]
    cos_all = jnp.cos(angles)
    sin_all = jnp.sin(angles) * jnp.where(lane < head // 2, -1.0, 1.0)

    crossing = next(front)
    phase("ng_cross")
    crossing.wait()
    phase("kv_part")

    for c in got_wkv:
        c.wait()
    n_own = dot(sel_kv, n_buf[0, links.slot_rows(0, 0, rows), 0:chunk]).astype(bf16)
    kvp[:, :, :head] = dot(n_own, wk_ref[...]).reshape(nx2, pad, head)
    kvp[:, :, head:] = dot(n_own, wv_ref[...]).reshape(nx2, pad, head)
    kv_got = rest(kvr, nx2)
    for p in LINE:
        kv_got.send(kvp.at[line_id(*p)], kvr.at[xid], links.at_line(*p))
    kvr[xid] = kvp[xid]

    phase("wait_wq")
    wq_got.wait()
    phase("q_mm")
    q_all = jnp.concatenate([
        (dot_t(n_buf[0, i * group:(i + 1) * group, :], wq_buf[0])
         + dot_t(n_buf[1, i * group:(i + 1) * group, :], wq_buf[1])).astype(bf16) for i in range(NZ)], axis=0)
    span = nyz * pad
    for i in range(nx2):
        chosen = dot(sel[i * span:(i + 1) * span, :], q_all)
        quarter = span // per
        packed = chosen[:quarter, :]
        for g in range(1, per):
            packed = packed + pltpu.roll(chosen[g * quarter:(g + 1) * quarter, :], g * qs, 1)
        qx[i] = packed.astype(bf16)
    q_got = rest(qr, nx2)
    for p in LINE:
        q_got.send(qx.at[line_id(*p)], qr.at[xid], links.at_line(*p))
    qr[xid] = qx[xid]

    phase("wait_w")
    for c in own_w:
        c.wait()
    for c in w_got:
        c.wait()
    phase("gate_up")

    def act_at(k, dx):
        return act.at[(z + k) % NZ, :, pl.ds(pl.multiple_of(line_id(dx, 0) * ff, ff), ff)]

    def act_out(k, dx, to_dx):
        return links.send(act_at(k, dx), act_at(k, dx), links.at_line(to_dx, 0))

    def act_give(k, dx):
        cross[k].send(act_at(k, dx), act_at(k, dx), partner)

    turns = (2, 1, 3, 0)
    early, late = turns[:2], turns[2:]
    near_act, far_act = {}, {}
    cross = {k: Group(links, act.at[0, :, 0:NX * ff]) for k in turns}
    def group_rows(k):
        return pl.ds(pl.multiple_of((z + k) % NZ * group, group), group)

    far = slice(2 * chunk, (NX - 1) * chunk)

    def over(k, part_cols):
        return dot(n_buf[0, group_rows(k), part_cols], w_buf[0, part_cols, :]) + dot(
            n_buf[1, group_rows(k), part_cols], w_buf[1, part_cols, :])

    for k in turns:
        gu_acc[k] = over(k, slice(0, far.start)) + over(k, slice(far.stop, NX * chunk))
    phase("wait_w_far")
    w_last.wait()
    phase("gate_up_far")
    for k in turns:
        both = (gu_acc[k] + over(k, far)).astype(bf16).astype(f32)
        gate, up = both[:, :ff], both[:, ff:]
        act_at(k, 0)[...] = (gate * jax.nn.sigmoid(gate) * up).astype(bf16)
        near_act[k] = [(dx, act_out(k, 0, dx)) for dx in HOPS[:2]]
        act_give(k, 0)

    def act_pass(k):
        for dx, c in near_act[k]:
            c.wait_recv()
            if (k in early) == (dx == 1):
                far_act[k] = act_out(k, NX - dx, dx)
            act_give(k, NX - dx)

    low, high = pl.ds(0, half), pl.ds(half, half)
    first_a, first_b = Group(links, ra1), Group(links, rb1)

    def act_use(k):
        cross[k].wait()
        g = (z + k) % NZ
        part[g] = dot(act[g], wd_buf[...]).reshape(NY, rows, chunk)
        if k:
            first_b.send(part.at[g, :, :, high], rb1.at[k - 1], links.at_plane(k, 0))

    def along_y(k):
        g = (z + k) % NZ
        for d in early + late[:1]:
            first_a.send(part.at[g, (y + d) % NY, :, low], ra1.at[d - 1, g], links.at_plane(0, d))

    def act_far(ks):
        for k in ks:
            far_act[k].wait_recv()
            act_give(k, 2)

    phase("wait_q")
    q_got.wait()
    phase("q_sum")
    lane_group = lax.broadcasted_iota(jnp.int32, (1, head), 1) // qs
    for j in range(qc // head):
        came = [qr[j * per + i].astype(f32) for i in range(per)]
        for g in range(per):
            piece = jnp.zeros((span // per, head), f32)
            for i in range(per):
                piece = piece + jnp.where(lane_group == i, pltpu.roll(came[i], (i - g) % per * qs, 1), 0.0)
            qy[g * per:(g + 1) * per, :, j * head:(j + 1) * head] = piece.reshape(per, pad, head)

    def plane_id(dz, dy):
        return (z + dz) % NZ * NY + (y + dy) % NY

    y_got = rest(qf, nyz)
    for p in PLANE:
        y_got.send(qy.at[plane_id(*p)], qf.at[yid], links.at_plane(*p))
    qf[yid] = qy[yid]

    def wo_rows(dz):
        return wo_all.at[pl.ds(pl.multiple_of((z + dz) % NZ * qc, qc), qc), :]

    wo_got = Group(links, wo_all.at[0:(NZ - 1) * qc])
    for d in HOPS:
        wo_got.send(wo_ref, wo_rows(0), links.at_plane(d, 0))
    own_wo = fetch(wo_ref, wo_rows(0))

    phase("act_pass")
    for k in early:
        act_pass(k)
    phase("wait_kv")
    kv_got.wait()
    kv_sum = kvr[0]
    for i in range(1, nx2):
        kv_sum = kv_sum + kvr[i]
    kv_new = kv_sum.astype(bf16).astype(f32)

    def turn(v, b=None):
        cos, sin = (cos_all, sin_all) if b is None else (cos_all[b:b + 1, :], sin_all[b:b + 1, :])
        return (v * cos + pltpu.roll(v, head // 2, 1) * sin).astype(bf16)

    k_new = turn(kv_new[:, :head])
    knew_ref[...] = k_new
    vnew_ref[...] = kv_new[:, head:].astype(bf16)
    k_row, v_row = k_new.astype(f32), kv_new[:, head:]
    phase("act_pass2")
    for k in late:
        act_pass(k)
    emb_out(ways[:2])
    phase("wait_qy")
    for c in got_kv:
        c.wait()
    y_got.wait()
    phase("attention")
    seq = k_buf.shape[1]
    score_scale = head ** -0.5
    position = lax.broadcasted_iota(jnp.int32, (1, seq), 1).astype(f32)
    o_buf[...] = jnp.zeros(o_buf.shape, f32)
    for b in range(own_rows):
        q_b = jnp.concatenate([turn(qf[:, b, j * head:(j + 1) * head], b) for j in range(qc // head)], axis=0)
        scores = dot_t(q_b, k_buf[b]) * score_scale
        score_new = lane_sum(q_b.astype(f32) * k_row[b:b + 1, :]) * score_scale
        valid = position < lengths[b:b + 1, :]
        top = jnp.maximum(jnp.max(jnp.where(valid, scores, -jnp.inf), axis=-1, keepdims=True), score_new)
        weights = jnp.where(valid, jnp.exp(scores - top), 0.0)
        weight_new = jnp.exp(score_new - top)
        denom = lane_sum(weights) + weight_new
        o_b = dot((weights / denom).astype(bf16), v_buf[b])
        o_b = o_b + (weight_new / denom).astype(bf16).astype(f32) * v_row[b:b + 1, :]
        o_b = o_b.astype(bf16).astype(f32)
        for j in range(qc // head):
            o_buf[:, :, b, j * head:(j + 1) * head] = o_b[j * nyz:(j + 1) * nyz, :].reshape(NZ, NY, head)
    o_back = rest(o_got, NY)
    for d in HOPS:
        o_back.send(o_buf.at[:, (y + d) % NY], o_got.at[y], links.at_plane(0, d))
    phase("act_early")
    act_far(turns)
    got_wd.wait()
    for k in turns:
        act_use(k)
        along_y(k)
    o_got[y] = o_buf[:, y]

    phase("wait_oy")
    o_back.wait()
    for i in range(NZ):
        o_all[xid, :, i * qc:(i + 1) * qc] = o_got[:, i].reshape(NY * pad, qc).astype(bf16)
    o_here = o_all.at[xid]
    o_line = [links.send(o_here, o_here, links.at_line(dx, 0)) for dx in HOPS]
    o_cross = rest(o_all, NX + 1)
    o_cross.send(o_here, o_here, partner)
    emb_out(ways[2:])
    emb_got[1].send(emb_piece(0, 1), emb_slot(0, 1), partner)
    emb_on(ways[:2], emb_far[:2])
    phase("wait_o")
    for dx, c in zip(HOPS, o_line):
        c.wait_recv()
        came = o_all.at[line_id(NX - dx, 0)]
        o_cross.send(came, came, partner)
    wo_got.wait()
    own_wo.wait()
    o_cross.wait()
    phase("out_mm")
    o_nat = dot(sel_t[...], o_all[...].reshape(nx2 * NY * pad, NZ * qc)).astype(bf16)
    att[...] = dot(o_nat, wo_all[...]).reshape(NY, rows, chunk)
    att_got = Group(links, rc)
    for d in HOPS:
        att_got.send(att.at[(y + d) % NY], rc.at[d - 1], links.at_plane(0, d))

    phase("wait_rs1")
    first_b.wait()
    acc_b[...] = (part[z, :, :, half:] + rb1[0]) + (rb1[1] + rb1[2])
    second = [Group(links, rb2), Group(links, ra2)]
    for d in HOPS:
        second[0].send(acc_b.at[(y + d) % NY], rb2.at[d - 1], links.at_plane(0, d))
    phase("wait_rs1a")
    first_a.wait()
    acc_a[...] = (part[:, y, :, :half] + ra1[0]) + (ra1[1] + ra1[2])
    for d in HOPS:
        second[1].send(acc_a.at[(z + d) % NZ], ra2.at[d - 1], links.at_plane(d, 0))
    phase("wait_att")
    att_got.wait()
    phase("wait_rs2")

    def own_residual():
        res = hid_ref[here_rows, :].astype(f32) + ((att[y] + rc[0]) + (rc[1] + rc[2]))
        second[0].wait()
        xbuf2[0, :, half:] = res[:, half:] + ((acc_b[y] + rb2[0]) + (rb2[1] + rb2[2]))
        yield high
        second[1].wait()
        xbuf2[0, :, :half] = res[:, :half] + ((acc_a[z] + ra2[0]) + (ra2[1] + ra2[2]))
        yield low

    back = norm_gather(links, own_residual, gains, 1, xbuf2, stat2, f_buf, gather_base, (lambda crossing: None, lambda: None))
    next(back)
    emb_on(ways[2:], emb_far[2:])
    for dx, oc in NEAR:
        emb_got[oc].send(emb_piece(dx, oc), emb_slot(dx, oc), links.at_line(dx, oc))
    phase.close()
    crossing = next(back)
    phase("wait_emb")
    own_emb.wait()
    for c in emb_got:
        c.wait()

    phase("logits")
    wide_n = 256
    for h in range(CORES):
        if h:
            crossing.wait()
        for i in range(total_rows // wide_n):
            cols = slice(i * wide_n, (i + 1) * wide_n)
            term = dot_t(emb_buf[h], f_buf[h, cols, :])
            z_ref[:, cols] = z_ref[:, cols] + term if h else term

    z_out = fetch(z_ref, z_hbm)

    phase("lse_own")
    shift = vocab_own * xid - emb_start(xid)
    vid = lax.broadcasted_iota(jnp.int32, (take, 1), 0)
    own = (vid >= shift) & (vid < shift + vocab_own)
    for b in range(blocks):
        zb = jnp.where(own, z_ref[:, b * 128:(b + 1) * 128], -jnp.inf)
        top = jnp.max(zb, axis=0, keepdims=True)
        lse_x[xid, b:b + 1, :] = top
        lse_x[xid, 8 + b:9 + b, :] = jnp.sum(jnp.exp(zb - top), axis=0, keepdims=True)
    for b in range(blocks, 8):
        lse_x[xid, b:b + 1, :] = jnp.zeros((1, 128), f32)
        lse_x[xid, 8 + b:9 + b, :] = jnp.ones((1, 128), f32)

    def merge(ref):
        tops = ref[:, :8, :]
        top = jnp.max(tops, axis=0)
        return top, jnp.sum(ref[:, 8:, :] * jnp.exp(tops - top[None]), axis=0)

    phase("lse_line")
    got = rest(lse_x, nx2)
    for p in LINE:
        got.send(lse_x.at[xid], lse_x.at[xid], links.at_line(*p))
    got.wait()
    top, mass = merge(lse_x)
    lse_y[yid, :8, :] = top
    lse_y[yid, 8:, :] = mass
    phase("lse_plane")
    got = rest(lse_y, nyz)
    for p in PLANE:
        got.send(lse_y.at[yid], lse_y.at[yid], links.at_plane(*p))
    got.wait()
    top, mass = merge(lse_y)
    norm_ref[...] = top + jnp.log(mass)
    phase("finish")
    z_out.wait()
    links.finish()
    phase.close()


def whole_step(hidden, freq, lens, k_cache, v_cache, g_attn, w_query, w_key, w_value,
               w_gate, w_up, w_out, w_down, g_final, embedding):
    total_rows, chunk = hidden.shape
    own_rows, seq, head = k_cache.shape
    rows = total_rows // (NY * NZ)
    vocab_own = embedding.shape[0] // (2 * NX)
    take = (vocab_own + 6 + 15) // 16 * 16
    half = chunk // 2
    qc = w_query.shape[1]
    ff = w_gate.shape[1] // (2 * NX)
    f32, bf16 = jnp.float32, jnp.bfloat16
    nyz, nx2, pad = NY * NZ, 2 * NX, 8
    vmem = pl.BlockSpec(memory_space=pltpu.VMEM)
    hbm = pl.BlockSpec(memory_space=pl.ANY)
    V = pltpu.VMEM
    return pl.pallas_call(
        lambda *refs: step_kernel(vocab_own, own_rows, *refs),
        out_shape=(jax.ShapeDtypeStruct((pad, head), bf16), jax.ShapeDtypeStruct((pad, head), bf16),
                   jax.ShapeDtypeStruct((take, total_rows), f32), jax.ShapeDtypeStruct((pad, head), f32)),
        in_specs=[vmem] * 5 + [hbm] * 10,
        out_specs=(vmem, vmem, hbm, vmem),
        scratch_shapes=[
            V((take, total_rows), f32),
            V((chunk, qc), bf16), V((chunk, head), bf16), V((chunk, head), bf16),
            V((own_rows, seq, head), bf16), V((own_rows, seq, head), bf16),
            V((nx2 * ff, chunk), bf16), V((NZ * qc, chunk), bf16), V((NY, rows, chunk), f32), V((3, rows, chunk), f32),
            V((NZ, NY * rows, 2 * ff), f32), V((2, total_rows, NX * chunk), bf16), V((2, NX * chunk, 2 * ff), bf16),
            V((qc, chunk), bf16), V((2, head, NX * chunk), bf16),
            V((nx2 * nyz * pad, total_rows), bf16), V((NY * rows, nx2 * NY * pad), bf16),
            V((nx2, nyz * pad // 4, head), bf16), V((nx2, nyz * pad // 4, head), bf16),
            V((nyz, pad, qc), f32), V((nyz, pad, qc), f32),
            V((nx2, pad, 2 * head), f32), V((nx2, pad, 2 * head), f32),
            V((NZ, NY, pad, qc), f32), V((NY, NZ, pad, qc), f32), V((nx2, NY * pad, NZ * qc), bf16),
            V((NZ, NY * rows, nx2 * ff), bf16),
            V((NZ, NY, rows, chunk), f32),
            V((3, NZ, rows, half), f32), V((3, NY, rows, half), f32), V((3, rows, half), f32), V((3, rows, half), f32),
            V((NZ, rows, half), f32), V((NY, rows, half), f32),
            V((NX, rows, chunk), bf16), V((2, rows, 128), f32), V((NX, rows, chunk), f32), V((2, rows, 128), f32),
            V((NX, 8, chunk), f32),
            V((2, total_rows, NX * chunk), bf16), V((2, take, NX * chunk), bf16),
            V((2, 2, chunk, ff), bf16), V((2, 2, (take // 2 + 15) // 16 * 16, chunk), bf16),
            V((nx2, 16, 128), f32), V((nx2, 16, 128), f32), V((nyz, 16, 128), f32),
            pltpu.SemaphoreType.DMA((SENDS,)), pltpu.SemaphoreType.DMA((TAGS,)), pltpu.SemaphoreType.DMA((11,)),
        ],
        compiler_params=pltpu.CompilerParams(
            collective_id=1, has_side_effects=True, vmem_limit_bytes=60 << 20),
        name="decode_step",
    )(hidden, g_attn[None, :], g_final[None, :], freq, lens, k_cache, v_cache,
      w_query, w_key, w_value, w_out, w_gate, w_up, w_down, embedding)


def solution(mesh):
    row_spec = P(("dp", "yax", "xax"))

    def local_step(hidden, cache_len, k_cache, v_cache, g_attn, w_query, w_key, w_value,
                   w_gate, w_up, w_out, w_down, g_final, embedding):
        rows = hidden.shape[0]
        half_dim = k_cache.shape[2] // 2
        inv_freq = ROPE_BASE ** (-(np.arange(half_dim, dtype=np.float64) * 2.0) / (2 * half_dim))
        freq = np.concatenate([inv_freq, inv_freq])[None, :].astype(np.float32)
        key_own, value_own, logits_wide, norm_tile = whole_step(
            hidden, freq, cache_len.reshape(rows // 128, 128), k_cache, v_cache, g_attn, w_query, w_key, w_value,
            w_gate, w_up, w_out, w_down, g_final, embedding)
        own_rows = k_cache.shape[0]
        vocab_own = embedding.shape[0] // (CORES * NX)
        first = vocab_own * lax.axis_index("xax")
        logits = lax.dynamic_slice_in_dim(logits_wide, first - first // 8 * 8, vocab_own, axis=0)
        log_norm = norm_tile[:rows // 128].reshape(rows)
        return key_own[:own_rows], value_own[:own_rows], (logits - log_norm).T, log_norm

    in_specs = (P("dp", "xax"), P("dp"), row_spec, row_spec, P("xax"), P("xax", "yax"),
                P("xax"), P("xax"), P("xax", "yax"), P("xax", "yax"),
                P("yax", "xax"), P("yax", "xax"), P("xax"), P("yax", "xax"))
    out_specs = (row_spec, row_spec, P("dp", ("yax", "xax")), P("dp"))
    return jax.shard_map(local_step, mesh=mesh, in_specs=in_specs, out_specs=out_specs, check_vma=False)
```

```python
import contextlib
import itertools

import jax
import jax.numpy as jnp
import numpy as np
from jax import lax
from jax.experimental import pallas as pl
from jax.experimental.pallas import tpu as pltpu
from jax.sharding import PartitionSpec as P

EPS = 1e-6
ROPE_BASE = 10000.0
MESH_ID = pl.DeviceIdType.MESH
NY = NZ = NX = 4
CORES = 2
POOL, SENDS, TAGS = 24, 59, 89
HOPS = (1, 3, 2)
FAR_FIRST = (2, 1, 3)
LINE = [(0, 1), (1, 0), (3, 0), (1, 1), (3, 1), (2, 0), (2, 1)]
NEAR = LINE[1:5]
NT = (((1,), (1,)), ((), ()))
PLANE = sorted([(dz, dy) for dz in range(NZ) for dy in range(NY) if dz or dy],
               key=lambda p: sum(abs(d - 2) for d in p))
FAR_LINE = LINE[::-1]


class Group:
    def __init__(self, links, whole):
        self.links, self.whole = links, whole
        self.tag, self.sem = next(links.tags), next(links.slow)
        links.groups.append(self)

    def send(self, src, dst, where):
        pltpu.make_async_remote_copy(
            src_ref=src, dst_ref=dst, send_sem=self.links.send_sem.at[self.sem],
            recv_sem=self.links.recv_sem.at[self.tag], device_id=where, device_id_type=MESH_ID).start()

    def wait(self):
        pltpu.make_async_copy(self.whole, self.whole, self.links.recv_sem.at[self.tag]).wait()

    def wait_sent(self):
        pltpu.make_async_copy(self.whole, self.whole, self.links.send_sem.at[self.sem]).wait()


class Phases:
    def __init__(self):
        self.stack = contextlib.ExitStack()

    def __call__(self, name):
        self.close()
        self.stack.enter_context(jax.named_scope(name))

    def close(self):
        self.stack.close()


class Links:
    def __init__(self, send_sem, recv_sem):
        self.send_sem, self.recv_sem = send_sem, recv_sem
        self.tags, self.slow, self.fast = itertools.count(), itertools.count(POOL), []
        self.pending, self.groups = [], []
        self.y_idx = lax.axis_index("yax")
        self.x_idx = lax.axis_index("xax")
        self.z, self.y = self.y_idx // NY, self.y_idx % NY
        self.chip, self.core = self.x_idx // CORES, self.x_idx % CORES

    def at_plane(self, dz, dy):
        return {"yax": (self.z + dz) % NZ * NY + (self.y + dy) % NY, "xax": self.x_idx}

    def slot_rows(self, dz, dy, rows):
        slot = (self.z + dz) % NZ * NY + (self.y + dy) % NY
        return pl.ds(pl.multiple_of(slot * rows, rows), rows)

    def line_id(self, dx, oc):
        core = 1 - self.core if oc else self.core
        return (self.chip + dx) % NX * CORES + core

    def at_line(self, dx, oc):
        return {"yax": self.y_idx, "xax": self.line_id(dx, oc)}

    def send(self, src, dst, where, tag=None, long=False):
        tag = next(self.tags) if tag is None else tag
        if long:
            sem = next(self.slow)
        else:
            sem = len(self.fast) % POOL
            if len(self.fast) >= POOL:
                self.fast[-POOL].wait_send()
        copy = pltpu.make_async_remote_copy(
            src_ref=src, dst_ref=dst, send_sem=self.send_sem.at[sem], recv_sem=self.recv_sem.at[tag],
            device_id=where, device_id_type=MESH_ID)
        copy.start()
        (self.pending if long else self.fast).append(copy)
        return copy

    def finish(self):
        for copy in self.pending + self.fast[-POOL:]:
            copy.wait_send()
        for group in self.groups:
            group.wait_sent()

    def barrier(self):
        barrier = pltpu.get_barrier_semaphore()
        peers = [self.at_line(*p) for p in LINE] + [self.at_plane(*p) for p in PLANE]
        for peer in peers:
            pl.semaphore_signal(barrier, inc=1, device_id=peer, device_id_type=MESH_ID)
        pl.semaphore_wait(barrier, len(peers))


def lane_sum(v):
    return jnp.sum(v, axis=-1, keepdims=True)


def plane_gather(links, buf, tags, hooks, crossing, start):
    cols = buf.shape[-1]
    rows = buf.shape[1] // (NY * NZ)
    span = (cols - start) // 2
    partner = links.at_line(0, 1)

    class Part:
        def __init__(self, index):
            self.index, self.lo, self.got = index, start + index * span, {}

        def order(self, du, dv):
            return (du, dv) if self.index else (dv, du)

        def block(self, at, half=0, piece=None):
            width = span if piece is None else span // 2
            lo = self.lo if not piece else self.lo + width
            return buf.at[half, links.slot_rows(*self.order(*at), rows), pl.ds(lo, width)]

        def push(self, name, at, to, piece=None):
            ref = self.block(at, piece=piece)
            self.got[name] = links.send(ref, ref, links.at_plane(*self.order(*to)), next(tags))

        def spread(self, k, at):
            self.push(("v+", k), at, (0, 1))
            self.push(("v-", k), at, (0, -1))

        def give(self, at):
            crossing.send(self.block(at), self.block(at, half=1), partner)

        def wait(self, name):
            self.got[name].wait_recv()

    parts = [Part(index) for index in range(2)]
    offset = (0, -1, 1, 2)
    for p in parts:
        p.push("u+", (0, 0), (1, 0))
        p.push("u-", (0, 0), (-1, 0))
        p.spread(0, (0, 0))
    for p in parts:
        p.give((0, 0))
    hooks[0](crossing)
    for k, name in enumerate(("u+", "u-"), 1):
        for p in parts:
            p.wait(name)
            at = (offset[k], 0)
            p.push(("far", k), at, (-offset[k], 0), piece=k - 1)
            p.spread(k, at)
            p.give(at)
    hooks[1]()

    def arrive(p, k):
        for name, step in (("v+", -1), ("v-", 1)):
            p.wait((name, k))
            at = (offset[k], step)
            if (name == "v+") == (k in (0, 3)):
                p.push(("relay", k), at, (0, -step))
            p.give(at)

    for p in parts:
        arrive(p, 0)
    for p in parts:
        p.wait(("far", 1))
        p.wait(("far", 2))
        p.spread(3, (2, 0))
        p.give((2, 0))
    for k in range(1, len(offset)):
        for p in parts:
            arrive(p, k)
    for k in range(len(offset)):
        for p in parts:
            p.wait(("relay", k))
            p.give((offset[k], 2))


def norm_gather(links, own_slot, gain_buf, which, xbuf, stat, out, base, hooks, skip=0):
    rows, chunk = xbuf.shape[1:]
    tags = itertools.count(base)
    line = []
    for cols in own_slot():
        line += [links.send(xbuf.at[0, :, cols], xbuf.at[NX - dx, :, cols], links.at_line(dx, 0), next(tags))
                 for dx in FAR_FIRST]
    yield
    phase = Phases()
    for n, c in enumerate(line):
        phase(f"ng_line{which}_{n}")
        c.wait_recv()
    phase("ng_stats")
    held = xbuf[...].astype(jnp.float32)
    count = NX * chunk
    mean = lane_sum(jnp.sum(held, axis=0)) / count
    dev = held - mean[None]
    square = lane_sum(jnp.sum(dev * dev, axis=0))
    lane = lax.broadcasted_iota(jnp.int32, (rows, 128), 1)
    stat[0] = jnp.where(lane == 0, mean, square)
    links.send(stat.at[0], stat.at[1], links.at_line(0, 1), next(tags)).wait_recv()
    other_mean, other_square = stat[1, :, 0:1], stat[1, :, 1:2]
    both = (mean + other_mean) * 0.5
    gap = mean - other_mean
    var = (square + other_square + gap * gap * (count * 0.5)) / (2 * count)
    scale = lax.rsqrt(var + EPS)
    for e in range(skip, NX):
        out[0, links.slot_rows(0, 0, rows), e * chunk:(e + 1) * chunk] = (
            (xbuf[e].astype(jnp.float32) - both) * scale * gain_buf[e, which:which + 1, :]).astype(jnp.bfloat16)
    phase("ng_plane")
    crossing = Group(links, out.at[1])
    plane_gather(links, out, tags, hooks, crossing, skip * chunk)
    phase.close()
    yield crossing


def step_kernel(vocab_own, own_rows, hid_ref, gain_a, gain_f, freq_ref, len_ref, k_hbm, v_hbm,
                wq_hbm, wk_hbm, wv_hbm, wo_ref, wg_ref, wu_ref, wd_hbm, emb_ref,
                knew_ref, vnew_ref, z_hbm, norm_ref,
                z_ref, wq_ref, wk_ref, wv_ref, k_buf, v_buf, wd_buf, wo_all, att, rc, gu_acc, n_buf, w_buf, wq_t, wq_buf, sel, sel_t, qx, qr, qy, qf,
                kvp, kvr, o_buf, o_got, o_all, act,
                part, ra1, rb1, ra2, rb2, acc_a, acc_b, xbuf, stat, xbuf2, stat2, gains, f_buf, emb_buf,
                w_relay, emb_relay, row_stats, lse_x, lse_y, send_sem, recv_sem, local_sem):
    links = Links(send_sem, recv_sem)
    phase = Phases()
    f32, bf16 = jnp.float32, jnp.bfloat16
    z, y, xid, yid = links.z, links.y, links.x_idx, links.y_idx
    total_rows, chunk = hid_ref.shape
    rows = total_rows // (NY * NZ)
    here_rows = links.slot_rows(0, 0, rows)
    half = chunk // 2
    nx2, nyz = 2 * NX, NY * NZ
    group = NY * rows
    head = 128
    pad = 8
    partner = links.at_line(0, 1)
    line_id = links.line_id
    gather_tags = 2 * len(HOPS) + 1 + len(PLANE) * CORES + CORES
    gather_base = [next(links.tags) for _ in range(gather_tags)][0]

    def dot(a, b):
        return jnp.dot(a, b, preferred_element_type=f32)

    def dot_t(a, b):
        return lax.dot_general(a, b, NT, preferred_element_type=f32)

    def rest(ref, n):
        return Group(links, ref.at[0:n - 1])

    local = []

    def fetch(src, dst):
        copy = pltpu.make_async_copy(src, dst, local_sem.at[len(local)])
        copy.start()
        local.append(copy)
        return copy

    ff = wg_ref.shape[1] // nx2

    def w_piece(ref, dx, oc):
        return ref.at[:, pl.ds(pl.multiple_of(line_id(dx, oc) * ff, ff), ff)]

    def w_slot(which, dx, oc):
        back = (NX - dx) % NX
        return w_buf.at[int(oc), pl.ds(back * chunk, chunk), pl.ds(which * ff, ff)]

    take = emb_buf.shape[1]

    def emb_start(xi):
        return pl.multiple_of(vocab_own * xi // pad * pad, pad)

    def emb_piece(dx, oc):
        return emb_ref.at[pl.ds(emb_start(line_id(dx, oc)), take), :]

    def emb_slot(dx, oc):
        return emb_buf.at[int(oc), :, pl.ds((NX - dx) % NX * chunk, chunk)]

    near_part = (take // 2 + 15) // 16 * 16
    far_parts = ((0, near_part), (near_part, take - near_part))

    def emb_half(oc, way):
        first, size = far_parts[way]
        return emb_ref.at[pl.ds(pl.multiple_of(emb_start(line_id(2, oc)) + first, pad), size), :]

    def emb_mid(oc, way):
        return emb_relay.at[way, oc, pl.ds(0, far_parts[way][1])]

    def emb_far_slot(oc, way):
        return emb_buf.at[int(oc), pl.ds(*far_parts[way]), pl.ds(2 * chunk, chunk)]

    got_wq = fetch(wq_hbm, wq_ref)
    own_w = [fetch(w_piece(wg_ref, 0, 0), w_slot(0, 0, 0)), fetch(w_piece(wu_ref, 0, 0), w_slot(1, 0, 0))]
    got_kv = [fetch(k_hbm, k_buf), fetch(v_hbm, v_buf)]
    got_wkv = [fetch(wk_hbm, wk_ref), fetch(wv_hbm, wv_ref)]
    got_wd = fetch(wd_hbm, wd_buf)
    own_emb = fetch(emb_piece(0, 0), emb_slot(0, 0))

    qc = wq_ref.shape[1]
    qs = qc // nx2
    per = head // qs
    wq_buf[...] = jnp.zeros(wq_buf.shape, bf16)

    phase("row_stats")
    eye = lax.broadcasted_iota(jnp.int32, (head, head), 0) == lax.broadcasted_iota(jnp.int32, (head, head), 1)
    blocks = total_rows // head

    def block_rows(b):
        return slice(b * head, (b + 1) * head)

    def to_row(v):
        return jnp.sum(jnp.where(eye, v, 0.0), axis=0, keepdims=True)

    def to_col(v):
        return lane_sum(jnp.where(eye, v, 0.0))

    row_stats[xid] = jnp.zeros((2 * pad, head), f32)
    for b in range(blocks):
        held = hid_ref[block_rows(b), :].astype(f32)
        mean = lane_sum(held) / chunk
        dev = held - mean
        row_stats[xid, b:b + 1, :] = to_row(mean)
        row_stats[xid, pad + b:pad + b + 1, :] = to_row(lane_sum(dev * dev))

    phase("barrier")
    links.barrier()

    phase("front_send")
    gains[0, 0:1, :] = gain_a[...]
    gains[0, 1:2, :] = gain_f[...]
    gains[0, 2:, :] = jnp.zeros((6, chunk), f32)

    def own_input():
        xbuf[0] = hid_ref[here_rows, :]
        yield pl.ds(0, chunk)

    w_far, emb_far = [], []
    w_got = [Group(links, w_buf.at[0, 0:2 * chunk]), Group(links, w_buf.at[1, 0:(NX - 1) * chunk])]
    w_last = Group(links, w_buf.at[0, 0:2 * chunk])
    emb_got = [Group(links, emb_buf.at[0, :, 0:(NX - 1) * chunk]), Group(links, emb_buf.at[1])]
    ways = [(way, hop, oc) for oc in (0, 1) for way, hop in enumerate(HOPS[:2])]

    def forward_weights():
        for (way, hop, oc), c in zip(ways, w_far):
            c.wait_recv()
            w_last.send(w_relay.at[way, oc], w_buf.at[oc, pl.ds(2 * chunk, chunk), pl.ds(way * ff, ff)],
                        links.at_line(hop, oc))

    def emb_out(some):
        for way, hop, oc in some:
            emb_far.append(links.send(emb_half(oc, way), emb_mid(oc, way), links.at_line(hop, 0), long=True))

    def emb_on(some, arrived):
        for (way, hop, oc), c in zip(some, arrived):
            c.wait_recv()
            emb_got[oc].send(emb_mid(oc, way), emb_far_slot(oc, way), links.at_line(hop, oc))

    def amid(crossing):
        stats_got.wait()
        means = row_stats[:, :pad, :]
        mean = jnp.sum(means, axis=0) / nx2
        gap = means - mean[None]
        square = jnp.sum(row_stats[:, pad:, :], axis=0) + jnp.sum(gap * gap, axis=0) * chunk
        scale = lax.rsqrt(square / (nx2 * chunk) + EPS)
        for b in range(blocks):
            n_buf[0, block_rows(b), 0:chunk] = (
                (hid_ref[block_rows(b), :].astype(f32) - to_col(mean[b:b + 1, :])) * to_col(scale[b:b + 1, :])
                * gains[0, 0:1, :]).astype(bf16)
        own = n_buf.at[0, :, 0:chunk]
        crossing.send(own, n_buf.at[1, :, 0:chunk], partner)

    front = norm_gather(links, own_input, gains, 0, xbuf, stat, n_buf, gather_base, (amid, forward_weights), skip=1)
    next(front)
    gain_got = rest(gains, NX)
    for dx in HOPS:
        gain_got.send(gains.at[0], gains.at[NX - dx], links.at_line(dx, 0))
    stats_got = rest(row_stats, nx2)
    for p in FAR_LINE:
        stats_got.send(row_stats.at[xid], row_stats.at[xid], links.at_line(*p))
    for way, hop, oc in ways:
        w_far.append(links.send(w_piece((wg_ref, wu_ref)[way], 2, oc), w_relay.at[way, oc], links.at_line(hop, 0),
                                long=True))

    got_wq.wait()
    eye_q = (lax.broadcasted_iota(jnp.int32, (qc, qc), 0) == lax.broadcasted_iota(jnp.int32, (qc, qc), 1))
    wq_t[...] = dot_t(eye_q.astype(bf16), wq_ref[...]).astype(bf16)
    wq_buf[0, 0:qs, 0:chunk] = wq_t[pl.ds(pl.multiple_of(xid * qs, qs), qs), :]

    def wq_rows(dx, oc):
        return wq_t.at[pl.ds(pl.multiple_of(line_id(dx, oc) * qs, qs), qs), :]

    def wq_slot(dx, oc):
        return wq_buf.at[oc, pl.ds(0, qs), pl.ds((NX - dx) % NX * chunk, chunk)]

    wq_got = Group(links, wq_t.at[0:qc - qs])
    for dx, oc in LINE:
        wq_got.send(wq_rows(dx, oc), wq_slot(dx, oc), links.at_line(dx, oc))
    for which, ref in enumerate((wg_ref, wu_ref)):
        for dx, oc in LINE[:1] + NEAR:
            w_got[oc].send(w_piece(ref, dx, oc), w_slot(which, dx, oc), links.at_line(dx, oc))

    phase("selections")
    r_id = lax.broadcasted_iota(jnp.int32, (nx2 * nyz * pad, 1), 0)
    r_j = r_id % pad
    r_src = jnp.where(r_j < own_rows, r_id // pad % nyz * rows + r_id // (pad * nyz) * own_rows + r_j, -1)
    s_id = lax.broadcasted_iota(jnp.int32, (1, total_rows), 1)
    sel[...] = jnp.where(r_src == s_id, 1.0, 0.0).astype(bf16)
    t_id = lax.broadcasted_iota(jnp.int32, (group, 1), 0)
    t_in = t_id % rows
    t_src = t_in // own_rows * (NY * pad) + t_id // rows * pad + t_in % own_rows
    u_id = lax.broadcasted_iota(jnp.int32, (1, nx2 * NY * pad), 1)
    sel_t[...] = jnp.where(t_src == u_id, 1.0, 0.0).astype(bf16)
    k_id = lax.broadcasted_iota(jnp.int32, (nx2 * pad, rows), 0)
    k_src = jnp.where(k_id % pad < own_rows, k_id // pad * own_rows + k_id % pad, -1)
    sel_kv = jnp.where(k_src == lax.broadcasted_iota(jnp.int32, (nx2 * pad, rows), 1), 1.0, 0.0).astype(bf16)

    phase.close()
    gain_got.wait()
    lane = lax.broadcasted_iota(jnp.int32, (1, head), 1)
    lengths = []
    for b in range(own_rows):
        index = (yid * nx2 + xid) * own_rows + b
        row = len_ref[pl.ds(index // head, 1), :].astype(f32)
        lengths.append(lane_sum(jnp.where(lane == index % head, row, 0.0)))
    lengths = jnp.concatenate(lengths + lengths[:pad - own_rows], axis=0)
    angles = lengths * freq_ref[...]
    cos_all = jnp.cos(angles)
    sin_all = jnp.sin(angles) * jnp.where(lane < head // 2, -1.0, 1.0)

    crossing = next(front)
    phase("ng_cross")
    crossing.wait()
    phase("kv_part")

    for c in got_wkv:
        c.wait()
    n_own = dot(sel_kv, n_buf[0, links.slot_rows(0, 0, rows), 0:chunk]).astype(bf16)
    kvp[:, :, :head] = dot(n_own, wk_ref[...]).reshape(nx2, pad, head)
    kvp[:, :, head:] = dot(n_own, wv_ref[...]).reshape(nx2, pad, head)
    kv_got = rest(kvr, nx2)
    for p in FAR_LINE:
        kv_got.send(kvp.at[line_id(*p)], kvr.at[xid], links.at_line(*p))
    kvr[xid] = kvp[xid]

    phase("wait_wq")
    wq_got.wait()
    phase("q_mm")
    q_all = jnp.concatenate([
        (dot_t(n_buf[0, i * group:(i + 1) * group, :], wq_buf[0])
         + dot_t(n_buf[1, i * group:(i + 1) * group, :], wq_buf[1])).astype(bf16) for i in range(NZ)], axis=0)
    span = nyz * pad
    for i in range(nx2):
        chosen = dot(sel[i * span:(i + 1) * span, :], q_all)
        quarter = span // per
        packed = chosen[:quarter, :]
        for g in range(1, per):
            packed = packed + pltpu.roll(chosen[g * quarter:(g + 1) * quarter, :], g * qs, 1)
        qx[i] = packed.astype(bf16)
    q_got = rest(qr, nx2)
    for p in FAR_LINE:
        q_got.send(qx.at[line_id(*p)], qr.at[xid], links.at_line(*p))
    qr[xid] = qx[xid]

    phase("wait_w")
    for c in own_w:
        c.wait()
    for c in w_got:
        c.wait()
    phase("gate_up")

    def act_at(k, dx):
        return act.at[(z + k) % NZ, :, pl.ds(pl.multiple_of(line_id(dx, 0) * ff, ff), ff)]

    def act_out(k, dx, to_dx):
        return links.send(act_at(k, dx), act_at(k, dx), links.at_line(to_dx, 0))

    def act_give(k, dx):
        cross[k].send(act_at(k, dx), act_at(k, dx), partner)

    turns = (2, 1, 3, 0)
    early, late = turns[:2], turns[2:]
    near_act, far_act = {}, {}
    cross = {k: Group(links, act.at[0, :, 0:NX * ff]) for k in turns}
    def group_rows(k):
        return pl.ds(pl.multiple_of((z + k) % NZ * group, group), group)

    far = slice(2 * chunk, (NX - 1) * chunk)

    def over(k, part_cols):
        return dot(n_buf[0, group_rows(k), part_cols], w_buf[0, part_cols, :]) + dot(
            n_buf[1, group_rows(k), part_cols], w_buf[1, part_cols, :])

    for k in turns:
        gu_acc[k] = over(k, slice(0, far.start)) + over(k, slice(far.stop, NX * chunk))
    phase("wait_w_far")
    w_last.wait()
    phase("gate_up_far")
    for k in turns:
        both = (gu_acc[k] + over(k, far)).astype(bf16).astype(f32)
        gate, up = both[:, :ff], both[:, ff:]
        act_at(k, 0)[...] = (gate * jax.nn.sigmoid(gate) * up).astype(bf16)
        near_act[k] = [(dx, act_out(k, 0, dx)) for dx in HOPS[:2]]
        act_give(k, 0)

    def act_pass(k):
        for dx, c in near_act[k]:
            c.wait_recv()
            if (k in early) == (dx == 1):
                far_act[k] = act_out(k, NX - dx, dx)
            act_give(k, NX - dx)

    low, high = pl.ds(0, half), pl.ds(half, half)
    first_a, first_b = Group(links, ra1), Group(links, rb1)

    def act_use(k):
        cross[k].wait()
        g = (z + k) % NZ
        part[g] = dot(act[g], wd_buf[...]).reshape(NY, rows, chunk)
        if k:
            first_b.send(part.at[g, :, :, high], rb1.at[k - 1], links.at_plane(k, 0))

    def along_y(k):
        g = (z + k) % NZ
        for d in early + late[:1]:
            first_a.send(part.at[g, (y + d) % NY, :, low], ra1.at[d - 1, g], links.at_plane(0, d))

    def act_far(ks):
        for k in ks:
            far_act[k].wait_recv()
            act_give(k, 2)

    phase("wait_q")
    q_got.wait()
    phase("q_sum")
    lane_group = lax.broadcasted_iota(jnp.int32, (1, head), 1) // qs
    for j in range(qc // head):
        came = [qr[j * per + i].astype(f32) for i in range(per)]
        for g in range(per):
            piece = jnp.zeros((span // per, head), f32)
            for i in range(per):
                piece = piece + jnp.where(lane_group == i, pltpu.roll(came[i], (i - g) % per * qs, 1), 0.0)
            qy[g * per:(g + 1) * per, :, j * head:(j + 1) * head] = piece.reshape(per, pad, head)

    def plane_id(dz, dy):
        return (z + dz) % NZ * NY + (y + dy) % NY

    y_got = rest(qf, nyz)
    for p in PLANE:
        y_got.send(qy.at[plane_id(*p)], qf.at[yid], links.at_plane(*p))
    qf[yid] = qy[yid]

    def wo_rows(dz):
        return wo_all.at[pl.ds(pl.multiple_of((z + dz) % NZ * qc, qc), qc), :]

    wo_got = Group(links, wo_all.at[0:(NZ - 1) * qc])
    for d in HOPS:
        wo_got.send(wo_ref, wo_rows(0), links.at_plane(d, 0))
    own_wo = fetch(wo_ref, wo_rows(0))

    phase("act_pass")
    for k in early:
        act_pass(k)
    phase("wait_kv")
    kv_got.wait()
    kv_sum = kvr[0]
    for i in range(1, nx2):
        kv_sum = kv_sum + kvr[i]
    kv_new = kv_sum.astype(bf16).astype(f32)

    def turn(v, b=None):
        cos, sin = (cos_all, sin_all) if b is None else (cos_all[b:b + 1, :], sin_all[b:b + 1, :])
        return (v * cos + pltpu.roll(v, head // 2, 1) * sin).astype(bf16)

    k_new = turn(kv_new[:, :head])
    knew_ref[...] = k_new
    vnew_ref[...] = kv_new[:, head:].astype(bf16)
    k_row, v_row = k_new.astype(f32), kv_new[:, head:]
    phase("act_pass2")
    for k in late:
        act_pass(k)
    emb_out(ways[:2])
    phase("wait_qy")
    for c in got_kv:
        c.wait()
    y_got.wait()
    phase("attention")
    seq = k_buf.shape[1]
    score_scale = head ** -0.5
    position = lax.broadcasted_iota(jnp.int32, (1, seq), 1).astype(f32)
    o_buf[...] = jnp.zeros(o_buf.shape, f32)
    for b in range(own_rows):
        q_b = jnp.concatenate([turn(qf[:, b, j * head:(j + 1) * head], b) for j in range(qc // head)], axis=0)
        scores = dot_t(q_b, k_buf[b]) * score_scale
        score_new = lane_sum(q_b.astype(f32) * k_row[b:b + 1, :]) * score_scale
        valid = position < lengths[b:b + 1, :]
        top = jnp.maximum(jnp.max(jnp.where(valid, scores, -jnp.inf), axis=-1, keepdims=True), score_new)
        weights = jnp.where(valid, jnp.exp(scores - top), 0.0)
        weight_new = jnp.exp(score_new - top)
        denom = lane_sum(weights) + weight_new
        o_b = dot((weights / denom).astype(bf16), v_buf[b])
        o_b = o_b + (weight_new / denom).astype(bf16).astype(f32) * v_row[b:b + 1, :]
        o_b = o_b.astype(bf16).astype(f32)
        for j in range(qc // head):
            o_buf[:, :, b, j * head:(j + 1) * head] = o_b[j * nyz:(j + 1) * nyz, :].reshape(NZ, NY, head)
    o_back = rest(o_got, NY)
    for d in HOPS:
        o_back.send(o_buf.at[:, (y + d) % NY], o_got.at[y], links.at_plane(0, d))
    phase("act_early")
    act_far(turns)
    got_wd.wait()
    for k in turns:
        act_use(k)
        along_y(k)
    o_got[y] = o_buf[:, y]

    phase("wait_oy")
    o_back.wait()
    for i in range(NZ):
        o_all[xid, :, i * qc:(i + 1) * qc] = o_got[:, i].reshape(NY * pad, qc).astype(bf16)
    o_here = o_all.at[xid]
    o_line = [links.send(o_here, o_here, links.at_line(dx, 0)) for dx in HOPS]
    o_cross = rest(o_all, NX + 1)
    o_cross.send(o_here, o_here, partner)
    emb_out(ways[2:])
    emb_got[1].send(emb_piece(0, 1), emb_slot(0, 1), partner)
    emb_on(ways[:2], emb_far[:2])
    phase("wait_o")
    for dx, c in zip(HOPS, o_line):
        c.wait_recv()
        came = o_all.at[line_id(NX - dx, 0)]
        o_cross.send(came, came, partner)
    wo_got.wait()
    own_wo.wait()
    o_cross.wait()
    phase("out_mm")
    o_nat = dot(sel_t[...], o_all[...].reshape(nx2 * NY * pad, NZ * qc)).astype(bf16)
    att[...] = dot(o_nat, wo_all[...]).reshape(NY, rows, chunk)
    att_got = Group(links, rc)
    for d in HOPS:
        att_got.send(att.at[(y + d) % NY], rc.at[d - 1], links.at_plane(0, d))

    phase("wait_rs1")
    first_b.wait()
    acc_b[...] = (part[z, :, :, half:] + rb1[0]) + (rb1[1] + rb1[2])
    second = [Group(links, rb2), Group(links, ra2)]
    for d in HOPS:
        second[0].send(acc_b.at[(y + d) % NY], rb2.at[d - 1], links.at_plane(0, d))
    phase("wait_rs1a")
    first_a.wait()
    acc_a[...] = (part[:, y, :, :half] + ra1[0]) + (ra1[1] + ra1[2])
    for d in HOPS:
        second[1].send(acc_a.at[(z + d) % NZ], ra2.at[d - 1], links.at_plane(d, 0))
    phase("wait_att")
    att_got.wait()
    phase("wait_rs2")

    def own_residual():
        res = hid_ref[here_rows, :].astype(f32) + ((att[y] + rc[0]) + (rc[1] + rc[2]))
        second[0].wait()
        xbuf2[0, :, half:] = res[:, half:] + ((acc_b[y] + rb2[0]) + (rb2[1] + rb2[2]))
        yield high
        second[1].wait()
        xbuf2[0, :, :half] = res[:, :half] + ((acc_a[z] + ra2[0]) + (ra2[1] + ra2[2]))
        yield low

    back = norm_gather(links, own_residual, gains, 1, xbuf2, stat2, f_buf, gather_base, (lambda crossing: None, lambda: None))
    next(back)
    emb_on(ways[2:], emb_far[2:])
    for dx, oc in NEAR:
        emb_got[oc].send(emb_piece(dx, oc), emb_slot(dx, oc), links.at_line(dx, oc))
    phase.close()
    crossing = next(back)
    phase("wait_emb")
    own_emb.wait()
    for c in emb_got:
        c.wait()

    phase("logits")
    wide_n = 256
    for h in range(CORES):
        if h:
            crossing.wait()
        for i in range(total_rows // wide_n):
            cols = slice(i * wide_n, (i + 1) * wide_n)
            term = dot_t(emb_buf[h], f_buf[h, cols, :])
            z_ref[:, cols] = z_ref[:, cols] + term if h else term

    z_out = fetch(z_ref, z_hbm)

    phase("lse_own")
    shift = vocab_own * xid - emb_start(xid)
    vid = lax.broadcasted_iota(jnp.int32, (take, 1), 0)
    own = (vid >= shift) & (vid < shift + vocab_own)
    for b in range(blocks):
        zb = jnp.where(own, z_ref[:, b * 128:(b + 1) * 128], -jnp.inf)
        top = jnp.max(zb, axis=0, keepdims=True)
        lse_x[xid, b:b + 1, :] = top
        lse_x[xid, 8 + b:9 + b, :] = jnp.sum(jnp.exp(zb - top), axis=0, keepdims=True)
    for b in range(blocks, 8):
        lse_x[xid, b:b + 1, :] = jnp.zeros((1, 128), f32)
        lse_x[xid, 8 + b:9 + b, :] = jnp.ones((1, 128), f32)

    def merge(ref):
        tops = ref[:, :8, :]
        top = jnp.max(tops, axis=0)
        return top, jnp.sum(ref[:, 8:, :] * jnp.exp(tops - top[None]), axis=0)

    phase("lse_line")
    got = rest(lse_x, nx2)
    for p in FAR_LINE:
        got.send(lse_x.at[xid], lse_x.at[xid], links.at_line(*p))
    got.wait()
    top, mass = merge(lse_x)
    lse_y[yid, :8, :] = top
    lse_y[yid, 8:, :] = mass
    phase("lse_plane")
    got = rest(lse_y, nyz)
    for p in PLANE:
        got.send(lse_y.at[yid], lse_y.at[yid], links.at_plane(*p))
    got.wait()
    top, mass = merge(lse_y)
    norm_ref[...] = top + jnp.log(mass)
    phase("finish")
    z_out.wait()
    links.finish()
    phase.close()


def whole_step(hidden, freq, lens, k_cache, v_cache, g_attn, w_query, w_key, w_value,
               w_gate, w_up, w_out, w_down, g_final, embedding):
    total_rows, chunk = hidden.shape
    own_rows, seq, head = k_cache.shape
    rows = total_rows // (NY * NZ)
    vocab_own = embedding.shape[0] // (2 * NX)
    take = (vocab_own + 6 + 15) // 16 * 16
    half = chunk // 2
    qc = w_query.shape[1]
    ff = w_gate.shape[1] // (2 * NX)
    f32, bf16 = jnp.float32, jnp.bfloat16
    nyz, nx2, pad = NY * NZ, 2 * NX, 8
    vmem = pl.BlockSpec(memory_space=pltpu.VMEM)
    hbm = pl.BlockSpec(memory_space=pl.ANY)
    V = pltpu.VMEM
    return pl.pallas_call(
        lambda *refs: step_kernel(vocab_own, own_rows, *refs),
        out_shape=(jax.ShapeDtypeStruct((pad, head), bf16), jax.ShapeDtypeStruct((pad, head), bf16),
                   jax.ShapeDtypeStruct((take, total_rows), f32), jax.ShapeDtypeStruct((pad, head), f32)),
        in_specs=[vmem] * 5 + [hbm] * 10,
        out_specs=(vmem, vmem, hbm, vmem),
        scratch_shapes=[
            V((take, total_rows), f32),
            V((chunk, qc), bf16), V((chunk, head), bf16), V((chunk, head), bf16),
            V((own_rows, seq, head), bf16), V((own_rows, seq, head), bf16),
            V((nx2 * ff, chunk), bf16), V((NZ * qc, chunk), bf16), V((NY, rows, chunk), f32), V((3, rows, chunk), f32),
            V((NZ, NY * rows, 2 * ff), f32), V((2, total_rows, NX * chunk), bf16), V((2, NX * chunk, 2 * ff), bf16),
            V((qc, chunk), bf16), V((2, head, NX * chunk), bf16),
            V((nx2 * nyz * pad, total_rows), bf16), V((NY * rows, nx2 * NY * pad), bf16),
            V((nx2, nyz * pad // 4, head), bf16), V((nx2, nyz * pad // 4, head), bf16),
            V((nyz, pad, qc), f32), V((nyz, pad, qc), f32),
            V((nx2, pad, 2 * head), f32), V((nx2, pad, 2 * head), f32),
            V((NZ, NY, pad, qc), f32), V((NY, NZ, pad, qc), f32), V((nx2, NY * pad, NZ * qc), bf16),
            V((NZ, NY * rows, nx2 * ff), bf16),
            V((NZ, NY, rows, chunk), f32),
            V((3, NZ, rows, half), f32), V((3, NY, rows, half), f32), V((3, rows, half), f32), V((3, rows, half), f32),
            V((NZ, rows, half), f32), V((NY, rows, half), f32),
            V((NX, rows, chunk), bf16), V((2, rows, 128), f32), V((NX, rows, chunk), f32), V((2, rows, 128), f32),
            V((NX, 8, chunk), f32),
            V((2, total_rows, NX * chunk), bf16), V((2, take, NX * chunk), bf16),
            V((2, 2, chunk, ff), bf16), V((2, 2, (take // 2 + 15) // 16 * 16, chunk), bf16),
            V((nx2, 16, 128), f32), V((nx2, 16, 128), f32), V((nyz, 16, 128), f32),
            pltpu.SemaphoreType.DMA((SENDS,)), pltpu.SemaphoreType.DMA((TAGS,)), pltpu.SemaphoreType.DMA((11,)),
        ],
        compiler_params=pltpu.CompilerParams(
            collective_id=1, has_side_effects=True, vmem_limit_bytes=60 << 20),
        name="decode_step",
    )(hidden, g_attn[None, :], g_final[None, :], freq, lens, k_cache, v_cache,
      w_query, w_key, w_value, w_out, w_gate, w_up, w_down, embedding)


def solution(mesh):
    row_spec = P(("dp", "yax", "xax"))

    def local_step(hidden, cache_len, k_cache, v_cache, g_attn, w_query, w_key, w_value,
                   w_gate, w_up, w_out, w_down, g_final, embedding):
        rows = hidden.shape[0]
        half_dim = k_cache.shape[2] // 2
        inv_freq = ROPE_BASE ** (-(np.arange(half_dim, dtype=np.float64) * 2.0) / (2 * half_dim))
        freq = np.concatenate([inv_freq, inv_freq])[None, :].astype(np.float32)
        key_own, value_own, logits_wide, norm_tile = whole_step(
            hidden, freq, cache_len.reshape(rows // 128, 128), k_cache, v_cache, g_attn, w_query, w_key, w_value,
            w_gate, w_up, w_out, w_down, g_final, embedding)
        own_rows = k_cache.shape[0]
        vocab_own = embedding.shape[0] // (CORES * NX)
        first = vocab_own * lax.axis_index("xax")
        logits = lax.dynamic_slice_in_dim(logits_wide, first - first // 8 * 8, vocab_own, axis=0)
        log_norm = norm_tile[:rows // 128].reshape(rows)
        return key_own[:own_rows], value_own[:own_rows], (logits - log_norm).T, log_norm

    in_specs = (P("dp", "xax"), P("dp"), row_spec, row_spec, P("xax"), P("xax", "yax"),
                P("xax"), P("xax"), P("xax", "yax"), P("xax", "yax"),
                P("yax", "xax"), P("yax", "xax"), P("xax"), P("yax", "xax"))
    out_specs = (row_spec, row_spec, P("dp", ("yax", "xax")), P("dp"))
    return jax.shard_map(local_step, mesh=mesh, in_specs=in_specs, out_specs=out_specs, check_vma=False)
```

```python
import contextlib
import itertools

import jax
import jax.numpy as jnp
import numpy as np
from jax import lax
from jax.experimental import pallas as pl
from jax.experimental.pallas import tpu as pltpu
from jax.sharding import PartitionSpec as P

EPS = 1e-6
ROPE_BASE = 10000.0
MESH_ID = pl.DeviceIdType.MESH
NY = NZ = NX = 4
CORES = 2
POOL, SENDS, TAGS = 24, 59, 89
HOPS = (1, 3, 2)
FAR_FIRST = (2, 1, 3)
LINE = [(0, 1), (1, 0), (3, 0), (1, 1), (3, 1), (2, 0), (2, 1)]
NEAR = LINE[1:5]
NT = (((1,), (1,)), ((), ()))
PLANE = sorted([(dz, dy) for dz in range(NZ) for dy in range(NY) if dz or dy],
               key=lambda p: sum(abs(d - 2) for d in p))
FAR_LINE = LINE[::-1]


class Group:
    def __init__(self, links, whole):
        self.links, self.whole = links, whole
        self.tag, self.sem = next(links.tags), next(links.slow)
        links.groups.append(self)

    def send(self, src, dst, where):
        pltpu.make_async_remote_copy(
            src_ref=src, dst_ref=dst, send_sem=self.links.send_sem.at[self.sem],
            recv_sem=self.links.recv_sem.at[self.tag], device_id=where, device_id_type=MESH_ID).start()

    def wait(self):
        pltpu.make_async_copy(self.whole, self.whole, self.links.recv_sem.at[self.tag]).wait()

    def wait_sent(self):
        pltpu.make_async_copy(self.whole, self.whole, self.links.send_sem.at[self.sem]).wait()


class Phases:
    def __init__(self):
        self.stack = contextlib.ExitStack()

    def __call__(self, name):
        self.close()
        self.stack.enter_context(jax.named_scope(name))

    def close(self):
        self.stack.close()


class Links:
    def __init__(self, send_sem, recv_sem):
        self.send_sem, self.recv_sem = send_sem, recv_sem
        self.tags, self.slow, self.fast = itertools.count(), itertools.count(POOL), []
        self.pending, self.groups = [], []
        self.y_idx = lax.axis_index("yax")
        self.x_idx = lax.axis_index("xax")
        self.z, self.y = self.y_idx // NY, self.y_idx % NY
        self.chip, self.core = self.x_idx // CORES, self.x_idx % CORES

    def at_plane(self, dz, dy):
        return {"yax": (self.z + dz) % NZ * NY + (self.y + dy) % NY, "xax": self.x_idx}

    def slot_rows(self, dz, dy, rows):
        slot = (self.z + dz) % NZ * NY + (self.y + dy) % NY
        return pl.ds(pl.multiple_of(slot * rows, rows), rows)

    def line_id(self, dx, oc):
        core = 1 - self.core if oc else self.core
        return (self.chip + dx) % NX * CORES + core

    def at_line(self, dx, oc):
        return {"yax": self.y_idx, "xax": self.line_id(dx, oc)}

    def send(self, src, dst, where, tag=None, long=False):
        tag = next(self.tags) if tag is None else tag
        if long:
            sem = next(self.slow)
        else:
            sem = len(self.fast) % POOL
            if len(self.fast) >= POOL:
                self.fast[-POOL].wait_send()
        copy = pltpu.make_async_remote_copy(
            src_ref=src, dst_ref=dst, send_sem=self.send_sem.at[sem], recv_sem=self.recv_sem.at[tag],
            device_id=where, device_id_type=MESH_ID)
        copy.start()
        (self.pending if long else self.fast).append(copy)
        return copy

    def finish(self):
        for copy in self.pending + self.fast[-POOL:]:
            copy.wait_send()
        for group in self.groups:
            group.wait_sent()

    def barrier(self):
        barrier = pltpu.get_barrier_semaphore()
        peers = [self.at_line(*p) for p in LINE] + [self.at_plane(*p) for p in PLANE]
        for peer in peers:
            pl.semaphore_signal(barrier, inc=1, device_id=peer, device_id_type=MESH_ID)
        pl.semaphore_wait(barrier, len(peers))


def lane_sum(v):
    return jnp.sum(v, axis=-1, keepdims=True)


def plane_gather(links, buf, tags, hooks, crossing, start):
    cols = buf.shape[-1]
    rows = buf.shape[1] // (NY * NZ)
    span = (cols - start) // 2
    partner = links.at_line(0, 1)

    class Part:
        def __init__(self, index):
            self.index, self.lo, self.got = index, start + index * span, {}

        def order(self, du, dv):
            return (du, dv) if self.index else (dv, du)

        def block(self, at, half=0, piece=None):
            width = span if piece is None else span // 2
            lo = self.lo if not piece else self.lo + width
            return buf.at[half, links.slot_rows(*self.order(*at), rows), pl.ds(lo, width)]

        def push(self, name, at, to, piece=None):
            ref = self.block(at, piece=piece)
            self.got[name] = links.send(ref, ref, links.at_plane(*self.order(*to)), next(tags))

        def spread(self, k, at):
            self.push(("v+", k), at, (0, 1))
            self.push(("v-", k), at, (0, -1))

        def give(self, at):
            crossing.send(self.block(at), self.block(at, half=1), partner)

        def wait(self, name):
            self.got[name].wait_recv()

    parts = [Part(index) for index in range(2)]
    offset = (0, -1, 1, 2)
    for p in parts:
        p.push("u+", (0, 0), (1, 0))
        p.push("u-", (0, 0), (-1, 0))
        p.spread(0, (0, 0))
    for p in parts:
        p.give((0, 0))
    hooks[0](crossing)
    for k, name in enumerate(("u+", "u-"), 1):
        for p in parts:
            p.wait(name)
            at = (offset[k], 0)
            p.push(("far", k), at, (-offset[k], 0), piece=k - 1)
            p.spread(k, at)
            p.give(at)
    hooks[1]()

    def arrive(p, k):
        for name, step in (("v+", -1), ("v-", 1)):
            p.wait((name, k))
            at = (offset[k], step)
            if (name == "v+") == (k in (0, 3)):
                p.push(("relay", k), at, (0, -step))
            p.give(at)

    for p in parts:
        arrive(p, 0)
    for p in parts:
        p.wait(("far", 1))
        p.wait(("far", 2))
        p.spread(3, (2, 0))
        p.give((2, 0))
    for k in range(1, len(offset)):
        for p in parts:
            arrive(p, k)
    for k in range(len(offset)):
        for p in parts:
            p.wait(("relay", k))
            p.give((offset[k], 2))


def norm_gather(links, own_slot, gain_buf, which, xbuf, stat, out, base, hooks, skip=0):
    rows, chunk = xbuf.shape[1:]
    tags = itertools.count(base)
    line = []
    for cols in own_slot():
        line += [links.send(xbuf.at[0, :, cols], xbuf.at[NX - dx, :, cols], links.at_line(dx, 0), next(tags))
                 for dx in FAR_FIRST]
    yield
    phase = Phases()
    for n, c in enumerate(line):
        phase(f"ng_line{which}_{n}")
        c.wait_recv()
    phase("ng_stats")
    held = xbuf[...].astype(jnp.float32)
    count = NX * chunk
    mean = lane_sum(jnp.sum(held, axis=0)) / count
    dev = held - mean[None]
    square = lane_sum(jnp.sum(dev * dev, axis=0))
    lane = lax.broadcasted_iota(jnp.int32, (rows, 128), 1)
    stat[0] = jnp.where(lane == 0, mean, square)
    links.send(stat.at[0], stat.at[1], links.at_line(0, 1), next(tags)).wait_recv()
    other_mean, other_square = stat[1, :, 0:1], stat[1, :, 1:2]
    both = (mean + other_mean) * 0.5
    gap = mean - other_mean
    var = (square + other_square + gap * gap * (count * 0.5)) / (2 * count)
    scale = lax.rsqrt(var + EPS)
    for e in range(skip, NX):
        out[0, links.slot_rows(0, 0, rows), e * chunk:(e + 1) * chunk] = (
            (xbuf[e].astype(jnp.float32) - both) * scale * gain_buf[e, which:which + 1, :]).astype(jnp.bfloat16)
    phase("ng_plane")
    crossing = Group(links, out.at[1])
    plane_gather(links, out, tags, hooks, crossing, skip * chunk)
    phase.close()
    yield crossing


def step_kernel(vocab_own, own_rows, hid_ref, gain_a, gain_f, freq_ref, len_ref, k_hbm, v_hbm,
                wq_hbm, wk_hbm, wv_hbm, wo_ref, wg_ref, wu_ref, wd_hbm, emb_ref,
                knew_ref, vnew_ref, z_hbm, norm_ref,
                z_ref, wq_ref, wk_ref, wv_ref, k_buf, v_buf, wd_buf, wo_all, att, rc, gu_acc, n_buf, w_buf, wq_t, wq_buf, sel, sel_t, qx, qr, qy, qf,
                kvp, kvr, o_buf, o_got, o_all, act,
                part, ra1, rb1, ra2, rb2, acc_a, acc_b, xbuf, stat, xbuf2, stat2, gains, f_buf, emb_buf,
                w_relay, emb_relay, row_stats, lse_x, lse_y, send_sem, recv_sem, local_sem):
    links = Links(send_sem, recv_sem)
    phase = Phases()
    f32, bf16 = jnp.float32, jnp.bfloat16
    z, y, xid, yid = links.z, links.y, links.x_idx, links.y_idx
    total_rows, chunk = hid_ref.shape
    rows = total_rows // (NY * NZ)
    here_rows = links.slot_rows(0, 0, rows)
    half = chunk // 2
    nx2, nyz = 2 * NX, NY * NZ
    group = NY * rows
    head = 128
    pad = 8
    partner = links.at_line(0, 1)
    line_id = links.line_id
    gather_tags = 2 * len(HOPS) + 1 + len(PLANE) * CORES + CORES
    gather_base = [next(links.tags) for _ in range(gather_tags)][0]

    def dot(a, b):
        return jnp.dot(a, b, preferred_element_type=f32)

    def dot_t(a, b):
        return lax.dot_general(a, b, NT, preferred_element_type=f32)

    def rest(ref, n):
        return Group(links, ref.at[0:n - 1])

    local = []

    def fetch(src, dst):
        copy = pltpu.make_async_copy(src, dst, local_sem.at[len(local)])
        copy.start()
        local.append(copy)
        return copy

    ff = wg_ref.shape[1] // nx2

    def w_piece(ref, dx, oc):
        return ref.at[:, pl.ds(pl.multiple_of(line_id(dx, oc) * ff, ff), ff)]

    def w_slot(which, dx, oc):
        back = (NX - dx) % NX
        return w_buf.at[int(oc), pl.ds(back * chunk, chunk), pl.ds(which * ff, ff)]

    take = emb_buf.shape[1]

    def emb_start(xi):
        return pl.multiple_of(vocab_own * xi // pad * pad, pad)

    def emb_piece(dx, oc):
        return emb_ref.at[pl.ds(emb_start(line_id(dx, oc)), take), :]

    def emb_slot(dx, oc):
        return emb_buf.at[int(oc), :, pl.ds((NX - dx) % NX * chunk, chunk)]

    near_part = (take // 2 + 15) // 16 * 16
    far_parts = ((0, near_part), (near_part, take - near_part))

    def emb_half(oc, way):
        first, size = far_parts[way]
        return emb_ref.at[pl.ds(pl.multiple_of(emb_start(line_id(2, oc)) + first, pad), size), :]

    def emb_mid(oc, way):
        return emb_relay.at[way, oc, pl.ds(0, far_parts[way][1])]

    def emb_far_slot(oc, way):
        return emb_buf.at[int(oc), pl.ds(*far_parts[way]), pl.ds(2 * chunk, chunk)]

    got_wq = fetch(wq_hbm, wq_ref)
    own_w = [fetch(w_piece(wg_ref, 0, 0), w_slot(0, 0, 0)), fetch(w_piece(wu_ref, 0, 0), w_slot(1, 0, 0))]
    got_kv = [fetch(k_hbm, k_buf), fetch(v_hbm, v_buf)]
    got_wkv = [fetch(wk_hbm, wk_ref), fetch(wv_hbm, wv_ref)]
    got_wd = fetch(wd_hbm, wd_buf)
    own_emb = fetch(emb_piece(0, 0), emb_slot(0, 0))

    qc = wq_ref.shape[1]
    qs = qc // nx2
    per = head // qs
    wq_buf[...] = jnp.zeros(wq_buf.shape, bf16)

    phase("row_stats")
    eye = lax.broadcasted_iota(jnp.int32, (head, head), 0) == lax.broadcasted_iota(jnp.int32, (head, head), 1)
    blocks = total_rows // head

    def block_rows(b):
        return slice(b * head, (b + 1) * head)

    def to_row(v):
        return jnp.sum(jnp.where(eye, v, 0.0), axis=0, keepdims=True)

    def to_col(v):
        return lane_sum(jnp.where(eye, v, 0.0))

    row_stats[xid] = jnp.zeros((2 * pad, head), f32)
    for b in range(blocks):
        held = hid_ref[block_rows(b), :].astype(f32)
        mean = lane_sum(held) / chunk
        dev = held - mean
        row_stats[xid, b:b + 1, :] = to_row(mean)
        row_stats[xid, pad + b:pad + b + 1, :] = to_row(lane_sum(dev * dev))

    phase("barrier")
    links.barrier()

    def wo_rows(dz):
        return wo_all.at[pl.ds(pl.multiple_of((z + dz) % NZ * qc, qc), qc), :]

    wo_got = Group(links, wo_all.at[0:(NZ - 1) * qc])
    for d in HOPS[:2]:
        wo_got.send(wo_ref, wo_rows(0), links.at_plane(d, 0))

    phase("front_send")
    gains[0, 0:1, :] = gain_a[...]
    gains[0, 1:2, :] = gain_f[...]
    gains[0, 2:, :] = jnp.zeros((6, chunk), f32)

    def own_input():
        xbuf[0] = hid_ref[here_rows, :]
        yield pl.ds(0, chunk)

    w_far, emb_far = [], []
    w_got = [Group(links, w_buf.at[0, 0:2 * chunk]), Group(links, w_buf.at[1, 0:(NX - 1) * chunk])]
    w_last = Group(links, w_buf.at[0, 0:2 * chunk])
    emb_got = [Group(links, emb_buf.at[0, :, 0:(NX - 1) * chunk]), Group(links, emb_buf.at[1])]
    ways = [(way, hop, oc) for oc in (0, 1) for way, hop in enumerate(HOPS[:2])]

    def forward_weights():
        for (way, hop, oc), c in zip(ways, w_far):
            c.wait_recv()
            w_last.send(w_relay.at[way, oc], w_buf.at[oc, pl.ds(2 * chunk, chunk), pl.ds(way * ff, ff)],
                        links.at_line(hop, oc))

    def emb_out(some):
        for way, hop, oc in some:
            emb_far.append(links.send(emb_half(oc, way), emb_mid(oc, way), links.at_line(hop, 0), long=True))

    def emb_on(some, arrived):
        for (way, hop, oc), c in zip(some, arrived):
            c.wait_recv()
            emb_got[oc].send(emb_mid(oc, way), emb_far_slot(oc, way), links.at_line(hop, oc))

    def amid(crossing):
        stats_got.wait()
        means = row_stats[:, :pad, :]
        mean = jnp.sum(means, axis=0) / nx2
        gap = means - mean[None]
        square = jnp.sum(row_stats[:, pad:, :], axis=0) + jnp.sum(gap * gap, axis=0) * chunk
        scale = lax.rsqrt(square / (nx2 * chunk) + EPS)
        for b in range(blocks):
            n_buf[0, block_rows(b), 0:chunk] = (
                (hid_ref[block_rows(b), :].astype(f32) - to_col(mean[b:b + 1, :])) * to_col(scale[b:b + 1, :])
                * gains[0, 0:1, :]).astype(bf16)
        own = n_buf.at[0, :, 0:chunk]
        crossing.send(own, n_buf.at[1, :, 0:chunk], partner)

    front = norm_gather(links, own_input, gains, 0, xbuf, stat, n_buf, gather_base, (amid, forward_weights), skip=1)
    next(front)
    gain_got = rest(gains, NX)
    for dx in HOPS:
        gain_got.send(gains.at[0], gains.at[NX - dx], links.at_line(dx, 0))
    stats_got = rest(row_stats, nx2)
    for p in FAR_LINE:
        stats_got.send(row_stats.at[xid], row_stats.at[xid], links.at_line(*p))
    for way, hop, oc in ways:
        w_far.append(links.send(w_piece((wg_ref, wu_ref)[way], 2, oc), w_relay.at[way, oc], links.at_line(hop, 0),
                                long=True))

    got_wq.wait()
    eye_q = (lax.broadcasted_iota(jnp.int32, (qc, qc), 0) == lax.broadcasted_iota(jnp.int32, (qc, qc), 1))
    wq_t[...] = dot_t(eye_q.astype(bf16), wq_ref[...]).astype(bf16)
    wq_buf[0, 0:qs, 0:chunk] = wq_t[pl.ds(pl.multiple_of(xid * qs, qs), qs), :]

    def wq_rows(dx, oc):
        return wq_t.at[pl.ds(pl.multiple_of(line_id(dx, oc) * qs, qs), qs), :]

    def wq_slot(dx, oc):
        return wq_buf.at[oc, pl.ds(0, qs), pl.ds((NX - dx) % NX * chunk, chunk)]

    wq_got = Group(links, wq_t.at[0:qc - qs])
    for dx, oc in LINE:
        wq_got.send(wq_rows(dx, oc), wq_slot(dx, oc), links.at_line(dx, oc))
    for which, ref in enumerate((wg_ref, wu_ref)):
        for dx, oc in LINE[:1] + NEAR:
            w_got[oc].send(w_piece(ref, dx, oc), w_slot(which, dx, oc), links.at_line(dx, oc))

    phase("selections")
    r_id = lax.broadcasted_iota(jnp.int32, (nx2 * nyz * pad, 1), 0)
    r_j = r_id % pad
    r_src = jnp.where(r_j < own_rows, r_id // pad % nyz * rows + r_id // (pad * nyz) * own_rows + r_j, -1)
    s_id = lax.broadcasted_iota(jnp.int32, (1, total_rows), 1)
    sel[...] = jnp.where(r_src == s_id, 1.0, 0.0).astype(bf16)
    t_id = lax.broadcasted_iota(jnp.int32, (group, 1), 0)
    t_in = t_id % rows
    t_src = t_in // own_rows * (NY * pad) + t_id // rows * pad + t_in % own_rows
    u_id = lax.broadcasted_iota(jnp.int32, (1, nx2 * NY * pad), 1)
    sel_t[...] = jnp.where(t_src == u_id, 1.0, 0.0).astype(bf16)
    k_id = lax.broadcasted_iota(jnp.int32, (nx2 * pad, rows), 0)
    k_src = jnp.where(k_id % pad < own_rows, k_id // pad * own_rows + k_id % pad, -1)
    sel_kv = jnp.where(k_src == lax.broadcasted_iota(jnp.int32, (nx2 * pad, rows), 1), 1.0, 0.0).astype(bf16)

    phase.close()
    gain_got.wait()
    lane = lax.broadcasted_iota(jnp.int32, (1, head), 1)
    lengths = []
    for b in range(own_rows):
        index = (yid * nx2 + xid) * own_rows + b
        row = len_ref[pl.ds(index // head, 1), :].astype(f32)
        lengths.append(lane_sum(jnp.where(lane == index % head, row, 0.0)))
    lengths = jnp.concatenate(lengths + lengths[:pad - own_rows], axis=0)
    angles = lengths * freq_ref[...]
    cos_all = jnp.cos(angles)
    sin_all = jnp.sin(angles) * jnp.where(lane < head // 2, -1.0, 1.0)

    crossing = next(front)
    phase("ng_cross")
    crossing.wait()
    phase("kv_part")

    for c in got_wkv:
        c.wait()
    n_own = dot(sel_kv, n_buf[0, links.slot_rows(0, 0, rows), 0:chunk]).astype(bf16)
    kvp[:, :, :head] = dot(n_own, wk_ref[...]).reshape(nx2, pad, head)
    kvp[:, :, head:] = dot(n_own, wv_ref[...]).reshape(nx2, pad, head)
    kv_got = rest(kvr, nx2)
    for p in FAR_LINE:
        kv_got.send(kvp.at[line_id(*p)], kvr.at[xid], links.at_line(*p))
    kvr[xid] = kvp[xid]

    phase("wait_wq")
    wq_got.wait()
    phase("q_mm")
    q_all = jnp.concatenate([
        (dot_t(n_buf[0, i * group:(i + 1) * group, :], wq_buf[0])
         + dot_t(n_buf[1, i * group:(i + 1) * group, :], wq_buf[1])).astype(bf16) for i in range(NZ)], axis=0)
    span = nyz * pad
    for i in range(nx2):
        chosen = dot(sel[i * span:(i + 1) * span, :], q_all)
        quarter = span // per
        packed = chosen[:quarter, :]
        for g in range(1, per):
            packed = packed + pltpu.roll(chosen[g * quarter:(g + 1) * quarter, :], g * qs, 1)
        qx[i] = packed.astype(bf16)
    q_got = rest(qr, nx2)
    for p in FAR_LINE:
        q_got.send(qx.at[line_id(*p)], qr.at[xid], links.at_line(*p))
    qr[xid] = qx[xid]

    phase("wait_w")
    for c in own_w:
        c.wait()
    for c in w_got:
        c.wait()
    phase("gate_up")

    def act_at(k, dx):
        return act.at[(z + k) % NZ, :, pl.ds(pl.multiple_of(line_id(dx, 0) * ff, ff), ff)]

    def act_out(k, dx, to_dx):
        return links.send(act_at(k, dx), act_at(k, dx), links.at_line(to_dx, 0))

    def act_give(k, dx):
        cross[k].send(act_at(k, dx), act_at(k, dx), partner)

    turns = (2, 1, 3, 0)
    early, late = turns[:2], turns[2:]
    near_act, far_act = {}, {}
    cross = {k: Group(links, act.at[0, :, 0:NX * ff]) for k in turns}
    def group_rows(k):
        return pl.ds(pl.multiple_of((z + k) % NZ * group, group), group)

    far = slice(2 * chunk, (NX - 1) * chunk)

    def over(k, part_cols):
        return dot(n_buf[0, group_rows(k), part_cols], w_buf[0, part_cols, :]) + dot(
            n_buf[1, group_rows(k), part_cols], w_buf[1, part_cols, :])

    for k in turns:
        gu_acc[k] = over(k, slice(0, far.start)) + over(k, slice(far.stop, NX * chunk))
    phase("wait_w_far")
    w_last.wait()
    phase("gate_up_far")
    for k in turns:
        both = (gu_acc[k] + over(k, far)).astype(bf16).astype(f32)
        gate, up = both[:, :ff], both[:, ff:]
        act_at(k, 0)[...] = (gate * jax.nn.sigmoid(gate) * up).astype(bf16)
        near_act[k] = [(dx, act_out(k, 0, dx)) for dx in HOPS[:2]]
        act_give(k, 0)

    def act_pass(k):
        for dx, c in near_act[k]:
            c.wait_recv()
            if (k in early) == (dx == 1):
                far_act[k] = act_out(k, NX - dx, dx)
            act_give(k, NX - dx)

    low, high = pl.ds(0, half), pl.ds(half, half)
    first_a, first_b = Group(links, ra1), Group(links, rb1)

    def act_use(k):
        cross[k].wait()
        g = (z + k) % NZ
        part[g] = dot(act[g], wd_buf[...]).reshape(NY, rows, chunk)
        if k:
            first_b.send(part.at[g, :, :, high], rb1.at[k - 1], links.at_plane(k, 0))

    def along_y(k):
        g = (z + k) % NZ
        for d in early + late[:1]:
            first_a.send(part.at[g, (y + d) % NY, :, low], ra1.at[d - 1, g], links.at_plane(0, d))

    def act_far(ks):
        for k in ks:
            far_act[k].wait_recv()
            act_give(k, 2)

    phase("wait_q")
    q_got.wait()
    phase("q_sum")
    lane_group = lax.broadcasted_iota(jnp.int32, (1, head), 1) // qs
    for j in range(qc // head):
        came = [qr[j * per + i].astype(f32) for i in range(per)]
        for g in range(per):
            piece = jnp.zeros((span // per, head), f32)
            for i in range(per):
                piece = piece + jnp.where(lane_group == i, pltpu.roll(came[i], (i - g) % per * qs, 1), 0.0)
            qy[g * per:(g + 1) * per, :, j * head:(j + 1) * head] = piece.reshape(per, pad, head)

    def plane_id(dz, dy):
        return (z + dz) % NZ * NY + (y + dy) % NY

    y_got = rest(qf, nyz)
    for p in PLANE:
        y_got.send(qy.at[plane_id(*p)], qf.at[yid], links.at_plane(*p))
    qf[yid] = qy[yid]

    wo_got.send(wo_ref, wo_rows(0), links.at_plane(FAR_FIRST[0], 0))
    own_wo = fetch(wo_ref, wo_rows(0))

    phase("act_pass")
    for k in early:
        act_pass(k)
    phase("wait_kv")
    kv_got.wait()
    kv_sum = kvr[0]
    for i in range(1, nx2):
        kv_sum = kv_sum + kvr[i]
    kv_new = kv_sum.astype(bf16).astype(f32)

    def turn(v, b=None):
        cos, sin = (cos_all, sin_all) if b is None else (cos_all[b:b + 1, :], sin_all[b:b + 1, :])
        return (v * cos + pltpu.roll(v, head // 2, 1) * sin).astype(bf16)

    k_new = turn(kv_new[:, :head])
    knew_ref[...] = k_new
    vnew_ref[...] = kv_new[:, head:].astype(bf16)
    k_row, v_row = k_new.astype(f32), kv_new[:, head:]
    phase("act_pass2")
    for k in late:
        act_pass(k)
    emb_out(ways[:2])
    phase("wait_qy")
    for c in got_kv:
        c.wait()
    y_got.wait()
    phase("attention")
    seq = k_buf.shape[1]
    score_scale = head ** -0.5
    position = lax.broadcasted_iota(jnp.int32, (1, seq), 1).astype(f32)
    o_buf[...] = jnp.zeros(o_buf.shape, f32)
    for b in range(own_rows):
        q_b = jnp.concatenate([turn(qf[:, b, j * head:(j + 1) * head], b) for j in range(qc // head)], axis=0)
        scores = dot_t(q_b, k_buf[b]) * score_scale
        score_new = lane_sum(q_b.astype(f32) * k_row[b:b + 1, :]) * score_scale
        valid = position < lengths[b:b + 1, :]
        top = jnp.maximum(jnp.max(jnp.where(valid, scores, -jnp.inf), axis=-1, keepdims=True), score_new)
        weights = jnp.where(valid, jnp.exp(scores - top), 0.0)
        weight_new = jnp.exp(score_new - top)
        denom = lane_sum(weights) + weight_new
        o_b = dot((weights / denom).astype(bf16), v_buf[b])
        o_b = o_b + (weight_new / denom).astype(bf16).astype(f32) * v_row[b:b + 1, :]
        o_b = o_b.astype(bf16).astype(f32)
        for j in range(qc // head):
            o_buf[:, :, b, j * head:(j + 1) * head] = o_b[j * nyz:(j + 1) * nyz, :].reshape(NZ, NY, head)
    o_back = rest(o_got, NY)
    for d in HOPS:
        o_back.send(o_buf.at[:, (y + d) % NY], o_got.at[y], links.at_plane(0, d))
    phase("act_early")
    act_far(turns)
    got_wd.wait()
    for k in turns:
        act_use(k)
        along_y(k)
    o_got[y] = o_buf[:, y]

    phase("wait_oy")
    o_back.wait()
    for i in range(NZ):
        o_all[xid, :, i * qc:(i + 1) * qc] = o_got[:, i].reshape(NY * pad, qc).astype(bf16)
    o_here = o_all.at[xid]
    o_line = [links.send(o_here, o_here, links.at_line(dx, 0)) for dx in HOPS]
    o_cross = rest(o_all, NX + 1)
    o_cross.send(o_here, o_here, partner)
    emb_out(ways[2:])
    emb_got[1].send(emb_piece(0, 1), emb_slot(0, 1), partner)
    emb_on(ways[:2], emb_far[:2])
    phase("wait_o")
    for dx, c in zip(HOPS, o_line):
        c.wait_recv()
        came = o_all.at[line_id(NX - dx, 0)]
        o_cross.send(came, came, partner)
    wo_got.wait()
    own_wo.wait()
    o_cross.wait()
    phase("out_mm")
    o_nat = dot(sel_t[...], o_all[...].reshape(nx2 * NY * pad, NZ * qc)).astype(bf16)
    att[...] = dot(o_nat, wo_all[...]).reshape(NY, rows, chunk)
    att_got = Group(links, rc)
    for d in HOPS:
        att_got.send(att.at[(y + d) % NY], rc.at[d - 1], links.at_plane(0, d))

    phase("wait_rs1")
    first_b.wait()
    acc_b[...] = (part[z, :, :, half:] + rb1[0]) + (rb1[1] + rb1[2])
    second = [Group(links, rb2), Group(links, ra2)]
    for d in HOPS:
        second[0].send(acc_b.at[(y + d) % NY], rb2.at[d - 1], links.at_plane(0, d))
    phase("wait_rs1a")
    first_a.wait()
    acc_a[...] = (part[:, y, :, :half] + ra1[0]) + (ra1[1] + ra1[2])
    for d in HOPS:
        second[1].send(acc_a.at[(z + d) % NZ], ra2.at[d - 1], links.at_plane(d, 0))
    phase("wait_att")
    att_got.wait()
    phase("wait_rs2")

    def own_residual():
        res = hid_ref[here_rows, :].astype(f32) + ((att[y] + rc[0]) + (rc[1] + rc[2]))
        second[0].wait()
        xbuf2[0, :, half:] = res[:, half:] + ((acc_b[y] + rb2[0]) + (rb2[1] + rb2[2]))
        yield high
        second[1].wait()
        xbuf2[0, :, :half] = res[:, :half] + ((acc_a[z] + ra2[0]) + (ra2[1] + ra2[2]))
        yield low

    back = norm_gather(links, own_residual, gains, 1, xbuf2, stat2, f_buf, gather_base, (lambda crossing: None, lambda: None))
    next(back)
    emb_on(ways[2:], emb_far[2:])
    for dx, oc in NEAR:
        emb_got[oc].send(emb_piece(dx, oc), emb_slot(dx, oc), links.at_line(dx, oc))
    phase.close()
    crossing = next(back)
    phase("wait_emb")
    own_emb.wait()
    for c in emb_got:
        c.wait()

    phase("logits")
    wide_n = 256
    for h in range(CORES):
        if h:
            crossing.wait()
        for i in range(total_rows // wide_n):
            cols = slice(i * wide_n, (i + 1) * wide_n)
            term = dot_t(emb_buf[h], f_buf[h, cols, :])
            z_ref[:, cols] = z_ref[:, cols] + term if h else term

    z_out = fetch(z_ref, z_hbm)

    phase("lse_own")
    shift = vocab_own * xid - emb_start(xid)
    vid = lax.broadcasted_iota(jnp.int32, (take, 1), 0)
    own = (vid >= shift) & (vid < shift + vocab_own)
    for b in range(blocks):
        zb = jnp.where(own, z_ref[:, b * 128:(b + 1) * 128], -jnp.inf)
        top = jnp.max(zb, axis=0, keepdims=True)
        lse_x[xid, b:b + 1, :] = top
        lse_x[xid, 8 + b:9 + b, :] = jnp.sum(jnp.exp(zb - top), axis=0, keepdims=True)
    for b in range(blocks, 8):
        lse_x[xid, b:b + 1, :] = jnp.zeros((1, 128), f32)
        lse_x[xid, 8 + b:9 + b, :] = jnp.ones((1, 128), f32)

    def merge(ref):
        tops = ref[:, :8, :]
        top = jnp.max(tops, axis=0)
        return top, jnp.sum(ref[:, 8:, :] * jnp.exp(tops - top[None]), axis=0)

    phase("lse_line")
    got = rest(lse_x, nx2)
    for p in FAR_LINE:
        got.send(lse_x.at[xid], lse_x.at[xid], links.at_line(*p))
    got.wait()
    top, mass = merge(lse_x)
    lse_y[yid, :8, :] = top
    lse_y[yid, 8:, :] = mass
    phase("lse_plane")
    got = rest(lse_y, nyz)
    for p in PLANE:
        got.send(lse_y.at[yid], lse_y.at[yid], links.at_plane(*p))
    got.wait()
    top, mass = merge(lse_y)
    norm_ref[...] = top + jnp.log(mass)
    phase("finish")
    z_out.wait()
    links.finish()
    phase.close()


def whole_step(hidden, freq, lens, k_cache, v_cache, g_attn, w_query, w_key, w_value,
               w_gate, w_up, w_out, w_down, g_final, embedding):
    total_rows, chunk = hidden.shape
    own_rows, seq, head = k_cache.shape
    rows = total_rows // (NY * NZ)
    vocab_own = embedding.shape[0] // (2 * NX)
    take = (vocab_own + 6 + 15) // 16 * 16
    half = chunk // 2
    qc = w_query.shape[1]
    ff = w_gate.shape[1] // (2 * NX)
    f32, bf16 = jnp.float32, jnp.bfloat16
    nyz, nx2, pad = NY * NZ, 2 * NX, 8
    vmem = pl.BlockSpec(memory_space=pltpu.VMEM)
    hbm = pl.BlockSpec(memory_space=pl.ANY)
    V = pltpu.VMEM
    return pl.pallas_call(
        lambda *refs: step_kernel(vocab_own, own_rows, *refs),
        out_shape=(jax.ShapeDtypeStruct((pad, head), bf16), jax.ShapeDtypeStruct((pad, head), bf16),
                   jax.ShapeDtypeStruct((take, total_rows), f32), jax.ShapeDtypeStruct((pad, head), f32)),
        in_specs=[vmem] * 5 + [hbm] * 10,
        out_specs=(vmem, vmem, hbm, vmem),
        scratch_shapes=[
            V((take, total_rows), f32),
            V((chunk, qc), bf16), V((chunk, head), bf16), V((chunk, head), bf16),
            V((own_rows, seq, head), bf16), V((own_rows, seq, head), bf16),
            V((nx2 * ff, chunk), bf16), V((NZ * qc, chunk), bf16), V((NY, rows, chunk), f32), V((3, rows, chunk), f32),
            V((NZ, NY * rows, 2 * ff), f32), V((2, total_rows, NX * chunk), bf16), V((2, NX * chunk, 2 * ff), bf16),
            V((qc, chunk), bf16), V((2, head, NX * chunk), bf16),
            V((nx2 * nyz * pad, total_rows), bf16), V((NY * rows, nx2 * NY * pad), bf16),
            V((nx2, nyz * pad // 4, head), bf16), V((nx2, nyz * pad // 4, head), bf16),
            V((nyz, pad, qc), f32), V((nyz, pad, qc), f32),
            V((nx2, pad, 2 * head), f32), V((nx2, pad, 2 * head), f32),
            V((NZ, NY, pad, qc), f32), V((NY, NZ, pad, qc), f32), V((nx2, NY * pad, NZ * qc), bf16),
            V((NZ, NY * rows, nx2 * ff), bf16),
            V((NZ, NY, rows, chunk), f32),
            V((3, NZ, rows, half), f32), V((3, NY, rows, half), f32), V((3, rows, half), f32), V((3, rows, half), f32),
            V((NZ, rows, half), f32), V((NY, rows, half), f32),
            V((NX, rows, chunk), bf16), V((2, rows, 128), f32), V((NX, rows, chunk), f32), V((2, rows, 128), f32),
            V((NX, 8, chunk), f32),
            V((2, total_rows, NX * chunk), bf16), V((2, take, NX * chunk), bf16),
            V((2, 2, chunk, ff), bf16), V((2, 2, (take // 2 + 15) // 16 * 16, chunk), bf16),
            V((nx2, 16, 128), f32), V((nx2, 16, 128), f32), V((nyz, 16, 128), f32),
            pltpu.SemaphoreType.DMA((SENDS,)), pltpu.SemaphoreType.DMA((TAGS,)), pltpu.SemaphoreType.DMA((11,)),
        ],
        compiler_params=pltpu.CompilerParams(
            collective_id=1, has_side_effects=True, vmem_limit_bytes=60 << 20),
        name="decode_step",
    )(hidden, g_attn[None, :], g_final[None, :], freq, lens, k_cache, v_cache,
      w_query, w_key, w_value, w_out, w_gate, w_up, w_down, embedding)


def solution(mesh):
    row_spec = P(("dp", "yax", "xax"))

    def local_step(hidden, cache_len, k_cache, v_cache, g_attn, w_query, w_key, w_value,
                   w_gate, w_up, w_out, w_down, g_final, embedding):
        rows = hidden.shape[0]
        half_dim = k_cache.shape[2] // 2
        inv_freq = ROPE_BASE ** (-(np.arange(half_dim, dtype=np.float64) * 2.0) / (2 * half_dim))
        freq = np.concatenate([inv_freq, inv_freq])[None, :].astype(np.float32)
        key_own, value_own, logits_wide, norm_tile = whole_step(
            hidden, freq, cache_len.reshape(rows // 128, 128), k_cache, v_cache, g_attn, w_query, w_key, w_value,
            w_gate, w_up, w_out, w_down, g_final, embedding)
        own_rows = k_cache.shape[0]
        vocab_own = embedding.shape[0] // (CORES * NX)
        first = vocab_own * lax.axis_index("xax")
        logits = lax.dynamic_slice_in_dim(logits_wide, first - first // 8 * 8, vocab_own, axis=0)
        log_norm = norm_tile[:rows // 128].reshape(rows)
        return key_own[:own_rows], value_own[:own_rows], (logits - log_norm).T, log_norm

    in_specs = (P("dp", "xax"), P("dp"), row_spec, row_spec, P("xax"), P("xax", "yax"),
                P("xax"), P("xax"), P("xax", "yax"), P("xax", "yax"),
                P("yax", "xax"), P("yax", "xax"), P("xax"), P("yax", "xax"))
    out_specs = (row_spec, row_spec, P("dp", ("yax", "xax")), P("dp"))
    return jax.shard_map(local_step, mesh=mesh, in_specs=in_specs, out_specs=out_specs, check_vma=False)
```

```python
import contextlib
import itertools

import jax
import jax.numpy as jnp
import numpy as np
from jax import lax
from jax.experimental import pallas as pl
from jax.experimental.pallas import tpu as pltpu
from jax.sharding import PartitionSpec as P

EPS = 1e-6
ROPE_BASE = 10000.0
MESH_ID = pl.DeviceIdType.MESH
NY = NZ = NX = 4
CORES = 2
POOL, SENDS, TAGS = 24, 59, 89
HOPS = (1, 3, 2)
FAR_FIRST = (2, 1, 3)
LINE = [(0, 1), (1, 0), (3, 0), (1, 1), (3, 1), (2, 0), (2, 1)]
NEAR = LINE[1:5]
NT = (((1,), (1,)), ((), ()))
PLANE = sorted([(dz, dy) for dz in range(NZ) for dy in range(NY) if dz or dy],
               key=lambda p: sum(abs(d - 2) for d in p))
FAR_LINE = LINE[::-1]


class Group:
    def __init__(self, links, whole):
        self.links, self.whole = links, whole
        self.tag, self.sem = next(links.tags), next(links.slow)
        links.groups.append(self)

    def send(self, src, dst, where):
        pltpu.make_async_remote_copy(
            src_ref=src, dst_ref=dst, send_sem=self.links.send_sem.at[self.sem],
            recv_sem=self.links.recv_sem.at[self.tag], device_id=where, device_id_type=MESH_ID).start()

    def wait(self):
        pltpu.make_async_copy(self.whole, self.whole, self.links.recv_sem.at[self.tag]).wait()

    def wait_sent(self):
        pltpu.make_async_copy(self.whole, self.whole, self.links.send_sem.at[self.sem]).wait()


class Phases:
    def __init__(self):
        self.stack = contextlib.ExitStack()

    def __call__(self, name):
        self.close()
        self.stack.enter_context(jax.named_scope(name))

    def close(self):
        self.stack.close()


class Links:
    def __init__(self, send_sem, recv_sem):
        self.send_sem, self.recv_sem = send_sem, recv_sem
        self.tags, self.slow, self.fast = itertools.count(), itertools.count(POOL), []
        self.pending, self.groups = [], []
        self.y_idx = lax.axis_index("yax")
        self.x_idx = lax.axis_index("xax")
        self.z, self.y = self.y_idx // NY, self.y_idx % NY
        self.chip, self.core = self.x_idx // CORES, self.x_idx % CORES

    def at_plane(self, dz, dy):
        return {"yax": (self.z + dz) % NZ * NY + (self.y + dy) % NY, "xax": self.x_idx}

    def slot_rows(self, dz, dy, rows):
        slot = (self.z + dz) % NZ * NY + (self.y + dy) % NY
        return pl.ds(pl.multiple_of(slot * rows, rows), rows)

    def line_id(self, dx, oc):
        core = 1 - self.core if oc else self.core
        return (self.chip + dx) % NX * CORES + core

    def at_line(self, dx, oc):
        return {"yax": self.y_idx, "xax": self.line_id(dx, oc)}

    def send(self, src, dst, where, tag=None, long=False):
        tag = next(self.tags) if tag is None else tag
        if long:
            sem = next(self.slow)
        else:
            sem = len(self.fast) % POOL
            if len(self.fast) >= POOL:
                self.fast[-POOL].wait_send()
        copy = pltpu.make_async_remote_copy(
            src_ref=src, dst_ref=dst, send_sem=self.send_sem.at[sem], recv_sem=self.recv_sem.at[tag],
            device_id=where, device_id_type=MESH_ID)
        copy.start()
        (self.pending if long else self.fast).append(copy)
        return copy

    def finish(self):
        for copy in self.pending + self.fast[-POOL:]:
            copy.wait_send()
        for group in self.groups:
            group.wait_sent()

    def barrier(self):
        barrier = pltpu.get_barrier_semaphore()
        peers = [self.at_line(*p) for p in LINE] + [self.at_plane(*p) for p in PLANE]
        for peer in peers:
            pl.semaphore_signal(barrier, inc=1, device_id=peer, device_id_type=MESH_ID)
        pl.semaphore_wait(barrier, len(peers))


def lane_sum(v):
    return jnp.sum(v, axis=-1, keepdims=True)


def plane_gather(links, buf, tags, hooks, crossing, start):
    cols = buf.shape[-1]
    rows = buf.shape[1] // (NY * NZ)
    span = (cols - start) // 2
    partner = links.at_line(0, 1)

    class Part:
        def __init__(self, index):
            self.index, self.lo, self.got = index, start + index * span, {}

        def order(self, du, dv):
            return (du, dv) if self.index else (dv, du)

        def block(self, at, half=0, piece=None):
            width = span if piece is None else span // 2
            lo = self.lo if not piece else self.lo + width
            return buf.at[half, links.slot_rows(*self.order(*at), rows), pl.ds(lo, width)]

        def push(self, name, at, to, piece=None):
            ref = self.block(at, piece=piece)
            self.got[name] = links.send(ref, ref, links.at_plane(*self.order(*to)), next(tags))

        def spread(self, k, at):
            self.push(("v+", k), at, (0, 1))
            self.push(("v-", k), at, (0, -1))

        def give(self, at):
            crossing.send(self.block(at), self.block(at, half=1), partner)

        def wait(self, name):
            self.got[name].wait_recv()

    parts = [Part(index) for index in range(2)]
    offset = (0, -1, 1, 2)
    for p in parts:
        p.push("u+", (0, 0), (1, 0))
        p.push("u-", (0, 0), (-1, 0))
        p.spread(0, (0, 0))
    for p in parts:
        p.give((0, 0))
    hooks[0](crossing)
    for k, name in enumerate(("u+", "u-"), 1):
        for p in parts:
            p.wait(name)
            at = (offset[k], 0)
            p.push(("far", k), at, (-offset[k], 0), piece=k - 1)
            p.spread(k, at)
            p.give(at)
    hooks[1]()

    def arrive(p, k):
        for name, step in (("v+", -1), ("v-", 1)):
            p.wait((name, k))
            at = (offset[k], step)
            if (name == "v+") == (k in (0, 3)):
                p.push(("relay", k), at, (0, -step))
            p.give(at)

    for p in parts:
        arrive(p, 0)
    for p in parts:
        p.wait(("far", 1))
        p.wait(("far", 2))
        p.spread(3, (2, 0))
        p.give((2, 0))
    for k in range(1, len(offset)):
        for p in parts:
            arrive(p, k)
    for k in range(len(offset)):
        for p in parts:
            p.wait(("relay", k))
            p.give((offset[k], 2))


def norm_gather(links, own_slot, gain_buf, which, xbuf, stat, out, base, hooks, skip=0):
    rows, chunk = xbuf.shape[1:]
    tags = itertools.count(base)
    line = []
    for cols in own_slot():
        line += [links.send(xbuf.at[0, :, cols], xbuf.at[NX - dx, :, cols], links.at_line(dx, 0), next(tags))
                 for dx in FAR_FIRST]
    yield
    phase = Phases()
    for n, c in enumerate(line):
        phase(f"ng_line{which}_{n}")
        c.wait_recv()
    phase("ng_stats")
    held = xbuf[...].astype(jnp.float32)
    count = NX * chunk
    mean = lane_sum(jnp.sum(held, axis=0)) / count
    dev = held - mean[None]
    square = lane_sum(jnp.sum(dev * dev, axis=0))
    lane = lax.broadcasted_iota(jnp.int32, (rows, 128), 1)
    stat[0] = jnp.where(lane == 0, mean, square)
    links.send(stat.at[0], stat.at[1], links.at_line(0, 1), next(tags)).wait_recv()
    other_mean, other_square = stat[1, :, 0:1], stat[1, :, 1:2]
    both = (mean + other_mean) * 0.5
    gap = mean - other_mean
    var = (square + other_square + gap * gap * (count * 0.5)) / (2 * count)
    scale = lax.rsqrt(var + EPS)
    for e in range(skip, NX):
        out[0, links.slot_rows(0, 0, rows), e * chunk:(e + 1) * chunk] = (
            (xbuf[e].astype(jnp.float32) - both) * scale * gain_buf[e, which:which + 1, :]).astype(jnp.bfloat16)
    phase("ng_plane")
    crossing = Group(links, out.at[1])
    plane_gather(links, out, tags, hooks, crossing, skip * chunk)
    phase.close()
    yield crossing


def step_kernel(vocab_own, own_rows, hid_ref, gain_a, gain_f, freq_ref, len_ref, k_hbm, v_hbm,
                wq_hbm, wk_hbm, wv_hbm, wo_ref, wg_ref, wu_ref, wd_hbm, emb_ref,
                knew_ref, vnew_ref, z_hbm, norm_ref,
                z_ref, wq_ref, wk_ref, wv_ref, k_buf, v_buf, wd_buf, wo_all, att, rc, gu_acc, n_buf, w_buf, wq_t, wq_buf, sel, sel_t, qx, qr, qy, qf,
                kvp, kvr, o_buf, o_got, o_all, act,
                part, ra1, rb1, ra2, rb2, acc_a, acc_b, xbuf, stat, xbuf2, stat2, gains, f_buf, emb_buf,
                w_relay, emb_relay, row_stats, lse_x, lse_y, send_sem, recv_sem, local_sem):
    links = Links(send_sem, recv_sem)
    phase = Phases()
    f32, bf16 = jnp.float32, jnp.bfloat16
    z, y, xid, yid = links.z, links.y, links.x_idx, links.y_idx
    total_rows, chunk = hid_ref.shape
    rows = total_rows // (NY * NZ)
    here_rows = links.slot_rows(0, 0, rows)
    half = chunk // 2
    nx2, nyz = 2 * NX, NY * NZ
    group = NY * rows
    head = 128
    pad = 8
    partner = links.at_line(0, 1)
    line_id = links.line_id
    gather_tags = 2 * len(HOPS) + 1 + len(PLANE) * CORES + CORES
    gather_base = [next(links.tags) for _ in range(gather_tags)][0]

    def dot(a, b):
        return jnp.dot(a, b, preferred_element_type=f32)

    def dot_t(a, b):
        return lax.dot_general(a, b, NT, preferred_element_type=f32)

    def rest(ref, n):
        return Group(links, ref.at[0:n - 1])

    local = []

    def fetch(src, dst):
        copy = pltpu.make_async_copy(src, dst, local_sem.at[len(local)])
        copy.start()
        local.append(copy)
        return copy

    ff = wg_ref.shape[1] // nx2

    def w_piece(ref, dx, oc):
        return ref.at[:, pl.ds(pl.multiple_of(line_id(dx, oc) * ff, ff), ff)]

    def w_slot(which, dx, oc):
        back = (NX - dx) % NX
        return w_buf.at[int(oc), pl.ds(back * chunk, chunk), pl.ds(which * ff, ff)]

    take = emb_buf.shape[1]

    def emb_start(xi):
        return pl.multiple_of(vocab_own * xi // pad * pad, pad)

    def emb_piece(dx, oc):
        return emb_ref.at[pl.ds(emb_start(line_id(dx, oc)), take), :]

    def emb_slot(dx, oc):
        return emb_buf.at[int(oc), :, pl.ds((NX - dx) % NX * chunk, chunk)]

    near_part = (take // 2 + 15) // 16 * 16
    far_parts = ((0, near_part), (near_part, take - near_part))

    def emb_half(oc, way):
        first, size = far_parts[way]
        return emb_ref.at[pl.ds(pl.multiple_of(emb_start(line_id(2, oc)) + first, pad), size), :]

    def emb_mid(oc, way):
        return emb_relay.at[way, oc, pl.ds(0, far_parts[way][1])]

    def emb_far_slot(oc, way):
        return emb_buf.at[int(oc), pl.ds(*far_parts[way]), pl.ds(2 * chunk, chunk)]

    got_wq = fetch(wq_hbm, wq_ref)
    own_w = [fetch(w_piece(wg_ref, 0, 0), w_slot(0, 0, 0)), fetch(w_piece(wu_ref, 0, 0), w_slot(1, 0, 0))]
    got_kv = [fetch(k_hbm, k_buf), fetch(v_hbm, v_buf)]
    got_wkv = [fetch(wk_hbm, wk_ref), fetch(wv_hbm, wv_ref)]
    got_wd = fetch(wd_hbm, wd_buf)
    own_emb = fetch(emb_piece(0, 0), emb_slot(0, 0))

    qc = wq_ref.shape[1]
    qs = qc // nx2
    per = head // qs
    wq_buf[...] = jnp.zeros(wq_buf.shape, bf16)

    phase("row_stats")
    eye = lax.broadcasted_iota(jnp.int32, (head, head), 0) == lax.broadcasted_iota(jnp.int32, (head, head), 1)
    blocks = total_rows // head

    def block_rows(b):
        return slice(b * head, (b + 1) * head)

    def to_row(v):
        return jnp.sum(jnp.where(eye, v, 0.0), axis=0, keepdims=True)

    def to_col(v):
        return lane_sum(jnp.where(eye, v, 0.0))

    row_stats[xid] = jnp.zeros((2 * pad, head), f32)
    for b in range(blocks):
        held = hid_ref[block_rows(b), :].astype(f32)
        mean = lane_sum(held) / chunk
        dev = held - mean
        row_stats[xid, b:b + 1, :] = to_row(mean)
        row_stats[xid, pad + b:pad + b + 1, :] = to_row(lane_sum(dev * dev))

    phase("barrier")
    links.barrier()

    phase("front_send")
    gains[0, 0:1, :] = gain_a[...]
    gains[0, 1:2, :] = gain_f[...]
    gains[0, 2:, :] = jnp.zeros((6, chunk), f32)

    def own_input():
        xbuf[0] = hid_ref[here_rows, :]
        yield pl.ds(0, chunk)

    w_far, emb_far = [], []
    w_got = [Group(links, w_buf.at[0, 0:2 * chunk]), Group(links, w_buf.at[1, 0:(NX - 1) * chunk])]
    w_last = Group(links, w_buf.at[0, 0:2 * chunk])
    emb_got = [Group(links, emb_buf.at[0, :, 0:(NX - 1) * chunk]), Group(links, emb_buf.at[1])]
    ways = [(way, hop, oc) for oc in (0, 1) for way, hop in enumerate(HOPS[:2])]

    def forward_weights():
        for (way, hop, oc), c in zip(ways, w_far):
            c.wait_recv()
            w_last.send(w_relay.at[way, oc], w_buf.at[oc, pl.ds(2 * chunk, chunk), pl.ds(way * ff, ff)],
                        links.at_line(hop, oc))

    def emb_out(some):
        for way, hop, oc in some:
            emb_far.append(links.send(emb_half(oc, way), emb_mid(oc, way), links.at_line(hop, 0), long=True))

    def emb_on(some, arrived):
        for (way, hop, oc), c in zip(some, arrived):
            c.wait_recv()
            emb_got[oc].send(emb_mid(oc, way), emb_far_slot(oc, way), links.at_line(hop, oc))

    def amid(crossing):
        stats_got.wait()
        means = row_stats[:, :pad, :]
        mean = jnp.sum(means, axis=0) / nx2
        gap = means - mean[None]
        square = jnp.sum(row_stats[:, pad:, :], axis=0) + jnp.sum(gap * gap, axis=0) * chunk
        scale = lax.rsqrt(square / (nx2 * chunk) + EPS)
        for b in range(blocks):
            n_buf[0, block_rows(b), 0:chunk] = (
                (hid_ref[block_rows(b), :].astype(f32) - to_col(mean[b:b + 1, :])) * to_col(scale[b:b + 1, :])
                * gains[0, 0:1, :]).astype(bf16)
        own = n_buf.at[0, :, 0:chunk]
        crossing.send(own, n_buf.at[1, :, 0:chunk], partner)

    front = norm_gather(links, own_input, gains, 0, xbuf, stat, n_buf, gather_base, (amid, forward_weights), skip=1)
    next(front)
    gain_got = rest(gains, NX)
    for dx in HOPS:
        gain_got.send(gains.at[0], gains.at[NX - dx], links.at_line(dx, 0))
    stats_got = rest(row_stats, nx2)
    for p in FAR_LINE:
        stats_got.send(row_stats.at[xid], row_stats.at[xid], links.at_line(*p))
    for way, hop, oc in ways:
        w_far.append(links.send(w_piece((wg_ref, wu_ref)[way], 2, oc), w_relay.at[way, oc], links.at_line(hop, 0),
                                long=True))

    got_wq.wait()
    eye_q = (lax.broadcasted_iota(jnp.int32, (qc, qc), 0) == lax.broadcasted_iota(jnp.int32, (qc, qc), 1))
    wq_t[...] = dot_t(eye_q.astype(bf16), wq_ref[...]).astype(bf16)
    wq_buf[0, 0:qs, 0:chunk] = wq_t[pl.ds(pl.multiple_of(xid * qs, qs), qs), :]

    def wq_rows(dx, oc):
        return wq_t.at[pl.ds(pl.multiple_of(line_id(dx, oc) * qs, qs), qs), :]

    def wq_slot(dx, oc):
        return wq_buf.at[oc, pl.ds(0, qs), pl.ds((NX - dx) % NX * chunk, chunk)]

    wq_got = Group(links, wq_t.at[0:qc - qs])
    for dx, oc in LINE:
        wq_got.send(wq_rows(dx, oc), wq_slot(dx, oc), links.at_line(dx, oc))
    for which, ref in enumerate((wg_ref, wu_ref)):
        for dx, oc in LINE[:1] + NEAR:
            w_got[oc].send(w_piece(ref, dx, oc), w_slot(which, dx, oc), links.at_line(dx, oc))

    phase("selections")
    r_id = lax.broadcasted_iota(jnp.int32, (nx2 * nyz * pad, 1), 0)
    r_j = r_id % pad
    r_src = jnp.where(r_j < own_rows, r_id // pad % nyz * rows + r_id // (pad * nyz) * own_rows + r_j, -1)
    s_id = lax.broadcasted_iota(jnp.int32, (1, total_rows), 1)
    sel[...] = jnp.where(r_src == s_id, 1.0, 0.0).astype(bf16)
    t_id = lax.broadcasted_iota(jnp.int32, (group, 1), 0)
    t_in = t_id % rows
    t_src = t_in // own_rows * (NY * pad) + t_id // rows * pad + t_in % own_rows
    u_id = lax.broadcasted_iota(jnp.int32, (1, nx2 * NY * pad), 1)
    sel_t[...] = jnp.where(t_src == u_id, 1.0, 0.0).astype(bf16)
    k_id = lax.broadcasted_iota(jnp.int32, (nx2 * pad, rows), 0)
    k_src = jnp.where(k_id % pad < own_rows, k_id // pad * own_rows + k_id % pad, -1)
    sel_kv = jnp.where(k_src == lax.broadcasted_iota(jnp.int32, (nx2 * pad, rows), 1), 1.0, 0.0).astype(bf16)

    phase.close()
    gain_got.wait()
    lane = lax.broadcasted_iota(jnp.int32, (1, head), 1)
    lengths = []
    for b in range(own_rows):
        index = (yid * nx2 + xid) * own_rows + b
        row = len_ref[pl.ds(index // head, 1), :].astype(f32)
        lengths.append(lane_sum(jnp.where(lane == index % head, row, 0.0)))
    lengths = jnp.concatenate(lengths + lengths[:pad - own_rows], axis=0)
    angles = lengths * freq_ref[...]
    cos_all = jnp.cos(angles)
    sin_all = jnp.sin(angles) * jnp.where(lane < head // 2, -1.0, 1.0)

    crossing = next(front)
    def wo_rows(dz):
        return wo_all.at[pl.ds(pl.multiple_of((z + dz) % NZ * qc, qc), qc), :]

    wo_got = Group(links, wo_all.at[0:(NZ - 1) * qc])
    for d in HOPS[:2]:
        wo_got.send(wo_ref, wo_rows(0), links.at_plane(d, 0))
    phase("ng_cross")
    crossing.wait()
    phase("kv_part")

    for c in got_wkv:
        c.wait()
    n_own = dot(sel_kv, n_buf[0, links.slot_rows(0, 0, rows), 0:chunk]).astype(bf16)
    kvp[:, :, :head] = dot(n_own, wk_ref[...]).reshape(nx2, pad, head)
    kvp[:, :, head:] = dot(n_own, wv_ref[...]).reshape(nx2, pad, head)
    kv_got = rest(kvr, nx2)
    for p in FAR_LINE:
        kv_got.send(kvp.at[line_id(*p)], kvr.at[xid], links.at_line(*p))
    kvr[xid] = kvp[xid]

    phase("wait_wq")
    wq_got.wait()
    phase("q_mm")
    q_all = jnp.concatenate([
        (dot_t(n_buf[0, i * group:(i + 1) * group, :], wq_buf[0])
         + dot_t(n_buf[1, i * group:(i + 1) * group, :], wq_buf[1])).astype(bf16) for i in range(NZ)], axis=0)
    span = nyz * pad
    for i in range(nx2):
        chosen = dot(sel[i * span:(i + 1) * span, :], q_all)
        quarter = span // per
        packed = chosen[:quarter, :]
        for g in range(1, per):
            packed = packed + pltpu.roll(chosen[g * quarter:(g + 1) * quarter, :], g * qs, 1)
        qx[i] = packed.astype(bf16)
    q_got = rest(qr, nx2)
    for p in FAR_LINE:
        q_got.send(qx.at[line_id(*p)], qr.at[xid], links.at_line(*p))
    qr[xid] = qx[xid]

    phase("wait_w")
    for c in own_w:
        c.wait()
    for c in w_got:
        c.wait()
    phase("gate_up")

    def act_at(k, dx):
        return act.at[(z + k) % NZ, :, pl.ds(pl.multiple_of(line_id(dx, 0) * ff, ff), ff)]

    def act_out(k, dx, to_dx):
        return links.send(act_at(k, dx), act_at(k, dx), links.at_line(to_dx, 0))

    def act_give(k, dx):
        cross[k].send(act_at(k, dx), act_at(k, dx), partner)

    turns = (2, 1, 3, 0)
    early, late = turns[:2], turns[2:]
    near_act, far_act = {}, {}
    cross = {k: Group(links, act.at[0, :, 0:NX * ff]) for k in turns}
    def group_rows(k):
        return pl.ds(pl.multiple_of((z + k) % NZ * group, group), group)

    far = slice(2 * chunk, (NX - 1) * chunk)

    def over(k, part_cols):
        return dot(n_buf[0, group_rows(k), part_cols], w_buf[0, part_cols, :]) + dot(
            n_buf[1, group_rows(k), part_cols], w_buf[1, part_cols, :])

    for k in turns:
        gu_acc[k] = over(k, slice(0, far.start)) + over(k, slice(far.stop, NX * chunk))
    phase("wait_w_far")
    w_last.wait()
    phase("gate_up_far")
    for k in turns:
        both = (gu_acc[k] + over(k, far)).astype(bf16).astype(f32)
        gate, up = both[:, :ff], both[:, ff:]
        act_at(k, 0)[...] = (gate * jax.nn.sigmoid(gate) * up).astype(bf16)
        near_act[k] = [(dx, act_out(k, 0, dx)) for dx in HOPS[:2]]
        act_give(k, 0)

    def act_pass(k):
        for dx, c in near_act[k]:
            c.wait_recv()
            if (k in early) == (dx == 1):
                far_act[k] = act_out(k, NX - dx, dx)
            act_give(k, NX - dx)

    low, high = pl.ds(0, half), pl.ds(half, half)
    first_a, first_b = Group(links, ra1), Group(links, rb1)

    def act_use(k):
        cross[k].wait()
        g = (z + k) % NZ
        part[g] = dot(act[g], wd_buf[...]).reshape(NY, rows, chunk)
        if k:
            first_b.send(part.at[g, :, :, high], rb1.at[k - 1], links.at_plane(k, 0))

    def along_y(k):
        g = (z + k) % NZ
        for d in early + late[:1]:
            first_a.send(part.at[g, (y + d) % NY, :, low], ra1.at[d - 1, g], links.at_plane(0, d))

    def act_far(ks):
        for k in ks:
            far_act[k].wait_recv()
            act_give(k, 2)

    phase("wait_q")
    q_got.wait()
    phase("q_sum")
    lane_group = lax.broadcasted_iota(jnp.int32, (1, head), 1) // qs
    for j in range(qc // head):
        came = [qr[j * per + i].astype(f32) for i in range(per)]
        for g in range(per):
            piece = jnp.zeros((span // per, head), f32)
            for i in range(per):
                piece = piece + jnp.where(lane_group == i, pltpu.roll(came[i], (i - g) % per * qs, 1), 0.0)
            qy[g * per:(g + 1) * per, :, j * head:(j + 1) * head] = piece.reshape(per, pad, head)

    def plane_id(dz, dy):
        return (z + dz) % NZ * NY + (y + dy) % NY

    y_got = rest(qf, nyz)
    for p in PLANE:
        y_got.send(qy.at[plane_id(*p)], qf.at[yid], links.at_plane(*p))
    qf[yid] = qy[yid]

    wo_got.send(wo_ref, wo_rows(0), links.at_plane(FAR_FIRST[0], 0))
    own_wo = fetch(wo_ref, wo_rows(0))

    phase("act_pass")
    for k in early:
        act_pass(k)
    phase("wait_kv")
    kv_got.wait()
    kv_sum = kvr[0]
    for i in range(1, nx2):
        kv_sum = kv_sum + kvr[i]
    kv_new = kv_sum.astype(bf16).astype(f32)

    def turn(v, b=None):
        cos, sin = (cos_all, sin_all) if b is None else (cos_all[b:b + 1, :], sin_all[b:b + 1, :])
        return (v * cos + pltpu.roll(v, head // 2, 1) * sin).astype(bf16)

    k_new = turn(kv_new[:, :head])
    knew_ref[...] = k_new
    vnew_ref[...] = kv_new[:, head:].astype(bf16)
    k_row, v_row = k_new.astype(f32), kv_new[:, head:]
    phase("act_pass2")
    for k in late:
        act_pass(k)
    emb_out(ways[:2])
    phase("wait_qy")
    for c in got_kv:
        c.wait()
    y_got.wait()
    phase("attention")
    seq = k_buf.shape[1]
    score_scale = head ** -0.5
    position = lax.broadcasted_iota(jnp.int32, (1, seq), 1).astype(f32)
    o_buf[...] = jnp.zeros(o_buf.shape, f32)
    for b in range(own_rows):
        q_b = jnp.concatenate([turn(qf[:, b, j * head:(j + 1) * head], b) for j in range(qc // head)], axis=0)
        scores = dot_t(q_b, k_buf[b]) * score_scale
        score_new = lane_sum(q_b.astype(f32) * k_row[b:b + 1, :]) * score_scale
        valid = position < lengths[b:b + 1, :]
        top = jnp.maximum(jnp.max(jnp.where(valid, scores, -jnp.inf), axis=-1, keepdims=True), score_new)
        weights = jnp.where(valid, jnp.exp(scores - top), 0.0)
        weight_new = jnp.exp(score_new - top)
        denom = lane_sum(weights) + weight_new
        o_b = dot((weights / denom).astype(bf16), v_buf[b])
        o_b = o_b + (weight_new / denom).astype(bf16).astype(f32) * v_row[b:b + 1, :]
        o_b = o_b.astype(bf16).astype(f32)
        for j in range(qc // head):
            o_buf[:, :, b, j * head:(j + 1) * head] = o_b[j * nyz:(j + 1) * nyz, :].reshape(NZ, NY, head)
    o_back = rest(o_got, NY)
    for d in HOPS:
        o_back.send(o_buf.at[:, (y + d) % NY], o_got.at[y], links.at_plane(0, d))
    phase("act_early")
    act_far(turns)
    got_wd.wait()
    for k in turns:
        act_use(k)
        along_y(k)
    o_got[y] = o_buf[:, y]

    phase("wait_oy")
    o_back.wait()
    for i in range(NZ):
        o_all[xid, :, i * qc:(i + 1) * qc] = o_got[:, i].reshape(NY * pad, qc).astype(bf16)
    o_here = o_all.at[xid]
    o_line = [links.send(o_here, o_here, links.at_line(dx, 0)) for dx in HOPS]
    o_cross = rest(o_all, NX + 1)
    o_cross.send(o_here, o_here, partner)
    emb_out(ways[2:])
    emb_got[1].send(emb_piece(0, 1), emb_slot(0, 1), partner)
    emb_on(ways[:2], emb_far[:2])
    phase("wait_o")
    for dx, c in zip(HOPS, o_line):
        c.wait_recv()
        came = o_all.at[line_id(NX - dx, 0)]
        o_cross.send(came, came, partner)
    wo_got.wait()
    own_wo.wait()
    o_cross.wait()
    phase("out_mm")
    o_nat = dot(sel_t[...], o_all[...].reshape(nx2 * NY * pad, NZ * qc)).astype(bf16)
    att[...] = dot(o_nat, wo_all[...]).reshape(NY, rows, chunk)
    att_got = Group(links, rc)
    for d in HOPS:
        att_got.send(att.at[(y + d) % NY], rc.at[d - 1], links.at_plane(0, d))

    phase("wait_rs1")
    first_b.wait()
    acc_b[...] = (part[z, :, :, half:] + rb1[0]) + (rb1[1] + rb1[2])
    second = [Group(links, rb2), Group(links, ra2)]
    for d in HOPS:
        second[0].send(acc_b.at[(y + d) % NY], rb2.at[d - 1], links.at_plane(0, d))
    phase("wait_rs1a")
    first_a.wait()
    acc_a[...] = (part[:, y, :, :half] + ra1[0]) + (ra1[1] + ra1[2])
    for d in HOPS:
        second[1].send(acc_a.at[(z + d) % NZ], ra2.at[d - 1], links.at_plane(d, 0))
    phase("wait_att")
    att_got.wait()
    phase("wait_rs2")

    def own_residual():
        res = hid_ref[here_rows, :].astype(f32) + ((att[y] + rc[0]) + (rc[1] + rc[2]))
        second[0].wait()
        xbuf2[0, :, half:] = res[:, half:] + ((acc_b[y] + rb2[0]) + (rb2[1] + rb2[2]))
        yield high
        second[1].wait()
        xbuf2[0, :, :half] = res[:, :half] + ((acc_a[z] + ra2[0]) + (ra2[1] + ra2[2]))
        yield low

    back = norm_gather(links, own_residual, gains, 1, xbuf2, stat2, f_buf, gather_base, (lambda crossing: None, lambda: None))
    next(back)
    emb_on(ways[2:], emb_far[2:])
    for dx, oc in NEAR:
        emb_got[oc].send(emb_piece(dx, oc), emb_slot(dx, oc), links.at_line(dx, oc))
    phase.close()
    crossing = next(back)
    phase("wait_emb")
    own_emb.wait()
    for c in emb_got:
        c.wait()

    phase("logits")
    wide_n = 256
    for h in range(CORES):
        if h:
            crossing.wait()
        for i in range(total_rows // wide_n):
            cols = slice(i * wide_n, (i + 1) * wide_n)
            term = dot_t(emb_buf[h], f_buf[h, cols, :])
            z_ref[:, cols] = z_ref[:, cols] + term if h else term

    z_out = fetch(z_ref, z_hbm)

    phase("lse_own")
    shift = vocab_own * xid - emb_start(xid)
    vid = lax.broadcasted_iota(jnp.int32, (take, 1), 0)
    own = (vid >= shift) & (vid < shift + vocab_own)
    for b in range(blocks):
        zb = jnp.where(own, z_ref[:, b * 128:(b + 1) * 128], -jnp.inf)
        top = jnp.max(zb, axis=0, keepdims=True)
        lse_x[xid, b:b + 1, :] = top
        lse_x[xid, 8 + b:9 + b, :] = jnp.sum(jnp.exp(zb - top), axis=0, keepdims=True)
    for b in range(blocks, 8):
        lse_x[xid, b:b + 1, :] = jnp.zeros((1, 128), f32)
        lse_x[xid, 8 + b:9 + b, :] = jnp.ones((1, 128), f32)

    def merge(ref):
        tops = ref[:, :8, :]
        top = jnp.max(tops, axis=0)
        return top, jnp.sum(ref[:, 8:, :] * jnp.exp(tops - top[None]), axis=0)

    phase("lse_line")
    got = rest(lse_x, nx2)
    for p in FAR_LINE:
        got.send(lse_x.at[xid], lse_x.at[xid], links.at_line(*p))
    got.wait()
    top, mass = merge(lse_x)
    lse_y[yid, :8, :] = top
    lse_y[yid, 8:, :] = mass
    phase("lse_plane")
    got = rest(lse_y, nyz)
    for p in PLANE:
        got.send(lse_y.at[yid], lse_y.at[yid], links.at_plane(*p))
    got.wait()
    top, mass = merge(lse_y)
    norm_ref[...] = top + jnp.log(mass)
    phase("finish")
    z_out.wait()
    links.finish()
    phase.close()


def whole_step(hidden, freq, lens, k_cache, v_cache, g_attn, w_query, w_key, w_value,
               w_gate, w_up, w_out, w_down, g_final, embedding):
    total_rows, chunk = hidden.shape
    own_rows, seq, head = k_cache.shape
    rows = total_rows // (NY * NZ)
    vocab_own = embedding.shape[0] // (2 * NX)
    take = (vocab_own + 6 + 15) // 16 * 16
    half = chunk // 2
    qc = w_query.shape[1]
    ff = w_gate.shape[1] // (2 * NX)
    f32, bf16 = jnp.float32, jnp.bfloat16
    nyz, nx2, pad = NY * NZ, 2 * NX, 8
    vmem = pl.BlockSpec(memory_space=pltpu.VMEM)
    hbm = pl.BlockSpec(memory_space=pl.ANY)
    V = pltpu.VMEM
    return pl.pallas_call(
        lambda *refs: step_kernel(vocab_own, own_rows, *refs),
        out_shape=(jax.ShapeDtypeStruct((pad, head), bf16), jax.ShapeDtypeStruct((pad, head), bf16),
                   jax.ShapeDtypeStruct((take, total_rows), f32), jax.ShapeDtypeStruct((pad, head), f32)),
        in_specs=[vmem] * 5 + [hbm] * 10,
        out_specs=(vmem, vmem, hbm, vmem),
        scratch_shapes=[
            V((take, total_rows), f32),
            V((chunk, qc), bf16), V((chunk, head), bf16), V((chunk, head), bf16),
            V((own_rows, seq, head), bf16), V((own_rows, seq, head), bf16),
            V((nx2 * ff, chunk), bf16), V((NZ * qc, chunk), bf16), V((NY, rows, chunk), f32), V((3, rows, chunk), f32),
            V((NZ, NY * rows, 2 * ff), f32), V((2, total_rows, NX * chunk), bf16), V((2, NX * chunk, 2 * ff), bf16),
            V((qc, chunk), bf16), V((2, head, NX * chunk), bf16),
            V((nx2 * nyz * pad, total_rows), bf16), V((NY * rows, nx2 * NY * pad), bf16),
            V((nx2, nyz * pad // 4, head), bf16), V((nx2, nyz * pad // 4, head), bf16),
            V((nyz, pad, qc), f32), V((nyz, pad, qc), f32),
            V((nx2, pad, 2 * head), f32), V((nx2, pad, 2 * head), f32),
            V((NZ, NY, pad, qc), f32), V((NY, NZ, pad, qc), f32), V((nx2, NY * pad, NZ * qc), bf16),
            V((NZ, NY * rows, nx2 * ff), bf16),
            V((NZ, NY, rows, chunk), f32),
            V((3, NZ, rows, half), f32), V((3, NY, rows, half), f32), V((3, rows, half), f32), V((3, rows, half), f32),
            V((NZ, rows, half), f32), V((NY, rows, half), f32),
            V((NX, rows, chunk), bf16), V((2, rows, 128), f32), V((NX, rows, chunk), f32), V((2, rows, 128), f32),
            V((NX, 8, chunk), f32),
            V((2, total_rows, NX * chunk), bf16), V((2, take, NX * chunk), bf16),
            V((2, 2, chunk, ff), bf16), V((2, 2, (take // 2 + 15) // 16 * 16, chunk), bf16),
            V((nx2, 16, 128), f32), V((nx2, 16, 128), f32), V((nyz, 16, 128), f32),
            pltpu.SemaphoreType.DMA((SENDS,)), pltpu.SemaphoreType.DMA((TAGS,)), pltpu.SemaphoreType.DMA((11,)),
        ],
        compiler_params=pltpu.CompilerParams(
            collective_id=1, has_side_effects=True, vmem_limit_bytes=60 << 20),
        name="decode_step",
    )(hidden, g_attn[None, :], g_final[None, :], freq, lens, k_cache, v_cache,
      w_query, w_key, w_value, w_out, w_gate, w_up, w_down, embedding)


def solution(mesh):
    row_spec = P(("dp", "yax", "xax"))

    def local_step(hidden, cache_len, k_cache, v_cache, g_attn, w_query, w_key, w_value,
                   w_gate, w_up, w_out, w_down, g_final, embedding):
        rows = hidden.shape[0]
        half_dim = k_cache.shape[2] // 2
        inv_freq = ROPE_BASE ** (-(np.arange(half_dim, dtype=np.float64) * 2.0) / (2 * half_dim))
        freq = np.concatenate([inv_freq, inv_freq])[None, :].astype(np.float32)
        key_own, value_own, logits_wide, norm_tile = whole_step(
            hidden, freq, cache_len.reshape(rows // 128, 128), k_cache, v_cache, g_attn, w_query, w_key, w_value,
            w_gate, w_up, w_out, w_down, g_final, embedding)
        own_rows = k_cache.shape[0]
        vocab_own = embedding.shape[0] // (CORES * NX)
        first = vocab_own * lax.axis_index("xax")
        logits = lax.dynamic_slice_in_dim(logits_wide, first - first // 8 * 8, vocab_own, axis=0)
        log_norm = norm_tile[:rows // 128].reshape(rows)
        return key_own[:own_rows], value_own[:own_rows], (logits - log_norm).T, log_norm

    in_specs = (P("dp", "xax"), P("dp"), row_spec, row_spec, P("xax"), P("xax", "yax"),
                P("xax"), P("xax"), P("xax", "yax"), P("xax", "yax"),
                P("yax", "xax"), P("yax", "xax"), P("xax"), P("yax", "xax"))
    out_specs = (row_spec, row_spec, P("dp", ("yax", "xax")), P("dp"))
    return jax.shard_map(local_step, mesh=mesh, in_specs=in_specs, out_specs=out_specs, check_vma=False)
```
